32 devices in a mesh: x: 4 (over z), yz: 8 (over y, x, core).
Axes of the slice: x: 2, y: 2, z: 4, core: 2. Of those that a mesh axis runs over, the one named last changes fastest.
Arguments:
- x_in: bfloat16 [512, 2048], P(None, ('x', 'yz'))
- ln_scale: float32 [2048], P(('x', 'yz'))
- w_gate_up: bfloat16 [2048, 2, 8192], P('x', None, 'yz')
- w_attn: bfloat16 [2048, 2304], P('x', 'yz')
- w_down: bfloat16 [8192, 2048], P('yz', 'x')
- w_out: bfloat16 [2048, 2048], P('yz', 'x')
- k_cache: bfloat16 [512, 2048, 128], P(('x', 'yz'))
- v_cache: bfloat16 [512, 2048, 128], P(('x', 'yz'))
- lengths: int32 [512], P(('x', 'yz'))
- positions: int32 [512], P(('x', 'yz'))
Outputs:
- output 1: bfloat16 [512, 2048], P(None, ('x', 'yz'))
- output 2: bfloat16 [512, 2048, 128], P(('x', 'yz'))
- output 3: bfloat16 [512, 2048, 128], P(('x', 'yz'))
All inputs are finite; a program needn't handle non-finite values.
Results may differ from the reference program's by a relative error of at most 0.00344997.
Values are sent between devices in bfloat16 or wider.
A program may use at most 1 GiB of HBM per device.

```python
import math
import jax
import jax.numpy as jnp
from jax import lax

D = 2048
FF = 8192
HEADS = 16
HEAD = 128
BATCH = 512
SEQ = 2048

LN_EPS = 1e-6
ROPE_BASE = 10000.0


def setup_inputs(seed: int = 0) -> dict:
    key_list = jax.random.split(jax.random.key(seed), 12)
    q_width = HEADS * HEAD
    key_scale = math.sqrt(math.log(SEQ / 16.0))
    x_in = jax.random.normal(key_list[0], (BATCH, D), jnp.float32)
    ln_scale = jax.random.uniform(key_list[1], (D,), jnp.float32, 0.5, 1.5)
    w_gate_up = jax.random.normal(key_list[2], (D, 2, FF), jnp.float32) * D ** -0.5
    w_attn = jax.random.normal(key_list[3], (D, q_width + 2 * HEAD), jnp.float32) * D ** -0.5
    w_down = jax.random.normal(key_list[4], (FF, D), jnp.float32) * FF ** -0.5
    w_out = jax.random.normal(key_list[5], (q_width, D), jnp.float32) * q_width ** -0.5
    k_cache = jax.random.normal(key_list[6], (BATCH, SEQ, HEAD), jnp.float32) * key_scale
    v_cache = jax.random.normal(key_list[7], (BATCH, SEQ, HEAD), jnp.float32) * 2.0
    len_keys = jax.random.split(key_list[8], 3)
    lengths = jax.random.randint(len_keys[0], (BATCH,), SEQ // 8, SEQ, jnp.int32)
    long_row = jax.random.randint(len_keys[1], (), 0, BATCH, jnp.int32)
    short_row = (long_row + 1 + jax.random.randint(len_keys[2], (), 0, BATCH - 1, jnp.int32)) % BATCH
    lengths = lengths.at[long_row].set(SEQ - 1).at[short_row].set(SEQ // 8)
    positions = jax.random.randint(key_list[9], (BATCH,), 0, 2 * SEQ, jnp.int32)
    return {
        'x_in': x_in.astype(jnp.bfloat16),
        'ln_scale': ln_scale,
        'w_gate_up': w_gate_up.astype(jnp.bfloat16),
        'w_attn': w_attn.astype(jnp.bfloat16),
        'w_down': w_down.astype(jnp.bfloat16),
        'w_out': w_out.astype(jnp.bfloat16),
        'k_cache': k_cache.astype(jnp.bfloat16),
        'v_cache': v_cache.astype(jnp.bfloat16),
        'lengths': lengths,
        'positions': positions,
    }


def rotary(values, positions):
    half_dim = values.shape[-1] // 2
    inv_freq = ROPE_BASE ** (-jnp.arange(half_dim, dtype=jnp.float32) / half_dim)
    angles = positions.astype(jnp.float32)[:, None, None] * inv_freq
    cos_part = jnp.cos(angles)
    sin_part = jnp.sin(angles)
    lo_half = values[..., :half_dim]
    hi_half = values[..., half_dim:]
    return jnp.concatenate([lo_half * cos_part - hi_half * sin_part, hi_half * cos_part + lo_half * sin_part], axis=-1)


def reference(x_in, ln_scale, w_gate_up, w_attn, w_down, w_out, k_cache, v_cache, lengths, positions):
    q_width = HEADS * HEAD
    x_float = x_in.astype(jnp.float32)
    mean_val = jnp.sum(x_float, axis=1, keepdims=True) / D
    var_val = jnp.sum(x_float * x_float, axis=1, keepdims=True) / D - mean_val * mean_val
    normed = ((x_float - mean_val) * lax.rsqrt(var_val + LN_EPS) * ln_scale).astype(jnp.bfloat16)
    gate_up = jnp.dot(normed, w_gate_up.reshape(D, 2 * FF), preferred_element_type=jnp.float32)
    gate_up = gate_up.astype(jnp.bfloat16).reshape(BATCH, 2, FF)
    hidden = (jax.nn.silu(gate_up[:, 0].astype(jnp.float32)) * gate_up[:, 1].astype(jnp.float32)).astype(jnp.bfloat16)
    proj_all = jnp.dot(normed, w_attn, preferred_element_type=jnp.float32).astype(jnp.bfloat16)
    q_raw = proj_all[:, :q_width].reshape(BATCH, HEADS, HEAD)
    k_tok = proj_all[:, q_width:q_width + HEAD]
    v_tok = proj_all[:, q_width + HEAD:]
    q_rot = rotary(q_raw.astype(jnp.float32), positions).astype(jnp.bfloat16)
    k_rot = rotary(k_tok[:, None, :].astype(jnp.float32), positions)[:, 0].astype(jnp.bfloat16)
    slot_ids = jnp.arange(SEQ)
    new_slot = (slot_ids[None, :] == lengths[:, None])[:, :, None]
    k_new = jnp.where(new_slot, k_rot[:, None, :], k_cache)
    v_new = jnp.where(new_slot, v_tok[:, None, :], v_cache)

    def row_attention(row_args):
        q_row, k_row, v_row, row_len = row_args
        scores = jnp.dot(q_row, k_row.T, preferred_element_type=jnp.float32) * HEAD ** -0.5
        scores = jnp.where(slot_ids[None, :] <= row_len, scores, -1e30)
        prob_row = jax.nn.softmax(scores, axis=-1).astype(jnp.bfloat16)
        return jnp.dot(prob_row, v_row, preferred_element_type=jnp.float32).astype(jnp.bfloat16)

    attn_out = lax.map(row_attention, (q_rot, k_new, v_new, lengths))
    o_flat = attn_out.reshape(BATCH, q_width)
    mixed_sum = jnp.dot(hidden, w_down, preferred_element_type=jnp.float32) + jnp.dot(o_flat, w_out, preferred_element_type=jnp.float32)
    y_out = (x_float + mixed_sum).astype(jnp.bfloat16)
    return (y_out, k_new, v_new)
```

```python
import functools

import jax
import jax.numpy as jnp
from jax import lax
from jax.experimental import pallas as pl
from jax.experimental.pallas import tpu as pltpu
from jax.sharding import PartitionSpec as P

LN_EPS = 1e-6
ROPE_BASE = 10000.0
MESH = pl.DeviceIdType.MESH
F32 = jnp.float32
BF16 = jnp.bfloat16

NZ = 4
NP = 8


def rotary(values, positions):
    half_dim = values.shape[-1] // 2
    inv_freq = ROPE_BASE ** (-jnp.arange(half_dim, dtype=jnp.float32) / half_dim)
    angles = positions.astype(jnp.float32)[:, None, None] * inv_freq
    cos_part = jnp.cos(angles)
    sin_part = jnp.sin(angles)
    lo_half = values[..., :half_dim]
    hi_half = values[..., half_dim:]
    return jnp.concatenate([lo_half * cos_part - hi_half * sin_part, hi_half * cos_part + lo_half * sin_part], axis=-1)


def coords():
    z = lax.axis_index('x')
    p = lax.axis_index('yz')
    core = p % 2
    xx = (p // 2) % 2
    y = p // 4
    partner = p + 1 - 2 * core
    xn = p + 2 - 4 * xx
    yn = p + 4 - 8 * y
    diag = xn + 4 - 8 * y
    z1 = z % 2
    z2 = z // 2
    zs = [z, 2 * z2 + 1 - z1, 2 * (1 - z2) + z1, 3 - z]
    return z, p, core, partner, xn, yn, diag, zs


def entry_barrier(z, p, zs):
    sem = pltpu.get_barrier_semaphore()
    for k in range(1, NZ):
        pl.semaphore_signal(sem, inc=1, device_id=(zs[k], p), device_id_type=MESH)
    for k in range(1, NP):
        pl.semaphore_signal(sem, inc=1, device_id=(z, (p + k) % NP), device_id_type=MESH)
    pl.semaphore_wait(sem, NZ - 1 + NP - 1)


def rcopy(src, dst, send, recv, dev):
    return pltpu.make_async_remote_copy(src_ref=src, dst_ref=dst, send_sem=send, recv_sem=recv, device_id=dev, device_id_type=MESH)


def kernel_a(xT_ref, ln_ref, wattn_ref, hT_ref, qkv_ref,
             xg, lng, zsend, zrecv, zq, s1, s2,
             xsend, xrecv, lsend, lrecv, zsend_sem, zrecv_sem, qsend, qrecv):
    z, p, core, partner, xn, yn, diag, zs = coords()
    xg[z, p] = xT_ref[...]
    lng[z, p] = ln_ref[...]
    entry_barrier(z, p, zs)
    sends = []

    def send(sem_i, src_z, src_p, dev):
        c = rcopy(xg.at[src_z, src_p], xg.at[src_z, src_p], xsend.at[sem_i], xrecv.at[src_z, src_p], dev)
        c.start()
        sends.append(c)

    def lsendf(sem_i, src_z, src_p, dev):
        c = rcopy(lng.at[src_z, src_p], lng.at[src_z, src_p], lsend.at[sem_i], lrecv.at[src_z, src_p], dev)
        c.start()
        sends.append(c)

    def wait_x(src_z, src_p):
        rcopy(xg.at[src_z, src_p], xg.at[src_z, src_p], xsend.at[0], xrecv.at[src_z, src_p], (z, p)).wait_recv()

    def wait_l(src_z, src_p):
        rcopy(lng.at[src_z, src_p], lng.at[src_z, src_p], lsend.at[0], lrecv.at[src_z, src_p], (z, p)).wait_recv()

    n = 0
    ln = 0
    for k in (3, 2, 1):
        lsendf(ln, z, p, (zs[k], p))
        send(n, z, p, (zs[k], p))
        n += 1
        ln += 1
    for k in range(NZ):
        if k:
            wait_x(zs[k], p)
            wait_l(zs[k], p)
        for dev in (xn, yn, partner):
            send(n, zs[k], p, (z, dev))
            n += 1
        for j in range(1, NP):
            lsendf(ln, zs[k], p, (z, (p + j) % NP))
            ln += 1
    for k in range(NZ):
        wait_x(zs[k], xn)
        if k < 2:
            send(n, zs[k], xn, (z, yn))
            n += 1
        send(n, zs[k], xn, (z, partner))
        n += 1
        wait_x(zs[k], yn)
        if k >= 2:
            send(n, zs[k], yn, (z, xn))
            n += 1
        send(n, zs[k], yn, (z, partner))
        n += 1
    for k in range(NZ):
        wait_x(zs[k], diag)
        send(n, zs[k], diag, (z, partner))
        n += 1
    pd = [partner + xn - p, partner + yn - p, partner + diag - p]
    for k in range(NZ):
        wait_x(zs[k], partner)
    for k in range(NZ):
        for q in pd:
            wait_x(zs[k], q)
    for k in range(NZ):
        for j in range(1, NP):
            wait_l(zs[k], (p + j) % NP)

    s1[...] = jnp.zeros_like(s1)
    s2[...] = jnp.zeros_like(s2)

    def stat(i, carry):
        blk = xg[i // NP, i % NP].astype(F32).reshape(8, 8, 512)
        s1[...] += jnp.sum(blk, axis=0)
        s2[...] += jnp.sum(blk * blk, axis=0)
        return carry

    lax.fori_loop(0, NZ * NP, stat, 0)
    mean = jnp.sum(s1[...], axis=0, keepdims=True) / 2048.0
    var = jnp.sum(s2[...], axis=0, keepdims=True) / 2048.0 - mean * mean
    rstd = lax.rsqrt(var + LN_EPS)
    lnT = jnp.concatenate([lng[i // NP, i % NP, 0:1, :] for i in range(32)] + [jnp.zeros((96, 128), F32)], axis=0).T
    for i in range(NZ * NP):
        sc = lnT[0:64, i:i + 1]
        hT_ref[i * 64:(i + 1) * 64, :] = ((xg[i // NP, i % NP].astype(F32) - mean) * rstd * sc).astype(BF16)

    h_mine = hT_ref[pl.ds(pl.multiple_of(z * 512, 512), 512), :]
    part = jnp.dot(wattn_ref[...], h_mine, preferred_element_type=F32)
    for q in range(NZ):
        zsend[q] = part[:, q * 128:(q + 1) * 128]
    for k in (3, 2, 1):
        c = rcopy(zsend.at[zs[k]], zrecv.at[z], zsend_sem.at[k], zrecv_sem.at[z], (zs[k], p))
        c.start()
        sends.append(c)
    for k in range(1, NZ):
        rcopy(zsend.at[0], zrecv.at[zs[k]], zsend_sem.at[0], zrecv_sem.at[zs[k]], (z, p)).wait_recv()
    zrecv[z] = zsend[z]
    zt = zrecv[0] + zrecv[1] + zrecv[2] + zrecv[3]
    ztt = zt.T.astype(BF16)
    zq[...] = ztt.reshape(NP, 16, 288)
    for j in range(1, NP):
        q = (p + j) % NP
        c = rcopy(zq.at[q], qkv_ref.at[p], qsend.at[j], qrecv.at[p], (z, q))
        c.start()
        sends.append(c)
    qkv_ref[p] = zq[p]
    for j in range(1, NP):
        q = (p + j) % NP
        rcopy(zq.at[0], qkv_ref.at[q], qsend.at[0], qrecv.at[q], (z, p)).wait_recv()
    for c in sends:
        c.wait_send()


def call_a(xT, lnb, wattnT):
    vm = pl.BlockSpec(memory_space=pltpu.VMEM)
    return pl.pallas_call(
        kernel_a,
        out_shape=(jax.ShapeDtypeStruct((2048, 512), BF16), jax.ShapeDtypeStruct((NP, 16, 288), BF16)),
        in_specs=[vm] * 3,
        out_specs=(vm, vm),
        scratch_shapes=[
            pltpu.VMEM((NZ, NP, 64, 512), BF16),
            pltpu.VMEM((NZ, NP, 8, 128), F32),
            pltpu.VMEM((NZ, 288, 128), F32),
            pltpu.VMEM((NZ, 288, 128), F32),
            pltpu.VMEM((NP, 16, 288), BF16),
            pltpu.VMEM((8, 512), F32),
            pltpu.VMEM((8, 512), F32),
            pltpu.SemaphoreType.DMA((40,)),
            pltpu.SemaphoreType.DMA((NZ, NP)),
            pltpu.SemaphoreType.DMA((40,)),
            pltpu.SemaphoreType.DMA((NZ, NP)),
            pltpu.SemaphoreType.DMA((NZ,)),
            pltpu.SemaphoreType.DMA((NZ,)),
            pltpu.SemaphoreType.DMA((NP,)),
            pltpu.SemaphoreType.DMA((NP,)),
        ],
        compiler_params=pltpu.CompilerParams(collective_id=0, has_side_effects=True, vmem_limit_bytes=32 * 1024 * 1024),
        name='gather_norm_qkv',
    )(xT, lnb, wattnT)


def kernel_b(len_ref, q_ref, k_ref, v_ref, kc_ref, vc_ref, o_ref, kn_ref, vn_ref):
    b = pl.program_id(0)
    length = len_ref[b]
    kn_ref[...] = kc_ref[...]
    vn_ref[...] = vc_ref[...]
    base = pl.multiple_of((length // 16) * 16, 16)
    rows = base + lax.broadcasted_iota(jnp.int32, (16, 128), 0)
    hit = rows == length
    kn_ref[0, pl.ds(base, 16), :] = jnp.where(hit, k_ref[0].astype(F32), kc_ref[0, pl.ds(base, 16), :].astype(F32)).astype(BF16)
    vn_ref[0, pl.ds(base, 16), :] = jnp.where(hit, v_ref[0].astype(F32), vc_ref[0, pl.ds(base, 16), :].astype(F32)).astype(BF16)
    scores = lax.dot_general(q_ref[0], kn_ref[0], (((1,), (1,)), ((), ())), preferred_element_type=F32) * (128.0 ** -0.5)
    slot = lax.broadcasted_iota(jnp.int32, scores.shape, 1)
    scores = jnp.where(slot <= length, scores, -1e30)
    top = jnp.max(scores, axis=1, keepdims=True)
    e = jnp.exp(scores - top)
    probs = (e / jnp.sum(e, axis=1, keepdims=True)).astype(BF16)
    o_ref[0] = jnp.dot(probs, vn_ref[0], preferred_element_type=F32).astype(BF16)


def call_b(lengths, q_rot, k_rot, v_tok, k_cache, v_cache):
    rows, seq, hd = k_cache.shape
    heads = q_rot.shape[1]
    blk = lambda *s: pl.BlockSpec((1,) + s, lambda i, *_: (i, 0, 0))
    return pl.pallas_call(
        kernel_b,
        grid_spec=pltpu.PrefetchScalarGridSpec(
            num_scalar_prefetch=1,
            grid=(rows,),
            in_specs=[blk(heads, hd), blk(1, hd), blk(1, hd), blk(seq, hd), blk(seq, hd)],
            out_specs=(blk(heads, hd), blk(seq, hd), blk(seq, hd)),
        ),
        out_shape=(
            jax.ShapeDtypeStruct((rows, heads, hd), BF16),
            jax.ShapeDtypeStruct(k_cache.shape, BF16),
            jax.ShapeDtypeStruct(v_cache.shape, BF16),
        ),
        compiler_params=pltpu.CompilerParams(vmem_limit_bytes=60 * 1024 * 1024),
        cost_estimate=pl.CostEstimate(flops=12_000_000_000, bytes_accessed=33_000_000, transcendentals=0),
        name='attend',
    )(lengths, q_rot, k_rot, v_tok, k_cache, v_cache)


def kernel_c(hT_ref, w0_ref, w1_ref, w2_ref, w3_ref, wd_ref, wo_ref, o_ref, xT_ref, y_ref,
             wdT, woT, og, hid, ysum, r1, r2, acc4,
             osend, orecv, gsend, grecv, hsend, hrecv, r1send, r1recv, r2send, r2recv):
    z, p, core, partner, xn, yn, diag, zs = coords()
    entry_barrier(z, p, zs)
    sends = []
    for j in range(1, NP):
        q = (p + j) % NP
        c = rcopy(o_ref.at[q], og.at[z, p], osend.at[j], orecv.at[p], (z, q))
        c.start()
        sends.append(c)
    og[z, p] = o_ref[p]
    g = None
    for i, w_ref in enumerate((w0_ref, w1_ref, w2_ref, w3_ref)):
        src = (z + NZ - i) % NZ
        h_blk = hT_ref[pl.ds(pl.multiple_of(src * 512, 512), 512), :]
        t = jnp.dot(w_ref[...], h_blk, preferred_element_type=F32)
        g = t if g is None else g + t
    gate = g[0:256].astype(BF16).astype(F32)
    up = g[256:512].astype(BF16).astype(F32)
    hid[z] = (jax.nn.silu(gate) * up).astype(BF16)

    def fwd(sem, src, dev):
        c = rcopy(hid.at[src], hid.at[src], hsend.at[sem], hrecv.at[src], dev)
        c.start()

    def fwd_wait_send(sem):
        rcopy(hid.at[0], hid.at[0], hsend.at[sem], hrecv.at[0], (z, p)).wait_send()

    def wait_hid(src):
        rcopy(hid.at[0], hid.at[src], hsend.at[0], hrecv.at[src], (z, p)).wait_recv()

    @pl.when(z < 3)
    def _():
        fwd(0, z, (z + 1, p))

    @pl.when(z > 0)
    def _():
        fwd(1, z, (z - 1, p))

    for j in range(1, NP):
        q = (p + j) % NP
        rcopy(o_ref.at[0], og.at[z, q], osend.at[0], orecv.at[q], (z, p)).wait_recv()
    for k in (3, 2, 1):
        c = rcopy(og.at[z], og.at[z], gsend.at[k], grecv.at[z], (zs[k], p))
        c.start()
        sends.append(c)
    wdT[...] = wd_ref[...].T
    woT[...] = wo_ref[...].T

    for k in range(1, NZ):
        @pl.when(z >= k)
        def _():
            wait_hid(z - k)

            @pl.when(z < 3)
            def _():
                fwd(2 * k, z - k, (z + 1, p))

        @pl.when(z + k <= 3)
        def _():
            wait_hid(z + k)

            @pl.when(z > 0)
            def _():
                fwd(2 * k + 1, z + k, (z - 1, p))

    for k in range(1, NZ):
        rcopy(og.at[0], og.at[zs[k]], gsend.at[0], grecv.at[zs[k]], (z, p)).wait_recv()

    hid_all = hid[...].reshape(1024, 512)
    o_all = og[...].reshape(512, 256)
    yt = jnp.dot(wdT[...], hid_all, preferred_element_type=F32)
    yt = yt + lax.dot_general(woT[...], o_all, (((1,), (1,)), ((), ())), preferred_element_type=F32)
    ysum[...] = yt.reshape(NP, 64, 512)
    for i in range(4):
        c = rcopy(ysum.at[2 * i + 1 - core], r1.at[i], r1send.at[i], r1recv.at[i], (z, partner))
        c.start()
        sends.append(c)
    chip = p // 2
    others = [xn // 2, yn // 2, diag // 2]
    for i, (t, dev) in enumerate(zip(others, (xn, yn, diag))):
        rcopy(ysum.at[0], r1.at[t], r1send.at[0], r1recv.at[t], (z, p)).wait_recv()
        acc4[i] = ysum[2 * t + core] + r1[t]
        c = rcopy(acc4.at[i], r2.at[i], r2send.at[i], r2recv.at[i], (z, dev))
        c.start()
        sends.append(c)
    rcopy(ysum.at[0], r1.at[chip], r1send.at[0], r1recv.at[chip], (z, p)).wait_recv()
    mine = ysum[p] + r1[chip]
    for i in range(3):
        rcopy(acc4.at[0], r2.at[i], r2send.at[0], r2recv.at[i], (z, p)).wait_recv()
        mine = mine + r2[i]
    y_ref[...] = (xT_ref[...].astype(F32) + mine).astype(BF16)
    for c in sends:
        c.wait_send()

    for k in range(NZ):
        @pl.when((z >= k) & (z < 3))
        def _():
            fwd_wait_send(2 * k)

        @pl.when((z + k <= 3) & (z > 0))
        def _():
            fwd_wait_send(2 * k + 1)


def call_c(hT, ws, wd, wo, o8, xT):
    vm = pl.BlockSpec(memory_space=pltpu.VMEM)
    return pl.pallas_call(
        kernel_c,
        out_shape=jax.ShapeDtypeStruct((64, 512), BF16),
        in_specs=[vm] * 9,
        out_specs=vm,
        scratch_shapes=[
            pltpu.VMEM((512, 1024), BF16),
            pltpu.VMEM((512, 256), BF16),
            pltpu.VMEM((NZ, NP, 16, 256), BF16),
            pltpu.VMEM((NZ, 256, 512), BF16),
            pltpu.VMEM((NP, 64, 512), F32),
            pltpu.VMEM((4, 64, 512), F32),
            pltpu.VMEM((3, 64, 512), F32),
            pltpu.VMEM((3, 64, 512), F32),
            pltpu.SemaphoreType.DMA((NP,)),
            pltpu.SemaphoreType.DMA((NP,)),
            pltpu.SemaphoreType.DMA((NZ,)),
            pltpu.SemaphoreType.DMA((NZ,)),
            pltpu.SemaphoreType.DMA((8,)),
            pltpu.SemaphoreType.DMA((NZ,)),
            pltpu.SemaphoreType.DMA((4,)),
            pltpu.SemaphoreType.DMA((4,)),
            pltpu.SemaphoreType.DMA((3,)),
            pltpu.SemaphoreType.DMA((3,)),
        ],
        compiler_params=pltpu.CompilerParams(collective_id=1, has_side_effects=True, vmem_limit_bytes=48 * 1024 * 1024),
        cost_estimate=pl.CostEstimate(flops=12_000_000_000, bytes_accessed=6_000_000, transcendentals=0),
        name='mlp_out',
    )(hT, *ws, wd, wo, o8, xT)


def solution(mesh):
    all_axes = ('x', 'yz')

    def local_step(x_in, ln_scale, w_gate_up, w_attn, w_down, w_out, k_cache, v_cache, lengths, positions):
        z = lax.axis_index('x')
        xT = x_in.T
        wattnT = w_attn.T
        lnb = jnp.broadcast_to(jnp.pad(ln_scale, (0, 64))[None, :], (8, 128))
        w4 = jnp.transpose(w_gate_up.reshape(512, 2, NZ, 256), (2, 1, 3, 0)).reshape(NZ, 512, 512)
        hT, qkv = call_a(xT, lnb, wattnT)
        w4, hT, qkv = lax.optimization_barrier((w4, hT, qkv))
        ws = [lax.dynamic_index_in_dim(w4, z, 0, keepdims=False)]
        for s in range(1, NZ):
            piece = lax.dynamic_index_in_dim(w4, (z + s) % NZ, 0, keepdims=False)
            ws.append(lax.ppermute(piece, 'x', [(i, (i + s) % NZ) for i in range(NZ)]))
        proj = jnp.transpose(qkv, (1, 0, 2)).reshape(16, 2304)
        q_raw = proj[:, :2048].reshape(16, 16, 128)
        k_tok = proj[:, 2048:2176]
        v_tok = proj[:, 2176:]
        q_rot = rotary(q_raw.astype(F32), positions).astype(BF16)
        k_rot = rotary(k_tok[:, None, :].astype(F32), positions).astype(BF16)
        o, k_new, v_new = call_b(lengths, q_rot, k_rot, v_tok[:, None, :], k_cache, v_cache)
        o8 = jnp.transpose(o.reshape(16, NP, 256), (1, 0, 2))
        yT = call_c(hT, ws, w_down, w_out, o8, xT)
        return yT.T, k_new, v_new

    row_spec = P(None, all_axes)
    vec_spec = P(all_axes)
    cache_spec = P(all_axes, None, None)
    return jax.shard_map(
        local_step,
        mesh=mesh,
        in_specs=(row_spec, vec_spec, P('x', None, 'yz'), P('x', 'yz'), P('yz', 'x'), P('yz', 'x'), cache_spec, cache_spec, vec_spec, vec_spec),
        out_specs=(row_spec, cache_spec, cache_spec),
        check_vma=False,
    )
```

```python
import functools

import jax
import jax.numpy as jnp
from jax import lax
from jax.experimental import pallas as pl
from jax.experimental.pallas import tpu as pltpu
from jax.sharding import PartitionSpec as P

LN_EPS = 1e-6
ROPE_BASE = 10000.0
MESH = pl.DeviceIdType.MESH
F32 = jnp.float32
BF16 = jnp.bfloat16

NZ = 4
NP = 8
C1 = 64
C2 = 96
C3 = 96
CA = C1 + C2
CHUNKS = 4
LANES = 512 // CHUNKS


def rotary(values, positions):
    half_dim = values.shape[-1] // 2
    inv_freq = ROPE_BASE ** (-jnp.arange(half_dim, dtype=jnp.float32) / half_dim)
    angles = positions.astype(jnp.float32)[:, None, None] * inv_freq
    cos_part = jnp.cos(angles)
    sin_part = jnp.sin(angles)
    lo_half = values[..., :half_dim]
    hi_half = values[..., half_dim:]
    return jnp.concatenate([lo_half * cos_part - hi_half * sin_part, hi_half * cos_part + lo_half * sin_part], axis=-1)


def coords():
    z = lax.axis_index('x')
    p = lax.axis_index('yz')
    core = p % 2
    xx = (p // 2) % 2
    y = p // 4
    partner = p + 1 - 2 * core
    xn = p + 2 - 4 * xx
    yn = p + 4 - 8 * y
    diag = xn + 4 - 8 * y
    z1 = z % 2
    z2 = z // 2
    zs = [z, 2 * z2 + 1 - z1, 2 * (1 - z2) + z1, 3 - z]
    return z, p, core, partner, xn, yn, diag, zs


def entry_barrier(z, p, zs):
    sem = pltpu.get_barrier_semaphore()
    for k in range(1, NZ):
        pl.semaphore_signal(sem, inc=1, device_id=(zs[k], p), device_id_type=MESH)
    for k in range(1, NP):
        pl.semaphore_signal(sem, inc=1, device_id=(z, (p + k) % NP), device_id_type=MESH)
    pl.semaphore_wait(sem, NZ - 1 + NP - 1)


def rcopy(src, dst, send, recv, dev):
    return pltpu.make_async_remote_copy(src_ref=src, dst_ref=dst, send_sem=send, recv_sem=recv, device_id=dev, device_id_type=MESH)


def attn_start(q):
    return pl.multiple_of(64 * q + 16 * (q // 2), 16)


def kernel_a(xT_ref, ln_ref, wattn_ref, w2_ref, hT_ref, qkv_ref, w1f_ref,
             xg, lng, watt, zsend, zrecv, zq, s1, s2,
             xsend, xrecv, lsend, lrecv, asend, arecv, zsend_sem, zrecv_sem, qsend, qrecv, wsend, wrecv):
    z, p, core, partner, xn, yn, diag, zs = coords()
    xg[z, p] = xT_ref[...]
    lng[z, p] = ln_ref[...]
    entry_barrier(z, p, zs)
    sends = []

    def send(sem_i, src_z, src_p, dev):
        c = rcopy(xg.at[src_z, src_p], xg.at[src_z, src_p], xsend.at[sem_i], xrecv.at[src_z, src_p], dev)
        c.start()
        sends.append(c)

    def lsendf(sem_i, src_z, src_p, dev):
        c = rcopy(lng.at[src_z, src_p], lng.at[src_z, src_p], lsend.at[sem_i], lrecv.at[src_z, src_p], dev)
        c.start()
        sends.append(c)

    def wait_x(src_z, src_p):
        rcopy(xg.at[src_z, src_p], xg.at[src_z, src_p], xsend.at[0], xrecv.at[src_z, src_p], (z, p)).wait_recv()

    def wait_l(src_z, src_p):
        rcopy(lng.at[src_z, src_p], lng.at[src_z, src_p], lsend.at[0], lrecv.at[src_z, src_p], (z, p)).wait_recv()

    half = C1 // 2

    def w_piece(i, src, dst, k, dev):
        return rcopy(
            w2_ref.at[:, pl.ds(pl.multiple_of(dst * 256 + i * half, 16), half), :],
            w1f_ref.at[src, :, pl.ds(i * half, half), :],
            wsend.at[i, k], wrecv.at[i, src], dev)

    def send_w(i):
        for k in (3, 2, 1):
            c = w_piece(i, z, zs[k], k, (zs[k], p))
            c.start()
            sends.append(c)

    n = 0
    ln = 0
    for k in (3, 2, 1):
        send(n, z, p, (zs[k], p))
        lsendf(ln, z, p, (zs[k], p))
        n += 1
        ln += 1
    for dev in (xn, yn, partner):
        send(n, z, p, (z, dev))
        n += 1
    for k in (3, 2, 1):
        c = rcopy(wattn_ref.at[pl.ds(attn_start(zs[k]), 80), :], watt.at[z], asend.at[k], arecv.at[z], (zs[k], p))
        c.start()
        sends.append(c)
    send_w(0)
    watt[z] = wattn_ref[pl.ds(attn_start(z), 80), :]
    for j in range(1, NP):
        lsendf(ln, z, p, (z, (p + j) % NP))
        ln += 1
    for k in range(1, NZ):
        wait_x(zs[k], p)
        for dev in (xn, yn, partner):
            send(n, zs[k], p, (z, dev))
            n += 1
        wait_l(zs[k], p)
        for j in range(1, NP):
            lsendf(ln, zs[k], p, (z, (p + j) % NP))
            ln += 1
    for k in range(NZ):
        wait_x(zs[k], xn)
        if k % 2:
            send(n, zs[k], xn, (z, yn))
            n += 1
        send(n, zs[k], xn, (z, partner))
        n += 1
        wait_x(zs[k], yn)
        if k % 2 == 0:
            send(n, zs[k], yn, (z, xn))
            n += 1
        send(n, zs[k], yn, (z, partner))
        n += 1
    for k in range(NZ):
        wait_x(zs[k], diag)
        send(n, zs[k], diag, (z, partner))
        n += 1
    pd = [partner + xn - p, partner + yn - p, partner + diag - p]
    for k in range(NZ):
        wait_x(zs[k], partner)
    for k in range(NZ):
        for q in pd:
            wait_x(zs[k], q)
    for k in range(NZ):
        for j in range(1, NP):
            wait_l(zs[k], (p + j) % NP)

    s1[...] = jnp.zeros_like(s1)
    s2[...] = jnp.zeros_like(s2)

    def stat(i, carry):
        blk = xg[i // NP, i % NP].astype(F32).reshape(8, 8, 512)
        s1[...] += jnp.sum(blk, axis=0)
        s2[...] += jnp.sum(blk * blk, axis=0)
        return carry

    lax.fori_loop(0, NZ * NP, stat, 0)
    mean = jnp.sum(s1[...], axis=0, keepdims=True) / 2048.0
    var = jnp.sum(s2[...], axis=0, keepdims=True) / 2048.0 - mean * mean
    rstd = lax.rsqrt(var + LN_EPS)
    lnT = jnp.concatenate([lng[i // NP, i % NP, 0:1, :] for i in range(32)] + [jnp.zeros((96, 128), F32)], axis=0).T
    for i in range(NZ * NP):
        sc = lnT[0:64, i:i + 1]
        hT_ref[i * 64:(i + 1) * 64, :] = ((xg[i // NP, i % NP].astype(F32) - mean) * rstd * sc).astype(BF16)

    for k in range(1, NZ):
        rcopy(watt.at[z], watt.at[zs[k]], asend.at[0], arecv.at[zs[k]], (z, p)).wait_recv()
    part = None
    for q in range(NZ):
        t = jnp.dot(watt[q], hT_ref[q * 512:(q + 1) * 512, :], preferred_element_type=F32)
        part = t if part is None else part + t
    part = part.astype(BF16)
    for q in range(NZ):
        zsend[q] = part[:, q * 128:(q + 1) * 128]
    for k in (3, 2, 1):
        c = rcopy(zsend.at[zs[k]], zrecv.at[z], zsend_sem.at[k], zrecv_sem.at[z], (zs[k], p))
        c.start()
        sends.append(c)
    send_w(1)
    zrecv[z] = zsend[z]
    for k in range(1, NZ):
        rcopy(zsend.at[0], zrecv.at[zs[k]], zsend_sem.at[0], zrecv_sem.at[zs[k]], (z, p)).wait_recv()
    zt = jnp.concatenate([zrecv[0].astype(F32), zrecv[1].astype(F32)[16:80], zrecv[2].astype(F32), zrecv[3].astype(F32)[16:80]], axis=0)
    zq[...] = zt.T.astype(BF16).reshape(NP, 16, 288)
    for j in range(1, NP):
        q = (p + j) % NP
        c = rcopy(zq.at[q], qkv_ref.at[p], qsend.at[j], qrecv.at[p], (z, q))
        c.start()
        sends.append(c)
    qkv_ref[p] = zq[p]
    for j in range(1, NP):
        q = (p + j) % NP
        rcopy(zq.at[0], qkv_ref.at[q], qsend.at[0], qrecv.at[q], (z, p)).wait_recv()
    for i in range(2):
        for k in range(1, NZ):
            w_piece(i, zs[k], z, 0, (z, p)).wait_recv()
    for c in sends:
        c.wait_send()


def call_a(xT, lnb, wattnT, w2):
    vm = pl.BlockSpec(memory_space=pltpu.VMEM)
    hbm = pl.BlockSpec(memory_space=pl.ANY)
    return pl.pallas_call(
        kernel_a,
        out_shape=(
            jax.ShapeDtypeStruct((2048, 512), BF16),
            jax.ShapeDtypeStruct((NP, 16, 288), BF16),
            jax.ShapeDtypeStruct((NZ, 2, C1, 512), BF16),
        ),
        in_specs=[vm] * 3 + [hbm],
        out_specs=(vm, vm, hbm),
        scratch_shapes=[
            pltpu.VMEM((NZ, NP, 64, 512), BF16),
            pltpu.VMEM((NZ, NP, 8, 128), F32),
            pltpu.VMEM((NZ, 80, 512), BF16),
            pltpu.VMEM((NZ, 80, 128), BF16),
            pltpu.VMEM((NZ, 80, 128), BF16),
            pltpu.VMEM((NP, 16, 288), BF16),
            pltpu.VMEM((8, 512), F32),
            pltpu.VMEM((8, 512), F32),
            pltpu.SemaphoreType.DMA((40,)),
            pltpu.SemaphoreType.DMA((NZ, NP)),
            pltpu.SemaphoreType.DMA((40,)),
            pltpu.SemaphoreType.DMA((NZ, NP)),
            pltpu.SemaphoreType.DMA((NZ,)),
            pltpu.SemaphoreType.DMA((NZ,)),
            pltpu.SemaphoreType.DMA((NZ,)),
            pltpu.SemaphoreType.DMA((NZ,)),
            pltpu.SemaphoreType.DMA((NP,)),
            pltpu.SemaphoreType.DMA((NP,)),
            pltpu.SemaphoreType.DMA((2, NZ)),
            pltpu.SemaphoreType.DMA((2, NZ)),
        ],
        compiler_params=pltpu.CompilerParams(collective_id=0, has_side_effects=True, vmem_limit_bytes=56 * 1024 * 1024),
        name='gather_norm_qkv',
    )(xT, lnb, wattnT, w2)


def kernel_b(len_ref, q_ref, k_ref, v_ref, kc_ref, vc_ref, o_ref, kn_ref, vn_ref, kbuf, vbuf, isem, osem):
    rows = kbuf.shape[0]
    seq = kbuf.shape[1]

    def load(b, t):
        return pltpu.make_async_copy((kc_ref, vc_ref)[t].at[b], (kbuf, vbuf)[t].at[b], isem.at[b, t])

    def store(b, t):
        return pltpu.make_async_copy((kbuf, vbuf)[t].at[b], (kn_ref, vn_ref)[t].at[b], osem.at[b, t])

    for b in range(rows):
        load(b, 0).start()
        load(b, 1).start()

    def insert(buf, b, length, new):
        base = pl.multiple_of((length // 16) * 16, 16)
        hit = base + lax.broadcasted_iota(jnp.int32, (16, 128), 0) == length
        buf[b, pl.ds(base, 16), :] = jnp.where(hit, new.astype(F32), buf[b, pl.ds(base, 16), :].astype(F32)).astype(BF16)

    def attend(b, length, n):
        scores = lax.dot_general(q_ref[b], kbuf[b, 0:n, :], (((1,), (1,)), ((), ())), preferred_element_type=F32) * (128.0 ** -0.5)
        slot = lax.broadcasted_iota(jnp.int32, scores.shape, 1)
        scores = jnp.where(slot <= length, scores, -1e30)
        top = jnp.max(scores, axis=1, keepdims=True)
        e = jnp.exp(scores - top)
        probs = (e / jnp.sum(e, axis=1, keepdims=True)).astype(BF16)
        return jnp.dot(probs, vbuf[b, 0:n, :], preferred_element_type=F32).astype(BF16)

    def pair(i, carry):
        b0 = 2 * i
        b1 = 2 * i + 1
        l0 = len_ref[b0]
        l1 = len_ref[b1]
        for b, length in ((b0, l0), (b1, l1)):
            load(b, 0).wait()
            load(b, 1).wait()
            insert(kbuf, b, length, k_ref[b])
            insert(vbuf, b, length, v_ref[b])
        last = jnp.maximum(l0, l1) // 512
        for t in range(seq // 512):
            @pl.when(last == t)
            def _():
                n = 512 * (t + 1)
                r0 = attend(b0, l0, n)
                r1 = attend(b1, l1, n)
                o_ref[b0] = r0
                o_ref[b1] = r1
        for b in (b0, b1):
            store(b, 0).start()
            store(b, 1).start()
        return carry

    lax.fori_loop(0, rows // 2, pair, 0)
    for b in range(rows):
        store(b, 0).wait()
        store(b, 1).wait()


def call_b(lengths, q_rot, k_rot, v_tok, k_cache, v_cache):
    rows, seq, hd = k_cache.shape
    heads = q_rot.shape[1]
    vm = pl.BlockSpec(memory_space=pltpu.VMEM)
    hbm = pl.BlockSpec(memory_space=pl.ANY)
    return pl.pallas_call(
        kernel_b,
        in_specs=[pl.BlockSpec(memory_space=pltpu.SMEM), vm, vm, vm, hbm, hbm],
        out_specs=(vm, hbm, hbm),
        out_shape=(
            jax.ShapeDtypeStruct((rows, heads, hd), BF16),
            jax.ShapeDtypeStruct(k_cache.shape, BF16),
            jax.ShapeDtypeStruct(v_cache.shape, BF16),
        ),
        scratch_shapes=[
            pltpu.VMEM((rows, seq, hd), BF16),
            pltpu.VMEM((rows, seq, hd), BF16),
            pltpu.SemaphoreType.DMA((rows, 2)),
            pltpu.SemaphoreType.DMA((rows, 2)),
        ],
        compiler_params=pltpu.CompilerParams(vmem_limit_bytes=58 * 1024 * 1024),
        cost_estimate=pl.CostEstimate(flops=12_000_000_000, bytes_accessed=33_000_000, transcendentals=0),
        name='attend',
    )(lengths, q_rot, k_rot, v_tok, k_cache, v_cache)


def kernel_c(hT_hbm, w2_ref, w1f_ref, p1_ref, p2_ref, p3_ref, wd_hbm, wo_hbm, o_ref, xT_ref, y_ref,
             hT, wvA, wvB, wd, wo, wdAT, wdBT, woT, og, hidA, hidB, yA, ysum, r1, acc, r2,
             lsem, wsem, wbsend, wbrecv, osend, orecv, gsend, grecv, hasend, harecv, hbsend, hbrecv,
             r1send, r1recv, r2send, r2recv):
    z, p, core, partner, xn, yn, diag, zs = coords()
    local = [pltpu.make_async_copy(hT_hbm, hT, lsem.at[0])]
    local.append(pltpu.make_async_copy(w2_ref.at[:, pl.ds(pl.multiple_of(z * 256, 256), CA), :], wvA.at[z], wsem.at[0]))
    for s, p_ref in ((1, p1_ref), (2, p2_ref), (3, p3_ref)):
        src = (z + NZ - s) % NZ
        local.append(pltpu.make_async_copy(w1f_ref.at[src], wvA.at[src, :, pl.ds(0, C1), :], wsem.at[2 * s]))
        local.append(pltpu.make_async_copy(p_ref, wvA.at[src, :, pl.ds(C1, C2), :], wsem.at[2 * s + 1]))
    late = [
        pltpu.make_async_copy(w2_ref.at[:, pl.ds(pl.multiple_of(z * 256 + CA, 32), C3), :], wvB.at[z], wsem.at[1]),
        pltpu.make_async_copy(wd_hbm, wd, lsem.at[1]),
        pltpu.make_async_copy(wo_hbm, wo, lsem.at[2]),
    ]
    for c in local + late:
        c.start()
    entry_barrier(z, p, zs)
    sends = []

    def w_piece(src, dst, k, dev):
        return rcopy(w2_ref.at[:, pl.ds(pl.multiple_of(dst * 256 + CA, 32), C3), :], wvB.at[src], wbsend.at[k], wbrecv.at[src], dev)

    for k in (3, 2, 1):
        c = w_piece(z, zs[k], k, (zs[k], p))
        c.start()
        sends.append(c)
    for j in range(1, NP):
        q = (p + j) % NP
        c = rcopy(o_ref.at[q], og.at[z, p], osend.at[j], orecv.at[p], (z, q))
        c.start()
        sends.append(c)
    og[z, p] = o_ref[p]

    def gated(wv, n):
        g = None
        for q in range(NZ):
            t = jnp.dot(wv[q].reshape(2 * n, 512), hT[q * 512:(q + 1) * 512, :], preferred_element_type=F32)
            g = t if g is None else g + t
        gate = g[0:n].astype(BF16).astype(F32)
        up = g[n:2 * n].astype(BF16).astype(F32)
        return (jax.nn.silu(gate) * up).astype(BF16)

    def fwd_a(sem, src, dev):
        return rcopy(hidA.at[src], hidA.at[src], hasend.at[sem], harecv.at[src], dev)

    def fwd_b(sem, src, ch, dev):
        return rcopy(hidB.at[ch, src], hidB.at[ch, src], hbsend.at[sem, ch], hbrecv.at[src, ch], dev)

    for c in local:
        c.wait()
    hidA[z] = gated(wvA, CA)

    @pl.when(z < 3)
    def _():
        fwd_a(0, z, (z + 1, p)).start()

    @pl.when(z > 0)
    def _():
        fwd_a(1, z, (z - 1, p)).start()

    for j in range(1, NP):
        q = (p + j) % NP
        rcopy(o_ref.at[0], og.at[z, q], osend.at[0], orecv.at[q], (z, p)).wait_recv()
    for k in (3, 2, 1):
        c = rcopy(og.at[z], og.at[z], gsend.at[k], grecv.at[z], (zs[k], p))
        c.start()
        sends.append(c)
    for c in late:
        c.wait()
    wdAT[...] = jnp.concatenate([wd[q * 256:q * 256 + CA, :] for q in range(NZ)], axis=0).T
    wdBT[...] = jnp.concatenate([wd[q * 256 + CA:(q + 1) * 256, :] for q in range(NZ)], axis=0).T
    woT[...] = wo[...].T

    def pass_a(k):
        @pl.when(z >= k)
        def _():
            fwd_a(0, z - k, (z, p)).wait_recv()

            @pl.when(z < 3)
            def _():
                fwd_a(2 * k, z - k, (z + 1, p)).start()

        @pl.when(z + k <= 3)
        def _():
            fwd_a(0, z + k, (z, p)).wait_recv()

            @pl.when(z > 0)
            def _():
                fwd_a(2 * k + 1, z + k, (z - 1, p)).start()

    for k in range(1, NZ):
        w_piece(zs[k], z, 0, (z, p)).wait_recv()
    hb = gated(wvB, C3)
    for ch in range(CHUNKS):
        hidB[ch, z] = hb[:, ch * LANES:(ch + 1) * LANES]
    pass_a(1)

    @pl.when(z < 3)
    def _():
        for ch in range(CHUNKS):
            fwd_b(0, z, ch, (z + 1, p)).start()

    @pl.when(z > 0)
    def _():
        for ch in range(CHUNKS):
            fwd_b(1, z, ch, (z - 1, p)).start()

    pass_a(2)
    pass_a(3)

    def pass_b(k, ch):
        @pl.when(z >= k)
        def _():
            fwd_b(0, z - k, ch, (z, p)).wait_recv()

            @pl.when(z < 3)
            def _():
                fwd_b(2 * k, z - k, ch, (z + 1, p)).start()

        @pl.when(z + k <= 3)
        def _():
            fwd_b(0, z + k, ch, (z, p)).wait_recv()

            @pl.when(z > 0)
            def _():
                fwd_b(2 * k + 1, z + k, ch, (z - 1, p)).start()

    for ch in range(CHUNKS):
        pass_b(1, ch)
    for k in range(1, NZ):
        rcopy(og.at[0], og.at[zs[k]], gsend.at[0], grecv.at[zs[k]], (z, p)).wait_recv()
    yA[...] = jnp.dot(wdAT[...], hidA[...].reshape(NZ * CA, 512), preferred_element_type=F32) + lax.dot_general(
        woT[...], og[...].reshape(512, 256), (((1,), (1,)), ((), ())), preferred_element_type=F32)
    for ch in range(CHUNKS):
        pass_b(2, ch)

    chip = p // 2
    others = [xn // 2, yn // 2, diag // 2]

    def d2d(ch):
        return rcopy(ysum.at[ch, 1 - core], r1.at[ch], r1send.at[ch], r1recv.at[ch], (z, partner))

    def hop(ch, i, dev):
        return rcopy(acc.at[ch, i], r2.at[ch, i], r2send.at[ch, i], r2recv.at[ch, i], (z, dev))

    def stage1(ch):
        pass_b(3, ch)
        lanes = slice(ch * LANES, (ch + 1) * LANES)
        yt = yA[:, lanes] + jnp.dot(wdBT[...], hidB[ch].reshape(NZ * C3, LANES), preferred_element_type=F32)
        yt = yt.reshape(4, 2, 64, LANES)
        for i in range(4):
            for j in range(2):
                ysum[ch, j, i] = yt[i, j]
        d2d(ch).start()

    def stage2(ch):
        d2d(ch).wait_recv()
        for i, (t, dev) in enumerate(zip(others, (xn, yn, diag))):
            acc[ch, i] = ysum[ch, core, t] + r1[ch, t]
            hop(ch, i, dev).start()

    def stage3(ch):
        lanes = slice(ch * LANES, (ch + 1) * LANES)
        mine = ysum[ch, core, chip] + r1[ch, chip]
        for i, dev in enumerate((xn, yn, diag)):
            hop(ch, i, dev).wait_recv()
            mine = mine + r2[ch, i]
        y_ref[:, lanes] = (xT_ref[:, lanes].astype(F32) + mine).astype(BF16)

    for t in range(CHUNKS + 2):
        if t < CHUNKS:
            stage1(t)
        if 1 <= t <= CHUNKS:
            stage2(t - 1)
        if t >= 2:
            stage3(t - 2)

    for c in sends:
        c.wait_send()
    for ch in range(CHUNKS):
        d2d(ch).wait_send()
        for i, dev in enumerate((xn, yn, diag)):
            hop(ch, i, dev).wait_send()
    for k in range(NZ - 1):
        @pl.when((z >= k) & (z < 3))
        def _():
            fwd_a(2 * k, z, (z, p)).wait_send()
            for ch in range(CHUNKS):
                fwd_b(2 * k, z, ch, (z, p)).wait_send()

        @pl.when((z + k <= 3) & (z > 0))
        def _():
            fwd_a(2 * k + 1, z, (z, p)).wait_send()
            for ch in range(CHUNKS):
                fwd_b(2 * k + 1, z, ch, (z, p)).wait_send()


def call_c(hT, w2, w1f, ps, wd, wo, o8, xT):
    vm = pl.BlockSpec(memory_space=pltpu.VMEM)
    hbm = pl.BlockSpec(memory_space=pl.ANY)
    return pl.pallas_call(
        kernel_c,
        out_shape=jax.ShapeDtypeStruct((64, 512), BF16),
        in_specs=[hbm] * 8 + [vm, vm],
        out_specs=vm,
        scratch_shapes=[
            pltpu.VMEM((2048, 512), BF16),
            pltpu.VMEM((NZ, 2, CA, 512), BF16),
            pltpu.VMEM((NZ, 2, C3, 512), BF16),
            pltpu.VMEM((1024, 512), BF16),
            pltpu.VMEM((256, 512), BF16),
            pltpu.VMEM((512, NZ * CA), BF16),
            pltpu.VMEM((512, NZ * C3), BF16),
            pltpu.VMEM((512, 256), BF16),
            pltpu.VMEM((NZ, NP, 16, 256), BF16),
            pltpu.VMEM((NZ, CA, 512), BF16),
            pltpu.VMEM((CHUNKS, NZ, C3, LANES), BF16),
            pltpu.VMEM((512, 512), F32),
            pltpu.VMEM((CHUNKS, 2, 4, 64, LANES), F32),
            pltpu.VMEM((CHUNKS, 4, 64, LANES), F32),
            pltpu.VMEM((CHUNKS, 3, 64, LANES), F32),
            pltpu.VMEM((CHUNKS, 3, 64, LANES), F32),
            pltpu.SemaphoreType.DMA((3,)),
            pltpu.SemaphoreType.DMA((8,)),
            pltpu.SemaphoreType.DMA((NZ,)),
            pltpu.SemaphoreType.DMA((NZ,)),
            pltpu.SemaphoreType.DMA((NP,)),
            pltpu.SemaphoreType.DMA((NP,)),
            pltpu.SemaphoreType.DMA((NZ,)),
            pltpu.SemaphoreType.DMA((NZ,)),
            pltpu.SemaphoreType.DMA((8,)),
            pltpu.SemaphoreType.DMA((NZ,)),
            pltpu.SemaphoreType.DMA((8, CHUNKS)),
            pltpu.SemaphoreType.DMA((NZ, CHUNKS)),
            pltpu.SemaphoreType.DMA((CHUNKS,)),
            pltpu.SemaphoreType.DMA((CHUNKS,)),
            pltpu.SemaphoreType.DMA((CHUNKS, 3)),
            pltpu.SemaphoreType.DMA((CHUNKS, 3)),
        ],
        compiler_params=pltpu.CompilerParams(collective_id=1, has_side_effects=True, vmem_limit_bytes=58 * 1024 * 1024),
        cost_estimate=pl.CostEstimate(flops=12_000_000_000, bytes_accessed=6_000_000, transcendentals=0),
        name='mlp_out',
    )(hT, w2, w1f, *ps, wd, wo, o8, xT)


def solution(mesh):
    all_axes = ('x', 'yz')

    def local_step(x_in, ln_scale, w_gate_up, w_attn, w_down, w_out, k_cache, v_cache, lengths, positions):
        z = lax.axis_index('x')
        xT = x_in.T
        wattnT = w_attn.T
        lnb = jnp.broadcast_to(jnp.pad(ln_scale, (0, 64))[None, :], (8, 128))
        w2 = jnp.transpose(w_gate_up, (1, 2, 0))
        hT, qkv, w1f = call_a(xT, lnb, wattnT, w2)
        w2b, hT, qkv, w1f = lax.optimization_barrier((w2, hT, qkv, w1f))
        ps = []
        for s in range(1, NZ):
            piece = lax.dynamic_slice(w2b, (0, ((z + s) % NZ) * 256 + C1, 0), (2, C2, 512))
            ps.append(lax.ppermute(piece, 'x', [(i, (i + s) % NZ) for i in range(NZ)]))
        proj = jnp.transpose(qkv, (1, 0, 2)).reshape(16, 2304)
        q_raw = proj[:, :2048].reshape(16, 16, 128)
        k_tok = proj[:, 2048:2176]
        v_tok = proj[:, 2176:]
        q_rot = rotary(q_raw.astype(F32), positions).astype(BF16)
        k_rot = rotary(k_tok[:, None, :].astype(F32), positions).astype(BF16)
        o, k_new, v_new = call_b(lengths, q_rot, k_rot, v_tok[:, None, :], k_cache, v_cache)
        o8 = jnp.transpose(o.reshape(16, NP, 256), (1, 0, 2))
        yT = call_c(hT, w2b, w1f, ps, w_down, w_out, o8, xT)
        return yT.T, k_new, v_new

    row_spec = P(None, all_axes)
    vec_spec = P(all_axes)
    cache_spec = P(all_axes, None, None)
    return jax.shard_map(
        local_step,
        mesh=mesh,
        in_specs=(row_spec, vec_spec, P('x', None, 'yz'), P('x', 'yz'), P('yz', 'x'), P('yz', 'x'), cache_spec, cache_spec, vec_spec, vec_spec),
        out_specs=(row_spec, cache_spec, cache_spec),
        check_vma=False,
    )
```

```python
import functools

import jax
import jax.numpy as jnp
from jax import lax
from jax.experimental import pallas as pl
from jax.experimental.pallas import tpu as pltpu
from jax.sharding import PartitionSpec as P

LN_EPS = 1e-6
ROPE_BASE = 10000.0
MESH = pl.DeviceIdType.MESH


class Phase:
    cm = None

    def __call__(self, name):
        if self.cm is not None:
            self.cm.__exit__(None, None, None)
            self.cm = None
        if name:
            self.cm = jax.named_scope(name)
            self.cm.__enter__()


ph = Phase()
F32 = jnp.float32
BF16 = jnp.bfloat16

NZ = 4
NP = 8
C1A = 16
C1 = 64
C2 = 128
C3 = 64
CA = C1 + C2
CHUNKS = 4
ROWS_A = CA // CHUNKS
LANES = 512 // CHUNKS


def rotary(values, positions):
    half_dim = values.shape[-1] // 2
    inv_freq = ROPE_BASE ** (-jnp.arange(half_dim, dtype=jnp.float32) / half_dim)
    angles = positions.astype(jnp.float32)[:, None, None] * inv_freq
    cos_part = jnp.cos(angles)
    sin_part = jnp.sin(angles)
    lo_half = values[..., :half_dim]
    hi_half = values[..., half_dim:]
    return jnp.concatenate([lo_half * cos_part - hi_half * sin_part, hi_half * cos_part + lo_half * sin_part], axis=-1)


def coords():
    z = lax.axis_index('x')
    p = lax.axis_index('yz')
    core = p % 2
    xx = (p // 2) % 2
    y = p // 4
    partner = p + 1 - 2 * core
    xn = p + 2 - 4 * xx
    yn = p + 4 - 8 * y
    diag = xn + 4 - 8 * y
    z1 = z % 2
    z2 = z // 2
    zs = [z, 2 * z2 + 1 - z1, 2 * (1 - z2) + z1, 3 - z]
    return z, p, core, partner, xn, yn, diag, zs


def entry_barrier(z, p, zs):
    sem = pltpu.get_barrier_semaphore()
    for k in range(1, NZ):
        pl.semaphore_signal(sem, inc=1, device_id=(zs[k], p), device_id_type=MESH)
    for k in range(1, NP):
        pl.semaphore_signal(sem, inc=1, device_id=(z, (p + k) % NP), device_id_type=MESH)
    pl.semaphore_wait(sem, NZ - 1 + NP - 1)


def rcopy(src, dst, send, recv, dev):
    return pltpu.make_async_remote_copy(src_ref=src, dst_ref=dst, send_sem=send, recv_sem=recv, device_id=dev, device_id_type=MESH)


class Relay:
    def __init__(self, z, p, at, send, recv):
        self.z, self.p, self.at, self.send, self.recv = z, p, at, send, recv

    def copy(self, way, src, ch, dev):
        ref = self.at(src, ch)
        return rcopy(ref, ref, self.send.at[way, ch], self.recv.at[src, ch], (dev, self.p))

    def own(self, chunks):
        z = self.z

        @pl.when(z < 3)
        def _():
            for ch in chunks:
                self.copy(0, z, ch, z + 1).start()

        @pl.when(z > 0)
        def _():
            for ch in chunks:
                self.copy(1, z, ch, z - 1).start()

    def step(self, k, ch):
        z = self.z

        @pl.when(z >= k)
        def _():
            self.copy(0, z - k, ch, z).wait_recv()

            @pl.when(z < 3)
            def _():
                self.copy(2 * k, z - k, ch, z + 1).start()

        @pl.when(z + k <= 3)
        def _():
            self.copy(0, z + k, ch, z).wait_recv()

            @pl.when(z > 0)
            def _():
                self.copy(2 * k + 1, z + k, ch, z - 1).start()

    def drain(self, chunks):
        z = self.z
        for k in range(NZ - 1):
            @pl.when((z >= k) & (z < 3))
            def _():
                for ch in chunks:
                    self.copy(2 * k, z, ch, z).wait_send()

            @pl.when((z + k <= 3) & (z > 0))
            def _():
                for ch in chunks:
                    self.copy(2 * k + 1, z, ch, z).wait_send()


def attn_start(q):
    return pl.multiple_of(64 * q + 16 * (q // 2), 16)


def kernel_a(xT_ref, ln_ref, wattn_ref, w_ref, hT_ref, qkv_ref, w1f_ref, w2_ref, ps1_ref, ps2_ref, ps3_ref,
             xg, lng, watt, zsend, zrecv, zq, s1, s2, wn, wt,
             xsend, xrecv, lsend, lrecv, asend, arecv, zsend_sem, zrecv_sem, qsend, qrecv, wsend, wrecv, lsem):
    z, p, core, partner, xn, yn, diag, zs = coords()
    ph('a_bar')
    wload = pltpu.make_async_copy(w_ref, wn, lsem.at[0])
    wload.start()
    xg[z, p] = xT_ref[...]
    lng[z, p] = jnp.zeros((8, 128), F32)
    lng[z, p, 0:1, 0:64] = ln_ref[...]
    entry_barrier(z, p, zs)
    ph('a_zsend')
    sends = []
    nx = iter(range(40))
    nl = iter(range(40))

    def send(src_z, src_p, dev):
        c = rcopy(xg.at[src_z, src_p], xg.at[src_z, src_p], xsend.at[next(nx)], xrecv.at[src_z, src_p], dev)
        c.start()
        sends.append(c)

    def send_l(src_z, src_p, dev):
        c = rcopy(lng.at[src_z, src_p], lng.at[src_z, src_p], lsend.at[next(nl)], lrecv.at[src_z, src_p], dev)
        c.start()
        sends.append(c)

    def wait_x(src_z, src_p):
        rcopy(xg.at[src_z, src_p], xg.at[src_z, src_p], xsend.at[0], xrecv.at[src_z, src_p], (z, p)).wait_recv()

    def wait_l(src_z, src_p):
        rcopy(lng.at[src_z, src_p], lng.at[src_z, src_p], lsend.at[0], lrecv.at[src_z, src_p], (z, p)).wait_recv()

    def stat(src_z, src_p):
        blk = xg[src_z, src_p].astype(F32).reshape(8, 8, 512)
        s1[...] += jnp.sum(blk, axis=0)
        s2[...] += jnp.sum(blk * blk, axis=0)

    spans = ((0, C1A), (C1A, C1 - C1A))

    def w_piece(i, src, dst, k, dev):
        o, n = spans[i]
        return rcopy(
            wt.at[:, pl.ds(pl.multiple_of(dst * 256 + o, 16), n), :],
            w1f_ref.at[src, :, pl.ds(o, n), :],
            wsend.at[i, k], wrecv.at[i, src], dev)

    def send_w(i):
        for k in (3, 2, 1):
            c = w_piece(i, z, zs[k], k, (zs[k], p))
            c.start()
            sends.append(c)

    def turn(odd):
        def body(i, carry):
            lanes = pl.ds(pl.multiple_of(i * 256 + odd * 128, 128), 128)
            blk = wn[:, :, lanes].astype(F32)
            for g in range(2):
                wt[g, lanes, :] = blk[:, g, :].T.astype(BF16)
            return carry

        lax.fori_loop(0, NZ, body, 0)

    for k in (3, 2, 1):
        send(z, p, (zs[k], p))
        send_l(z, p, (zs[k], p))
    for dev in (xn, yn, partner):
        send(z, p, (z, dev))
    for j in range(1, NP):
        send_l(z, p, (z, (p + j) % NP))
    s1[...] = jnp.zeros_like(s1)
    s2[...] = jnp.zeros_like(s2)
    stat(z, p)
    watt[z] = wattn_ref[pl.ds(attn_start(z), 80), :]
    wload.wait()
    turn(0)

    def column(k):
        wait_x(zs[k], p)
        for dev in (xn, yn, partner):
            send(zs[k], p, (z, dev))
        stat(zs[k], p)

    def neighbours(k):
        wait_x(zs[k], xn)
        if k % 2:
            send(zs[k], xn, (z, yn))
        send(zs[k], xn, (z, partner))
        stat(zs[k], xn)
        wait_x(zs[k], yn)
        if k % 2 == 0:
            send(zs[k], yn, (z, xn))
        send(zs[k], yn, (z, partner))
        stat(zs[k], yn)

    def diagonal(k):
        wait_x(zs[k], diag)
        send(zs[k], diag, (z, partner))
        stat(zs[k], diag)

    ph('a_col1')
    column(1)
    neighbours(0)
    ph('a_col2')
    column(2)
    neighbours(1)
    diagonal(0)
    ph('a_col3')
    column(3)
    for k in (3, 2, 1):
        c = rcopy(wattn_ref.at[pl.ds(attn_start(zs[k]), 80), :], watt.at[z], asend.at[k], arecv.at[z], (zs[k], p))
        c.start()
        sends.append(c)
    send_w(0)
    ph('a_lnsend')
    for k in range(1, NZ):
        wait_l(zs[k], p)
        for j in range(1, NP):
            send_l(zs[k], p, (z, (p + j) % NP))
    ph('a_nbr')
    neighbours(2)
    diagonal(1)
    neighbours(3)
    ph('a_diag')
    diagonal(2)
    diagonal(3)
    ph('a_rest')
    pd = [partner + xn - p, partner + yn - p, partner + diag - p]
    for q in [partner] + pd:
        for k in range(NZ):
            wait_x(zs[k], q)
            stat(zs[k], q)
    for k in range(NZ):
        for j in range(1, NP):
            wait_l(zs[k], (p + j) % NP)

    ph('a_norm')
    mean = jnp.sum(s1[...], axis=0, keepdims=True) / 2048.0
    var = jnp.sum(s2[...], axis=0, keepdims=True) / 2048.0 - mean * mean
    rstd = lax.rsqrt(var + LN_EPS)
    lnT = jnp.concatenate([lng[i // NP, i % NP, 0:1, :] for i in range(32)] + [jnp.zeros((96, 128), F32)], axis=0).T
    for i in range(NZ * NP):
        sc = lnT[0:64, i:i + 1]
        hT_ref[i * 64:(i + 1) * 64, :] = ((xg[i // NP, i % NP].astype(F32) - mean) * rstd * sc).astype(BF16)

    ph('a_attw')
    for k in range(1, NZ):
        rcopy(watt.at[z], watt.at[zs[k]], asend.at[0], arecv.at[zs[k]], (z, p)).wait_recv()
    ph('a_zdot')
    part = None
    for q in range(NZ):
        t = jnp.dot(watt[q], hT_ref[q * 512:(q + 1) * 512, :], preferred_element_type=F32)
        part = t if part is None else part + t
    part = part.astype(BF16)
    for q in range(NZ):
        zsend[q] = part[:, q * 128:(q + 1) * 128]
    for k in (3, 2, 1):
        c = rcopy(zsend.at[zs[k]], zrecv.at[z], zsend_sem.at[k], zrecv_sem.at[z], (zs[k], p))
        c.start()
        sends.append(c)
    send_w(1)
    zrecv[z] = zsend[z]
    ph('a_turn')
    turn(1)
    outs = [pltpu.make_async_copy(wt, w2_ref, lsem.at[1])]
    for i, ps_ref in enumerate((ps1_ref, ps2_ref, ps3_ref)):
        dst = (z + i + 1) % NZ
        outs.append(pltpu.make_async_copy(wt.at[:, pl.ds(pl.multiple_of(dst * 256 + C1, 16), C2), :], ps_ref, lsem.at[2 + i]))
    for c in outs[1:] + outs[:1]:
        c.start()
    ph('a_zwait')
    for k in range(1, NZ):
        rcopy(zsend.at[0], zrecv.at[zs[k]], zsend_sem.at[0], zrecv_sem.at[zs[k]], (z, p)).wait_recv()
    ph('a_a2a')
    zt = jnp.concatenate([zrecv[0].astype(F32), zrecv[1].astype(F32)[16:80], zrecv[2].astype(F32), zrecv[3].astype(F32)[16:80]], axis=0)
    zq[...] = zt.T.astype(BF16).reshape(NP, 16, 288)
    for j in range(1, NP):
        q = (p + j) % NP
        c = rcopy(zq.at[q], qkv_ref.at[p], qsend.at[j], qrecv.at[p], (z, q))
        c.start()
        sends.append(c)
    qkv_ref[p] = zq[p]
    for j in range(1, NP):
        q = (p + j) % NP
        rcopy(zq.at[0], qkv_ref.at[q], qsend.at[0], qrecv.at[q], (z, p)).wait_recv()
    ph('a_wwait')
    for i in range(2):
        for k in range(1, NZ):
            w_piece(i, zs[k], z, 0, (z, p)).wait_recv()
    ph('a_sendwait')
    for c in outs:
        c.wait()
    for c in sends:
        c.wait_send()
    ph('')


def call_a(xT, ln, wattnT, w):
    vm = pl.BlockSpec(memory_space=pltpu.VMEM)
    hbm = pl.BlockSpec(memory_space=pl.ANY)
    return pl.pallas_call(
        kernel_a,
        out_shape=(
            jax.ShapeDtypeStruct((2048, 512), BF16),
            jax.ShapeDtypeStruct((NP, 16, 288), BF16),
            jax.ShapeDtypeStruct((NZ, 2, C1, 512), BF16),
            jax.ShapeDtypeStruct((2, 1024, 512), BF16),
        ) + (jax.ShapeDtypeStruct((2, C2, 512), BF16),) * 3,
        in_specs=[vm] * 3 + [hbm],
        out_specs=(vm, vm) + (hbm,) * 5,
        scratch_shapes=[
            pltpu.VMEM((NZ, NP, 64, 512), BF16),
            pltpu.VMEM((NZ, NP, 8, 128), F32),
            pltpu.VMEM((NZ, 80, 512), BF16),
            pltpu.VMEM((NZ, 80, 128), BF16),
            pltpu.VMEM((NZ, 80, 128), BF16),
            pltpu.VMEM((NP, 16, 288), BF16),
            pltpu.VMEM((8, 512), F32),
            pltpu.VMEM((8, 512), F32),
            pltpu.VMEM((512, 2, 1024), BF16),
            pltpu.VMEM((2, 1024, 512), BF16),
            pltpu.SemaphoreType.DMA((40,)),
            pltpu.SemaphoreType.DMA((NZ, NP)),
            pltpu.SemaphoreType.DMA((40,)),
            pltpu.SemaphoreType.DMA((NZ, NP)),
            pltpu.SemaphoreType.DMA((NZ,)),
            pltpu.SemaphoreType.DMA((NZ,)),
            pltpu.SemaphoreType.DMA((NZ,)),
            pltpu.SemaphoreType.DMA((NZ,)),
            pltpu.SemaphoreType.DMA((NP,)),
            pltpu.SemaphoreType.DMA((NP,)),
            pltpu.SemaphoreType.DMA((2, NZ)),
            pltpu.SemaphoreType.DMA((2, NZ)),
            pltpu.SemaphoreType.DMA((5,)),
        ],
        compiler_params=pltpu.CompilerParams(collective_id=0, has_side_effects=True, vmem_limit_bytes=56 * 1024 * 1024),
        name='gather_norm_qkv',
    )(xT, ln, wattnT, w)


def kernel_b(len_ref, q_ref, k_ref, v_ref, kc_ref, vc_ref, o_ref, kn_ref, vn_ref, kbuf, vbuf, oscr, isem, osem):
    rows = kbuf.shape[0]
    seq = kbuf.shape[1]

    def load(b, t):
        return pltpu.make_async_copy((kc_ref, vc_ref)[t].at[b], (kbuf, vbuf)[t].at[b], isem.at[b, t])

    def store(b, t):
        return pltpu.make_async_copy((kbuf, vbuf)[t].at[b], (kn_ref, vn_ref)[t].at[b], osem.at[b, t])

    for b in range(rows):
        load(b, 0).start()
        load(b, 1).start()

    def insert(buf, b, length, new):
        base = pl.multiple_of((length // 16) * 16, 16)
        hit = base + lax.broadcasted_iota(jnp.int32, (16, 128), 0) == length
        buf[b, pl.ds(base, 16), :] = jnp.where(hit, new.astype(F32), buf[b, pl.ds(base, 16), :].astype(F32)).astype(BF16)

    def attend(b, length, n):
        scores = lax.dot_general(q_ref[b], kbuf[b, 0:n, :], (((1,), (1,)), ((), ())), preferred_element_type=F32) * (128.0 ** -0.5)
        slot = lax.broadcasted_iota(jnp.int32, scores.shape, 1)
        scores = jnp.where(slot <= length, scores, -1e30)
        top = jnp.max(scores, axis=1, keepdims=True)
        e = jnp.exp(scores - top)
        probs = (e / jnp.sum(e, axis=1, keepdims=True)).astype(BF16)
        return jnp.dot(probs, vbuf[b, 0:n, :], preferred_element_type=F32)

    def pair(i, carry):
        b0 = 2 * i
        b1 = 2 * i + 1
        l0 = len_ref[b0]
        l1 = len_ref[b1]
        for b, length in ((b0, l0), (b1, l1)):
            load(b, 0).wait()
            load(b, 1).wait()
            insert(kbuf, b, length, k_ref[b])
            insert(vbuf, b, length, v_ref[b])
        last = jnp.maximum(l0, l1) // 512
        for t in range(seq // 512):
            @pl.when(last == t)
            def _():
                n = 512 * (t + 1)
                r0 = attend(b0, l0, n)
                r1 = attend(b1, l1, n)
                oscr[b0] = r0
                oscr[b1] = r1
        for b in (b0, b1):
            store(b, 0).start()
            store(b, 1).start()
        return carry

    lax.fori_loop(0, rows // 2, pair, 0)
    for h in range(16):
        o_ref[h // 2, :, (h % 2) * 128:(h % 2 + 1) * 128] = oscr[:, h, :].astype(BF16)
    for b in range(rows):
        store(b, 0).wait()
        store(b, 1).wait()


def call_b(lengths, q_rot, k_rot, v_tok, k_cache, v_cache):
    rows, seq, hd = k_cache.shape
    heads = q_rot.shape[1]
    vm = pl.BlockSpec(memory_space=pltpu.VMEM)
    hbm = pl.BlockSpec(memory_space=pl.ANY)
    return pl.pallas_call(
        kernel_b,
        in_specs=[pl.BlockSpec(memory_space=pltpu.SMEM), vm, vm, vm, hbm, hbm],
        out_specs=(vm, hbm, hbm),
        out_shape=(
            jax.ShapeDtypeStruct((NP, rows, heads * hd // NP), BF16),
            jax.ShapeDtypeStruct(k_cache.shape, BF16),
            jax.ShapeDtypeStruct(v_cache.shape, BF16),
        ),
        scratch_shapes=[
            pltpu.VMEM((rows, seq, hd), BF16),
            pltpu.VMEM((rows, seq, hd), BF16),
            pltpu.VMEM((rows, heads, hd), F32),
            pltpu.SemaphoreType.DMA((rows, 2)),
            pltpu.SemaphoreType.DMA((rows, 2)),
        ],
        compiler_params=pltpu.CompilerParams(vmem_limit_bytes=58 * 1024 * 1024),
        cost_estimate=pl.CostEstimate(flops=12_000_000_000, bytes_accessed=33_000_000, transcendentals=0),
        name='attend',
    )(lengths, q_rot, k_rot, v_tok, k_cache, v_cache)


def kernel_c(hT_hbm, w2_ref, w1f_ref, p1_ref, p2_ref, p3_ref, wd_hbm, wo_hbm, o_ref, xT_ref, y_ref,
             hT, wvA, wvB, wd, wo, wdAT, wdBT, woT, og, hidA, hidB, yA, ysum, r1, acc, r2,
             lsem, wsem, wbsend, wbrecv, osend, orecv, gsend, grecv, hasend, harecv, hbsend, hbrecv,
             r1send, r1recv, r2send, r2recv):
    z, p, core, partner, xn, yn, diag, zs = coords()
    ph('c_bar')
    local = [pltpu.make_async_copy(hT_hbm, hT, lsem.at[0])]
    local.append(pltpu.make_async_copy(w2_ref.at[:, pl.ds(pl.multiple_of(z * 256, 256), CA), :], wvA.at[z], wsem.at[0]))
    for s, p_ref in ((1, p1_ref), (2, p2_ref), (3, p3_ref)):
        src = (z + NZ - s) % NZ
        local.append(pltpu.make_async_copy(w1f_ref.at[src], wvA.at[src, :, pl.ds(0, C1), :], wsem.at[2 * s]))
        local.append(pltpu.make_async_copy(p_ref, wvA.at[src, :, pl.ds(C1, C2), :], wsem.at[2 * s + 1]))
    late = [
        pltpu.make_async_copy(w2_ref.at[:, pl.ds(pl.multiple_of(z * 256 + CA, 32), C3), :], wvB.at[z], wsem.at[1]),
        pltpu.make_async_copy(wd_hbm, wd, lsem.at[1]),
        pltpu.make_async_copy(wo_hbm, wo, lsem.at[2]),
    ]
    for c in local + late:
        c.start()
    entry_barrier(z, p, zs)
    sends = []

    ph('c_send')
    def w_piece(src, dst, k, dev):
        return rcopy(w2_ref.at[:, pl.ds(pl.multiple_of(dst * 256 + CA, 32), C3), :], wvB.at[src], wbsend.at[k], wbrecv.at[src], dev)

    for k in (3, 2, 1):
        c = w_piece(z, zs[k], k, (zs[k], p))
        c.start()
        sends.append(c)
    for j in range(1, NP):
        q = (p + j) % NP
        c = rcopy(o_ref.at[q], og.at[z, p], osend.at[j], orecv.at[p], (z, q))
        c.start()
        sends.append(c)
    og[z, p] = o_ref[p]

    def gated(wv, n):
        g = None
        for q in range(NZ):
            t = jnp.dot(wv[q].reshape(2 * n, 512), hT[q * 512:(q + 1) * 512, :], preferred_element_type=F32)
            g = t if g is None else g + t
        gate = g[0:n].astype(BF16).astype(F32)
        up = g[n:2 * n].astype(BF16).astype(F32)
        return (jax.nn.silu(gate) * up).astype(BF16)

    ra = Relay(z, p, lambda src, ch: hidA.at[src, pl.ds(ch * ROWS_A, ROWS_A), :], hasend, harecv)
    rb = Relay(z, p, lambda src, ch: hidB.at[ch, src], hbsend, hbrecv)
    ro = Relay(z, p, lambda src, ch: og.at[src], gsend, grecv)
    every = range(CHUNKS)

    ph('c_localwait')
    for c in local:
        c.wait()
    ph('c_gA')
    hidA[z] = gated(wvA, CA)

    ra.own(every)
    ph('c_owait')
    for j in range(1, NP):
        q = (p + j) % NP
        rcopy(o_ref.at[0], og.at[z, q], osend.at[0], orecv.at[q], (z, p)).wait_recv()
    ro.own(range(1))
    ph('c_transp')
    for c in late:
        c.wait()
    wdAT[...] = jnp.concatenate([wd[q * 256:q * 256 + CA, :] for q in range(NZ)], axis=0).T
    wdBT[...] = jnp.concatenate([wd[q * 256 + CA:(q + 1) * 256, :] for q in range(NZ)], axis=0).T
    woT[...] = wo[...].T

    ph('c_wBwait')
    for k in range(1, NZ):
        w_piece(zs[k], z, 0, (z, p)).wait_recv()
    ph('c_gB')
    hb = gated(wvB, C3)
    for ch in range(CHUNKS):
        hidB[ch, z] = hb[:, ch * LANES:(ch + 1) * LANES]
    ph('c_passA1')
    rb.own(every)
    for ch in every:
        ra.step(1, ch)
    ph('c_passB1')
    ro.step(1, 0)
    for ch in every:
        rb.step(1, ch)
    ph('c_passA2')
    for ch in every:
        ra.step(2, ch)
    ph('c_passB2')
    ro.step(2, 0)
    for ch in every:
        rb.step(2, ch)
    ph('c_passA3')
    for ch in every:
        ra.step(3, ch)
    ro.step(3, 0)
    ph('c_yA')
    yA[...] = jnp.dot(wdAT[...], hidA[...].reshape(NZ * CA, 512), preferred_element_type=F32) + lax.dot_general(
        woT[...], og[...].reshape(512, 256), (((1,), (1,)), ((), ())), preferred_element_type=F32)

    chip = p // 2
    others = [xn // 2, yn // 2, diag // 2]

    def d2d(ch):
        return rcopy(ysum.at[ch, 1 - core], r1.at[ch], r1send.at[ch], r1recv.at[ch], (z, partner))

    def hop(ch, i, dev):
        return rcopy(acc.at[ch, i], r2.at[ch, i], r2send.at[ch, i], r2recv.at[ch, i], (z, dev))

    def stage1(ch):
        rb.step(3, ch)
        lanes = slice(ch * LANES, (ch + 1) * LANES)
        yt = yA[:, lanes] + jnp.dot(wdBT[...], hidB[ch].reshape(NZ * C3, LANES), preferred_element_type=F32)
        yt = yt.reshape(4, 2, 64, LANES)
        for i in range(4):
            for j in range(2):
                ysum[ch, j, i] = yt[i, j]
        d2d(ch).start()

    def stage2(ch):
        d2d(ch).wait_recv()
        for i, (t, dev) in enumerate(zip(others, (xn, yn, diag))):
            acc[ch, i] = ysum[ch, core, t] + r1[ch, t]
            hop(ch, i, dev).start()

    def stage3(ch):
        lanes = slice(ch * LANES, (ch + 1) * LANES)
        mine = ysum[ch, core, chip] + r1[ch, chip]
        for i, dev in enumerate((xn, yn, diag)):
            hop(ch, i, dev).wait_recv()
            mine = mine + r2[ch, i]
        y_ref[:, lanes] = (xT_ref[:, lanes].astype(F32) + mine).astype(BF16)

    ph('c_rs')
    for t in range(CHUNKS + 2):
        if t < CHUNKS:
            stage1(t)
        if 1 <= t <= CHUNKS:
            stage2(t - 1)
        if t >= 2:
            stage3(t - 2)

    ph('c_end')
    for c in sends:
        c.wait_send()
    for ch in range(CHUNKS):
        d2d(ch).wait_send()
        for i, dev in enumerate((xn, yn, diag)):
            hop(ch, i, dev).wait_send()
    ra.drain(every)
    rb.drain(every)
    ro.drain(range(1))
    ph('')


def call_c(hT, w2, w1f, ps, wd, wo, o8, xT):
    vm = pl.BlockSpec(memory_space=pltpu.VMEM)
    hbm = pl.BlockSpec(memory_space=pl.ANY)
    return pl.pallas_call(
        kernel_c,
        out_shape=jax.ShapeDtypeStruct((64, 512), BF16),
        in_specs=[hbm] * 8 + [vm, vm],
        out_specs=vm,
        scratch_shapes=[
            pltpu.VMEM((2048, 512), BF16),
            pltpu.VMEM((NZ, 2, CA, 512), BF16),
            pltpu.VMEM((NZ, 2, C3, 512), BF16),
            pltpu.VMEM((1024, 512), BF16),
            pltpu.VMEM((256, 512), BF16),
            pltpu.VMEM((512, NZ * CA), BF16),
            pltpu.VMEM((512, NZ * C3), BF16),
            pltpu.VMEM((512, 256), BF16),
            pltpu.VMEM((NZ, NP, 16, 256), BF16),
            pltpu.VMEM((NZ, CA, 512), BF16),
            pltpu.VMEM((CHUNKS, NZ, C3, LANES), BF16),
            pltpu.VMEM((512, 512), F32),
            pltpu.VMEM((CHUNKS, 2, 4, 64, LANES), F32),
            pltpu.VMEM((CHUNKS, 4, 64, LANES), F32),
            pltpu.VMEM((CHUNKS, 3, 64, LANES), F32),
            pltpu.VMEM((CHUNKS, 3, 64, LANES), F32),
            pltpu.SemaphoreType.DMA((3,)),
            pltpu.SemaphoreType.DMA((8,)),
            pltpu.SemaphoreType.DMA((NZ,)),
            pltpu.SemaphoreType.DMA((NZ,)),
            pltpu.SemaphoreType.DMA((NP,)),
            pltpu.SemaphoreType.DMA((NP,)),
            pltpu.SemaphoreType.DMA((8, 1)),
            pltpu.SemaphoreType.DMA((NZ, 1)),
            pltpu.SemaphoreType.DMA((8, CHUNKS)),
            pltpu.SemaphoreType.DMA((NZ, CHUNKS)),
            pltpu.SemaphoreType.DMA((8, CHUNKS)),
            pltpu.SemaphoreType.DMA((NZ, CHUNKS)),
            pltpu.SemaphoreType.DMA((CHUNKS,)),
            pltpu.SemaphoreType.DMA((CHUNKS,)),
            pltpu.SemaphoreType.DMA((CHUNKS, 3)),
            pltpu.SemaphoreType.DMA((CHUNKS, 3)),
        ],
        compiler_params=pltpu.CompilerParams(collective_id=1, has_side_effects=True, vmem_limit_bytes=58 * 1024 * 1024),
        cost_estimate=pl.CostEstimate(flops=12_000_000_000, bytes_accessed=6_000_000, transcendentals=0),
        name='mlp_out',
    )(hT, w2, w1f, *ps, wd, wo, o8, xT)


def solution(mesh):
    all_axes = ('x', 'yz')

    def local_step(x_in, ln_scale, w_gate_up, w_attn, w_down, w_out, k_cache, v_cache, lengths, positions):
        xT = x_in.T
        wattnT = w_attn.T
        hT, qkv, w1f, w2, *pieces = call_a(xT, ln_scale[None, :], wattnT, w_gate_up)
        ps = [lax.ppermute(pieces[i], 'x', [(q, (q + i + 1) % NZ) for q in range(NZ)]) for i in range(NZ - 1)]
        proj = jnp.transpose(qkv, (1, 0, 2)).reshape(16, 2304)
        q_raw = proj[:, :2048].reshape(16, 16, 128)
        k_tok = proj[:, 2048:2176]
        v_tok = proj[:, 2176:]
        q_rot = rotary(q_raw.astype(F32), positions).astype(BF16)
        k_rot = rotary(k_tok[:, None, :].astype(F32), positions).astype(BF16)
        o8, k_new, v_new = call_b(lengths, q_rot, k_rot, v_tok[:, None, :], k_cache, v_cache)
        yT = call_c(hT, w2, w1f, ps, w_down, w_out, o8, xT)
        return yT.T, k_new, v_new

    row_spec = P(None, all_axes)
    vec_spec = P(all_axes)
    cache_spec = P(all_axes, None, None)
    return jax.shard_map(
        local_step,
        mesh=mesh,
        in_specs=(row_spec, vec_spec, P('x', None, 'yz'), P('x', 'yz'), P('yz', 'x'), P('yz', 'x'), cache_spec, cache_spec, vec_spec, vec_spec),
        out_specs=(row_spec, cache_spec, cache_spec),
        check_vma=False,
    )
```

```python
import functools

import jax
import jax.numpy as jnp
from jax import lax
from jax.experimental import pallas as pl
from jax.experimental.pallas import tpu as pltpu
from jax.sharding import PartitionSpec as P

LN_EPS = 1e-6
ROPE_BASE = 10000.0
MESH = pl.DeviceIdType.MESH


class Phase:
    cm = None

    def __call__(self, name):
        if self.cm is not None:
            self.cm.__exit__(None, None, None)
            self.cm = None
        if name:
            self.cm = jax.named_scope(name)
            self.cm.__enter__()


ph = Phase()
F32 = jnp.float32
BF16 = jnp.bfloat16

NZ = 4
NP = 8
C1A = 16
C1 = 64
C2 = 128
C3 = 64
CA = C1 + C2
CHUNKS = 4
ROWS_A = CA // CHUNKS
LANES = 512 // CHUNKS


def rotary(values, positions):
    half_dim = values.shape[-1] // 2
    inv_freq = ROPE_BASE ** (-jnp.arange(half_dim, dtype=jnp.float32) / half_dim)
    angles = positions.astype(jnp.float32)[:, None, None] * inv_freq
    cos_part = jnp.cos(angles)
    sin_part = jnp.sin(angles)
    lo_half = values[..., :half_dim]
    hi_half = values[..., half_dim:]
    return jnp.concatenate([lo_half * cos_part - hi_half * sin_part, hi_half * cos_part + lo_half * sin_part], axis=-1)


def coords():
    z = lax.axis_index('x')
    p = lax.axis_index('yz')
    core = p % 2
    xx = (p // 2) % 2
    y = p // 4
    partner = p + 1 - 2 * core
    xn = p + 2 - 4 * xx
    yn = p + 4 - 8 * y
    diag = xn + 4 - 8 * y
    z1 = z % 2
    z2 = z // 2
    zs = [z, 2 * z2 + 1 - z1, 2 * (1 - z2) + z1, 3 - z]
    return z, p, core, partner, xn, yn, diag, zs


def entry_barrier(z, p, zs):
    sem = pltpu.get_barrier_semaphore()
    for k in range(1, NZ):
        pl.semaphore_signal(sem, inc=1, device_id=(zs[k], p), device_id_type=MESH)
    for k in range(1, NP):
        pl.semaphore_signal(sem, inc=1, device_id=(z, (p + k) % NP), device_id_type=MESH)
    pl.semaphore_wait(sem, NZ - 1 + NP - 1)


def rcopy(src, dst, send, recv, dev):
    return pltpu.make_async_remote_copy(src_ref=src, dst_ref=dst, send_sem=send, recv_sem=recv, device_id=dev, device_id_type=MESH)


class Relay:
    def __init__(self, z, p, at, send, recv):
        self.z, self.p, self.at, self.send, self.recv = z, p, at, send, recv

    def copy(self, way, src, ch, dev):
        ref = self.at(src, ch)
        return rcopy(ref, ref, self.send.at[way, ch], self.recv.at[src, ch], (dev, self.p))

    def own(self, chunks):
        z = self.z

        @pl.when(z < 3)
        def _():
            for ch in chunks:
                self.copy(0, z, ch, z + 1).start()

        @pl.when(z > 0)
        def _():
            for ch in chunks:
                self.copy(1, z, ch, z - 1).start()

    def step(self, k, ch):
        z = self.z

        @pl.when(z >= k)
        def _():
            self.copy(0, z - k, ch, z).wait_recv()

            @pl.when(z < 3)
            def _():
                self.copy(2 * k, z - k, ch, z + 1).start()

        @pl.when(z + k <= 3)
        def _():
            self.copy(0, z + k, ch, z).wait_recv()

            @pl.when(z > 0)
            def _():
                self.copy(2 * k + 1, z + k, ch, z - 1).start()

    def drain(self, chunks):
        z = self.z
        for k in range(NZ - 1):
            @pl.when((z >= k) & (z < 3))
            def _():
                for ch in chunks:
                    self.copy(2 * k, z, ch, z).wait_send()

            @pl.when((z + k <= 3) & (z > 0))
            def _():
                for ch in chunks:
                    self.copy(2 * k + 1, z, ch, z).wait_send()


def attn_start(q):
    return pl.multiple_of(64 * q + 16 * (q // 2), 16)


def kernel_a(xT_ref, ln_ref, wattn_ref, w_ref, h_ref, qkv_ref, w1f_ref, w2_ref, ps1_ref, ps2_ref, ps3_ref,
             xg, lng, watt, zsend, zrecv, zq, s1, s2, wn, wt, hT_ref,
             xsend, xrecv, lsend, lrecv, asend, arecv, zsend_sem, zrecv_sem, qsend, qrecv, wsend, wrecv, lsem, osem):
    z, p, core, partner, xn, yn, diag, zs = coords()
    ph('a_bar')
    wload = pltpu.make_async_copy(w_ref, wn, lsem.at[0])
    wload.start()
    xg[z, p] = xT_ref[...]
    lng[z, p] = jnp.zeros((1, 128), F32)
    lng[z, p, 0:1, 0:64] = ln_ref[...]
    entry_barrier(z, p, zs)
    ph('a_zsend')
    sends = []
    nx = iter(range(40))
    nl = iter(range(40))

    def send(src_z, src_p, dev):
        c = rcopy(xg.at[src_z, src_p], xg.at[src_z, src_p], xsend.at[next(nx)], xrecv.at[src_z, src_p], dev)
        c.start()
        sends.append(c)

    def send_l(src_z, src_p, dev):
        c = rcopy(lng.at[src_z, src_p], lng.at[src_z, src_p], lsend.at[next(nl)], lrecv.at[src_z, src_p], dev)
        c.start()
        sends.append(c)

    def wait_x(src_z, src_p):
        rcopy(xg.at[src_z, src_p], xg.at[src_z, src_p], xsend.at[0], xrecv.at[src_z, src_p], (z, p)).wait_recv()

    def wait_l(src_z, src_p):
        rcopy(lng.at[src_z, src_p], lng.at[src_z, src_p], lsend.at[0], lrecv.at[src_z, src_p], (z, p)).wait_recv()

    def stat(src_z, src_p):
        blk = xg[src_z, src_p].astype(F32).reshape(8, 8, 512)
        s1[...] += jnp.sum(blk, axis=0)
        s2[...] += jnp.sum(blk * blk, axis=0)

    spans = ((0, C1A), (C1A, C1 - C1A))

    def w_piece(i, src, dst, k, dev):
        o, n = spans[i]
        return rcopy(
            wt.at[:, pl.ds(pl.multiple_of(dst * 256 + o, 16), n), :],
            w1f_ref.at[src, :, pl.ds(o, n), :],
            wsend.at[i, k], wrecv.at[i, src], dev)

    def send_w(i):
        for k in (3, 2, 1):
            c = w_piece(i, z, zs[k], k, (zs[k], p))
            c.start()
            sends.append(c)

    def turn(odd):
        def body(i, carry):
            lanes = pl.ds(pl.multiple_of(i * 256 + odd * 128, 128), 128)
            blk = wn[:, :, lanes].astype(F32)
            for g in range(2):
                wt[g, lanes, :] = blk[:, g, :].T.astype(BF16)
            return carry

        lax.fori_loop(0, NZ, body, 0)

    mid = 2 - z // 2
    far = 3 - 3 * (z // 2)
    zo = [z, zs[1], mid, far]
    inner = (z == 1) | (z == 2)
    send(z, p, (mid, p))
    send(z, p, (zs[1], p))
    for k in (3, 2, 1):
        send_l(z, p, (zs[k], p))
    for dev in (xn, yn, partner):
        send(z, p, (z, dev))

    def outward(k):
        return rcopy(xg.at[zo[k], p], xg.at[zo[k], p], osem.at[k - 2], xrecv.at[zo[k], p], (zs[1], p))

    for j in range(1, NP):
        send_l(z, p, (z, (p + j) % NP))
    s1[...] = jnp.zeros_like(s1)
    s2[...] = jnp.zeros_like(s2)
    stat(z, p)
    watt[z] = wattn_ref[pl.ds(attn_start(z), 80), :]
    wload.wait()
    turn(0)

    def column(k):
        wait_x(zo[k], p)
        if k >= 2:
            @pl.when(inner)
            def _():
                outward(k).start()
        if k == 3:
            send(zo[k], p, (z, diag))
        for dev in (xn, yn, partner):
            send(zo[k], p, (z, dev))
        stat(zo[k], p)

    two_src = xn + core * (yn - xn)
    two_dst = yn + core * (xn - yn)

    def neighbours(k):
        wait_x(zo[k], xn)
        if k == 2:
            wait_x(zo[k], yn)
        if k == 1:
            send(zo[k], xn, (z, yn))
        if k == 2:
            send(zo[k], two_src, (z, two_dst))
        send(zo[k], xn, (z, partner))
        stat(zo[k], xn)
        if k != 2:
            wait_x(zo[k], yn)
        if k == 0:
            send(zo[k], yn, (z, xn))
        send(zo[k], yn, (z, partner))
        stat(zo[k], yn)

    def diagonal(k):
        wait_x(zo[k], diag)
        send(zo[k], diag, (z, partner))
        stat(zo[k], diag)

    ph('a_col1')
    column(1)
    neighbours(0)
    ph('a_col2')
    column(2)
    neighbours(1)
    diagonal(0)
    ph('a_col3')
    column(3)
    ph('a_wattn')
    for k in (3, 2, 1):
        c = rcopy(wattn_ref.at[pl.ds(attn_start(zs[k]), 80), :], watt.at[z], asend.at[k], arecv.at[z], (zs[k], p))
        c.start()
        sends.append(c)
    send_w(0)
    ph('a_lnsend')
    for k in range(1, NZ):
        wait_l(zs[k], p)
        for j in range(1, NP):
            send_l(zs[k], p, (z, (p + j) % NP))
    ph('a_nbr')
    neighbours(2)
    diagonal(1)
    neighbours(3)
    ph('a_diag')
    diagonal(2)
    diagonal(3)
    ph('a_rest')
    pd = [partner + xn - p, partner + yn - p, partner + diag - p]
    for q in [partner] + pd:
        for k in range(NZ):
            wait_x(zo[k], q)
            stat(zo[k], q)
    for k in range(NZ):
        for j in range(1, NP):
            wait_l(zs[k], (p + j) % NP)

    ph('a_norm')
    mean = jnp.sum(s1[...], axis=0, keepdims=True) / 2048.0
    var = jnp.sum(s2[...], axis=0, keepdims=True) / 2048.0 - mean * mean
    rstd = lax.rsqrt(var + LN_EPS)
    lnT = jnp.concatenate([lng[i // NP, i % NP, 0:1, :] for i in range(32)] + [jnp.zeros((96, 128), F32)], axis=0).T
    for i in range(NZ * NP):
        sc = lnT[0:64, i:i + 1]
        hT_ref[i * 64:(i + 1) * 64, :] = ((xg[i // NP, i % NP].astype(F32) - mean) * rstd * sc).astype(BF16)

    hout = pltpu.make_async_copy(hT_ref, h_ref, lsem.at[5])
    hout.start()
    ph('a_attw')
    for k in range(1, NZ):
        rcopy(watt.at[z], watt.at[zs[k]], asend.at[0], arecv.at[zs[k]], (z, p)).wait_recv()
    ph('a_zdot')
    part = None
    for q in range(NZ):
        t = jnp.dot(watt[q], hT_ref[q * 512:(q + 1) * 512, :], preferred_element_type=F32)
        part = t if part is None else part + t
    part = part.astype(BF16)
    for q in range(NZ):
        zsend[q] = part[:, q * 128:(q + 1) * 128]
    for k in (3, 2, 1):
        c = rcopy(zsend.at[zs[k]], zrecv.at[z], zsend_sem.at[k], zrecv_sem.at[z], (zs[k], p))
        c.start()
        sends.append(c)
    zrecv[z] = zsend[z]
    ph('a_turn')
    turn(1)
    send_w(1)
    outs = [pltpu.make_async_copy(wt, w2_ref, lsem.at[1])]
    for i, ps_ref in enumerate((ps1_ref, ps2_ref, ps3_ref)):
        dst = (z + i + 1) % NZ
        outs.append(pltpu.make_async_copy(wt.at[:, pl.ds(pl.multiple_of(dst * 256 + C1, 16), C2), :], ps_ref, lsem.at[2 + i]))
    for c in outs[1:] + outs[:1]:
        c.start()
    ph('a_zwait')
    for k in range(1, NZ):
        rcopy(zsend.at[0], zrecv.at[zs[k]], zsend_sem.at[0], zrecv_sem.at[zs[k]], (z, p)).wait_recv()
    ph('a_a2a')
    zt = jnp.concatenate([zrecv[0].astype(F32), zrecv[1].astype(F32)[16:80], zrecv[2].astype(F32), zrecv[3].astype(F32)[16:80]], axis=0)
    zq[...] = zt.T.astype(BF16).reshape(NP, 16, 288)
    for j in range(1, NP):
        q = (p + j) % NP
        c = rcopy(zq.at[q], qkv_ref.at[p], qsend.at[j], qrecv.at[p], (z, q))
        c.start()
        sends.append(c)
    qkv_ref[p] = zq[p]
    for j in range(1, NP):
        q = (p + j) % NP
        rcopy(zq.at[0], qkv_ref.at[q], qsend.at[0], qrecv.at[q], (z, p)).wait_recv()
    ph('a_wwait')
    for i in range(2):
        for k in range(1, NZ):
            w_piece(i, zs[k], z, 0, (z, p)).wait_recv()
    ph('a_sendwait')
    hout.wait()
    for c in outs:
        c.wait()
    for c in sends:
        c.wait_send()

    @pl.when(inner)
    def _():
        outward(2).wait_send()
        outward(3).wait_send()
    ph('')


def call_a(xT, ln, wattnT, w):
    vm = pl.BlockSpec(memory_space=pltpu.VMEM)
    hbm = pl.BlockSpec(memory_space=pl.ANY)
    return pl.pallas_call(
        kernel_a,
        out_shape=(
            jax.ShapeDtypeStruct((2048, 512), BF16),
            jax.ShapeDtypeStruct((NP, 16, 288), BF16),
            jax.ShapeDtypeStruct((NZ, 2, C1, 512), BF16),
            jax.ShapeDtypeStruct((2, 1024, 512), BF16),
        ) + (jax.ShapeDtypeStruct((2, C2, 512), BF16),) * 3,
        in_specs=[vm] * 3 + [hbm],
        out_specs=(hbm, vm) + (hbm,) * 5,
        scratch_shapes=[
            pltpu.VMEM((NZ, NP, 64, 512), BF16),
            pltpu.VMEM((NZ, NP, 1, 128), F32),
            pltpu.VMEM((NZ, 80, 512), BF16),
            pltpu.VMEM((NZ, 80, 128), BF16),
            pltpu.VMEM((NZ, 80, 128), BF16),
            pltpu.VMEM((NP, 16, 288), BF16),
            pltpu.VMEM((8, 512), F32),
            pltpu.VMEM((8, 512), F32),
            pltpu.VMEM((512, 2, 1024), BF16),
            pltpu.VMEM((2, 1024, 512), BF16),
            pltpu.VMEM((2048, 512), BF16),
            pltpu.SemaphoreType.DMA((40,)),
            pltpu.SemaphoreType.DMA((NZ, NP)),
            pltpu.SemaphoreType.DMA((40,)),
            pltpu.SemaphoreType.DMA((NZ, NP)),
            pltpu.SemaphoreType.DMA((NZ,)),
            pltpu.SemaphoreType.DMA((NZ,)),
            pltpu.SemaphoreType.DMA((NZ,)),
            pltpu.SemaphoreType.DMA((NZ,)),
            pltpu.SemaphoreType.DMA((NP,)),
            pltpu.SemaphoreType.DMA((NP,)),
            pltpu.SemaphoreType.DMA((2, NZ)),
            pltpu.SemaphoreType.DMA((2, NZ)),
            pltpu.SemaphoreType.DMA((6,)),
            pltpu.SemaphoreType.DMA((2,)),
        ],
        compiler_params=pltpu.CompilerParams(collective_id=0, has_side_effects=True, vmem_limit_bytes=56 * 1024 * 1024),
        name='gather_norm_qkv',
    )(xT, ln, wattnT, w)


def kernel_b(len_ref, q_ref, k_ref, v_ref, kc_ref, vc_ref, o_ref, kn_ref, vn_ref, kbuf, vbuf, oscr, isem, osem):
    rows = kbuf.shape[0]
    seq = kbuf.shape[1]

    def load(b, t):
        return pltpu.make_async_copy((kc_ref, vc_ref)[t].at[b], (kbuf, vbuf)[t].at[b], isem.at[b, t])

    def store(b, t):
        return pltpu.make_async_copy((kbuf, vbuf)[t].at[b], (kn_ref, vn_ref)[t].at[b], osem.at[b, t])

    for b in range(rows):
        load(b, 0).start()
        load(b, 1).start()

    def insert(buf, b, length, new):
        base = pl.multiple_of((length // 16) * 16, 16)
        hit = base + lax.broadcasted_iota(jnp.int32, (16, 128), 0) == length
        buf[b, pl.ds(base, 16), :] = jnp.where(hit, new.astype(F32), buf[b, pl.ds(base, 16), :].astype(F32)).astype(BF16)

    def attend(b, length, n):
        scores = lax.dot_general(q_ref[b], kbuf[b, 0:n, :], (((1,), (1,)), ((), ())), preferred_element_type=F32) * (128.0 ** -0.5)
        slot = lax.broadcasted_iota(jnp.int32, scores.shape, 1)
        scores = jnp.where(slot <= length, scores, -1e30)
        top = jnp.max(scores, axis=1, keepdims=True)
        e = jnp.exp(scores - top)
        probs = (e / jnp.sum(e, axis=1, keepdims=True)).astype(BF16)
        return jnp.dot(probs, vbuf[b, 0:n, :], preferred_element_type=F32)

    def pair(i, carry):
        b0 = 2 * i
        b1 = 2 * i + 1
        l0 = len_ref[b0]
        l1 = len_ref[b1]
        for b, length in ((b0, l0), (b1, l1)):
            load(b, 0).wait()
            load(b, 1).wait()
            insert(kbuf, b, length, k_ref[b])
            insert(vbuf, b, length, v_ref[b])
        last = jnp.maximum(l0, l1) // 512
        for t in range(seq // 512):
            @pl.when(last == t)
            def _():
                n = 512 * (t + 1)
                r0 = attend(b0, l0, n)
                r1 = attend(b1, l1, n)
                oscr[b0] = r0
                oscr[b1] = r1
        for b in (b0, b1):
            store(b, 0).start()
            store(b, 1).start()
        return carry

    lax.fori_loop(0, rows // 2, pair, 0)
    for h in range(16):
        o_ref[h // 2, :, (h % 2) * 128:(h % 2 + 1) * 128] = oscr[:, h, :].astype(BF16)
    for b in range(rows):
        store(b, 0).wait()
        store(b, 1).wait()


def call_b(lengths, q_rot, k_rot, v_tok, k_cache, v_cache):
    rows, seq, hd = k_cache.shape
    heads = q_rot.shape[1]
    vm = pl.BlockSpec(memory_space=pltpu.VMEM)
    hbm = pl.BlockSpec(memory_space=pl.ANY)
    return pl.pallas_call(
        kernel_b,
        in_specs=[pl.BlockSpec(memory_space=pltpu.SMEM), vm, vm, vm, hbm, hbm],
        out_specs=(vm, hbm, hbm),
        out_shape=(
            jax.ShapeDtypeStruct((NP, rows, heads * hd // NP), BF16),
            jax.ShapeDtypeStruct(k_cache.shape, BF16),
            jax.ShapeDtypeStruct(v_cache.shape, BF16),
        ),
        scratch_shapes=[
            pltpu.VMEM((rows, seq, hd), BF16),
            pltpu.VMEM((rows, seq, hd), BF16),
            pltpu.VMEM((rows, heads, hd), F32),
            pltpu.SemaphoreType.DMA((rows, 2)),
            pltpu.SemaphoreType.DMA((rows, 2)),
        ],
        compiler_params=pltpu.CompilerParams(vmem_limit_bytes=58 * 1024 * 1024),
        cost_estimate=pl.CostEstimate(flops=12_000_000_000, bytes_accessed=33_000_000, transcendentals=0),
        name='attend',
    )(lengths, q_rot, k_rot, v_tok, k_cache, v_cache)


def kernel_c(hT, w2_ref, w1f_ref, p1_ref, p2_ref, p3_ref, wd, wo, o_ref, xT_ref, y_ref,
             wvA, wvB, wdAT, wdBT, woT, og, hidA, hidB, yA, ysum, r1, acc, r2,
             wsem, wbsend, wbrecv, osend, orecv, gsend, grecv, hasend, harecv, hbsend, hbrecv,
             r1send, r1recv, r2send, r2recv):
    z, p, core, partner, xn, yn, diag, zs = coords()
    ph('c_bar')
    local = [pltpu.make_async_copy(w2_ref.at[:, pl.ds(pl.multiple_of(z * 256, 256), CA), :], wvA.at[z], wsem.at[0])]
    for s, p_ref in ((1, p1_ref), (2, p2_ref), (3, p3_ref)):
        src = (z + NZ - s) % NZ
        local.append(pltpu.make_async_copy(w1f_ref.at[src], wvA.at[src, :, pl.ds(0, C1), :], wsem.at[2 * s]))
        local.append(pltpu.make_async_copy(p_ref, wvA.at[src, :, pl.ds(C1, C2), :], wsem.at[2 * s + 1]))
    late = [
        pltpu.make_async_copy(w2_ref.at[:, pl.ds(pl.multiple_of(z * 256 + CA, 32), C3), :], wvB.at[z], wsem.at[1]),
    ]
    for c in local + late:
        c.start()
    entry_barrier(z, p, zs)
    sends = []

    ph('c_send')
    def w_piece(src, dst, k, dev):
        return rcopy(w2_ref.at[:, pl.ds(pl.multiple_of(dst * 256 + CA, 32), C3), :], wvB.at[src], wbsend.at[k], wbrecv.at[src], dev)

    for k in (3, 2, 1):
        c = w_piece(z, zs[k], k, (zs[k], p))
        c.start()
        sends.append(c)
    for j in range(1, NP):
        q = (p + j) % NP
        c = rcopy(o_ref.at[q], og.at[z, p], osend.at[j], orecv.at[p], (z, q))
        c.start()
        sends.append(c)
    og[z, p] = o_ref[p]

    def gated(wv, n):
        g = None
        for q in range(NZ):
            t = jnp.dot(wv[q].reshape(2 * n, 512), hT[q * 512:(q + 1) * 512, :], preferred_element_type=F32)
            g = t if g is None else g + t
        gate = g[0:n].astype(BF16).astype(F32)
        up = g[n:2 * n].astype(BF16).astype(F32)
        return (jax.nn.silu(gate) * up).astype(BF16)

    ra = Relay(z, p, lambda src, ch: hidA.at[src, pl.ds(ch * ROWS_A, ROWS_A), :], hasend, harecv)
    rb = Relay(z, p, lambda src, ch: hidB.at[ch, src], hbsend, hbrecv)
    ro = Relay(z, p, lambda src, ch: og.at[src], gsend, grecv)
    every = range(CHUNKS)

    ph('c_localwait')
    for c in local:
        c.wait()
    ph('c_gA')
    hidA[z] = gated(wvA, CA)

    ra.own(every)
    ph('c_owait')
    for j in range(1, NP):
        q = (p + j) % NP
        rcopy(o_ref.at[0], og.at[z, q], osend.at[0], orecv.at[q], (z, p)).wait_recv()
    ro.own(range(1))
    ph('c_transp')
    for c in late:
        c.wait()
    wdAT[...] = jnp.concatenate([wd[q * 256:q * 256 + CA, :] for q in range(NZ)], axis=0).T
    wdBT[...] = jnp.concatenate([wd[q * 256 + CA:(q + 1) * 256, :] for q in range(NZ)], axis=0).T
    woT[...] = wo[...].T

    ph('c_wBwait')
    for k in range(1, NZ):
        w_piece(zs[k], z, 0, (z, p)).wait_recv()
    ph('c_gB')
    hb = gated(wvB, C3)
    for ch in range(CHUNKS):
        hidB[ch, z] = hb[:, ch * LANES:(ch + 1) * LANES]
    ph('c_passA1')
    rb.own(every)
    for ch in every:
        ra.step(1, ch)
    ph('c_passB1')
    ro.step(1, 0)
    for ch in every:
        rb.step(1, ch)
    ph('c_passA2')
    for ch in every:
        ra.step(2, ch)
    ph('c_passB2')
    ro.step(2, 0)
    for ch in every:
        rb.step(2, ch)
    ph('c_passA3')
    for ch in every:
        ra.step(3, ch)
    ro.step(3, 0)
    ph('c_yA')
    yA[...] = jnp.dot(wdAT[...], hidA[...].reshape(NZ * CA, 512), preferred_element_type=F32) + lax.dot_general(
        woT[...], og[...].reshape(512, 256), (((1,), (1,)), ((), ())), preferred_element_type=F32)

    chip = p // 2
    others = [xn // 2, yn // 2, diag // 2]

    def d2d(ch):
        return rcopy(ysum.at[ch, 1 - core], r1.at[ch], r1send.at[ch], r1recv.at[ch], (z, partner))

    def hop(ch, i, dev):
        return rcopy(acc.at[ch, i], r2.at[ch, i], r2send.at[ch, i], r2recv.at[ch, i], (z, dev))

    def stage1(ch):
        rb.step(3, ch)
        lanes = slice(ch * LANES, (ch + 1) * LANES)
        yt = yA[:, lanes] + jnp.dot(wdBT[...], hidB[ch].reshape(NZ * C3, LANES), preferred_element_type=F32)
        yt = yt.reshape(4, 2, 64, LANES)
        for i in range(4):
            for j in range(2):
                ysum[ch, j, i] = yt[i, j]
        d2d(ch).start()

    def stage2(ch):
        d2d(ch).wait_recv()
        for i, (t, dev) in enumerate(zip(others, (xn, yn, diag))):
            acc[ch, i] = ysum[ch, core, t] + r1[ch, t]
            hop(ch, i, dev).start()

    def stage3(ch):
        lanes = slice(ch * LANES, (ch + 1) * LANES)
        mine = ysum[ch, core, chip] + r1[ch, chip]
        for i, dev in enumerate((xn, yn, diag)):
            hop(ch, i, dev).wait_recv()
            mine = mine + r2[ch, i]
        y_ref[:, lanes] = (xT_ref[:, lanes].astype(F32) + mine).astype(BF16)

    ph('c_rs')
    for t in range(CHUNKS + 2):
        if t < CHUNKS:
            stage1(t)
        if 1 <= t <= CHUNKS:
            stage2(t - 1)
        if t >= 2:
            stage3(t - 2)

    ph('c_end')
    for c in sends:
        c.wait_send()
    for ch in range(CHUNKS):
        d2d(ch).wait_send()
        for i, dev in enumerate((xn, yn, diag)):
            hop(ch, i, dev).wait_send()
    ra.drain(every)
    rb.drain(every)
    ro.drain(range(1))
    ph('')


def call_c(hT, w2, w1f, ps, wd, wo, o8, xT):
    vm = pl.BlockSpec(memory_space=pltpu.VMEM)
    hbm = pl.BlockSpec(memory_space=pl.ANY)
    return pl.pallas_call(
        kernel_c,
        out_shape=jax.ShapeDtypeStruct((64, 512), BF16),
        in_specs=[vm] + [hbm] * 5 + [vm] * 4,
        out_specs=vm,
        scratch_shapes=[
            pltpu.VMEM((NZ, 2, CA, 512), BF16),
            pltpu.VMEM((NZ, 2, C3, 512), BF16),
            pltpu.VMEM((512, NZ * CA), BF16),
            pltpu.VMEM((512, NZ * C3), BF16),
            pltpu.VMEM((512, 256), BF16),
            pltpu.VMEM((NZ, NP, 16, 256), BF16),
            pltpu.VMEM((NZ, CA, 512), BF16),
            pltpu.VMEM((CHUNKS, NZ, C3, LANES), BF16),
            pltpu.VMEM((512, 512), F32),
            pltpu.VMEM((CHUNKS, 2, 4, 64, LANES), F32),
            pltpu.VMEM((CHUNKS, 4, 64, LANES), F32),
            pltpu.VMEM((CHUNKS, 3, 64, LANES), F32),
            pltpu.VMEM((CHUNKS, 3, 64, LANES), F32),
            pltpu.SemaphoreType.DMA((8,)),
            pltpu.SemaphoreType.DMA((NZ,)),
            pltpu.SemaphoreType.DMA((NZ,)),
            pltpu.SemaphoreType.DMA((NP,)),
            pltpu.SemaphoreType.DMA((NP,)),
            pltpu.SemaphoreType.DMA((8, 1)),
            pltpu.SemaphoreType.DMA((NZ, 1)),
            pltpu.SemaphoreType.DMA((8, CHUNKS)),
            pltpu.SemaphoreType.DMA((NZ, CHUNKS)),
            pltpu.SemaphoreType.DMA((8, CHUNKS)),
            pltpu.SemaphoreType.DMA((NZ, CHUNKS)),
            pltpu.SemaphoreType.DMA((CHUNKS,)),
            pltpu.SemaphoreType.DMA((CHUNKS,)),
            pltpu.SemaphoreType.DMA((CHUNKS, 3)),
            pltpu.SemaphoreType.DMA((CHUNKS, 3)),
        ],
        compiler_params=pltpu.CompilerParams(collective_id=1, has_side_effects=True, vmem_limit_bytes=40 * 1024 * 1024),
        cost_estimate=pl.CostEstimate(flops=12_000_000_000, bytes_accessed=6_000_000, transcendentals=0),
        name='mlp_out',
    )(hT, w2, w1f, *ps, wd, wo, o8, xT)


def solution(mesh):
    all_axes = ('x', 'yz')

    def local_step(x_in, ln_scale, w_gate_up, w_attn, w_down, w_out, k_cache, v_cache, lengths, positions):
        xT = x_in.T
        wattnT = w_attn.T
        hT, qkv, w1f, w2, *pieces = call_a(xT, ln_scale[None, :], wattnT, w_gate_up)
        ps = [lax.ppermute(pieces[i], 'x', [(q, (q + i + 1) % NZ) for q in range(NZ)]) for i in range(NZ - 1)]
        proj = jnp.transpose(qkv, (1, 0, 2)).reshape(16, 2304)
        q_raw = proj[:, :2048].reshape(16, 16, 128)
        k_tok = proj[:, 2048:2176]
        v_tok = proj[:, 2176:]
        q_rot = rotary(q_raw.astype(F32), positions).astype(BF16)
        k_rot = rotary(k_tok[:, None, :].astype(F32), positions).astype(BF16)
        o8, k_new, v_new = call_b(lengths, q_rot, k_rot, v_tok[:, None, :], k_cache, v_cache)
        yT = call_c(hT, w2, w1f, ps, w_down, w_out, o8, xT)
        return yT.T, k_new, v_new

    row_spec = P(None, all_axes)
    vec_spec = P(all_axes)
    cache_spec = P(all_axes, None, None)
    return jax.shard_map(
        local_step,
        mesh=mesh,
        in_specs=(row_spec, vec_spec, P('x', None, 'yz'), P('x', 'yz'), P('yz', 'x'), P('yz', 'x'), cache_spec, cache_spec, vec_spec, vec_spec),
        out_specs=(row_spec, cache_spec, cache_spec),
        check_vma=False,
    )
```

```python
import functools

import jax
import jax.numpy as jnp
from jax import lax
from jax.experimental import pallas as pl
from jax.experimental.pallas import tpu as pltpu
from jax.sharding import PartitionSpec as P

LN_EPS = 1e-6
ROPE_BASE = 10000.0
MESH = pl.DeviceIdType.MESH


class Phase:
    cm = None

    def __call__(self, name):
        if self.cm is not None:
            self.cm.__exit__(None, None, None)
            self.cm = None
        if name:
            self.cm = jax.named_scope(name)
            self.cm.__enter__()


ph = Phase()
F32 = jnp.float32
BF16 = jnp.bfloat16

NZ = 4
NP = 8
C1A = 16
C1 = 64
C2 = 128
C3 = 64
CA = C1 + C2
CHUNKS = 4
LANES = 512 // CHUNKS


def rotary(values, positions):
    half_dim = values.shape[-1] // 2
    inv_freq = ROPE_BASE ** (-jnp.arange(half_dim, dtype=jnp.float32) / half_dim)
    angles = positions.astype(jnp.float32)[:, None, None] * inv_freq
    cos_part = jnp.cos(angles)
    sin_part = jnp.sin(angles)
    lo_half = values[..., :half_dim]
    hi_half = values[..., half_dim:]
    return jnp.concatenate([lo_half * cos_part - hi_half * sin_part, hi_half * cos_part + lo_half * sin_part], axis=-1)


def coords():
    z = lax.axis_index('x')
    p = lax.axis_index('yz')
    core = p % 2
    xx = (p // 2) % 2
    y = p // 4
    partner = p + 1 - 2 * core
    xn = p + 2 - 4 * xx
    yn = p + 4 - 8 * y
    diag = xn + 4 - 8 * y
    z1 = z % 2
    z2 = z // 2
    zs = [z, 2 * z2 + 1 - z1, 2 * (1 - z2) + z1, 3 - z]
    return z, p, core, partner, xn, yn, diag, zs


def entry_barrier(z, p, zs):
    sem = pltpu.get_barrier_semaphore()
    for k in range(1, NZ):
        pl.semaphore_signal(sem, inc=1, device_id=(zs[k], p), device_id_type=MESH)
    for k in range(1, NP):
        pl.semaphore_signal(sem, inc=1, device_id=(z, (p + k) % NP), device_id_type=MESH)
    pl.semaphore_wait(sem, NZ - 1 + NP - 1)


def rcopy(src, dst, send, recv, dev):
    return pltpu.make_async_remote_copy(src_ref=src, dst_ref=dst, send_sem=send, recv_sem=recv, device_id=dev, device_id_type=MESH)


class Relay:
    def __init__(self, z, p, at, send, recv):
        self.z, self.p, self.at, self.send, self.recv = z, p, at, send, recv

    def copy(self, way, src, ch, dev):
        ref = self.at(src, ch)
        return rcopy(ref, ref, self.send.at[way, ch], self.recv.at[src, ch], (dev, self.p))

    def own(self, chunks):
        z = self.z

        @pl.when(z < 3)
        def _():
            for ch in chunks:
                self.copy(0, z, ch, z + 1).start()

        @pl.when(z > 0)
        def _():
            for ch in chunks:
                self.copy(1, z, ch, z - 1).start()

    def step(self, k, ch):
        z = self.z

        @pl.when(z >= k)
        def _():
            self.copy(0, z - k, ch, z).wait_recv()

            @pl.when(z < 3)
            def _():
                self.copy(2 * k, z - k, ch, z + 1).start()

        @pl.when(z + k <= 3)
        def _():
            self.copy(0, z + k, ch, z).wait_recv()

            @pl.when(z > 0)
            def _():
                self.copy(2 * k + 1, z + k, ch, z - 1).start()

    def drain(self, chunks):
        z = self.z
        for k in range(NZ - 1):
            @pl.when((z >= k) & (z < 3))
            def _():
                for ch in chunks:
                    self.copy(2 * k, z, ch, z).wait_send()

            @pl.when((z + k <= 3) & (z > 0))
            def _():
                for ch in chunks:
                    self.copy(2 * k + 1, z, ch, z).wait_send()


def attn_start(q):
    return pl.multiple_of(64 * q + 16 * (q // 2), 16)


def kernel_a(xT_ref, ln_ref, wattn_ref, w_ref, h_ref, qkv_ref, w1f_ref, w2_ref, ps1_ref, ps2_ref, ps3_ref,
             xg, lng, watt, zsend, zrecv, zq, s1, s2, wn, wt, hT_ref,
             xsend, xrecv, lsend, lrecv, asend, arecv, zsend_sem, zrecv_sem, qsend, qrecv, wsend, wrecv, lsem, osem):
    z, p, core, partner, xn, yn, diag, zs = coords()
    ph('a_bar')
    wload = pltpu.make_async_copy(w_ref, wn, lsem.at[0])
    wload.start()
    xg[z, p] = xT_ref[...]
    lng[z, p] = jnp.zeros((1, 128), F32)
    lng[z, p, 0:1, 0:64] = ln_ref[...]
    entry_barrier(z, p, zs)
    ph('a_zsend')
    sends = []
    nx = iter(range(40))
    nl = iter(range(40))

    def send(src_z, src_p, dev):
        c = rcopy(xg.at[src_z, src_p], xg.at[src_z, src_p], xsend.at[next(nx)], xrecv.at[src_z, src_p], dev)
        c.start()
        sends.append(c)

    def send_l(src_z, src_p, dev):
        c = rcopy(lng.at[src_z, src_p], lng.at[src_z, src_p], lsend.at[next(nl)], lrecv.at[src_z, src_p], dev)
        c.start()
        sends.append(c)

    def wait_x(src_z, src_p):
        rcopy(xg.at[src_z, src_p], xg.at[src_z, src_p], xsend.at[0], xrecv.at[src_z, src_p], (z, p)).wait_recv()

    def wait_l(src_z, src_p):
        rcopy(lng.at[src_z, src_p], lng.at[src_z, src_p], lsend.at[0], lrecv.at[src_z, src_p], (z, p)).wait_recv()

    def stat(src_z, src_p):
        blk = xg[src_z, src_p].astype(F32).reshape(8, 8, 512)
        s1[...] += jnp.sum(blk, axis=0)
        s2[...] += jnp.sum(blk * blk, axis=0)

    spans = ((0, C1A), (C1A, C1 - C1A))

    def w_piece(i, src, dst, k, dev):
        o, n = spans[i]
        return rcopy(
            wt.at[:, pl.ds(pl.multiple_of(dst * 256 + o, 16), n), :],
            w1f_ref.at[src, :, pl.ds(o, n), :],
            wsend.at[i, k], wrecv.at[i, src], dev)

    def send_w(i):
        for k in (3, 2, 1):
            c = w_piece(i, z, zs[k], k, (zs[k], p))
            c.start()
            sends.append(c)

    def turn(odd):
        def body(i, carry):
            lanes = pl.ds(pl.multiple_of(i * 256 + odd * 128, 128), 128)
            blk = wn[:, :, lanes].astype(F32)
            for g in range(2):
                wt[g, lanes, :] = blk[:, g, :].T.astype(BF16)
            return carry

        lax.fori_loop(0, NZ, body, 0)

    mid = 2 - z // 2
    far = 3 - 3 * (z // 2)
    zo = [z, zs[1], mid, far]
    inner = (z == 1) | (z == 2)
    send(z, p, (mid, p))
    send(z, p, (zs[1], p))
    for k in (3, 2, 1):
        send_l(z, p, (zs[k], p))
    for dev in (xn, yn, partner):
        send(z, p, (z, dev))

    def outward(k):
        return rcopy(xg.at[zo[k], p], xg.at[zo[k], p], osem.at[k - 2], xrecv.at[zo[k], p], (zs[1], p))

    for j in range(1, NP):
        send_l(z, p, (z, (p + j) % NP))
    s1[...] = jnp.zeros_like(s1)
    s2[...] = jnp.zeros_like(s2)
    stat(z, p)
    watt[z] = wattn_ref[pl.ds(attn_start(z), 80), :]
    wload.wait()
    turn(0)

    def column(k):
        wait_x(zo[k], p)
        if k >= 2:
            @pl.when(inner)
            def _():
                outward(k).start()
        if k == 3:
            send(zo[k], p, (z, diag))
        for dev in (xn, yn, partner):
            send(zo[k], p, (z, dev))
        stat(zo[k], p)

    two_src = xn + core * (yn - xn)
    two_dst = yn + core * (xn - yn)

    def neighbours(k):
        wait_x(zo[k], xn)
        if k == 2:
            wait_x(zo[k], yn)
        if k == 1:
            send(zo[k], xn, (z, yn))
        if k == 2:
            send(zo[k], two_src, (z, two_dst))
        send(zo[k], xn, (z, partner))
        stat(zo[k], xn)
        if k != 2:
            wait_x(zo[k], yn)
        if k == 0:
            send(zo[k], yn, (z, xn))
        send(zo[k], yn, (z, partner))
        stat(zo[k], yn)

    def diagonal(k):
        wait_x(zo[k], diag)
        send(zo[k], diag, (z, partner))
        stat(zo[k], diag)

    ph('a_col1')
    column(1)
    column(2)
    ph('a_col3')
    column(3)
    ph('a_wattn')
    for k in (3, 2, 1):
        c = rcopy(wattn_ref.at[pl.ds(attn_start(zs[k]), 80), :], watt.at[z], asend.at[k], arecv.at[z], (zs[k], p))
        c.start()
        sends.append(c)
    send_w(0)
    ph('a_lnsend')
    for k in range(1, NZ):
        wait_l(zs[k], p)
        for j in range(1, NP):
            send_l(zs[k], p, (z, (p + j) % NP))
    ph('a_nbr')
    neighbours(0)
    neighbours(1)
    ph('a_nbr2')
    diagonal(0)
    neighbours(2)
    diagonal(1)
    neighbours(3)
    ph('a_diag')
    diagonal(2)
    diagonal(3)
    ph('a_rest')
    pd = [partner + xn - p, partner + yn - p, partner + diag - p]
    for q in [partner] + pd:
        for k in range(NZ):
            wait_x(zo[k], q)
            stat(zo[k], q)
    for k in range(NZ):
        for j in range(1, NP):
            wait_l(zs[k], (p + j) % NP)

    ph('a_norm')
    mean = jnp.sum(s1[...], axis=0, keepdims=True) / 2048.0
    var = jnp.sum(s2[...], axis=0, keepdims=True) / 2048.0 - mean * mean
    rstd = lax.rsqrt(var + LN_EPS)
    lnT = jnp.concatenate([lng[i // NP, i % NP, 0:1, :] for i in range(32)] + [jnp.zeros((96, 128), F32)], axis=0).T
    for i in range(NZ * NP):
        sc = lnT[0:64, i:i + 1]
        hT_ref[i * 64:(i + 1) * 64, :] = ((xg[i // NP, i % NP].astype(F32) - mean) * rstd * sc).astype(BF16)

    hout = pltpu.make_async_copy(hT_ref, h_ref, lsem.at[5])
    hout.start()
    ph('a_attw')
    for k in range(1, NZ):
        rcopy(watt.at[z], watt.at[zs[k]], asend.at[0], arecv.at[zs[k]], (z, p)).wait_recv()
    ph('a_zdot')
    part = None
    for q in range(NZ):
        t = jnp.dot(watt[q], hT_ref[q * 512:(q + 1) * 512, :], preferred_element_type=F32)
        part = t if part is None else part + t
    part = part.astype(BF16)
    for q in range(NZ):
        zsend[q] = part[:, q * 128:(q + 1) * 128]
    for k in (3, 2, 1):
        c = rcopy(zsend.at[zs[k]], zrecv.at[z], zsend_sem.at[k], zrecv_sem.at[z], (zs[k], p))
        c.start()
        sends.append(c)
    zrecv[z] = zsend[z]
    ph('a_turn')
    turn(1)
    send_w(1)
    outs = [pltpu.make_async_copy(wt, w2_ref, lsem.at[1])]
    for i, ps_ref in enumerate((ps1_ref, ps2_ref, ps3_ref)):
        dst = (z + i + 1) % NZ
        outs.append(pltpu.make_async_copy(wt.at[:, pl.ds(pl.multiple_of(dst * 256 + C1, 16), C2), :], ps_ref, lsem.at[2 + i]))
    for c in outs[1:] + outs[:1]:
        c.start()
    ph('a_zwait')
    for k in range(1, NZ):
        rcopy(zsend.at[0], zrecv.at[zs[k]], zsend_sem.at[0], zrecv_sem.at[zs[k]], (z, p)).wait_recv()
    ph('a_a2a')
    zt = jnp.concatenate([zrecv[0].astype(F32), zrecv[1].astype(F32)[16:80], zrecv[2].astype(F32), zrecv[3].astype(F32)[16:80]], axis=0)
    zq[...] = zt.T.astype(BF16).reshape(NP, 16, 288)
    for j in range(1, NP):
        q = (p + j) % NP
        c = rcopy(zq.at[q], qkv_ref.at[p], qsend.at[j], qrecv.at[p], (z, q))
        c.start()
        sends.append(c)
    qkv_ref[p] = zq[p]
    for j in range(1, NP):
        q = (p + j) % NP
        rcopy(zq.at[0], qkv_ref.at[q], qsend.at[0], qrecv.at[q], (z, p)).wait_recv()
    ph('a_wwait')
    for i in range(2):
        for k in range(1, NZ):
            w_piece(i, zs[k], z, 0, (z, p)).wait_recv()
    ph('a_sendwait')
    hout.wait()
    for c in outs:
        c.wait()
    for c in sends:
        c.wait_send()

    @pl.when(inner)
    def _():
        outward(2).wait_send()
        outward(3).wait_send()
    ph('')


def call_a(xT, ln, wattnT, w):
    vm = pl.BlockSpec(memory_space=pltpu.VMEM)
    hbm = pl.BlockSpec(memory_space=pl.ANY)
    return pl.pallas_call(
        kernel_a,
        out_shape=(
            jax.ShapeDtypeStruct((2048, 512), BF16),
            jax.ShapeDtypeStruct((NP, 16, 288), BF16),
            jax.ShapeDtypeStruct((NZ, 2, C1, 512), BF16),
            jax.ShapeDtypeStruct((2, 1024, 512), BF16),
        ) + (jax.ShapeDtypeStruct((2, C2, 512), BF16),) * 3,
        in_specs=[vm] * 3 + [hbm],
        out_specs=(hbm, vm) + (hbm,) * 5,
        scratch_shapes=[
            pltpu.VMEM((NZ, NP, 64, 512), BF16),
            pltpu.VMEM((NZ, NP, 1, 128), F32),
            pltpu.VMEM((NZ, 80, 512), BF16),
            pltpu.VMEM((NZ, 80, 128), BF16),
            pltpu.VMEM((NZ, 80, 128), BF16),
            pltpu.VMEM((NP, 16, 288), BF16),
            pltpu.VMEM((8, 512), F32),
            pltpu.VMEM((8, 512), F32),
            pltpu.VMEM((512, 2, 1024), BF16),
            pltpu.VMEM((2, 1024, 512), BF16),
            pltpu.VMEM((2048, 512), BF16),
            pltpu.SemaphoreType.DMA((40,)),
            pltpu.SemaphoreType.DMA((NZ, NP)),
            pltpu.SemaphoreType.DMA((40,)),
            pltpu.SemaphoreType.DMA((NZ, NP)),
            pltpu.SemaphoreType.DMA((NZ,)),
            pltpu.SemaphoreType.DMA((NZ,)),
            pltpu.SemaphoreType.DMA((NZ,)),
            pltpu.SemaphoreType.DMA((NZ,)),
            pltpu.SemaphoreType.DMA((NP,)),
            pltpu.SemaphoreType.DMA((NP,)),
            pltpu.SemaphoreType.DMA((2, NZ)),
            pltpu.SemaphoreType.DMA((2, NZ)),
            pltpu.SemaphoreType.DMA((6,)),
            pltpu.SemaphoreType.DMA((2,)),
        ],
        compiler_params=pltpu.CompilerParams(collective_id=0, has_side_effects=True, vmem_limit_bytes=56 * 1024 * 1024),
        name='gather_norm_qkv',
    )(xT, ln, wattnT, w)


def kernel_b(len_ref, q_ref, k_ref, v_ref, kc_ref, vc_ref, o_ref, kn_ref, vn_ref, kbuf, vbuf, oscr, isem, osem):
    rows = kbuf.shape[0]
    seq = kbuf.shape[1]

    def load(b, t):
        return pltpu.make_async_copy((kc_ref, vc_ref)[t].at[b], (kbuf, vbuf)[t].at[b], isem.at[b, t])

    def store(b, t):
        return pltpu.make_async_copy((kbuf, vbuf)[t].at[b], (kn_ref, vn_ref)[t].at[b], osem.at[b, t])

    for b in range(rows):
        load(b, 0).start()
        load(b, 1).start()

    def insert(buf, b, length, new):
        base = pl.multiple_of((length // 16) * 16, 16)
        hit = base + lax.broadcasted_iota(jnp.int32, (16, 128), 0) == length
        buf[b, pl.ds(base, 16), :] = jnp.where(hit, new.astype(F32), buf[b, pl.ds(base, 16), :].astype(F32)).astype(BF16)

    def attend(b, length, n):
        scores = lax.dot_general(q_ref[b], kbuf[b, 0:n, :], (((1,), (1,)), ((), ())), preferred_element_type=F32) * (128.0 ** -0.5)
        slot = lax.broadcasted_iota(jnp.int32, scores.shape, 1)
        scores = jnp.where(slot <= length, scores, -1e30)
        top = jnp.max(scores, axis=1, keepdims=True)
        e = jnp.exp(scores - top)
        probs = (e / jnp.sum(e, axis=1, keepdims=True)).astype(BF16)
        return jnp.dot(probs, vbuf[b, 0:n, :], preferred_element_type=F32)

    def pair(i, carry):
        b0 = 2 * i
        b1 = 2 * i + 1
        l0 = len_ref[b0]
        l1 = len_ref[b1]
        for b, length in ((b0, l0), (b1, l1)):
            load(b, 0).wait()
            load(b, 1).wait()
            insert(kbuf, b, length, k_ref[b])
            insert(vbuf, b, length, v_ref[b])
        last = jnp.maximum(l0, l1) // 512
        for t in range(seq // 512):
            @pl.when(last == t)
            def _():
                n = 512 * (t + 1)
                r0 = attend(b0, l0, n)
                r1 = attend(b1, l1, n)
                oscr[b0] = r0
                oscr[b1] = r1
        for b in (b0, b1):
            store(b, 0).start()
            store(b, 1).start()
        return carry

    lax.fori_loop(0, rows // 2, pair, 0)
    for h in range(16):
        o_ref[h // 2, :, (h % 2) * 128:(h % 2 + 1) * 128] = oscr[:, h, :].astype(BF16)
    for b in range(rows):
        store(b, 0).wait()
        store(b, 1).wait()


def call_b(lengths, q_rot, k_rot, v_tok, k_cache, v_cache):
    rows, seq, hd = k_cache.shape
    heads = q_rot.shape[1]
    vm = pl.BlockSpec(memory_space=pltpu.VMEM)
    hbm = pl.BlockSpec(memory_space=pl.ANY)
    return pl.pallas_call(
        kernel_b,
        in_specs=[pl.BlockSpec(memory_space=pltpu.SMEM), vm, vm, vm, hbm, hbm],
        out_specs=(vm, hbm, hbm),
        out_shape=(
            jax.ShapeDtypeStruct((NP, rows, heads * hd // NP), BF16),
            jax.ShapeDtypeStruct(k_cache.shape, BF16),
            jax.ShapeDtypeStruct(v_cache.shape, BF16),
        ),
        scratch_shapes=[
            pltpu.VMEM((rows, seq, hd), BF16),
            pltpu.VMEM((rows, seq, hd), BF16),
            pltpu.VMEM((rows, heads, hd), F32),
            pltpu.SemaphoreType.DMA((rows, 2)),
            pltpu.SemaphoreType.DMA((rows, 2)),
        ],
        compiler_params=pltpu.CompilerParams(vmem_limit_bytes=58 * 1024 * 1024),
        cost_estimate=pl.CostEstimate(flops=12_000_000_000, bytes_accessed=33_000_000, transcendentals=0),
        name='attend',
    )(lengths, q_rot, k_rot, v_tok, k_cache, v_cache)


def kernel_c(hT, w2_ref, w1f_ref, p1_ref, p2_ref, p3_ref, wd, wo, o_ref, xT_ref, y_ref,
             wvA, wvB, wdAT, wdBT, woT, og, hidA, hidB, ysum, r1, acc, r2,
             wsem, wbsend, wbrecv, osend, orecv, gsend, grecv, hasend, harecv, hbsend, hbrecv,
             r1send, r1recv, r2send, r2recv):
    z, p, core, partner, xn, yn, diag, zs = coords()
    ph('c_bar')
    local = [pltpu.make_async_copy(w2_ref.at[:, pl.ds(pl.multiple_of(z * 256, 256), CA), :], wvA.at[z], wsem.at[0])]
    for s, p_ref in ((1, p1_ref), (2, p2_ref), (3, p3_ref)):
        src = (z + NZ - s) % NZ
        local.append(pltpu.make_async_copy(w1f_ref.at[src], wvA.at[src, :, pl.ds(0, C1), :], wsem.at[2 * s]))
        local.append(pltpu.make_async_copy(p_ref, wvA.at[src, :, pl.ds(C1, C2), :], wsem.at[2 * s + 1]))
    late = [
        pltpu.make_async_copy(w2_ref.at[:, pl.ds(pl.multiple_of(z * 256 + CA, 32), C3), :], wvB.at[z], wsem.at[1]),
    ]
    for c in local + late:
        c.start()
    entry_barrier(z, p, zs)
    sends = []

    ph('c_send')
    def w_piece(src, dst, k, dev):
        return rcopy(w2_ref.at[:, pl.ds(pl.multiple_of(dst * 256 + CA, 32), C3), :], wvB.at[src], wbsend.at[k], wbrecv.at[src], dev)

    for k in (3, 2, 1):
        c = w_piece(z, zs[k], k, (zs[k], p))
        c.start()
        sends.append(c)
    for j in range(1, NP):
        q = (p + j) % NP
        c = rcopy(o_ref.at[q], og.at[z, p], osend.at[j], orecv.at[p], (z, q))
        c.start()
        sends.append(c)
    og[z, p] = o_ref[p]

    def gated(wv, n):
        g = None
        for q in range(NZ):
            t = jnp.dot(wv[q].reshape(2 * n, 512), hT[q * 512:(q + 1) * 512, :], preferred_element_type=F32)
            g = t if g is None else g + t
        gate = g[0:n].astype(BF16).astype(F32)
        up = g[n:2 * n].astype(BF16).astype(F32)
        return (jax.nn.silu(gate) * up).astype(BF16)

    ra = Relay(z, p, lambda src, ch: hidA.at[ch, src], hasend, harecv)
    rb = Relay(z, p, lambda src, ch: hidB.at[ch, src], hbsend, hbrecv)
    ro = Relay(z, p, lambda src, ch: og.at[src], gsend, grecv)
    every = range(CHUNKS)

    ph('c_localwait')
    for c in local:
        c.wait()
    ph('c_gA')
    ha = gated(wvA, CA)
    for ch in every:
        hidA[ch, z] = ha[:, ch * LANES:(ch + 1) * LANES]

    ra.own(range(2))
    ph('c_owait')
    for j in range(1, NP):
        q = (p + j) % NP
        rcopy(o_ref.at[0], og.at[z, q], osend.at[0], orecv.at[q], (z, p)).wait_recv()
    ro.own(range(1))
    ph('c_transp')
    for c in late:
        c.wait()
    wdAT[...] = jnp.concatenate([wd[q * 256:q * 256 + CA, :] for q in range(NZ)], axis=0).T
    wdBT[...] = jnp.concatenate([wd[q * 256 + CA:(q + 1) * 256, :] for q in range(NZ)], axis=0).T
    woT[...] = wo[...].T

    ph('c_wBwait')
    for k in range(1, NZ):
        w_piece(zs[k], z, 0, (z, p)).wait_recv()
    ph('c_gB')
    hb = gated(wvB, C3)
    for ch in range(CHUNKS):
        hidB[ch, z] = hb[:, ch * LANES:(ch + 1) * LANES]
    ph('c_own')
    rb.own(range(2))
    for ch in range(2, CHUNKS):
        ra.own((ch,))
        rb.own((ch,))
    ro.step(1, 0)

    chip = p // 2
    others = [xn // 2, yn // 2, diag // 2]

    def d2d(ch):
        return rcopy(ysum.at[ch, 1 - core], r1.at[ch], r1send.at[ch], r1recv.at[ch], (z, partner))

    def hop(ch, i, dev):
        return rcopy(acc.at[ch, i], r2.at[ch, i], r2send.at[ch, i], r2recv.at[ch, i], (z, dev))

    def stage1(ch):
        o_rows = og[ch * NZ // CHUNKS].reshape(128, 256)
        yt = jnp.dot(wdAT[...], hidA[ch].reshape(NZ * CA, LANES), preferred_element_type=F32)
        yt = yt + jnp.dot(wdBT[...], hidB[ch].reshape(NZ * C3, LANES), preferred_element_type=F32)
        yt = yt + lax.dot_general(woT[...], o_rows, (((1,), (1,)), ((), ())), preferred_element_type=F32)
        yt = yt.reshape(4, 2, 64, LANES)
        for i in range(4):
            for j in range(2):
                ysum[ch, j, i] = yt[i, j]
        d2d(ch).start()

    def stage2(ch):
        d2d(ch).wait_recv()
        for i, (t, dev) in enumerate(zip(others, (xn, yn, diag))):
            acc[ch, i] = ysum[ch, core, t] + r1[ch, t]
            hop(ch, i, dev).start()

    def stage3(ch):
        lanes = slice(ch * LANES, (ch + 1) * LANES)
        mine = ysum[ch, core, chip] + r1[ch, chip]
        for i, dev in enumerate((xn, yn, diag)):
            hop(ch, i, dev).wait_recv()
            mine = mine + r2[ch, i]
        y_ref[:, lanes] = (xT_ref[:, lanes].astype(F32) + mine).astype(BF16)

    for t in range(1, CHUNKS + 6):
        ph(f'c_wave{t}')
        for k in range(1, NZ):
            ch = t - k
            if 0 <= ch < CHUNKS:
                ra.step(k, ch)
                rb.step(k, ch)
        if t < 3:
            ro.step(t + 1, 0)
        ph(f'c_sum{t}')
        if 0 <= t - 3 < CHUNKS:
            stage1(t - 3)
            if t - 3 == CHUNKS - 2:
                stage2(t - 3)
        if 0 <= t - 4 < CHUNKS and t - 4 != CHUNKS - 2:
            stage2(t - 4)
        if 0 <= t - 5 < CHUNKS:
            stage3(t - 5)

    ph('c_end')
    for c in sends:
        c.wait_send()
    for ch in range(CHUNKS):
        d2d(ch).wait_send()
        for i, dev in enumerate((xn, yn, diag)):
            hop(ch, i, dev).wait_send()
    ra.drain(every)
    rb.drain(every)
    ro.drain(range(1))
    ph('')


def call_c(hT, w2, w1f, ps, wd, wo, o8, xT):
    vm = pl.BlockSpec(memory_space=pltpu.VMEM)
    hbm = pl.BlockSpec(memory_space=pl.ANY)
    return pl.pallas_call(
        kernel_c,
        out_shape=jax.ShapeDtypeStruct((64, 512), BF16),
        in_specs=[vm] + [hbm] * 5 + [vm] * 4,
        out_specs=vm,
        scratch_shapes=[
            pltpu.VMEM((NZ, 2, CA, 512), BF16),
            pltpu.VMEM((NZ, 2, C3, 512), BF16),
            pltpu.VMEM((512, NZ * CA), BF16),
            pltpu.VMEM((512, NZ * C3), BF16),
            pltpu.VMEM((512, 256), BF16),
            pltpu.VMEM((NZ, NP, 16, 256), BF16),
            pltpu.VMEM((CHUNKS, NZ, CA, LANES), BF16),
            pltpu.VMEM((CHUNKS, NZ, C3, LANES), BF16),
            pltpu.VMEM((CHUNKS, 2, 4, 64, LANES), F32),
            pltpu.VMEM((CHUNKS, 4, 64, LANES), F32),
            pltpu.VMEM((CHUNKS, 3, 64, LANES), F32),
            pltpu.VMEM((CHUNKS, 3, 64, LANES), F32),
            pltpu.SemaphoreType.DMA((8,)),
            pltpu.SemaphoreType.DMA((NZ,)),
            pltpu.SemaphoreType.DMA((NZ,)),
            pltpu.SemaphoreType.DMA((NP,)),
            pltpu.SemaphoreType.DMA((NP,)),
            pltpu.SemaphoreType.DMA((8, 1)),
            pltpu.SemaphoreType.DMA((NZ, 1)),
            pltpu.SemaphoreType.DMA((8, CHUNKS)),
            pltpu.SemaphoreType.DMA((NZ, CHUNKS)),
            pltpu.SemaphoreType.DMA((8, CHUNKS)),
            pltpu.SemaphoreType.DMA((NZ, CHUNKS)),
            pltpu.SemaphoreType.DMA((CHUNKS,)),
            pltpu.SemaphoreType.DMA((CHUNKS,)),
            pltpu.SemaphoreType.DMA((CHUNKS, 3)),
            pltpu.SemaphoreType.DMA((CHUNKS, 3)),
        ],
        compiler_params=pltpu.CompilerParams(collective_id=1, has_side_effects=True, vmem_limit_bytes=40 * 1024 * 1024),
        cost_estimate=pl.CostEstimate(flops=12_000_000_000, bytes_accessed=6_000_000, transcendentals=0),
        name='mlp_out',
    )(hT, w2, w1f, *ps, wd, wo, o8, xT)


def solution(mesh):
    all_axes = ('x', 'yz')

    def local_step(x_in, ln_scale, w_gate_up, w_attn, w_down, w_out, k_cache, v_cache, lengths, positions):
        xT = x_in.T
        wattnT = w_attn.T
        hT, qkv, w1f, w2, *pieces = call_a(xT, ln_scale[None, :], wattnT, w_gate_up)
        ps = [lax.ppermute(pieces[i], 'x', [(q, (q + i + 1) % NZ) for q in range(NZ)]) for i in range(NZ - 1)]
        proj = jnp.transpose(qkv, (1, 0, 2)).reshape(16, 2304)
        q_raw = proj[:, :2048].reshape(16, 16, 128)
        k_tok = proj[:, 2048:2176]
        v_tok = proj[:, 2176:]
        q_rot = rotary(q_raw.astype(F32), positions).astype(BF16)
        k_rot = rotary(k_tok[:, None, :].astype(F32), positions).astype(BF16)
        o8, k_new, v_new = call_b(lengths, q_rot, k_rot, v_tok[:, None, :], k_cache, v_cache)
        yT = call_c(hT, w2, w1f, ps, w_down, w_out, o8, xT)
        return yT.T, k_new, v_new

    row_spec = P(None, all_axes)
    vec_spec = P(all_axes)
    cache_spec = P(all_axes, None, None)
    return jax.shard_map(
        local_step,
        mesh=mesh,
        in_specs=(row_spec, vec_spec, P('x', None, 'yz'), P('x', 'yz'), P('yz', 'x'), P('yz', 'x'), cache_spec, cache_spec, vec_spec, vec_spec),
        out_specs=(row_spec, cache_spec, cache_spec),
        check_vma=False,
    )
```

```python
import functools

import jax
import jax.numpy as jnp
from jax import lax
from jax.experimental import pallas as pl
from jax.experimental.pallas import tpu as pltpu
from jax.sharding import PartitionSpec as P

LN_EPS = 1e-6
ROPE_BASE = 10000.0
MESH = pl.DeviceIdType.MESH


class Phase:
    cm = None

    def __call__(self, name):
        if self.cm is not None:
            self.cm.__exit__(None, None, None)
            self.cm = None
        if name:
            self.cm = jax.named_scope(name)
            self.cm.__enter__()


ph = Phase()
F32 = jnp.float32
BF16 = jnp.bfloat16

NZ = 4
NP = 8
C1 = 48
C2 = 144
C3 = 64
CA = C1 + C2
CHUNKS = 4
LANES = 512 // CHUNKS


def rotary(values, positions):
    half_dim = values.shape[-1] // 2
    inv_freq = ROPE_BASE ** (-jnp.arange(half_dim, dtype=jnp.float32) / half_dim)
    angles = positions.astype(jnp.float32)[:, None, None] * inv_freq
    cos_part = jnp.cos(angles)
    sin_part = jnp.sin(angles)
    lo_half = values[..., :half_dim]
    hi_half = values[..., half_dim:]
    return jnp.concatenate([lo_half * cos_part - hi_half * sin_part, hi_half * cos_part + lo_half * sin_part], axis=-1)


def coords():
    z = lax.axis_index('x')
    p = lax.axis_index('yz')
    core = p % 2
    xx = (p // 2) % 2
    y = p // 4
    partner = p + 1 - 2 * core
    xn = p + 2 - 4 * xx
    yn = p + 4 - 8 * y
    diag = xn + 4 - 8 * y
    z1 = z % 2
    z2 = z // 2
    zs = [z, 2 * z2 + 1 - z1, 2 * (1 - z2) + z1, 3 - z]
    return z, p, core, partner, xn, yn, diag, zs


def entry_barrier(z, p, zs):
    sem = pltpu.get_barrier_semaphore()
    for k in range(1, NZ):
        pl.semaphore_signal(sem, inc=1, device_id=(zs[k], p), device_id_type=MESH)
    for k in range(1, NP):
        pl.semaphore_signal(sem, inc=1, device_id=(z, (p + k) % NP), device_id_type=MESH)
    pl.semaphore_wait(sem, NZ - 1 + NP - 1)


def rcopy(src, dst, send, recv, dev):
    return pltpu.make_async_remote_copy(src_ref=src, dst_ref=dst, send_sem=send, recv_sem=recv, device_id=dev, device_id_type=MESH)


class Relay:
    def __init__(self, z, p, at, send, recv):
        self.z, self.p, self.at, self.send, self.recv = z, p, at, send, recv

    def copy(self, way, src, ch, dev):
        ref = self.at(src, ch)
        return rcopy(ref, ref, self.send.at[way, ch], self.recv.at[src, ch], (dev, self.p))

    def own(self, chunks):
        z = self.z

        @pl.when(z < 3)
        def _():
            for ch in chunks:
                self.copy(0, z, ch, z + 1).start()

        @pl.when(z > 0)
        def _():
            for ch in chunks:
                self.copy(1, z, ch, z - 1).start()

    def step(self, k, ch):
        z = self.z

        @pl.when(z >= k)
        def _():
            self.copy(0, z - k, ch, z).wait_recv()

            @pl.when(z < 3)
            def _():
                self.copy(2 * k, z - k, ch, z + 1).start()

        @pl.when(z + k <= 3)
        def _():
            self.copy(0, z + k, ch, z).wait_recv()

            @pl.when(z > 0)
            def _():
                self.copy(2 * k + 1, z + k, ch, z - 1).start()

    def drain(self, chunks):
        z = self.z
        for k in range(NZ - 1):
            @pl.when((z >= k) & (z < 3))
            def _():
                for ch in chunks:
                    self.copy(2 * k, z, ch, z).wait_send()

            @pl.when((z + k <= 3) & (z > 0))
            def _():
                for ch in chunks:
                    self.copy(2 * k + 1, z, ch, z).wait_send()


def attn_start(q):
    return pl.multiple_of(64 * q + 16 * (q // 2), 16)


def kernel_a(xT_ref, ln_ref, wattn_ref, w_ref, h_ref, qkv_ref, w1f_ref, w2_ref, ps1_ref, ps2_ref, ps3_ref,
             xg, lng, watt, zsend, zrecv, zq, s1, s2, wn, wt, hT_ref,
             xsend, xrecv, lsend, lrecv, asend, arecv, zsend_sem, zrecv_sem, qsend, qrecv, wsend, wrecv, lsem, osem):
    z, p, core, partner, xn, yn, diag, zs = coords()
    ph('a_bar')
    wload = pltpu.make_async_copy(w_ref, wn, lsem.at[0])
    wload.start()
    xg[z, p] = xT_ref[...]
    lng[z, p] = jnp.zeros((1, 128), F32)
    lng[z, p, 0:1, 0:64] = ln_ref[...]
    entry_barrier(z, p, zs)
    ph('a_zsend')
    sends = []
    nx = iter(range(40))
    nl = iter(range(40))

    def send(src_z, src_p, dev):
        c = rcopy(xg.at[src_z, src_p], xg.at[src_z, src_p], xsend.at[next(nx)], xrecv.at[src_z, src_p], dev)
        c.start()
        sends.append(c)

    def send_l(src_z, src_p, dev):
        c = rcopy(lng.at[src_z, src_p], lng.at[src_z, src_p], lsend.at[next(nl)], lrecv.at[src_z, src_p], dev)
        c.start()
        sends.append(c)

    def wait_x(src_z, src_p):
        rcopy(xg.at[src_z, src_p], xg.at[src_z, src_p], xsend.at[0], xrecv.at[src_z, src_p], (z, p)).wait_recv()

    def wait_l(src_z, src_p):
        rcopy(lng.at[src_z, src_p], lng.at[src_z, src_p], lsend.at[0], lrecv.at[src_z, src_p], (z, p)).wait_recv()

    def stat(src_z, src_p):
        blk = xg[src_z, src_p].astype(F32).reshape(8, 8, 512)
        s1[...] += jnp.sum(blk, axis=0)
        s2[...] += jnp.sum(blk * blk, axis=0)

    def w_piece(src, dst, k, dev):
        return rcopy(
            wt.at[:, pl.ds(pl.multiple_of(dst * 256, 256), C1), :],
            w1f_ref.at[src], wsend.at[k], wrecv.at[src], dev)

    def turn(odd):
        def body(i, carry):
            lanes = pl.ds(pl.multiple_of(i * 256 + odd * 128, 128), 128)
            blk = wn[:, :, lanes].astype(F32)
            for g in range(2):
                wt[g, lanes, :] = blk[:, g, :].T.astype(BF16)
            return carry

        lax.fori_loop(0, NZ, body, 0)

    mid = 2 - z // 2
    far = 3 - 3 * (z // 2)
    zo = [z, zs[1], mid, far]
    inner = (z == 1) | (z == 2)
    send(z, p, (mid, p))
    send(z, p, (zs[1], p))
    for k in (3, 2, 1):
        send_l(z, p, (zs[k], p))
    for dev in (xn, yn, partner):
        send(z, p, (z, dev))

    def outward(k):
        return rcopy(xg.at[zo[k], p], xg.at[zo[k], p], osem.at[k - 2], xrecv.at[zo[k], p], (zs[1], p))

    for j in range(1, NP):
        send_l(z, p, (z, (p + j) % NP))
    s1[...] = jnp.zeros_like(s1)
    s2[...] = jnp.zeros_like(s2)
    stat(z, p)
    watt[z] = wattn_ref[pl.ds(attn_start(z), 80), :]
    wload.wait()
    turn(0)

    def column(k):
        wait_x(zo[k], p)
        if k >= 2:
            @pl.when(inner)
            def _():
                outward(k).start()
        if k == 3:
            send(zo[k], p, (z, diag))
        for dev in (xn, yn, partner):
            send(zo[k], p, (z, dev))
        stat(zo[k], p)

    two_src = xn + core * (yn - xn)
    two_dst = yn + core * (xn - yn)

    def neighbours(k):
        wait_x(zo[k], xn)
        if k == 2:
            wait_x(zo[k], yn)
        if k == 1:
            send(zo[k], xn, (z, yn))
        if k == 2:
            send(zo[k], two_src, (z, two_dst))
        send(zo[k], xn, (z, partner))
        stat(zo[k], xn)
        if k != 2:
            wait_x(zo[k], yn)
        if k == 0:
            send(zo[k], yn, (z, xn))
        send(zo[k], yn, (z, partner))
        stat(zo[k], yn)

    def diagonal(k):
        wait_x(zo[k], diag)
        send(zo[k], diag, (z, partner))
        stat(zo[k], diag)

    ph('a_col1')
    column(1)
    column(2)
    ph('a_col3')
    column(3)
    ph('a_lnsend')
    for k in range(1, NZ):
        wait_l(zs[k], p)
        for j in range(1, NP):
            send_l(zs[k], p, (z, (p + j) % NP))
    ph('a_nbr')
    neighbours(0)
    neighbours(1)
    ph('a_nbr2')
    diagonal(0)
    ph('a_wattn')
    for k in (3, 2, 1):
        c = rcopy(wattn_ref.at[pl.ds(attn_start(zs[k]), 80), :], watt.at[z], asend.at[k], arecv.at[z], (zs[k], p))
        c.start()
        sends.append(c)
    ph('a_nbr3')
    neighbours(2)
    diagonal(1)
    neighbours(3)
    ph('a_diag')
    diagonal(2)
    diagonal(3)
    ph('a_rest')
    pd = [partner + xn - p, partner + yn - p, partner + diag - p]
    for q in [partner] + pd:
        for k in range(NZ):
            wait_x(zo[k], q)
            stat(zo[k], q)
    for k in range(NZ):
        for j in range(1, NP):
            wait_l(zs[k], (p + j) % NP)

    ph('a_norm')
    mean = jnp.sum(s1[...], axis=0, keepdims=True) / 2048.0
    var = jnp.sum(s2[...], axis=0, keepdims=True) / 2048.0 - mean * mean
    rstd = lax.rsqrt(var + LN_EPS)
    lnT = jnp.concatenate([lng[i // NP, i % NP, 0:1, :] for i in range(32)] + [jnp.zeros((96, 128), F32)], axis=0).T
    for i in range(NZ * NP):
        sc = lnT[0:64, i:i + 1]
        hT_ref[i * 64:(i + 1) * 64, :] = ((xg[i // NP, i % NP].astype(F32) - mean) * rstd * sc).astype(BF16)

    hout = pltpu.make_async_copy(hT_ref, h_ref, lsem.at[5])
    hout.start()
    ph('a_attw')
    for k in range(1, NZ):
        rcopy(watt.at[z], watt.at[zs[k]], asend.at[0], arecv.at[zs[k]], (z, p)).wait_recv()
    ph('a_zdot')
    part = None
    for q in range(NZ):
        t = jnp.dot(watt[q], hT_ref[q * 512:(q + 1) * 512, :], preferred_element_type=F32)
        part = t if part is None else part + t
    part = part.astype(BF16)
    for q in range(NZ):
        zsend[q] = part[:, q * 128:(q + 1) * 128]
    for k in (3, 2, 1):
        c = rcopy(zsend.at[zs[k]], zrecv.at[z], zsend_sem.at[k], zrecv_sem.at[z], (zs[k], p))
        c.start()
        sends.append(c)
    zrecv[z] = zsend[z]
    ph('a_turn')
    turn(1)
    for k in (3, 2, 1):
        c = w_piece(z, zs[k], k, (zs[k], p))
        c.start()
        sends.append(c)
    outs = [pltpu.make_async_copy(wt, w2_ref, lsem.at[1])]
    for i, ps_ref in enumerate((ps1_ref, ps2_ref, ps3_ref)):
        dst = (z + i + 1) % NZ
        outs.append(pltpu.make_async_copy(wt.at[:, pl.ds(pl.multiple_of(dst * 256 + C1, 16), C2), :], ps_ref, lsem.at[2 + i]))
    for c in outs[1:] + outs[:1]:
        c.start()
    ph('a_zwait')
    for k in range(1, NZ):
        rcopy(zsend.at[0], zrecv.at[zs[k]], zsend_sem.at[0], zrecv_sem.at[zs[k]], (z, p)).wait_recv()
    ph('a_a2a')
    zt = jnp.concatenate([zrecv[0].astype(F32), zrecv[1].astype(F32)[16:80], zrecv[2].astype(F32), zrecv[3].astype(F32)[16:80]], axis=0)
    zq[...] = zt.T.astype(BF16).reshape(NP, 16, 288)
    for j in range(1, NP):
        q = (p + j) % NP
        c = rcopy(zq.at[q], qkv_ref.at[p], qsend.at[j], qrecv.at[p], (z, q))
        c.start()
        sends.append(c)
    qkv_ref[p] = zq[p]
    for j in range(1, NP):
        q = (p + j) % NP
        rcopy(zq.at[0], qkv_ref.at[q], qsend.at[0], qrecv.at[q], (z, p)).wait_recv()
    ph('a_wwait')
    for k in range(1, NZ):
        w_piece(zs[k], z, 0, (z, p)).wait_recv()
    ph('a_sendwait')
    hout.wait()
    for c in outs:
        c.wait()
    for c in sends:
        c.wait_send()

    @pl.when(inner)
    def _():
        outward(2).wait_send()
        outward(3).wait_send()
    ph('')


def call_a(xT, ln, wattnT, w):
    vm = pl.BlockSpec(memory_space=pltpu.VMEM)
    hbm = pl.BlockSpec(memory_space=pl.ANY)
    return pl.pallas_call(
        kernel_a,
        out_shape=(
            jax.ShapeDtypeStruct((2048, 512), BF16),
            jax.ShapeDtypeStruct((NP, 16, 288), BF16),
            jax.ShapeDtypeStruct((NZ, 2, C1, 512), BF16),
            jax.ShapeDtypeStruct((2, 1024, 512), BF16),
        ) + (jax.ShapeDtypeStruct((2, C2, 512), BF16),) * 3,
        in_specs=[vm] * 3 + [hbm],
        out_specs=(hbm, vm) + (hbm,) * 5,
        scratch_shapes=[
            pltpu.VMEM((NZ, NP, 64, 512), BF16),
            pltpu.VMEM((NZ, NP, 1, 128), F32),
            pltpu.VMEM((NZ, 80, 512), BF16),
            pltpu.VMEM((NZ, 80, 128), BF16),
            pltpu.VMEM((NZ, 80, 128), BF16),
            pltpu.VMEM((NP, 16, 288), BF16),
            pltpu.VMEM((8, 512), F32),
            pltpu.VMEM((8, 512), F32),
            pltpu.VMEM((512, 2, 1024), BF16),
            pltpu.VMEM((2, 1024, 512), BF16),
            pltpu.VMEM((2048, 512), BF16),
            pltpu.SemaphoreType.DMA((40,)),
            pltpu.SemaphoreType.DMA((NZ, NP)),
            pltpu.SemaphoreType.DMA((40,)),
            pltpu.SemaphoreType.DMA((NZ, NP)),
            pltpu.SemaphoreType.DMA((NZ,)),
            pltpu.SemaphoreType.DMA((NZ,)),
            pltpu.SemaphoreType.DMA((NZ,)),
            pltpu.SemaphoreType.DMA((NZ,)),
            pltpu.SemaphoreType.DMA((NP,)),
            pltpu.SemaphoreType.DMA((NP,)),
            pltpu.SemaphoreType.DMA((NZ,)),
            pltpu.SemaphoreType.DMA((NZ,)),
            pltpu.SemaphoreType.DMA((6,)),
            pltpu.SemaphoreType.DMA((2,)),
        ],
        compiler_params=pltpu.CompilerParams(collective_id=0, has_side_effects=True, vmem_limit_bytes=56 * 1024 * 1024),
        name='gather_norm_qkv',
    )(xT, ln, wattnT, w)


def kernel_b(len_ref, q_ref, k_ref, v_ref, kc_ref, vc_ref, o_ref, kn_ref, vn_ref, kbuf, vbuf, oscr, isem, osem):
    rows = kbuf.shape[0]
    seq = kbuf.shape[1]

    def load(b, t):
        return pltpu.make_async_copy((kc_ref, vc_ref)[t].at[b], (kbuf, vbuf)[t].at[b], isem.at[b, t])

    def store(b, t):
        return pltpu.make_async_copy((kbuf, vbuf)[t].at[b], (kn_ref, vn_ref)[t].at[b], osem.at[b, t])

    for b in range(rows):
        load(b, 0).start()
        load(b, 1).start()

    def insert(buf, b, length, new):
        base = pl.multiple_of((length // 16) * 16, 16)
        hit = base + lax.broadcasted_iota(jnp.int32, (16, 128), 0) == length
        buf[b, pl.ds(base, 16), :] = jnp.where(hit, new.astype(F32), buf[b, pl.ds(base, 16), :].astype(F32)).astype(BF16)

    def attend(b, length, n):
        scores = lax.dot_general(q_ref[b], kbuf[b, 0:n, :], (((1,), (1,)), ((), ())), preferred_element_type=F32) * (128.0 ** -0.5)
        slot = lax.broadcasted_iota(jnp.int32, scores.shape, 1)
        scores = jnp.where(slot <= length, scores, -1e30)
        top = jnp.max(scores, axis=1, keepdims=True)
        e = jnp.exp(scores - top)
        probs = (e / jnp.sum(e, axis=1, keepdims=True)).astype(BF16)
        return jnp.dot(probs, vbuf[b, 0:n, :], preferred_element_type=F32)

    def pair(i, carry):
        b0 = 2 * i
        b1 = 2 * i + 1
        l0 = len_ref[b0]
        l1 = len_ref[b1]
        for b, length in ((b0, l0), (b1, l1)):
            load(b, 0).wait()
            load(b, 1).wait()
            insert(kbuf, b, length, k_ref[b])
            insert(vbuf, b, length, v_ref[b])
        last = jnp.maximum(l0, l1) // 512
        for t in range(seq // 512):
            @pl.when(last == t)
            def _():
                n = 512 * (t + 1)
                r0 = attend(b0, l0, n)
                r1 = attend(b1, l1, n)
                oscr[b0] = r0
                oscr[b1] = r1
        for b in (b0, b1):
            store(b, 0).start()
            store(b, 1).start()
        return carry

    lax.fori_loop(0, rows // 2, pair, 0)
    for h in range(16):
        o_ref[h // 2, :, (h % 2) * 128:(h % 2 + 1) * 128] = oscr[:, h, :].astype(BF16)
    for b in range(rows):
        store(b, 0).wait()
        store(b, 1).wait()


def call_b(lengths, q_rot, k_rot, v_tok, k_cache, v_cache):
    rows, seq, hd = k_cache.shape
    heads = q_rot.shape[1]
    vm = pl.BlockSpec(memory_space=pltpu.VMEM)
    hbm = pl.BlockSpec(memory_space=pl.ANY)
    return pl.pallas_call(
        kernel_b,
        in_specs=[pl.BlockSpec(memory_space=pltpu.SMEM), vm, vm, vm, hbm, hbm],
        out_specs=(vm, hbm, hbm),
        out_shape=(
            jax.ShapeDtypeStruct((NP, rows, heads * hd // NP), BF16),
            jax.ShapeDtypeStruct(k_cache.shape, BF16),
            jax.ShapeDtypeStruct(v_cache.shape, BF16),
        ),
        scratch_shapes=[
            pltpu.VMEM((rows, seq, hd), BF16),
            pltpu.VMEM((rows, seq, hd), BF16),
            pltpu.VMEM((rows, heads, hd), F32),
            pltpu.SemaphoreType.DMA((rows, 2)),
            pltpu.SemaphoreType.DMA((rows, 2)),
        ],
        compiler_params=pltpu.CompilerParams(vmem_limit_bytes=58 * 1024 * 1024),
        cost_estimate=pl.CostEstimate(flops=12_000_000_000, bytes_accessed=33_000_000, transcendentals=0),
        name='attend',
    )(lengths, q_rot, k_rot, v_tok, k_cache, v_cache)


def kernel_c(hT, w2_ref, w1f_ref, p1_ref, p2_ref, p3_ref, wd, wo, o_ref, xT_ref, y_ref,
             wvA, wvB, wdAT, wdBT, woT, og, hidA, hidB, ysum, r1, acc, r2,
             wsem, wbsend, wbrecv, osend, orecv, gsend, grecv, hasend, harecv, hbsend, hbrecv,
             r1send, r1recv, r2send, r2recv):
    z, p, core, partner, xn, yn, diag, zs = coords()
    ph('c_bar')
    local = [pltpu.make_async_copy(w2_ref.at[:, pl.ds(pl.multiple_of(z * 256, 256), CA), :], wvA.at[z], wsem.at[0])]
    for s, p_ref in ((1, p1_ref), (2, p2_ref), (3, p3_ref)):
        src = (z + NZ - s) % NZ
        local.append(pltpu.make_async_copy(w1f_ref.at[src], wvA.at[src, :, pl.ds(0, C1), :], wsem.at[2 * s]))
        local.append(pltpu.make_async_copy(p_ref, wvA.at[src, :, pl.ds(C1, C2), :], wsem.at[2 * s + 1]))
    late = [
        pltpu.make_async_copy(w2_ref.at[:, pl.ds(pl.multiple_of(z * 256 + CA, 32), C3), :], wvB.at[z], wsem.at[1]),
    ]
    for c in local + late:
        c.start()
    entry_barrier(z, p, zs)
    sends = []

    ph('c_send')
    def w_piece(src, dst, k, dev):
        return rcopy(w2_ref.at[:, pl.ds(pl.multiple_of(dst * 256 + CA, 32), C3), :], wvB.at[src], wbsend.at[k], wbrecv.at[src], dev)

    for k in (3, 2, 1):
        c = w_piece(z, zs[k], k, (zs[k], p))
        c.start()
        sends.append(c)
    for j in range(1, NP):
        q = (p + j) % NP
        c = rcopy(o_ref.at[q], og.at[z, p], osend.at[j], orecv.at[p], (z, q))
        c.start()
        sends.append(c)
    og[z, p] = o_ref[p]

    def gated(wv, n):
        g = None
        for q in range(NZ):
            t = jnp.dot(wv[q].reshape(2 * n, 512), hT[q * 512:(q + 1) * 512, :], preferred_element_type=F32)
            g = t if g is None else g + t
        gate = g[0:n].astype(BF16).astype(F32)
        up = g[n:2 * n].astype(BF16).astype(F32)
        return (jax.nn.silu(gate) * up).astype(BF16)

    ra = Relay(z, p, lambda src, ch: hidA.at[ch, src], hasend, harecv)
    rb = Relay(z, p, lambda src, ch: hidB.at[ch, src], hbsend, hbrecv)
    ro = Relay(z, p, lambda src, ch: og.at[src], gsend, grecv)
    every = range(CHUNKS)

    ph('c_localwait')
    for c in local:
        c.wait()
    ph('c_gA')
    ha = gated(wvA, CA)
    for ch in every:
        hidA[ch, z] = ha[:, ch * LANES:(ch + 1) * LANES]

    ra.own(range(2))
    ph('c_owait')
    for j in range(1, NP):
        q = (p + j) % NP
        rcopy(o_ref.at[0], og.at[z, q], osend.at[0], orecv.at[q], (z, p)).wait_recv()
    ro.own(range(1))
    ph('c_transp')
    for c in late:
        c.wait()
    wdAT[...] = jnp.concatenate([wd[q * 256:q * 256 + CA, :] for q in range(NZ)], axis=0).T
    wdBT[...] = jnp.concatenate([wd[q * 256 + CA:(q + 1) * 256, :] for q in range(NZ)], axis=0).T
    woT[...] = wo[...].T

    ph('c_wBwait')
    for k in range(1, NZ):
        w_piece(zs[k], z, 0, (z, p)).wait_recv()
    ph('c_gB')
    hb = gated(wvB, C3)
    for ch in range(CHUNKS):
        hidB[ch, z] = hb[:, ch * LANES:(ch + 1) * LANES]
    ph('c_own')
    rb.own(range(2))
    for ch in range(2, CHUNKS):
        ra.own((ch,))
        rb.own((ch,))
    ro.step(1, 0)

    chip = p // 2
    others = [xn // 2, yn // 2, diag // 2]

    def d2d(ch):
        return rcopy(ysum.at[ch, 1 - core], r1.at[ch], r1send.at[ch], r1recv.at[ch], (z, partner))

    def hop(ch, i, dev):
        return rcopy(acc.at[ch, i], r2.at[ch, i], r2send.at[ch, i], r2recv.at[ch, i], (z, dev))

    def stage1(ch):
        o_rows = og[ch * NZ // CHUNKS].reshape(128, 256)
        yt = jnp.dot(wdAT[...], hidA[ch].reshape(NZ * CA, LANES), preferred_element_type=F32)
        yt = yt + jnp.dot(wdBT[...], hidB[ch].reshape(NZ * C3, LANES), preferred_element_type=F32)
        yt = yt + lax.dot_general(woT[...], o_rows, (((1,), (1,)), ((), ())), preferred_element_type=F32)
        yt = yt.reshape(4, 2, 64, LANES)
        for i in range(4):
            for j in range(2):
                ysum[ch, j, i] = yt[i, j]
        d2d(ch).start()

    def stage2(ch):
        d2d(ch).wait_recv()
        for i, (t, dev) in enumerate(zip(others, (xn, yn, diag))):
            acc[ch, i] = ysum[ch, core, t] + r1[ch, t]
            hop(ch, i, dev).start()

    def stage3(ch):
        lanes = slice(ch * LANES, (ch + 1) * LANES)
        mine = ysum[ch, core, chip] + r1[ch, chip]
        for i, dev in enumerate((xn, yn, diag)):
            hop(ch, i, dev).wait_recv()
            mine = mine + r2[ch, i]
        y_ref[:, lanes] = (xT_ref[:, lanes].astype(F32) + mine).astype(BF16)

    for t in range(1, CHUNKS + 3):
        ph(f'c_wave{t}')
        for k in range(1, NZ):
            ch = t - k
            if 0 <= ch < CHUNKS:
                ra.step(k, ch)
                rb.step(k, ch)
        if t < 3:
            ro.step(t + 1, 0)
        ph(f'c_sum{t}')
        if t >= 3:
            stage1(t - 3)
        if t >= 4:
            stage2(t - 4)
    ph('c_last2')
    stage2(CHUNKS - 1)
    ph('c_last3')
    for ch in every:
        stage3(ch)

    ph('c_end')
    for c in sends:
        c.wait_send()
    for ch in range(CHUNKS):
        d2d(ch).wait_send()
        for i, dev in enumerate((xn, yn, diag)):
            hop(ch, i, dev).wait_send()
    ra.drain(every)
    rb.drain(every)
    ro.drain(range(1))
    ph('')


def call_c(hT, w2, w1f, ps, wd, wo, o8, xT):
    vm = pl.BlockSpec(memory_space=pltpu.VMEM)
    hbm = pl.BlockSpec(memory_space=pl.ANY)
    return pl.pallas_call(
        kernel_c,
        out_shape=jax.ShapeDtypeStruct((64, 512), BF16),
        in_specs=[vm] + [hbm] * 5 + [vm] * 4,
        out_specs=vm,
        scratch_shapes=[
            pltpu.VMEM((NZ, 2, CA, 512), BF16),
            pltpu.VMEM((NZ, 2, C3, 512), BF16),
            pltpu.VMEM((512, NZ * CA), BF16),
            pltpu.VMEM((512, NZ * C3), BF16),
            pltpu.VMEM((512, 256), BF16),
            pltpu.VMEM((NZ, NP, 16, 256), BF16),
            pltpu.VMEM((CHUNKS, NZ, CA, LANES), BF16),
            pltpu.VMEM((CHUNKS, NZ, C3, LANES), BF16),
            pltpu.VMEM((CHUNKS, 2, 4, 64, LANES), F32),
            pltpu.VMEM((CHUNKS, 4, 64, LANES), F32),
            pltpu.VMEM((CHUNKS, 3, 64, LANES), F32),
            pltpu.VMEM((CHUNKS, 3, 64, LANES), F32),
            pltpu.SemaphoreType.DMA((8,)),
            pltpu.SemaphoreType.DMA((NZ,)),
            pltpu.SemaphoreType.DMA((NZ,)),
            pltpu.SemaphoreType.DMA((NP,)),
            pltpu.SemaphoreType.DMA((NP,)),
            pltpu.SemaphoreType.DMA((8, 1)),
            pltpu.SemaphoreType.DMA((NZ, 1)),
            pltpu.SemaphoreType.DMA((8, CHUNKS)),
            pltpu.SemaphoreType.DMA((NZ, CHUNKS)),
            pltpu.SemaphoreType.DMA((8, CHUNKS)),
            pltpu.SemaphoreType.DMA((NZ, CHUNKS)),
            pltpu.SemaphoreType.DMA((CHUNKS,)),
            pltpu.SemaphoreType.DMA((CHUNKS,)),
            pltpu.SemaphoreType.DMA((CHUNKS, 3)),
            pltpu.SemaphoreType.DMA((CHUNKS, 3)),
        ],
        compiler_params=pltpu.CompilerParams(collective_id=1, has_side_effects=True, vmem_limit_bytes=40 * 1024 * 1024),
        cost_estimate=pl.CostEstimate(flops=12_000_000_000, bytes_accessed=6_000_000, transcendentals=0),
        name='mlp_out',
    )(hT, w2, w1f, *ps, wd, wo, o8, xT)


def solution(mesh):
    all_axes = ('x', 'yz')

    def local_step(x_in, ln_scale, w_gate_up, w_attn, w_down, w_out, k_cache, v_cache, lengths, positions):
        xT = x_in.T
        wattnT = w_attn.T
        hT, qkv, w1f, w2, *pieces = call_a(xT, ln_scale[None, :], wattnT, w_gate_up)
        ps = [lax.ppermute(pieces[i], 'x', [(q, (q + i + 1) % NZ) for q in range(NZ)]) for i in range(NZ - 1)]
        proj = jnp.transpose(qkv, (1, 0, 2)).reshape(16, 2304)
        q_raw = proj[:, :2048].reshape(16, 16, 128)
        k_tok = proj[:, 2048:2176]
        v_tok = proj[:, 2176:]
        q_rot = rotary(q_raw.astype(F32), positions).astype(BF16)
        k_rot = rotary(k_tok[:, None, :].astype(F32), positions).astype(BF16)
        o8, k_new, v_new = call_b(lengths, q_rot, k_rot, v_tok[:, None, :], k_cache, v_cache)
        yT = call_c(hT, w2, w1f, ps, w_down, w_out, o8, xT)
        return yT.T, k_new, v_new

    row_spec = P(None, all_axes)
    vec_spec = P(all_axes)
    cache_spec = P(all_axes, None, None)
    return jax.shard_map(
        local_step,
        mesh=mesh,
        in_specs=(row_spec, vec_spec, P('x', None, 'yz'), P('x', 'yz'), P('yz', 'x'), P('yz', 'x'), cache_spec, cache_spec, vec_spec, vec_spec),
        out_specs=(row_spec, cache_spec, cache_spec),
        check_vma=False,
    )
```

```python
import functools

import jax
import jax.numpy as jnp
from jax import lax
from jax.experimental import pallas as pl
from jax.experimental.pallas import tpu as pltpu
from jax.sharding import PartitionSpec as P

LN_EPS = 1e-6
ROPE_BASE = 10000.0
MESH = pl.DeviceIdType.MESH


class Phase:
    cm = None

    def __call__(self, name):
        if self.cm is not None:
            self.cm.__exit__(None, None, None)
            self.cm = None
        if name:
            self.cm = jax.named_scope(name)
            self.cm.__enter__()


ph = Phase()
F32 = jnp.float32
BF16 = jnp.bfloat16

NZ = 4
NP = 8
C1A = 16
C1 = 48
C2 = 128
C3 = 80
CA = C1 + C2
CHUNKS = 4
LANES = 512 // CHUNKS


def rotary(values, positions):
    half_dim = values.shape[-1] // 2
    inv_freq = ROPE_BASE ** (-jnp.arange(half_dim, dtype=jnp.float32) / half_dim)
    angles = positions.astype(jnp.float32)[:, None, None] * inv_freq
    cos_part = jnp.cos(angles)
    sin_part = jnp.sin(angles)
    lo_half = values[..., :half_dim]
    hi_half = values[..., half_dim:]
    return jnp.concatenate([lo_half * cos_part - hi_half * sin_part, hi_half * cos_part + lo_half * sin_part], axis=-1)


def coords():
    z = lax.axis_index('x')
    p = lax.axis_index('yz')
    core = p % 2
    xx = (p // 2) % 2
    y = p // 4
    partner = p + 1 - 2 * core
    xn = p + 2 - 4 * xx
    yn = p + 4 - 8 * y
    diag = xn + 4 - 8 * y
    z1 = z % 2
    z2 = z // 2
    zs = [z, 2 * z2 + 1 - z1, 2 * (1 - z2) + z1, 3 - z]
    return z, p, core, partner, xn, yn, diag, zs


def entry_barrier(z, p, zs):
    sem = pltpu.get_barrier_semaphore()
    for k in range(1, NZ):
        pl.semaphore_signal(sem, inc=1, device_id=(zs[k], p), device_id_type=MESH)
    for k in range(1, NP):
        pl.semaphore_signal(sem, inc=1, device_id=(z, (p + k) % NP), device_id_type=MESH)
    pl.semaphore_wait(sem, NZ - 1 + NP - 1)


def rcopy(src, dst, send, recv, dev):
    return pltpu.make_async_remote_copy(src_ref=src, dst_ref=dst, send_sem=send, recv_sem=recv, device_id=dev, device_id_type=MESH)


class Relay:
    def __init__(self, z, p, at, send, recv):
        self.z, self.p, self.at, self.send, self.recv = z, p, at, send, recv

    def copy(self, way, src, ch, dev):
        ref = self.at(src, ch)
        return rcopy(ref, ref, self.send.at[way, ch], self.recv.at[src, ch], (dev, self.p))

    def own(self, chunks):
        z = self.z

        @pl.when(z < 3)
        def _():
            for ch in chunks:
                self.copy(0, z, ch, z + 1).start()

        @pl.when(z > 0)
        def _():
            for ch in chunks:
                self.copy(1, z, ch, z - 1).start()

    def step(self, k, ch):
        z = self.z

        @pl.when(z >= k)
        def _():
            self.copy(0, z - k, ch, z).wait_recv()

            @pl.when(z < 3)
            def _():
                self.copy(2 * k, z - k, ch, z + 1).start()

        @pl.when(z + k <= 3)
        def _():
            self.copy(0, z + k, ch, z).wait_recv()

            @pl.when(z > 0)
            def _():
                self.copy(2 * k + 1, z + k, ch, z - 1).start()

    def drain(self, chunks):
        z = self.z
        for k in range(NZ - 1):
            @pl.when((z >= k) & (z < 3))
            def _():
                for ch in chunks:
                    self.copy(2 * k, z, ch, z).wait_send()

            @pl.when((z + k <= 3) & (z > 0))
            def _():
                for ch in chunks:
                    self.copy(2 * k + 1, z, ch, z).wait_send()


def attn_start(q):
    return pl.multiple_of(64 * q + 16 * (q // 2), 16)


def kernel_a(xT_ref, ln_ref, wattn_ref, w_ref, h_ref, qkv_ref, w1f_ref, w2_ref, ps1_ref, ps2_ref, ps3_ref,
             xg, lng, watt, zsend, zrecv, zq, s1, s2, wn, wt, hT_ref,
             xsend, xrecv, lsend, lrecv, asend, arecv, zsend_sem, zrecv_sem, qsend, qrecv, wsend, wrecv, lsem, osem):
    z, p, core, partner, xn, yn, diag, zs = coords()
    ph('a_bar')
    wload = pltpu.make_async_copy(w_ref, wn, lsem.at[0])
    wload.start()
    xg[z, p] = xT_ref[...]
    lng[z, p] = jnp.zeros((1, 128), F32)
    lng[z, p, 0:1, 0:64] = ln_ref[...]
    entry_barrier(z, p, zs)
    ph('a_zsend')
    sends = []
    nx = iter(range(40))
    nl = iter(range(40))

    def send(src_z, src_p, dev):
        c = rcopy(xg.at[src_z, src_p], xg.at[src_z, src_p], xsend.at[next(nx)], xrecv.at[src_z, src_p], dev)
        c.start()
        sends.append(c)

    def send_l(src_z, src_p, dev):
        c = rcopy(lng.at[src_z, src_p], lng.at[src_z, src_p], lsend.at[next(nl)], lrecv.at[src_z, src_p], dev)
        c.start()
        sends.append(c)

    def wait_x(src_z, src_p):
        rcopy(xg.at[src_z, src_p], xg.at[src_z, src_p], xsend.at[0], xrecv.at[src_z, src_p], (z, p)).wait_recv()

    def wait_l(src_z, src_p):
        rcopy(lng.at[src_z, src_p], lng.at[src_z, src_p], lsend.at[0], lrecv.at[src_z, src_p], (z, p)).wait_recv()

    def stat(src_z, src_p):
        blk = xg[src_z, src_p].astype(F32).reshape(8, 8, 512)
        s1[...] += jnp.sum(blk, axis=0)
        s2[...] += jnp.sum(blk * blk, axis=0)

    spans = ((0, C1A), (C1A, C1 - C1A))

    def w_piece(i, src, dst, k, dev):
        o, n = spans[i]
        return rcopy(
            wt.at[:, pl.ds(pl.multiple_of(dst * 256 + o, 16), n), :],
            w1f_ref.at[src, :, pl.ds(o, n), :],
            wsend.at[i, k], wrecv.at[i, src], dev)

    def send_w(i):
        for k in (3, 2, 1):
            c = w_piece(i, z, zs[k], k, (zs[k], p))
            c.start()
            sends.append(c)

    def turn(odd):
        def body(i, carry):
            lanes = pl.ds(pl.multiple_of(i * 256 + odd * 128, 128), 128)
            blk = wn[:, :, lanes].astype(F32)
            for g in range(2):
                wt[g, lanes, :] = blk[:, g, :].T.astype(BF16)
            return carry

        lax.fori_loop(0, NZ, body, 0)

    mid = 2 - z // 2
    far = 3 - 3 * (z // 2)
    zo = [z, zs[1], mid, far]
    inner = (z == 1) | (z == 2)
    send(z, p, (mid, p))
    send(z, p, (zs[1], p))
    for k in (3, 2, 1):
        send_l(z, p, (zs[k], p))
    for dev in (diag, xn, yn, partner):
        send(z, p, (z, dev))

    def outward(k):
        return rcopy(xg.at[zo[k], p], xg.at[zo[k], p], osem.at[k - 2], xrecv.at[zo[k], p], (zs[1], p))

    for j in range(1, NP):
        send_l(z, p, (z, (p + j) % NP))
    s1[...] = jnp.zeros_like(s1)
    s2[...] = jnp.zeros_like(s2)
    stat(z, p)
    watt[z] = wattn_ref[pl.ds(attn_start(z), 80), :]
    wload.wait()
    turn(0)

    def column(k):
        wait_x(zo[k], p)
        if k >= 2:
            @pl.when(inner)
            def _():
                outward(k).start()
        for dev in (diag, xn, yn, partner):
            send(zo[k], p, (z, dev))
        stat(zo[k], p)

    def pass_on(k, src):
        wait_x(zo[k], src)
        send(zo[k], src, (z, partner))
        stat(zo[k], src)

    ph('a_col1')
    column(1)
    column(2)
    ph('a_col3')
    column(3)
    ph('a_lnsend')
    for k in range(1, NZ):
        wait_l(zs[k], p)
        for j in range(1, NP):
            send_l(zs[k], p, (z, (p + j) % NP))
    ph('a_nbr')
    for k in range(2):
        pass_on(k, xn)
        pass_on(k, yn)
    ph('a_wattn')
    for k in (3, 2, 1):
        c = rcopy(wattn_ref.at[pl.ds(attn_start(zs[k]), 80), :], watt.at[z], asend.at[k], arecv.at[z], (zs[k], p))
        c.start()
        sends.append(c)
    send_w(0)
    ph('a_nbr2')
    pass_on(0, diag)
    pass_on(1, diag)
    ph('a_nbr3')
    for k in range(2, NZ):
        pass_on(k, xn)
        pass_on(k, yn)
        pass_on(k, diag)
    ph('a_rest')
    pd = [partner + xn - p, partner + yn - p, partner + diag - p]
    for q in [partner] + pd:
        for k in range(NZ):
            wait_x(zo[k], q)
            stat(zo[k], q)
    for k in range(NZ):
        for j in range(1, NP):
            wait_l(zs[k], (p + j) % NP)

    ph('a_norm')
    mean = jnp.sum(s1[...], axis=0, keepdims=True) / 2048.0
    var = jnp.sum(s2[...], axis=0, keepdims=True) / 2048.0 - mean * mean
    rstd = lax.rsqrt(var + LN_EPS)
    lnT = jnp.concatenate([lng[i // NP, i % NP, 0:1, :] for i in range(32)] + [jnp.zeros((96, 128), F32)], axis=0).T
    for i in range(NZ * NP):
        sc = lnT[0:64, i:i + 1]
        hT_ref[i * 64:(i + 1) * 64, :] = ((xg[i // NP, i % NP].astype(F32) - mean) * rstd * sc).astype(BF16)

    hout = pltpu.make_async_copy(hT_ref, h_ref, lsem.at[5])
    hout.start()
    ph('a_attw')
    for k in range(1, NZ):
        rcopy(watt.at[z], watt.at[zs[k]], asend.at[0], arecv.at[zs[k]], (z, p)).wait_recv()
    ph('a_zdot')
    part = None
    for q in range(NZ):
        t = jnp.dot(watt[q], hT_ref[q * 512:(q + 1) * 512, :], preferred_element_type=F32)
        part = t if part is None else part + t
    part = part.astype(BF16)
    for q in range(NZ):
        zsend[q] = part[:, q * 128:(q + 1) * 128]
    for k in (3, 2, 1):
        c = rcopy(zsend.at[zs[k]], zrecv.at[z], zsend_sem.at[k], zrecv_sem.at[z], (zs[k], p))
        c.start()
        sends.append(c)
    zrecv[z] = zsend[z]
    ph('a_turn')
    turn(1)
    send_w(1)
    outs = [pltpu.make_async_copy(wt, w2_ref, lsem.at[1])]
    for i, ps_ref in enumerate((ps1_ref, ps2_ref, ps3_ref)):
        dst = (z + i + 1) % NZ
        outs.append(pltpu.make_async_copy(wt.at[:, pl.ds(pl.multiple_of(dst * 256 + C1, 16), C2), :], ps_ref, lsem.at[2 + i]))
    for c in outs[1:] + outs[:1]:
        c.start()
    ph('a_zwait')
    for k in range(1, NZ):
        rcopy(zsend.at[0], zrecv.at[zs[k]], zsend_sem.at[0], zrecv_sem.at[zs[k]], (z, p)).wait_recv()
    ph('a_a2a')
    zt = jnp.concatenate([zrecv[0].astype(F32), zrecv[1].astype(F32)[16:80], zrecv[2].astype(F32), zrecv[3].astype(F32)[16:80]], axis=0)
    zq[...] = zt.T.astype(BF16).reshape(NP, 16, 288)
    for j in range(1, NP):
        q = (p + j) % NP
        c = rcopy(zq.at[q], qkv_ref.at[p], qsend.at[j], qrecv.at[p], (z, q))
        c.start()
        sends.append(c)
    qkv_ref[p] = zq[p]
    for j in range(1, NP):
        q = (p + j) % NP
        rcopy(zq.at[0], qkv_ref.at[q], qsend.at[0], qrecv.at[q], (z, p)).wait_recv()
    ph('a_wwait')
    for i in range(2):
        for k in range(1, NZ):
            w_piece(i, zs[k], z, 0, (z, p)).wait_recv()
    ph('a_sendwait')
    hout.wait()
    for c in outs:
        c.wait()
    for c in sends:
        c.wait_send()

    @pl.when(inner)
    def _():
        outward(2).wait_send()
        outward(3).wait_send()
    ph('')


def call_a(xT, ln, wattnT, w):
    vm = pl.BlockSpec(memory_space=pltpu.VMEM)
    hbm = pl.BlockSpec(memory_space=pl.ANY)
    return pl.pallas_call(
        kernel_a,
        out_shape=(
            jax.ShapeDtypeStruct((2048, 512), BF16),
            jax.ShapeDtypeStruct((NP, 16, 288), BF16),
            jax.ShapeDtypeStruct((NZ, 2, C1, 512), BF16),
            jax.ShapeDtypeStruct((2, 1024, 512), BF16),
        ) + (jax.ShapeDtypeStruct((2, C2, 512), BF16),) * 3,
        in_specs=[vm] * 3 + [hbm],
        out_specs=(hbm, vm) + (hbm,) * 5,
        scratch_shapes=[
            pltpu.VMEM((NZ, NP, 64, 512), BF16),
            pltpu.VMEM((NZ, NP, 1, 128), F32),
            pltpu.VMEM((NZ, 80, 512), BF16),
            pltpu.VMEM((NZ, 80, 128), BF16),
            pltpu.VMEM((NZ, 80, 128), BF16),
            pltpu.VMEM((NP, 16, 288), BF16),
            pltpu.VMEM((8, 512), F32),
            pltpu.VMEM((8, 512), F32),
            pltpu.VMEM((512, 2, 1024), BF16),
            pltpu.VMEM((2, 1024, 512), BF16),
            pltpu.VMEM((2048, 512), BF16),
            pltpu.SemaphoreType.DMA((40,)),
            pltpu.SemaphoreType.DMA((NZ, NP)),
            pltpu.SemaphoreType.DMA((40,)),
            pltpu.SemaphoreType.DMA((NZ, NP)),
            pltpu.SemaphoreType.DMA((NZ,)),
            pltpu.SemaphoreType.DMA((NZ,)),
            pltpu.SemaphoreType.DMA((NZ,)),
            pltpu.SemaphoreType.DMA((NZ,)),
            pltpu.SemaphoreType.DMA((NP,)),
            pltpu.SemaphoreType.DMA((NP,)),
            pltpu.SemaphoreType.DMA((2, NZ)),
            pltpu.SemaphoreType.DMA((2, NZ)),
            pltpu.SemaphoreType.DMA((6,)),
            pltpu.SemaphoreType.DMA((2,)),
        ],
        compiler_params=pltpu.CompilerParams(collective_id=0, has_side_effects=True, vmem_limit_bytes=56 * 1024 * 1024),
        name='gather_norm_qkv',
    )(xT, ln, wattnT, w)


def kernel_b(len_ref, q_ref, k_ref, v_ref, kc_ref, vc_ref, o_ref, kn_ref, vn_ref, kbuf, vbuf, oscr, isem, osem):
    rows = kbuf.shape[0]
    seq = kbuf.shape[1]

    def load(b, t):
        return pltpu.make_async_copy((kc_ref, vc_ref)[t].at[b], (kbuf, vbuf)[t].at[b], isem.at[b, t])

    def store(b, t):
        return pltpu.make_async_copy((kbuf, vbuf)[t].at[b], (kn_ref, vn_ref)[t].at[b], osem.at[b, t])

    for b in range(rows):
        load(b, 0).start()
        load(b, 1).start()

    def insert(buf, b, length, new):
        base = pl.multiple_of((length // 16) * 16, 16)
        hit = base + lax.broadcasted_iota(jnp.int32, (16, 128), 0) == length
        buf[b, pl.ds(base, 16), :] = jnp.where(hit, new.astype(F32), buf[b, pl.ds(base, 16), :].astype(F32)).astype(BF16)

    def attend(b, length, n):
        scores = lax.dot_general(q_ref[b], kbuf[b, 0:n, :], (((1,), (1,)), ((), ())), preferred_element_type=F32) * (128.0 ** -0.5)
        slot = lax.broadcasted_iota(jnp.int32, scores.shape, 1)
        scores = jnp.where(slot <= length, scores, -1e30)
        top = jnp.max(scores, axis=1, keepdims=True)
        e = jnp.exp(scores - top)
        probs = (e / jnp.sum(e, axis=1, keepdims=True)).astype(BF16)
        return jnp.dot(probs, vbuf[b, 0:n, :], preferred_element_type=F32)

    def pair(i, carry):
        b0 = 2 * i
        b1 = 2 * i + 1
        l0 = len_ref[b0]
        l1 = len_ref[b1]
        for b, length in ((b0, l0), (b1, l1)):
            load(b, 0).wait()
            load(b, 1).wait()
            insert(kbuf, b, length, k_ref[b])
            insert(vbuf, b, length, v_ref[b])
        last = jnp.maximum(l0, l1) // 512
        for t in range(seq // 512):
            @pl.when(last == t)
            def _():
                n = 512 * (t + 1)
                r0 = attend(b0, l0, n)
                r1 = attend(b1, l1, n)
                oscr[b0] = r0
                oscr[b1] = r1
        for b in (b0, b1):
            store(b, 0).start()
            store(b, 1).start()
        return carry

    lax.fori_loop(0, rows // 2, pair, 0)
    for h in range(16):
        o_ref[h // 2, :, (h % 2) * 128:(h % 2 + 1) * 128] = oscr[:, h, :].astype(BF16)
    for b in range(rows):
        store(b, 0).wait()
        store(b, 1).wait()


def call_b(lengths, q_rot, k_rot, v_tok, k_cache, v_cache):
    rows, seq, hd = k_cache.shape
    heads = q_rot.shape[1]
    vm = pl.BlockSpec(memory_space=pltpu.VMEM)
    hbm = pl.BlockSpec(memory_space=pl.ANY)
    return pl.pallas_call(
        kernel_b,
        in_specs=[pl.BlockSpec(memory_space=pltpu.SMEM), vm, vm, vm, hbm, hbm],
        out_specs=(vm, hbm, hbm),
        out_shape=(
            jax.ShapeDtypeStruct((NP, rows, heads * hd // NP), BF16),
            jax.ShapeDtypeStruct(k_cache.shape, BF16),
            jax.ShapeDtypeStruct(v_cache.shape, BF16),
        ),
        scratch_shapes=[
            pltpu.VMEM((rows, seq, hd), BF16),
            pltpu.VMEM((rows, seq, hd), BF16),
            pltpu.VMEM((rows, heads, hd), F32),
            pltpu.SemaphoreType.DMA((rows, 2)),
            pltpu.SemaphoreType.DMA((rows, 2)),
        ],
        compiler_params=pltpu.CompilerParams(vmem_limit_bytes=58 * 1024 * 1024),
        cost_estimate=pl.CostEstimate(flops=12_000_000_000, bytes_accessed=33_000_000, transcendentals=0),
        name='attend',
    )(lengths, q_rot, k_rot, v_tok, k_cache, v_cache)


def kernel_c(hT, w2_ref, w1f_ref, p1_ref, p2_ref, p3_ref, wd, wo, o_ref, xT_ref, y_ref,
             wvA, wvB, wdAT, wdBT, woT, og, hidA, hidB, ysum, r1, acc, r2,
             wsem, wbsend, wbrecv, osend, orecv, gsend, grecv, hasend, harecv, hbsend, hbrecv,
             r1send, r1recv, r2send, r2recv):
    z, p, core, partner, xn, yn, diag, zs = coords()
    ph('c_bar')
    local = [pltpu.make_async_copy(w2_ref.at[:, pl.ds(pl.multiple_of(z * 256, 256), CA), :], wvA.at[z], wsem.at[0])]
    for s, p_ref in ((1, p1_ref), (2, p2_ref), (3, p3_ref)):
        src = (z + NZ - s) % NZ
        local.append(pltpu.make_async_copy(w1f_ref.at[src], wvA.at[src, :, pl.ds(0, C1), :], wsem.at[2 * s]))
        local.append(pltpu.make_async_copy(p_ref, wvA.at[src, :, pl.ds(C1, C2), :], wsem.at[2 * s + 1]))
    late = [
        pltpu.make_async_copy(w2_ref.at[:, pl.ds(pl.multiple_of(z * 256 + CA, 16), C3), :], wvB.at[z], wsem.at[1]),
    ]
    for c in local + late:
        c.start()
    entry_barrier(z, p, zs)
    sends = []

    ph('c_send')
    def w_piece(src, dst, k, dev):
        return rcopy(w2_ref.at[:, pl.ds(pl.multiple_of(dst * 256 + CA, 16), C3), :], wvB.at[src], wbsend.at[k], wbrecv.at[src], dev)

    for k in (3, 2, 1):
        c = w_piece(z, zs[k], k, (zs[k], p))
        c.start()
        sends.append(c)
    for j in range(1, NP):
        q = (p + j) % NP
        c = rcopy(o_ref.at[q], og.at[z, p], osend.at[j], orecv.at[p], (z, q))
        c.start()
        sends.append(c)
    og[z, p] = o_ref[p]

    def gated(wv, n):
        g = None
        for q in range(NZ):
            t = jnp.dot(wv[q].reshape(2 * n, 512), hT[q * 512:(q + 1) * 512, :], preferred_element_type=F32)
            g = t if g is None else g + t
        gate = g[0:n].astype(BF16).astype(F32)
        up = g[n:2 * n].astype(BF16).astype(F32)
        return (jax.nn.silu(gate) * up).astype(BF16)

    ra = Relay(z, p, lambda src, ch: hidA.at[ch, src], hasend, harecv)
    rb = Relay(z, p, lambda src, ch: hidB.at[ch, src], hbsend, hbrecv)
    ro = Relay(z, p, lambda src, ch: og.at[src], gsend, grecv)
    every = range(CHUNKS)

    ph('c_localwait')
    for c in local:
        c.wait()
    ph('c_gA')
    ha = gated(wvA, CA)
    for ch in every:
        hidA[ch, z] = ha[:, ch * LANES:(ch + 1) * LANES]

    ra.own(range(2))
    ph('c_owait')
    for j in range(1, NP):
        q = (p + j) % NP
        rcopy(o_ref.at[0], og.at[z, q], osend.at[0], orecv.at[q], (z, p)).wait_recv()
    ro.own(range(1))
    ph('c_transp')
    for c in late:
        c.wait()
    wdAT[...] = jnp.concatenate([wd[q * 256:q * 256 + CA, :] for q in range(NZ)], axis=0).T
    wdBT[...] = jnp.concatenate([wd[q * 256 + CA:(q + 1) * 256, :] for q in range(NZ)], axis=0).T
    woT[...] = wo[...].T

    ph('c_wBwait')
    for k in range(1, NZ):
        w_piece(zs[k], z, 0, (z, p)).wait_recv()
    ph('c_gB')
    hb = gated(wvB, C3)
    for ch in range(CHUNKS):
        hidB[ch, z] = hb[:, ch * LANES:(ch + 1) * LANES]
    ph('c_own')
    rb.own(range(2))
    for ch in range(2, CHUNKS):
        ra.own((ch,))
        rb.own((ch,))
    ro.step(1, 0)

    chip = p // 2
    others = [xn // 2, yn // 2, diag // 2]

    def d2d(ch):
        return rcopy(ysum.at[ch, 1 - core], r1.at[ch], r1send.at[ch], r1recv.at[ch], (z, partner))

    def hop(ch, i, dev):
        return rcopy(acc.at[ch, i], r2.at[ch, i], r2send.at[ch, i], r2recv.at[ch, i], (z, dev))

    def stage1(ch):
        o_rows = og[ch * NZ // CHUNKS].reshape(128, 256)
        yt = jnp.dot(wdAT[...], hidA[ch].reshape(NZ * CA, LANES), preferred_element_type=F32)
        yt = yt + jnp.dot(wdBT[...], hidB[ch].reshape(NZ * C3, LANES), preferred_element_type=F32)
        yt = yt + lax.dot_general(woT[...], o_rows, (((1,), (1,)), ((), ())), preferred_element_type=F32)
        yt = yt.reshape(4, 2, 64, LANES)
        for i in range(4):
            for j in range(2):
                ysum[ch, j, i] = yt[i, j]
        d2d(ch).start()

    def stage2(ch):
        d2d(ch).wait_recv()
        for i, (t, dev) in enumerate(zip(others, (xn, yn, diag))):
            acc[ch, i] = ysum[ch, core, t] + r1[ch, t]
            hop(ch, i, dev).start()

    def stage3(ch):
        lanes = slice(ch * LANES, (ch + 1) * LANES)
        mine = ysum[ch, core, chip] + r1[ch, chip]
        for i, dev in enumerate((xn, yn, diag)):
            hop(ch, i, dev).wait_recv()
            mine = mine + r2[ch, i]
        y_ref[:, lanes] = (xT_ref[:, lanes].astype(F32) + mine).astype(BF16)

    for t in range(1, CHUNKS + 3):
        ph(f'c_wave{t}')
        for k in range(1, NZ):
            ch = t - k
            if 0 <= ch < CHUNKS:
                ra.step(k, ch)
                rb.step(k, ch)
        if t < 3:
            ro.step(t + 1, 0)
        ph(f'c_sum{t}')
        if t >= 3:
            stage1(t - 3)
        if t >= 4:
            stage2(t - 4)
    ph('c_last2')
    stage2(CHUNKS - 1)
    ph('c_last3')
    for ch in every:
        stage3(ch)

    ph('c_end')
    for c in sends:
        c.wait_send()
    for ch in range(CHUNKS):
        d2d(ch).wait_send()
        for i, dev in enumerate((xn, yn, diag)):
            hop(ch, i, dev).wait_send()
    ra.drain(every)
    rb.drain(every)
    ro.drain(range(1))
    ph('')


def call_c(hT, w2, w1f, ps, wd, wo, o8, xT):
    vm = pl.BlockSpec(memory_space=pltpu.VMEM)
    hbm = pl.BlockSpec(memory_space=pl.ANY)
    return pl.pallas_call(
        kernel_c,
        out_shape=jax.ShapeDtypeStruct((64, 512), BF16),
        in_specs=[vm] + [hbm] * 5 + [vm] * 4,
        out_specs=vm,
        scratch_shapes=[
            pltpu.VMEM((NZ, 2, CA, 512), BF16),
            pltpu.VMEM((NZ, 2, C3, 512), BF16),
            pltpu.VMEM((512, NZ * CA), BF16),
            pltpu.VMEM((512, NZ * C3), BF16),
            pltpu.VMEM((512, 256), BF16),
            pltpu.VMEM((NZ, NP, 16, 256), BF16),
            pltpu.VMEM((CHUNKS, NZ, CA, LANES), BF16),
            pltpu.VMEM((CHUNKS, NZ, C3, LANES), BF16),
            pltpu.VMEM((CHUNKS, 2, 4, 64, LANES), F32),
            pltpu.VMEM((CHUNKS, 4, 64, LANES), F32),
            pltpu.VMEM((CHUNKS, 3, 64, LANES), F32),
            pltpu.VMEM((CHUNKS, 3, 64, LANES), F32),
            pltpu.SemaphoreType.DMA((8,)),
            pltpu.SemaphoreType.DMA((NZ,)),
            pltpu.SemaphoreType.DMA((NZ,)),
            pltpu.SemaphoreType.DMA((NP,)),
            pltpu.SemaphoreType.DMA((NP,)),
            pltpu.SemaphoreType.DMA((8, 1)),
            pltpu.SemaphoreType.DMA((NZ, 1)),
            pltpu.SemaphoreType.DMA((8, CHUNKS)),
            pltpu.SemaphoreType.DMA((NZ, CHUNKS)),
            pltpu.SemaphoreType.DMA((8, CHUNKS)),
            pltpu.SemaphoreType.DMA((NZ, CHUNKS)),
            pltpu.SemaphoreType.DMA((CHUNKS,)),
            pltpu.SemaphoreType.DMA((CHUNKS,)),
            pltpu.SemaphoreType.DMA((CHUNKS, 3)),
            pltpu.SemaphoreType.DMA((CHUNKS, 3)),
        ],
        compiler_params=pltpu.CompilerParams(collective_id=1, has_side_effects=True, vmem_limit_bytes=40 * 1024 * 1024),
        cost_estimate=pl.CostEstimate(flops=12_000_000_000, bytes_accessed=6_000_000, transcendentals=0),
        name='mlp_out',
    )(hT, w2, w1f, *ps, wd, wo, o8, xT)


def solution(mesh):
    all_axes = ('x', 'yz')

    def local_step(x_in, ln_scale, w_gate_up, w_attn, w_down, w_out, k_cache, v_cache, lengths, positions):
        xT = x_in.T
        wattnT = w_attn.T
        hT, qkv, w1f, w2, *pieces = call_a(xT, ln_scale[None, :], wattnT, w_gate_up)
        ps = [lax.ppermute(pieces[i], 'x', [(q, (q + i + 1) % NZ) for q in range(NZ)]) for i in range(NZ - 1)]
        proj = jnp.transpose(qkv, (1, 0, 2)).reshape(16, 2304)
        q_raw = proj[:, :2048].reshape(16, 16, 128)
        k_tok = proj[:, 2048:2176]
        v_tok = proj[:, 2176:]
        q_rot = rotary(q_raw.astype(F32), positions).astype(BF16)
        k_rot = rotary(k_tok[:, None, :].astype(F32), positions).astype(BF16)
        o8, k_new, v_new = call_b(lengths, q_rot, k_rot, v_tok[:, None, :], k_cache, v_cache)
        yT = call_c(hT, w2, w1f, ps, w_down, w_out, o8, xT)
        return yT.T, k_new, v_new

    row_spec = P(None, all_axes)
    vec_spec = P(all_axes)
    cache_spec = P(all_axes, None, None)
    return jax.shard_map(
        local_step,
        mesh=mesh,
        in_specs=(row_spec, vec_spec, P('x', None, 'yz'), P('x', 'yz'), P('yz', 'x'), P('yz', 'x'), cache_spec, cache_spec, vec_spec, vec_spec),
        out_specs=(row_spec, cache_spec, cache_spec),
        check_vma=False,
    )
```

```python
import functools

import jax
import jax.numpy as jnp
from jax import lax
from jax.experimental import pallas as pl
from jax.experimental.pallas import tpu as pltpu
from jax.sharding import PartitionSpec as P

LN_EPS = 1e-6
ROPE_BASE = 10000.0
MESH = pl.DeviceIdType.MESH


class Phase:
    cm = None

    def __call__(self, name):
        if self.cm is not None:
            self.cm.__exit__(None, None, None)
            self.cm = None
        if name:
            self.cm = jax.named_scope(name)
            self.cm.__enter__()


ph = Phase()
F32 = jnp.float32
BF16 = jnp.bfloat16

NZ = 4
NP = 8
C1A = 16
C1 = 48
C2 = 128
C3 = 80
C3A = 48
CA = C1 + C2
CHUNKS = 4
LANES = 512 // CHUNKS


def rotary(values, positions):
    half_dim = values.shape[-1] // 2
    inv_freq = ROPE_BASE ** (-jnp.arange(half_dim, dtype=jnp.float32) / half_dim)
    angles = positions.astype(jnp.float32)[:, None, None] * inv_freq
    cos_part = jnp.cos(angles)
    sin_part = jnp.sin(angles)
    lo_half = values[..., :half_dim]
    hi_half = values[..., half_dim:]
    return jnp.concatenate([lo_half * cos_part - hi_half * sin_part, hi_half * cos_part + lo_half * sin_part], axis=-1)


def coords():
    z = lax.axis_index('x')
    p = lax.axis_index('yz')
    core = p % 2
    xx = (p // 2) % 2
    y = p // 4
    partner = p + 1 - 2 * core
    xn = p + 2 - 4 * xx
    yn = p + 4 - 8 * y
    diag = xn + 4 - 8 * y
    z1 = z % 2
    z2 = z // 2
    zs = [z, 2 * z2 + 1 - z1, 2 * (1 - z2) + z1, 3 - z]
    return z, p, core, partner, xn, yn, diag, zs


def entry_barrier(z, p, zs):
    sem = pltpu.get_barrier_semaphore()
    for k in range(1, NZ):
        pl.semaphore_signal(sem, inc=1, device_id=(zs[k], p), device_id_type=MESH)
    for k in range(1, NP):
        pl.semaphore_signal(sem, inc=1, device_id=(z, (p + k) % NP), device_id_type=MESH)
    pl.semaphore_wait(sem, NZ - 1 + NP - 1)


def rcopy(src, dst, send, recv, dev):
    return pltpu.make_async_remote_copy(src_ref=src, dst_ref=dst, send_sem=send, recv_sem=recv, device_id=dev, device_id_type=MESH)


class Relay:
    def __init__(self, z, p, at, send, recv):
        self.z, self.p, self.at, self.send, self.recv = z, p, at, send, recv

    def copy(self, way, src, ch, dev):
        ref = self.at(src, ch)
        return rcopy(ref, ref, self.send.at[way, ch], self.recv.at[src, ch], (dev, self.p))

    def own(self, chunks):
        z = self.z

        @pl.when(z < 3)
        def _():
            for ch in chunks:
                self.copy(0, z, ch, z + 1).start()

        @pl.when(z > 0)
        def _():
            for ch in chunks:
                self.copy(1, z, ch, z - 1).start()

    def step(self, k, ch):
        z = self.z

        @pl.when(z >= k)
        def _():
            self.copy(0, z - k, ch, z).wait_recv()

            @pl.when(z < 3)
            def _():
                self.copy(2 * k, z - k, ch, z + 1).start()

        @pl.when(z + k <= 3)
        def _():
            self.copy(0, z + k, ch, z).wait_recv()

            @pl.when(z > 0)
            def _():
                self.copy(2 * k + 1, z + k, ch, z - 1).start()

    def drain(self, chunks):
        z = self.z
        for k in range(NZ - 1):
            @pl.when((z >= k) & (z < 3))
            def _():
                for ch in chunks:
                    self.copy(2 * k, z, ch, z).wait_send()

            @pl.when((z + k <= 3) & (z > 0))
            def _():
                for ch in chunks:
                    self.copy(2 * k + 1, z, ch, z).wait_send()


def attn_start(q):
    return pl.multiple_of(64 * q + 16 * (q // 2), 16)


def kernel_a(xT_hbm, ln_hbm, wattn_hbm, w_ref, h_ref, qkv_ref, w1f_ref, w2_ref, ps1_ref, ps2_ref, ps3_ref,
             xg, lng, watt, zsend, zrecv, zq, s1, s2, wn, wt, hT_ref, ln_ref, wattn_ref,
             xsend, xrecv, lsend, lrecv, asend, arecv, zsend_sem, zrecv_sem, qsend, qrecv, wsend, wrecv, lsem, osem):
    z, p, core, partner, xn, yn, diag, zs = coords()
    ph('a_bar')
    wload = pltpu.make_async_copy(w_ref, wn, lsem.at[0])
    loads = [
        pltpu.make_async_copy(xT_hbm, xg.at[z, p], lsem.at[6]),
        pltpu.make_async_copy(ln_hbm, ln_ref, lsem.at[7]),
        pltpu.make_async_copy(wattn_hbm, wattn_ref, lsem.at[8]),
        wload,
    ]
    for c in loads:
        c.start()
    loads[1].wait()
    lng[z, p] = jnp.zeros((1, 128), F32)
    lng[z, p, 0:1, 0:64] = ln_ref[...]
    entry_barrier(z, p, zs)
    loads[0].wait()
    ph('a_zsend')
    sends = []
    nx = iter(range(40))
    nl = iter(range(40))

    def send(src_z, src_p, dev):
        c = rcopy(xg.at[src_z, src_p], xg.at[src_z, src_p], xsend.at[next(nx)], xrecv.at[src_z, src_p], dev)
        c.start()
        sends.append(c)

    def send_l(src_z, src_p, dev):
        c = rcopy(lng.at[src_z, src_p], lng.at[src_z, src_p], lsend.at[next(nl)], lrecv.at[src_z, src_p], dev)
        c.start()
        sends.append(c)

    def wait_x(src_z, src_p):
        rcopy(xg.at[src_z, src_p], xg.at[src_z, src_p], xsend.at[0], xrecv.at[src_z, src_p], (z, p)).wait_recv()

    def wait_l(src_z, src_p):
        rcopy(lng.at[src_z, src_p], lng.at[src_z, src_p], lsend.at[0], lrecv.at[src_z, src_p], (z, p)).wait_recv()

    def stat(src_z, src_p):
        blk = xg[src_z, src_p].astype(F32).reshape(8, 8, 512)
        s1[...] += jnp.sum(blk, axis=0)
        s2[...] += jnp.sum(blk * blk, axis=0)

    spans = ((0, C1A), (C1A, C1 - C1A))

    def w_piece(i, src, dst, k, dev):
        o, n = spans[i]
        return rcopy(
            wt.at[:, pl.ds(pl.multiple_of(dst * 256 + o, 16), n), :],
            w1f_ref.at[src, :, pl.ds(o, n), :],
            wsend.at[i, k], wrecv.at[i, src], dev)

    def send_w(i):
        for k in (3, 2, 1):
            c = w_piece(i, z, zs[k], k, (zs[k], p))
            c.start()
            sends.append(c)

    def turn(odd):
        def body(i, carry):
            lanes = pl.ds(pl.multiple_of(i * 256 + odd * 128, 128), 128)
            blk = wn[:, :, lanes].astype(F32)
            for g in range(2):
                wt[g, lanes, :] = blk[:, g, :].T.astype(BF16)
            return carry

        lax.fori_loop(0, NZ, body, 0)

    mid = 2 - z // 2
    far = 3 - 3 * (z // 2)
    zo = [z, zs[1], mid, far]
    inner = (z == 1) | (z == 2)
    send(z, p, (mid, p))
    send(z, p, (zs[1], p))
    for k in (3, 2, 1):
        send_l(z, p, (zs[k], p))
    for dev in (diag, xn, yn, partner):
        send(z, p, (z, dev))

    def outward(k):
        return rcopy(xg.at[zo[k], p], xg.at[zo[k], p], osem.at[k - 2], xrecv.at[zo[k], p], (zs[1], p))

    for j in range(1, NP):
        send_l(z, p, (z, (p + j) % NP))
    s1[...] = jnp.zeros_like(s1)
    s2[...] = jnp.zeros_like(s2)
    stat(z, p)
    loads[2].wait()
    watt[z] = wattn_ref[pl.ds(attn_start(z), 80), :]
    wload.wait()
    turn(0)

    def column(k):
        wait_x(zo[k], p)
        if k >= 2:
            @pl.when(inner)
            def _():
                outward(k).start()
        for dev in (diag, xn, yn, partner):
            send(zo[k], p, (z, dev))
        stat(zo[k], p)

    def pass_on(k, src):
        wait_x(zo[k], src)
        send(zo[k], src, (z, partner))
        stat(zo[k], src)

    ph('a_col1')
    column(1)
    column(2)
    ph('a_col3')
    column(3)
    ph('a_lnsend')
    for k in range(1, NZ):
        wait_l(zs[k], p)
        for j in range(1, NP):
            send_l(zs[k], p, (z, (p + j) % NP))
    ph('a_nbr')
    for k in range(2):
        pass_on(k, xn)
        pass_on(k, yn)
    ph('a_wattn')
    for k in (3, 2, 1):
        c = rcopy(wattn_ref.at[pl.ds(attn_start(zs[k]), 80), :], watt.at[z], asend.at[k], arecv.at[z], (zs[k], p))
        c.start()
        sends.append(c)
    ph('a_nbr2')
    pass_on(0, diag)
    pass_on(1, diag)
    ph('a_nbr3')
    for k in range(2, NZ):
        pass_on(k, xn)
        pass_on(k, yn)
        pass_on(k, diag)
    send_w(0)
    ph('a_rest')
    pd = [partner + xn - p, partner + yn - p, partner + diag - p]
    for q in [partner] + pd:
        for k in range(NZ):
            wait_x(zo[k], q)
            stat(zo[k], q)
    for k in range(NZ):
        for j in range(1, NP):
            wait_l(zs[k], (p + j) % NP)

    ph('a_norm')
    mean = jnp.sum(s1[...], axis=0, keepdims=True) / 2048.0
    var = jnp.sum(s2[...], axis=0, keepdims=True) / 2048.0 - mean * mean
    rstd = lax.rsqrt(var + LN_EPS)
    lnT = jnp.concatenate([lng[i // NP, i % NP, 0:1, :] for i in range(32)] + [jnp.zeros((96, 128), F32)], axis=0).T
    for i in range(NZ * NP):
        sc = lnT[0:64, i:i + 1]
        hT_ref[i * 64:(i + 1) * 64, :] = ((xg[i // NP, i % NP].astype(F32) - mean) * rstd * sc).astype(BF16)

    hout = pltpu.make_async_copy(hT_ref, h_ref, lsem.at[5])
    hout.start()
    ph('a_attw')
    for k in range(1, NZ):
        rcopy(watt.at[z], watt.at[zs[k]], asend.at[0], arecv.at[zs[k]], (z, p)).wait_recv()
    ph('a_zdot')
    part = None
    for q in range(NZ):
        t = jnp.dot(watt[q], hT_ref[q * 512:(q + 1) * 512, :], preferred_element_type=F32)
        part = t if part is None else part + t
    part = part.astype(BF16)
    for q in range(NZ):
        zsend[q] = part[:, q * 128:(q + 1) * 128]
    for k in (3, 2, 1):
        c = rcopy(zsend.at[zs[k]], zrecv.at[z], zsend_sem.at[k], zrecv_sem.at[z], (zs[k], p))
        c.start()
        sends.append(c)
    zrecv[z] = zsend[z]
    ph('a_turn')
    turn(1)
    send_w(1)
    outs = [pltpu.make_async_copy(wt, w2_ref, lsem.at[1])]
    for i, ps_ref in enumerate((ps1_ref, ps2_ref, ps3_ref)):
        dst = (z + i + 1) % NZ
        outs.append(pltpu.make_async_copy(wt.at[:, pl.ds(pl.multiple_of(dst * 256 + C1, 16), C2), :], ps_ref, lsem.at[2 + i]))
    for c in outs[1:] + outs[:1]:
        c.start()
    ph('a_zwait')
    for k in range(1, NZ):
        rcopy(zsend.at[0], zrecv.at[zs[k]], zsend_sem.at[0], zrecv_sem.at[zs[k]], (z, p)).wait_recv()
    ph('a_a2a')
    zt = jnp.concatenate([zrecv[0].astype(F32), zrecv[1].astype(F32)[16:80], zrecv[2].astype(F32), zrecv[3].astype(F32)[16:80]], axis=0)
    zq[...] = zt.T.astype(BF16).reshape(NP, 16, 288)
    for j in range(1, NP):
        q = (p + j) % NP
        c = rcopy(zq.at[q], qkv_ref.at[p], qsend.at[j], qrecv.at[p], (z, q))
        c.start()
        sends.append(c)
    qown = pltpu.make_async_copy(zq.at[p], qkv_ref.at[p], lsem.at[9])
    qown.start()
    for j in range(1, NP):
        q = (p + j) % NP
        rcopy(zq.at[0], qkv_ref.at[q], qsend.at[0], qrecv.at[q], (z, p)).wait_recv()
    ph('a_wwait')
    for i in range(2):
        for k in range(1, NZ):
            w_piece(i, zs[k], z, 0, (z, p)).wait_recv()
    ph('a_sendwait')
    hout.wait()
    qown.wait()
    for c in outs:
        c.wait()
    for c in sends:
        c.wait_send()

    @pl.when(inner)
    def _():
        outward(2).wait_send()
        outward(3).wait_send()
    ph('')


def call_a(xT, ln, wattnT, w):
    hbm = pl.BlockSpec(memory_space=pl.ANY)
    return pl.pallas_call(
        kernel_a,
        out_shape=(
            jax.ShapeDtypeStruct((2048, 512), BF16),
            jax.ShapeDtypeStruct((NP, 16, 288), BF16),
            jax.ShapeDtypeStruct((NZ, 2, C1, 512), BF16),
            jax.ShapeDtypeStruct((2, 1024, 512), BF16),
        ) + (jax.ShapeDtypeStruct((2, C2, 512), BF16),) * 3,
        in_specs=[hbm] * 4,
        out_specs=(hbm,) * 7,
        scratch_shapes=[
            pltpu.VMEM((NZ, NP, 64, 512), BF16),
            pltpu.VMEM((NZ, NP, 1, 128), F32),
            pltpu.VMEM((NZ, 80, 512), BF16),
            pltpu.VMEM((NZ, 80, 128), BF16),
            pltpu.VMEM((NZ, 80, 128), BF16),
            pltpu.VMEM((NP, 16, 288), BF16),
            pltpu.VMEM((8, 512), F32),
            pltpu.VMEM((8, 512), F32),
            pltpu.VMEM((512, 2, 1024), BF16),
            pltpu.VMEM((2, 1024, 512), BF16),
            pltpu.VMEM((2048, 512), BF16),
            pltpu.VMEM((1, 64), F32),
            pltpu.VMEM((288, 512), BF16),
            pltpu.SemaphoreType.DMA((40,)),
            pltpu.SemaphoreType.DMA((NZ, NP)),
            pltpu.SemaphoreType.DMA((40,)),
            pltpu.SemaphoreType.DMA((NZ, NP)),
            pltpu.SemaphoreType.DMA((NZ,)),
            pltpu.SemaphoreType.DMA((NZ,)),
            pltpu.SemaphoreType.DMA((NZ,)),
            pltpu.SemaphoreType.DMA((NZ,)),
            pltpu.SemaphoreType.DMA((NP,)),
            pltpu.SemaphoreType.DMA((NP,)),
            pltpu.SemaphoreType.DMA((2, NZ)),
            pltpu.SemaphoreType.DMA((2, NZ)),
            pltpu.SemaphoreType.DMA((10,)),
            pltpu.SemaphoreType.DMA((2,)),
        ],
        compiler_params=pltpu.CompilerParams(collective_id=0, has_side_effects=True, vmem_limit_bytes=56 * 1024 * 1024),
        name='gather_norm_qkv',
    )(xT, ln, wattnT, w)


def kernel_b(len_ref, q_ref, k_ref, v_ref, kc_ref, vc_ref, o_ref, kn_ref, vn_ref, kbuf, vbuf, oscr, isem, osem):
    rows = kbuf.shape[0]
    seq = kbuf.shape[1]

    def load(b, t):
        return pltpu.make_async_copy((kc_ref, vc_ref)[t].at[b], (kbuf, vbuf)[t].at[b], isem.at[b, t])

    def store(b, t):
        return pltpu.make_async_copy((kbuf, vbuf)[t].at[b], (kn_ref, vn_ref)[t].at[b], osem.at[b, t])

    for b in range(rows):
        load(b, 0).start()
        load(b, 1).start()

    def insert(buf, b, length, new):
        base = pl.multiple_of((length // 16) * 16, 16)
        hit = base + lax.broadcasted_iota(jnp.int32, (16, 128), 0) == length
        buf[b, pl.ds(base, 16), :] = jnp.where(hit, new.astype(F32), buf[b, pl.ds(base, 16), :].astype(F32)).astype(BF16)

    def attend(b, length, n):
        scores = lax.dot_general(q_ref[b], kbuf[b, 0:n, :], (((1,), (1,)), ((), ())), preferred_element_type=F32) * (128.0 ** -0.5)
        slot = lax.broadcasted_iota(jnp.int32, scores.shape, 1)
        scores = jnp.where(slot <= length, scores, -1e30)
        top = jnp.max(scores, axis=1, keepdims=True)
        e = jnp.exp(scores - top)
        probs = (e / jnp.sum(e, axis=1, keepdims=True)).astype(BF16)
        return jnp.dot(probs, vbuf[b, 0:n, :], preferred_element_type=F32)

    def pair(i, carry):
        b0 = 2 * i
        b1 = 2 * i + 1
        l0 = len_ref[b0]
        l1 = len_ref[b1]
        for b, length in ((b0, l0), (b1, l1)):
            load(b, 0).wait()
            load(b, 1).wait()
            insert(kbuf, b, length, k_ref[b])
            insert(vbuf, b, length, v_ref[b])
        last = jnp.maximum(l0, l1) // 512
        for t in range(seq // 512):
            @pl.when(last == t)
            def _():
                n = 512 * (t + 1)
                r0 = attend(b0, l0, n)
                r1 = attend(b1, l1, n)
                oscr[b0] = r0
                oscr[b1] = r1
        for b in (b0, b1):
            store(b, 0).start()
            store(b, 1).start()
        return carry

    lax.fori_loop(0, rows // 2, pair, 0)
    for h in range(16):
        o_ref[h // 2, :, (h % 2) * 128:(h % 2 + 1) * 128] = oscr[:, h, :].astype(BF16)
    for b in range(rows):
        store(b, 0).wait()
        store(b, 1).wait()


def call_b(lengths, q_rot, k_rot, v_tok, k_cache, v_cache):
    rows, seq, hd = k_cache.shape
    heads = q_rot.shape[1]
    vm = pl.BlockSpec(memory_space=pltpu.VMEM)
    hbm = pl.BlockSpec(memory_space=pl.ANY)
    return pl.pallas_call(
        kernel_b,
        in_specs=[pl.BlockSpec(memory_space=pltpu.SMEM), vm, vm, vm, hbm, hbm],
        out_specs=(vm, hbm, hbm),
        out_shape=(
            jax.ShapeDtypeStruct((NP, rows, heads * hd // NP), BF16),
            jax.ShapeDtypeStruct(k_cache.shape, BF16),
            jax.ShapeDtypeStruct(v_cache.shape, BF16),
        ),
        scratch_shapes=[
            pltpu.VMEM((rows, seq, hd), BF16),
            pltpu.VMEM((rows, seq, hd), BF16),
            pltpu.VMEM((rows, heads, hd), F32),
            pltpu.SemaphoreType.DMA((rows, 2)),
            pltpu.SemaphoreType.DMA((rows, 2)),
        ],
        compiler_params=pltpu.CompilerParams(vmem_limit_bytes=58 * 1024 * 1024),
        cost_estimate=pl.CostEstimate(flops=12_000_000_000, bytes_accessed=33_000_000, transcendentals=0),
        name='attend',
    )(lengths, q_rot, k_rot, v_tok, k_cache, v_cache)


def kernel_c(hT, w2_ref, w1f_ref, p1_ref, p2_ref, p3_ref, wd, wo, o_ref, xT_ref, y_ref,
             wvA, wvB, wdAT, wdBT, woT, og, hidA, hidB, ysum, r1, acc, r2,
             wsem, wbsend, wbrecv, osend, orecv, gsend, grecv, hasend, harecv, hbsend, hbrecv,
             r1send, r1recv, r2send, r2recv):
    z, p, core, partner, xn, yn, diag, zs = coords()
    ph('c_bar')
    local = [pltpu.make_async_copy(w2_ref.at[:, pl.ds(pl.multiple_of(z * 256, 256), CA), :], wvA.at[z], wsem.at[0])]
    for s, p_ref in ((1, p1_ref), (2, p2_ref), (3, p3_ref)):
        src = (z + NZ - s) % NZ
        local.append(pltpu.make_async_copy(w1f_ref.at[src], wvA.at[src, :, pl.ds(0, C1), :], wsem.at[2 * s]))
        local.append(pltpu.make_async_copy(p_ref, wvA.at[src, :, pl.ds(C1, C2), :], wsem.at[2 * s + 1]))
    late = [
        pltpu.make_async_copy(w2_ref.at[:, pl.ds(pl.multiple_of(z * 256 + CA, 16), C3), :], wvB.at[z], wsem.at[1]),
    ]
    for c in local + late:
        c.start()
    entry_barrier(z, p, zs)
    sends = []

    ph('c_send')
    spans = ((0, C3A), (C3A, C3 - C3A))

    def w_piece(i, src, dst, k, dev):
        o, n = spans[i]
        return rcopy(
            w2_ref.at[:, pl.ds(pl.multiple_of(dst * 256 + CA + o, 16), n), :],
            wvB.at[src, :, pl.ds(o, n), :], wbsend.at[i, k], wbrecv.at[i, src], dev)

    def send_w(i):
        for k in (3, 2, 1):
            c = w_piece(i, z, zs[k], k, (zs[k], p))
            c.start()
            sends.append(c)

    send_w(0)
    for j in range(1, NP):
        q = (p + j) % NP
        c = rcopy(o_ref.at[q], og.at[z, p], osend.at[j], orecv.at[p], (z, q))
        c.start()
        sends.append(c)
    og[z, p] = o_ref[p]

    def gated(wv, n):
        g = None
        for q in range(NZ):
            t = jnp.dot(wv[q].reshape(2 * n, 512), hT[q * 512:(q + 1) * 512, :], preferred_element_type=F32)
            g = t if g is None else g + t
        gate = g[0:n].astype(BF16).astype(F32)
        up = g[n:2 * n].astype(BF16).astype(F32)
        return (jax.nn.silu(gate) * up).astype(BF16)

    ra = Relay(z, p, lambda src, ch: hidA.at[ch, src], hasend, harecv)
    rb = Relay(z, p, lambda src, ch: hidB.at[ch, src], hbsend, hbrecv)
    ro = Relay(z, p, lambda src, ch: og.at[src], gsend, grecv)
    every = range(CHUNKS)

    ph('c_localwait')
    for c in local:
        c.wait()
    ph('c_gA')
    ha = gated(wvA, CA)
    for ch in every:
        hidA[ch, z] = ha[:, ch * LANES:(ch + 1) * LANES]

    ra.own(range(2))
    send_w(1)
    ph('c_owait')
    for j in range(1, NP):
        q = (p + j) % NP
        rcopy(o_ref.at[0], og.at[z, q], osend.at[0], orecv.at[q], (z, p)).wait_recv()
    ro.own(range(1))
    ph('c_transp')
    for c in late:
        c.wait()
    wdAT[...] = jnp.concatenate([wd[q * 256:q * 256 + CA, :] for q in range(NZ)], axis=0).T
    wdBT[...] = jnp.concatenate([wd[q * 256 + CA:(q + 1) * 256, :] for q in range(NZ)], axis=0).T
    woT[...] = wo[...].T

    ph('c_wBwait')
    for ch in range(2):
        ra.step(1, ch)
    ro.step(1, 0)
    for ch in range(2):
        ra.step(2, ch)
    ph('c_wBwait2')
    for i in range(2):
        for k in range(1, NZ):
            w_piece(i, zs[k], z, 0, (z, p)).wait_recv()
    ph('c_gB')
    hb = gated(wvB, C3)
    for ch in range(CHUNKS):
        hidB[ch, z] = hb[:, ch * LANES:(ch + 1) * LANES]
    ph('c_own')
    rb.own(range(2))
    for ch in range(2, CHUNKS):
        ra.own((ch,))
        rb.own((ch,))

    chip = p // 2
    others = [diag // 2, xn // 2, yn // 2]

    def d2d(ch):
        return rcopy(ysum.at[ch, 1 - core], r1.at[ch], r1send.at[ch], r1recv.at[ch], (z, partner))

    def hop(ch, i, dev):
        return rcopy(acc.at[ch, i], r2.at[ch, i], r2send.at[ch, i], r2recv.at[ch, i], (z, dev))

    def stage1(ch):
        o_rows = og[ch * NZ // CHUNKS].reshape(128, 256)
        yt = jnp.dot(wdAT[...], hidA[ch].reshape(NZ * CA, LANES), preferred_element_type=F32)
        yt = yt + jnp.dot(wdBT[...], hidB[ch].reshape(NZ * C3, LANES), preferred_element_type=F32)
        yt = yt + lax.dot_general(woT[...], o_rows, (((1,), (1,)), ((), ())), preferred_element_type=F32)
        yt = yt.reshape(4, 2, 64, LANES)
        for i in range(4):
            for j in range(2):
                ysum[ch, j, i] = yt[i, j]
        d2d(ch).start()

    def stage2(ch):
        d2d(ch).wait_recv()
        for i, (t, dev) in enumerate(zip(others, (diag, xn, yn))):
            acc[ch, i] = ysum[ch, core, t] + r1[ch, t]
            hop(ch, i, dev).start()

    def stage3(ch):
        lanes = slice(ch * LANES, (ch + 1) * LANES)
        mine = ysum[ch, core, chip] + r1[ch, chip]
        for i, dev in enumerate((diag, xn, yn)):
            hop(ch, i, dev).wait_recv()
            mine = mine + r2[ch, i]
        y_ref[:, lanes] = (xT_ref[:, lanes].astype(F32) + mine).astype(BF16)

    for t in range(1, CHUNKS + 3):
        ph(f'c_wave{t}')
        for k in range(1, NZ):
            ch = t - k
            if 0 <= ch < CHUNKS:
                if k == 3 or ch >= 2:
                    ra.step(k, ch)
                rb.step(k, ch)
        if t < 3:
            ro.step(t + 1, 0)
        ph(f'c_sum{t}')
        if t >= 3:
            stage1(t - 3)
        if t >= 4:
            stage2(t - 4)
    ph('c_last2')
    stage2(CHUNKS - 1)
    ph('c_last3')
    for ch in every:
        stage3(ch)

    ph('c_end')
    for c in sends:
        c.wait_send()
    for ch in range(CHUNKS):
        d2d(ch).wait_send()
        for i, dev in enumerate((diag, xn, yn)):
            hop(ch, i, dev).wait_send()
    ra.drain(every)
    rb.drain(every)
    ro.drain(range(1))
    ph('')


def call_c(hT, w2, w1f, ps, wd, wo, o8, xT):
    vm = pl.BlockSpec(memory_space=pltpu.VMEM)
    hbm = pl.BlockSpec(memory_space=pl.ANY)
    return pl.pallas_call(
        kernel_c,
        out_shape=jax.ShapeDtypeStruct((64, 512), BF16),
        in_specs=[vm] + [hbm] * 5 + [vm] * 4,
        out_specs=vm,
        scratch_shapes=[
            pltpu.VMEM((NZ, 2, CA, 512), BF16),
            pltpu.VMEM((NZ, 2, C3, 512), BF16),
            pltpu.VMEM((512, NZ * CA), BF16),
            pltpu.VMEM((512, NZ * C3), BF16),
            pltpu.VMEM((512, 256), BF16),
            pltpu.VMEM((NZ, NP, 16, 256), BF16),
            pltpu.VMEM((CHUNKS, NZ, CA, LANES), BF16),
            pltpu.VMEM((CHUNKS, NZ, C3, LANES), BF16),
            pltpu.VMEM((CHUNKS, 2, 4, 64, LANES), F32),
            pltpu.VMEM((CHUNKS, 4, 64, LANES), F32),
            pltpu.VMEM((CHUNKS, 3, 64, LANES), F32),
            pltpu.VMEM((CHUNKS, 3, 64, LANES), F32),
            pltpu.SemaphoreType.DMA((8,)),
            pltpu.SemaphoreType.DMA((2, NZ)),
            pltpu.SemaphoreType.DMA((2, NZ)),
            pltpu.SemaphoreType.DMA((NP,)),
            pltpu.SemaphoreType.DMA((NP,)),
            pltpu.SemaphoreType.DMA((8, 1)),
            pltpu.SemaphoreType.DMA((NZ, 1)),
            pltpu.SemaphoreType.DMA((8, CHUNKS)),
            pltpu.SemaphoreType.DMA((NZ, CHUNKS)),
            pltpu.SemaphoreType.DMA((8, CHUNKS)),
            pltpu.SemaphoreType.DMA((NZ, CHUNKS)),
            pltpu.SemaphoreType.DMA((CHUNKS,)),
            pltpu.SemaphoreType.DMA((CHUNKS,)),
            pltpu.SemaphoreType.DMA((CHUNKS, 3)),
            pltpu.SemaphoreType.DMA((CHUNKS, 3)),
        ],
        compiler_params=pltpu.CompilerParams(collective_id=1, has_side_effects=True, vmem_limit_bytes=40 * 1024 * 1024),
        cost_estimate=pl.CostEstimate(flops=12_000_000_000, bytes_accessed=6_000_000, transcendentals=0),
        name='mlp_out',
    )(hT, w2, w1f, *ps, wd, wo, o8, xT)


def solution(mesh):
    all_axes = ('x', 'yz')

    def local_step(x_in, ln_scale, w_gate_up, w_attn, w_down, w_out, k_cache, v_cache, lengths, positions):
        xT = x_in.T
        wattnT = w_attn.T
        hT, qkv, w1f, w2, *pieces = call_a(xT, ln_scale[None, :], wattnT, w_gate_up)
        ps = [lax.ppermute(pieces[i], 'x', [(q, (q + i + 1) % NZ) for q in range(NZ)]) for i in range(NZ - 1)]
        proj = jnp.transpose(qkv, (1, 0, 2)).reshape(16, 2304)
        q_raw = proj[:, :2048].reshape(16, 16, 128)
        k_tok = proj[:, 2048:2176]
        v_tok = proj[:, 2176:]
        q_rot = rotary(q_raw.astype(F32), positions).astype(BF16)
        k_rot = rotary(k_tok[:, None, :].astype(F32), positions).astype(BF16)
        o8, k_new, v_new = call_b(lengths, q_rot, k_rot, v_tok[:, None, :], k_cache, v_cache)
        yT = call_c(hT, w2, w1f, ps, w_down, w_out, o8, xT)
        return yT.T, k_new, v_new

    row_spec = P(None, all_axes)
    vec_spec = P(all_axes)
    cache_spec = P(all_axes, None, None)
    return jax.shard_map(
        local_step,
        mesh=mesh,
        in_specs=(row_spec, vec_spec, P('x', None, 'yz'), P('x', 'yz'), P('yz', 'x'), P('yz', 'x'), cache_spec, cache_spec, vec_spec, vec_spec),
        out_specs=(row_spec, cache_spec, cache_spec),
        check_vma=False,
    )
```

```python
import functools

import jax
import jax.numpy as jnp
from jax import lax
from jax.experimental import pallas as pl
from jax.experimental.pallas import tpu as pltpu
from jax.sharding import PartitionSpec as P

LN_EPS = 1e-6
ROPE_BASE = 10000.0
MESH = pl.DeviceIdType.MESH


class Phase:
    cm = None

    def __call__(self, name):
        if self.cm is not None:
            self.cm.__exit__(None, None, None)
            self.cm = None
        if name:
            self.cm = jax.named_scope(name)
            self.cm.__enter__()


ph = Phase()
F32 = jnp.float32
BF16 = jnp.bfloat16

NZ = 4
NP = 8
C1A = 16
C1 = 48
C2 = 128
C3 = 80
C3A = 48
CA = C1 + C2
CHUNKS = 4
LANES = 512 // CHUNKS


def rotary(values, positions):
    half_dim = values.shape[-1] // 2
    inv_freq = ROPE_BASE ** (-jnp.arange(half_dim, dtype=jnp.float32) / half_dim)
    angles = positions.astype(jnp.float32)[:, None, None] * inv_freq
    cos_part = jnp.cos(angles)
    sin_part = jnp.sin(angles)
    lo_half = values[..., :half_dim]
    hi_half = values[..., half_dim:]
    return jnp.concatenate([lo_half * cos_part - hi_half * sin_part, hi_half * cos_part + lo_half * sin_part], axis=-1)


def coords():
    z = lax.axis_index('x')
    p = lax.axis_index('yz')
    core = p % 2
    xx = (p // 2) % 2
    y = p // 4
    partner = p + 1 - 2 * core
    xn = p + 2 - 4 * xx
    yn = p + 4 - 8 * y
    diag = xn + 4 - 8 * y
    z1 = z % 2
    z2 = z // 2
    zs = [z, 2 * z2 + 1 - z1, 2 * (1 - z2) + z1, 3 - z]
    return z, p, core, partner, xn, yn, diag, zs


def entry_barrier(z, p, zs):
    sem = pltpu.get_barrier_semaphore()
    for k in range(1, NZ):
        pl.semaphore_signal(sem, inc=1, device_id=(zs[k], p), device_id_type=MESH)
    for k in range(1, NP):
        pl.semaphore_signal(sem, inc=1, device_id=(z, (p + k) % NP), device_id_type=MESH)
    pl.semaphore_wait(sem, NZ - 1 + NP - 1)


def rcopy(src, dst, send, recv, dev):
    return pltpu.make_async_remote_copy(src_ref=src, dst_ref=dst, send_sem=send, recv_sem=recv, device_id=dev, device_id_type=MESH)


class Relay:
    def __init__(self, z, p, at, whole, send, recv):
        self.z, self.p, self.at, self.whole, self.send, self.recv = z, p, at, whole, send, recv

    def copy(self, way, src, ch, dev):
        ref = self.at(src, ch)
        return rcopy(ref, ref, self.send.at[way], self.recv.at[src, ch], (dev, self.p))

    def own(self, chunks):
        z = self.z

        @pl.when(z < 3)
        def _():
            for ch in chunks:
                self.copy(0, z, ch, z + 1).start()

        @pl.when(z > 0)
        def _():
            for ch in chunks:
                self.copy(1, z, ch, z - 1).start()

    def step(self, k, ch):
        z = self.z

        @pl.when(z >= k)
        def _():
            self.copy(0, z - k, ch, z).wait_recv()

            @pl.when(z < 3)
            def _():
                self.copy(2 * k, z - k, ch, z + 1).start()

        @pl.when(z + k <= 3)
        def _():
            self.copy(0, z + k, ch, z).wait_recv()

            @pl.when(z > 0)
            def _():
                self.copy(2 * k + 1, z + k, ch, z - 1).start()

    def sent(self, way):
        rcopy(self.whole, self.whole, self.send.at[way], self.recv.at[0, 0], (self.z, self.p)).wait_send()

    def drain(self):
        z = self.z
        for k in range(NZ - 1):
            @pl.when((z >= k) & (z < 3))
            def _():
                self.sent(2 * k)

            @pl.when((z + k <= 3) & (z > 0))
            def _():
                self.sent(2 * k + 1)


def attn_start(q):
    return pl.multiple_of(64 * q + 16 * (q // 2), 16)


def kernel_a(xT_hbm, ln_hbm, wattn_hbm, w_ref, h_ref, qkv_ref, w1f_ref, w2_ref, ps1_ref, ps2_ref, ps3_ref,
             xg, lng, watt, zsend, zrecv, zq, s1, s2, wn, wt, hT_ref, ln_ref, wattn_ref,
             xsend, xrecv, rpart, lsend, lrecv, asend, arecv, zsend_sem, zrecv_sem, qsend, qrecv, wsend, wrecv, lsem, osem, ldummy):
    z, p, core, partner, xn, yn, diag, zs = coords()
    ph('a_bar')
    wload = pltpu.make_async_copy(w_ref, wn, lsem.at[0])
    loads = [
        pltpu.make_async_copy(xT_hbm, xg.at[z, p], lsem.at[6]),
        pltpu.make_async_copy(ln_hbm, ln_ref, lsem.at[7]),
        pltpu.make_async_copy(wattn_hbm, wattn_ref, lsem.at[8]),
        wload,
    ]
    for c in loads:
        c.start()
    loads[1].wait()
    lng[z, p] = jnp.zeros((1, 128), F32)
    lng[z, p, 0:1, 0:64] = ln_ref[...]
    entry_barrier(z, p, zs)
    loads[0].wait()
    ph('a_zsend')
    here = (z, p)

    def send(src_z, src_p, dev, way=0):
        recv = rpart.at[0] if way == 4 else xrecv.at[way, src_z]
        rcopy(xg.at[src_z, src_p], xg.at[src_z, src_p], xsend.at[0], recv, dev).start()

    def send_l(src_z, dev, phase):
        rcopy(lng.at[src_z, p], lng.at[src_z, p], lsend.at[0], lrecv.at[phase], dev).start()

    def wait_x(src_z, src_p, way):
        rcopy(xg.at[src_z, src_p], xg.at[src_z, src_p], xsend.at[0], xrecv.at[way, src_z], here).wait_recv()

    def stat(src_z, src_p):
        blk = xg[src_z, src_p].astype(F32).reshape(8, 8, 512)
        s1[...] += jnp.sum(blk, axis=0)
        s2[...] += jnp.sum(blk * blk, axis=0)

    spans = ((0, C1A), (C1A, C1 - C1A))

    def w_piece(i, src, dst, dev):
        o, n = spans[i]
        return rcopy(
            wt.at[:, pl.ds(pl.multiple_of(dst * 256 + o, 16), n), :],
            w1f_ref.at[src, :, pl.ds(o, n), :],
            wsend.at[0], wrecv.at[0], dev)

    def send_w(i):
        for k in (3, 2, 1):
            w_piece(i, z, zs[k], (zs[k], p)).start()

    def turn(odd):
        def body(i, carry):
            lanes = pl.ds(pl.multiple_of(i * 256 + odd * 128, 128), 128)
            blk = wn[:, :, lanes].astype(F32)
            for g in range(2):
                wt[g, lanes, :] = blk[:, g, :].T.astype(BF16)
            return carry

        lax.fori_loop(0, NZ, body, 0)

    mid = 2 - z // 2
    far = 3 - 3 * (z // 2)
    zo = [z, zs[1], mid, far]
    inner = (z == 1) | (z == 2)
    send(z, p, (mid, p))
    send(z, p, (zs[1], p))
    for k in (3, 2, 1):
        send_l(z, (zs[k], p), 0)
    targets = ((diag, 3), (xn, 1), (yn, 2), (partner, 4))
    for dev, way in targets:
        send(z, p, (z, dev), way)
    for j in range(1, NP):
        send_l(z, (z, (p + j) % NP), 1)

    def attn_piece(q):
        return rcopy(wattn_ref.at[pl.ds(attn_start(q), 80), :], watt.at[z], asend.at[0], arecv.at[0], (q, p))

    loads[2].wait()
    attn_piece(mid).start()

    @pl.when(jnp.logical_not(inner))
    def _():
        attn_piece(zs[1]).start()

    def outward(k):
        return rcopy(xg.at[zo[k], p], xg.at[zo[k], p], osem.at[k - 2], xrecv.at[0, zo[k]], (zs[1], p))

    s1[...] = jnp.zeros_like(s1)
    s2[...] = jnp.zeros_like(s2)
    stat(z, p)
    watt[z] = wattn_ref[pl.ds(attn_start(z), 80), :]
    wload.wait()
    turn(0)

    def column(k):
        wait_x(zo[k], p, 0)
        if k >= 2:
            @pl.when(inner)
            def _():
                outward(k).start()
        for dev, way in targets:
            send(zo[k], p, (z, dev), way)
        stat(zo[k], p)

    def pass_on(k, src, way):
        wait_x(zo[k], src, way)
        send(zo[k], src, (z, partner), 4)
        stat(zo[k], src)

    ph('a_col1')
    column(1)
    column(2)
    ph('a_col3')
    column(3)
    ph('a_lnsend')
    rcopy(ldummy.at[pl.ds(0, 3)], ldummy.at[pl.ds(0, 3)], lsend.at[0], lrecv.at[0], here).wait_recv()
    for k in range(1, NZ):
        for j in range(1, NP):
            send_l(zs[k], (z, (p + j) % NP), 1)
    ph('a_nbr')
    for k in range(2):
        pass_on(k, xn, 1)
        pass_on(k, yn, 2)
    ph('a_wattn')
    attn_piece(far).start()

    @pl.when(inner)
    def _():
        attn_piece(zs[1]).start()

    ph('a_nbr2')
    pass_on(0, diag, 3)
    pass_on(1, diag, 3)
    ph('a_nbr3')
    for k in range(2, NZ):
        pass_on(k, xn, 1)
        pass_on(k, yn, 2)
        pass_on(k, diag, 3)
    send_w(0)
    ph('a_rest')
    half = xg.at[pl.ds(0, 2)]
    rcopy(half, half, xsend.at[0], rpart.at[0], here).wait_recv()
    for q in (partner, partner + xn - p, partner + yn - p, partner + diag - p):
        for k in range(NZ):
            stat(zo[k], q)
    rcopy(ldummy.at[pl.ds(0, 28)], ldummy.at[pl.ds(0, 28)], lsend.at[0], lrecv.at[1], here).wait_recv()

    ph('a_norm')
    mean = jnp.sum(s1[...], axis=0, keepdims=True) / 2048.0
    var = jnp.sum(s2[...], axis=0, keepdims=True) / 2048.0 - mean * mean
    rstd = lax.rsqrt(var + LN_EPS)
    lnT = jnp.concatenate([lng[i // NP, i % NP, 0:1, :] for i in range(32)] + [jnp.zeros((96, 128), F32)], axis=0).T
    for i in range(NZ * NP):
        sc = lnT[0:64, i:i + 1]
        hT_ref[i * 64:(i + 1) * 64, :] = ((xg[i // NP, i % NP].astype(F32) - mean) * rstd * sc).astype(BF16)

    hout = pltpu.make_async_copy(hT_ref, h_ref, lsem.at[5])
    hout.start()
    ph('a_attw')
    three = watt.at[pl.ds(0, 3)]
    rcopy(three, three, asend.at[0], arecv.at[0], here).wait_recv()
    ph('a_zdot')
    part = None
    for q in range(NZ):
        t = jnp.dot(watt[q], hT_ref[q * 512:(q + 1) * 512, :], preferred_element_type=F32)
        part = t if part is None else part + t
    part = part.astype(BF16)
    for q in range(NZ):
        zsend[q] = part[:, q * 128:(q + 1) * 128]
    for k in (3, 2, 1):
        rcopy(zsend.at[zs[k]], zrecv.at[z], zsend_sem.at[0], zrecv_sem.at[0], (zs[k], p)).start()
    zrecv[z] = zsend[z]
    ph('a_turn')
    turn(1)
    send_w(1)
    outs = [pltpu.make_async_copy(wt, w2_ref, lsem.at[1])]
    for i, ps_ref in enumerate((ps1_ref, ps2_ref, ps3_ref)):
        dst = (z + i + 1) % NZ
        outs.append(pltpu.make_async_copy(wt.at[:, pl.ds(pl.multiple_of(dst * 256 + C1, 16), C2), :], ps_ref, lsem.at[2 + i]))
    for c in outs[1:] + outs[:1]:
        c.start()
    ph('a_zwait')
    zthree = rcopy(zsend.at[pl.ds(0, 3)], zrecv.at[pl.ds(0, 3)], zsend_sem.at[0], zrecv_sem.at[0], here)
    zthree.wait_recv()
    ph('a_a2a')
    zt = jnp.concatenate([zrecv[0].astype(F32), zrecv[1].astype(F32)[16:80], zrecv[2].astype(F32), zrecv[3].astype(F32)[16:80]], axis=0)
    zq[...] = zt.T.astype(BF16).reshape(NP, 16, 288)
    for j in range(1, NP):
        q = (p + j) % NP
        rcopy(zq.at[q], qkv_ref.at[p], qsend.at[0], qrecv.at[0], (z, q)).start()
    qown = pltpu.make_async_copy(zq.at[p], qkv_ref.at[p], lsem.at[9])
    qown.start()
    qseven = rcopy(zq.at[pl.ds(0, 7)], qkv_ref.at[pl.ds(0, 7)], qsend.at[0], qrecv.at[0], here)
    qseven.wait_recv()
    ph('a_wwait')
    wthree = w1f_ref.at[pl.ds(0, 3)]
    wall = rcopy(wthree, wthree, wsend.at[0], wrecv.at[0], here)
    wall.wait_recv()
    ph('a_sendwait')
    hout.wait()
    qown.wait()
    for c in outs:
        c.wait()
    sent30 = w2_ref.at[:, pl.ds(0, 960), :]
    rcopy(sent30, sent30, xsend.at[0], rpart.at[0], here).wait_send()
    rcopy(ldummy, ldummy, lsend.at[0], lrecv.at[0], here).wait_send()
    rcopy(three, three, asend.at[0], arecv.at[0], here).wait_send()
    zthree.wait_send()
    qseven.wait_send()
    wall.wait_send()

    @pl.when(inner)
    def _():
        outward(2).wait_send()
        outward(3).wait_send()
    ph('')


def call_a(xT, ln, wattnT, w):
    hbm = pl.BlockSpec(memory_space=pl.ANY)
    return pl.pallas_call(
        kernel_a,
        out_shape=(
            jax.ShapeDtypeStruct((2048, 512), BF16),
            jax.ShapeDtypeStruct((NP, 16, 288), BF16),
            jax.ShapeDtypeStruct((NZ, 2, C1, 512), BF16),
            jax.ShapeDtypeStruct((2, 1024, 512), BF16),
        ) + (jax.ShapeDtypeStruct((2, C2, 512), BF16),) * 3,
        in_specs=[hbm] * 4,
        out_specs=(hbm,) * 7,
        scratch_shapes=[
            pltpu.VMEM((NZ, NP, 64, 512), BF16),
            pltpu.VMEM((NZ, NP, 1, 128), F32),
            pltpu.VMEM((NZ, 80, 512), BF16),
            pltpu.VMEM((NZ, 80, 128), BF16),
            pltpu.VMEM((NZ, 80, 128), BF16),
            pltpu.VMEM((NP, 16, 288), BF16),
            pltpu.VMEM((8, 512), F32),
            pltpu.VMEM((8, 512), F32),
            pltpu.VMEM((512, 2, 1024), BF16),
            pltpu.VMEM((2, 1024, 512), BF16),
            pltpu.VMEM((2048, 512), BF16),
            pltpu.VMEM((1, 64), F32),
            pltpu.VMEM((288, 512), BF16),
            pltpu.SemaphoreType.DMA((1,)),
            pltpu.SemaphoreType.DMA((4, NZ)),
            pltpu.SemaphoreType.DMA((1,)),
            pltpu.SemaphoreType.DMA((1,)),
            pltpu.SemaphoreType.DMA((2,)),
            pltpu.SemaphoreType.DMA((1,)),
            pltpu.SemaphoreType.DMA((1,)),
            pltpu.SemaphoreType.DMA((1,)),
            pltpu.SemaphoreType.DMA((1,)),
            pltpu.SemaphoreType.DMA((1,)),
            pltpu.SemaphoreType.DMA((1,)),
            pltpu.SemaphoreType.DMA((1,)),
            pltpu.SemaphoreType.DMA((1,)),
            pltpu.SemaphoreType.DMA((10,)),
            pltpu.SemaphoreType.DMA((2,)),
            pltpu.VMEM((31, 1, 128), F32),
        ],
        compiler_params=pltpu.CompilerParams(collective_id=0, has_side_effects=True, vmem_limit_bytes=56 * 1024 * 1024),
        name='gather_norm_qkv',
    )(xT, ln, wattnT, w)


def kernel_b(len_ref, q_ref, k_ref, v_ref, kc_ref, vc_ref, o_ref, kn_ref, vn_ref, kbuf, vbuf, oscr, isem, osem):
    rows = kbuf.shape[0]
    seq = kbuf.shape[1]

    def load(b, t):
        return pltpu.make_async_copy((kc_ref, vc_ref)[t].at[b], (kbuf, vbuf)[t].at[b], isem.at[b])

    def store(b, t):
        return pltpu.make_async_copy((kbuf, vbuf)[t].at[b], (kn_ref, vn_ref)[t].at[b], osem.at[0])

    for b in range(rows):
        load(b, 0).start()
        load(b, 1).start()

    def insert(buf, b, length, new):
        base = pl.multiple_of((length // 16) * 16, 16)
        hit = base + lax.broadcasted_iota(jnp.int32, (16, 128), 0) == length
        buf[b, pl.ds(base, 16), :] = jnp.where(hit, new.astype(F32), buf[b, pl.ds(base, 16), :].astype(F32)).astype(BF16)

    def attend(b, length, n):
        scores = lax.dot_general(q_ref[b], kbuf[b, 0:n, :], (((1,), (1,)), ((), ())), preferred_element_type=F32) * (128.0 ** -0.5)
        slot = lax.broadcasted_iota(jnp.int32, scores.shape, 1)
        scores = jnp.where(slot <= length, scores, -1e30)
        top = jnp.max(scores, axis=1, keepdims=True)
        e = jnp.exp(scores - top)
        probs = (e / jnp.sum(e, axis=1, keepdims=True)).astype(BF16)
        return jnp.dot(probs, vbuf[b, 0:n, :], preferred_element_type=F32)

    def pair(i, carry):
        b0 = 2 * i
        b1 = 2 * i + 1
        l0 = len_ref[b0]
        l1 = len_ref[b1]
        for b, length in ((b0, l0), (b1, l1)):
            pltpu.make_async_copy(kc_ref.at[pl.ds(0, 2)], kbuf.at[pl.ds(0, 2)], isem.at[b]).wait()
            insert(kbuf, b, length, k_ref[b])
            insert(vbuf, b, length, v_ref[b])
        last = jnp.maximum(l0, l1) // 512
        for t in range(seq // 512):
            @pl.when(last == t)
            def _():
                n = 512 * (t + 1)
                r0 = attend(b0, l0, n)
                r1 = attend(b1, l1, n)
                oscr[b0] = r0
                oscr[b1] = r1
        for b in (b0, b1):
            store(b, 0).start()
            store(b, 1).start()
        return carry

    lax.fori_loop(0, rows // 2, pair, 0)
    for h in range(16):
        o_ref[h // 2, :, (h % 2) * 128:(h % 2 + 1) * 128] = oscr[:, h, :].astype(BF16)
    pltpu.make_async_copy(kbuf, kn_ref, osem.at[0]).wait()
    pltpu.make_async_copy(vbuf, vn_ref, osem.at[0]).wait()


def call_b(lengths, q_rot, k_rot, v_tok, k_cache, v_cache):
    rows, seq, hd = k_cache.shape
    heads = q_rot.shape[1]
    vm = pl.BlockSpec(memory_space=pltpu.VMEM)
    hbm = pl.BlockSpec(memory_space=pl.ANY)
    return pl.pallas_call(
        kernel_b,
        in_specs=[pl.BlockSpec(memory_space=pltpu.SMEM), vm, vm, vm, hbm, hbm],
        out_specs=(vm, hbm, hbm),
        out_shape=(
            jax.ShapeDtypeStruct((NP, rows, heads * hd // NP), BF16),
            jax.ShapeDtypeStruct(k_cache.shape, BF16),
            jax.ShapeDtypeStruct(v_cache.shape, BF16),
        ),
        scratch_shapes=[
            pltpu.VMEM((rows, seq, hd), BF16),
            pltpu.VMEM((rows, seq, hd), BF16),
            pltpu.VMEM((rows, heads, hd), F32),
            pltpu.SemaphoreType.DMA((rows,)),
            pltpu.SemaphoreType.DMA((1,)),
        ],
        compiler_params=pltpu.CompilerParams(vmem_limit_bytes=58 * 1024 * 1024),
        cost_estimate=pl.CostEstimate(flops=12_000_000_000, bytes_accessed=33_000_000, transcendentals=0),
        name='attend',
    )(lengths, q_rot, k_rot, v_tok, k_cache, v_cache)


def kernel_c(hT, w2_ref, w1f_ref, p1_ref, p2_ref, p3_ref, wd, wo, o_ref, xT_ref, y_ref,
             wvA, wvB, wdAT, wdBT, woT, og, hidA, hidB, yA, ysum, r1, acc, r2,
             wsem, wbsend, wbrecv, osend, orecv, gsend, grecv, hasend, harecv, hbsend, hbrecv,
             r1send, r1recv, r2send, r2recv):
    z, p, core, partner, xn, yn, diag, zs = coords()
    ph('c_bar')
    local = [pltpu.make_async_copy(w2_ref.at[:, pl.ds(pl.multiple_of(z * 256, 256), CA), :], wvA.at[z], wsem.at[0])]
    for s, p_ref in ((1, p1_ref), (2, p2_ref), (3, p3_ref)):
        src = (z + NZ - s) % NZ
        local.append(pltpu.make_async_copy(w1f_ref.at[src], wvA.at[src, :, pl.ds(0, C1), :], wsem.at[0]))
        local.append(pltpu.make_async_copy(p_ref, wvA.at[src, :, pl.ds(C1, C2), :], wsem.at[0]))
    late = [
        pltpu.make_async_copy(w2_ref.at[:, pl.ds(pl.multiple_of(z * 256 + CA, 16), C3), :], wvB.at[z], wsem.at[1]),
    ]
    for c in local + late:
        c.start()
    entry_barrier(z, p, zs)
    here = (z, p)

    ph('c_send')
    spans = ((0, C3A), (C3A, C3 - C3A))

    def w_piece(i, src, dst, dev):
        o, n = spans[i]
        return rcopy(
            w2_ref.at[:, pl.ds(pl.multiple_of(dst * 256 + CA + o, 16), n), :],
            wvB.at[src, :, pl.ds(o, n), :], wbsend.at[0], wbrecv.at[0], dev)

    def send_w(i):
        for k in (3, 2, 1):
            w_piece(i, z, zs[k], (zs[k], p)).start()

    send_w(0)
    for j in range(1, NP):
        q = (p + j) % NP
        rcopy(o_ref.at[q], og.at[z, p], osend.at[0], orecv.at[0], (z, q)).start()
    og[z, p] = o_ref[p]

    def gated(wv, n):
        g = None
        for q in range(NZ):
            t = jnp.dot(wv[q].reshape(2 * n, 512), hT[q * 512:(q + 1) * 512, :], preferred_element_type=F32)
            g = t if g is None else g + t
        gate = g[0:n].astype(BF16).astype(F32)
        up = g[n:2 * n].astype(BF16).astype(F32)
        return (jax.nn.silu(gate) * up).astype(BF16)

    ra = Relay(z, p, lambda src, ch: hidA.at[ch, src], hidA.at[0], hasend, harecv)
    rb = Relay(z, p, lambda src, ch: hidB.at[ch, src], hidB.at[0], hbsend, hbrecv)
    ro = Relay(z, p, lambda src, ch: og.at[src], og.at[0], gsend, grecv)
    every = range(CHUNKS)

    ph('c_localwait')
    pltpu.make_async_copy(wvA, wvA, wsem.at[0]).wait()
    ph('c_gA')
    ha = gated(wvA, CA)
    for ch in every:
        hidA[ch, z] = ha[:, ch * LANES:(ch + 1) * LANES]

    ra.own(range(2))
    send_w(1)
    ph('c_owait')
    oseven = rcopy(o_ref.at[pl.ds(0, 7)], og.at[z, pl.ds(0, 7)], osend.at[0], orecv.at[0], here)
    oseven.wait_recv()
    ro.own(range(1))
    ph('c_transp')
    for c in late:
        c.wait()
    wdAT[...] = jnp.concatenate([wd[q * 256:q * 256 + CA, :] for q in range(NZ)], axis=0).T
    wdBT[...] = jnp.concatenate([wd[q * 256 + CA:(q + 1) * 256, :] for q in range(NZ)], axis=0).T
    woT[...] = wo[...].T

    ph('c_wBwait')
    for ch in range(2):
        ra.step(1, ch)
    ro.step(1, 0)
    for ch in range(2):
        ra.step(2, ch)
    ph('c_wBwait2')
    wthree = wvB.at[pl.ds(0, 3)]
    wall = rcopy(wthree, wthree, wbsend.at[0], wbrecv.at[0], here)
    wall.wait_recv()
    ph('c_gB')
    hb = gated(wvB, C3)
    for ch in range(CHUNKS):
        hidB[ch, z] = hb[:, ch * LANES:(ch + 1) * LANES]
    ph('c_own')
    rb.own(range(2))
    for ch in range(2, CHUNKS):
        ra.own((ch,))
        rb.own((ch,))

    chip = p // 2
    others = [diag // 2, xn // 2, yn // 2]

    def d2d(ch):
        return rcopy(ysum.at[ch, 1 - core], r1.at[ch], r1send.at[0], r1recv.at[ch], (z, partner))

    def hop(ch, i, dev):
        return rcopy(acc.at[ch, i], r2.at[ch, i], r2send.at[0], r2recv.at[ch], (z, dev))

    def stage0(ch):
        o_rows = og[ch * NZ // CHUNKS].reshape(128, 256)
        yA[...] = jnp.dot(wdAT[...], hidA[ch].reshape(NZ * CA, LANES), preferred_element_type=F32) + lax.dot_general(
            woT[...], o_rows, (((1,), (1,)), ((), ())), preferred_element_type=F32)

    def stage1(ch):
        yt = yA[...] + jnp.dot(wdBT[...], hidB[ch].reshape(NZ * C3, LANES), preferred_element_type=F32)
        yt = yt.reshape(4, 2, 64, LANES)
        for i in range(4):
            for j in range(2):
                ysum[ch, j, i] = yt[i, j]
        d2d(ch).start()

    def stage2(ch):
        d2d(ch).wait_recv()
        for i, (t, dev) in enumerate(zip(others, (diag, xn, yn))):
            acc[ch, i] = ysum[ch, core, t] + r1[ch, t]
            hop(ch, i, dev).start()

    def stage3(ch):
        lanes = slice(ch * LANES, (ch + 1) * LANES)
        mine = ysum[ch, core, chip] + r1[ch, chip]
        rcopy(acc.at[ch], r2.at[ch], r2send.at[0], r2recv.at[ch], here).wait_recv()
        for i in range(3):
            mine = mine + r2[ch, i]
        y_ref[:, lanes] = (xT_ref[:, lanes].astype(F32) + mine).astype(BF16)

    for t in range(1, CHUNKS + 3):
        ph(f'c_wave{t}')
        for k in range(1, NZ - 1):
            ch = t - k
            if 0 <= ch < CHUNKS:
                if ch >= 2:
                    ra.step(k, ch)
                rb.step(k, ch)
        if t < 3:
            ro.step(t + 1, 0)
        ph(f'c_sum{t}')
        if t >= 3:
            ra.step(3, t - 3)
            stage0(t - 3)
            rb.step(3, t - 3)
            stage1(t - 3)
        if t >= 4:
            stage2(t - 4)
    ph('c_last2')
    stage2(CHUNKS - 1)
    ph('c_last3')
    for ch in every:
        stage3(ch)

    ph('c_end')
    wall.wait_send()
    oseven.wait_send()
    rcopy(r1, r1, r1send.at[0], r1recv.at[0], here).wait_send()
    rcopy(acc, acc, r2send.at[0], r2recv.at[0], here).wait_send()
    ra.drain()
    rb.drain()
    ro.drain()
    ph('')


def call_c(hT, w2, w1f, ps, wd, wo, o8, xT):
    vm = pl.BlockSpec(memory_space=pltpu.VMEM)
    hbm = pl.BlockSpec(memory_space=pl.ANY)
    return pl.pallas_call(
        kernel_c,
        out_shape=jax.ShapeDtypeStruct((64, 512), BF16),
        in_specs=[vm] + [hbm] * 5 + [vm] * 4,
        out_specs=vm,
        scratch_shapes=[
            pltpu.VMEM((NZ, 2, CA, 512), BF16),
            pltpu.VMEM((NZ, 2, C3, 512), BF16),
            pltpu.VMEM((512, NZ * CA), BF16),
            pltpu.VMEM((512, NZ * C3), BF16),
            pltpu.VMEM((512, 256), BF16),
            pltpu.VMEM((NZ, NP, 16, 256), BF16),
            pltpu.VMEM((CHUNKS, NZ, CA, LANES), BF16),
            pltpu.VMEM((CHUNKS, NZ, C3, LANES), BF16),
            pltpu.VMEM((512, LANES), F32),
            pltpu.VMEM((CHUNKS, 2, 4, 64, LANES), F32),
            pltpu.VMEM((CHUNKS, 4, 64, LANES), F32),
            pltpu.VMEM((CHUNKS, 3, 64, LANES), F32),
            pltpu.VMEM((CHUNKS, 3, 64, LANES), F32),
            pltpu.SemaphoreType.DMA((2,)),
            pltpu.SemaphoreType.DMA((1,)),
            pltpu.SemaphoreType.DMA((1,)),
            pltpu.SemaphoreType.DMA((1,)),
            pltpu.SemaphoreType.DMA((1,)),
            pltpu.SemaphoreType.DMA((6,)),
            pltpu.SemaphoreType.DMA((NZ, 1)),
            pltpu.SemaphoreType.DMA((6,)),
            pltpu.SemaphoreType.DMA((NZ, CHUNKS)),
            pltpu.SemaphoreType.DMA((6,)),
            pltpu.SemaphoreType.DMA((NZ, CHUNKS)),
            pltpu.SemaphoreType.DMA((1,)),
            pltpu.SemaphoreType.DMA((CHUNKS,)),
            pltpu.SemaphoreType.DMA((1,)),
            pltpu.SemaphoreType.DMA((CHUNKS,)),
        ],
        compiler_params=pltpu.CompilerParams(collective_id=1, has_side_effects=True, vmem_limit_bytes=40 * 1024 * 1024),
        cost_estimate=pl.CostEstimate(flops=12_000_000_000, bytes_accessed=6_000_000, transcendentals=0),
        name='mlp_out',
    )(hT, w2, w1f, *ps, wd, wo, o8, xT)


def solution(mesh):
    all_axes = ('x', 'yz')

    def local_step(x_in, ln_scale, w_gate_up, w_attn, w_down, w_out, k_cache, v_cache, lengths, positions):
        xT = x_in.T
        wattnT = w_attn.T
        hT, qkv, w1f, w2, *pieces = call_a(xT, ln_scale[None, :], wattnT, w_gate_up)
        ps = [lax.ppermute(pieces[i], 'x', [(q, (q + i + 1) % NZ) for q in range(NZ)]) for i in range(NZ - 1)]
        proj = jnp.transpose(qkv, (1, 0, 2)).reshape(16, 2304)
        q_raw = proj[:, :2048].reshape(16, 16, 128)
        k_tok = proj[:, 2048:2176]
        v_tok = proj[:, 2176:]
        q_rot = rotary(q_raw.astype(F32), positions).astype(BF16)
        k_rot = rotary(k_tok[:, None, :].astype(F32), positions).astype(BF16)
        o8, k_new, v_new = call_b(lengths, q_rot, k_rot, v_tok[:, None, :], k_cache, v_cache)
        yT = call_c(hT, w2, w1f, ps, w_down, w_out, o8, xT)
        return yT.T, k_new, v_new

    row_spec = P(None, all_axes)
    vec_spec = P(all_axes)
    cache_spec = P(all_axes, None, None)
    return jax.shard_map(
        local_step,
        mesh=mesh,
        in_specs=(row_spec, vec_spec, P('x', None, 'yz'), P('x', 'yz'), P('yz', 'x'), P('yz', 'x'), cache_spec, cache_spec, vec_spec, vec_spec),
        out_specs=(row_spec, cache_spec, cache_spec),
        check_vma=False,
    )
```

```python
import functools

import jax
import jax.numpy as jnp
from jax import lax
from jax.experimental import pallas as pl
from jax.experimental.pallas import tpu as pltpu
from jax.sharding import PartitionSpec as P

LN_EPS = 1e-6
ROPE_BASE = 10000.0
MESH = pl.DeviceIdType.MESH


class Phase:
    cm = None

    def __call__(self, name):
        if self.cm is not None:
            self.cm.__exit__(None, None, None)
            self.cm = None
        if name:
            self.cm = jax.named_scope(name)
            self.cm.__enter__()


ph = Phase()
F32 = jnp.float32
BF16 = jnp.bfloat16

NZ = 4
NP = 8
C1A = 16
C1 = 48
C2 = 112
C3 = 96
C3A = 48
CA = C1 + C2
CHUNKS = 4
LANES = 512 // CHUNKS


def rotary(values, positions):
    half_dim = values.shape[-1] // 2
    inv_freq = ROPE_BASE ** (-jnp.arange(half_dim, dtype=jnp.float32) / half_dim)
    angles = positions.astype(jnp.float32)[:, None, None] * inv_freq
    cos_part = jnp.cos(angles)
    sin_part = jnp.sin(angles)
    lo_half = values[..., :half_dim]
    hi_half = values[..., half_dim:]
    return jnp.concatenate([lo_half * cos_part - hi_half * sin_part, hi_half * cos_part + lo_half * sin_part], axis=-1)


def coords():
    z = lax.axis_index('x')
    p = lax.axis_index('yz')
    core = p % 2
    xx = (p // 2) % 2
    y = p // 4
    partner = p + 1 - 2 * core
    xn = p + 2 - 4 * xx
    yn = p + 4 - 8 * y
    diag = xn + 4 - 8 * y
    z1 = z % 2
    z2 = z // 2
    zs = [z, 2 * z2 + 1 - z1, 2 * (1 - z2) + z1, 3 - z]
    return z, p, core, partner, xn, yn, diag, zs


def entry_barrier(z, p, zs):
    sem = pltpu.get_barrier_semaphore()
    for k in range(1, NZ):
        pl.semaphore_signal(sem, inc=1, device_id=(zs[k], p), device_id_type=MESH)
    for k in range(1, NP):
        pl.semaphore_signal(sem, inc=1, device_id=(z, (p + k) % NP), device_id_type=MESH)
    pl.semaphore_wait(sem, NZ - 1 + NP - 1)


def rcopy(src, dst, send, recv, dev):
    return pltpu.make_async_remote_copy(src_ref=src, dst_ref=dst, send_sem=send, recv_sem=recv, device_id=dev, device_id_type=MESH)


class Relay:
    def __init__(self, z, p, at, whole, send, recv):
        self.z, self.p, self.at, self.whole, self.send, self.recv = z, p, at, whole, send, recv

    def copy(self, way, src, ch, dev):
        ref = self.at(src, ch)
        return rcopy(ref, ref, self.send.at[way], self.recv.at[src, ch], (dev, self.p))

    def own(self, chunks):
        z = self.z

        @pl.when(z < 3)
        def _():
            for ch in chunks:
                self.copy(0, z, ch, z + 1).start()

        @pl.when(z > 0)
        def _():
            for ch in chunks:
                self.copy(1, z, ch, z - 1).start()

    def step(self, k, ch):
        z = self.z

        @pl.when(z >= k)
        def _():
            self.copy(0, z - k, ch, z).wait_recv()

            @pl.when(z < 3)
            def _():
                self.copy(2 * k, z - k, ch, z + 1).start()

        @pl.when(z + k <= 3)
        def _():
            self.copy(0, z + k, ch, z).wait_recv()

            @pl.when(z > 0)
            def _():
                self.copy(2 * k + 1, z + k, ch, z - 1).start()

    def sent(self, way):
        rcopy(self.whole, self.whole, self.send.at[way], self.recv.at[0, 0], (self.z, self.p)).wait_send()

    def drain(self):
        z = self.z
        for k in range(NZ - 1):
            @pl.when((z >= k) & (z < 3))
            def _():
                self.sent(2 * k)

            @pl.when((z + k <= 3) & (z > 0))
            def _():
                self.sent(2 * k + 1)


def attn_start(q):
    return pl.multiple_of(64 * q + 16 * (q // 2), 16)


def kernel_a(xT_hbm, ln_hbm, wattn_hbm, w_ref, h_ref, qkv_ref, w1f_ref, w2_ref, ps1_ref, ps2_ref, ps3_ref,
             xg, lng, watt, zsend, zrecv, zq, s1, s2, wn, wt, hT_ref, ln_ref, wattn_ref,
             xsend, xrecv, rpart, lsend, lrecv, asend, arecv, zsend_sem, zrecv_sem, qsend, qrecv, wsend, wrecv, lsem, osem, ldummy):
    z, p, core, partner, xn, yn, diag, zs = coords()
    ph('a_bar')
    wload = pltpu.make_async_copy(w_ref, wn, lsem.at[0])
    loads = [
        pltpu.make_async_copy(xT_hbm, xg.at[z, p], lsem.at[6]),
        pltpu.make_async_copy(ln_hbm, ln_ref, lsem.at[7]),
        pltpu.make_async_copy(wattn_hbm, wattn_ref, lsem.at[8]),
        wload,
    ]
    for c in loads:
        c.start()
    loads[1].wait()
    lng[z, p] = jnp.zeros((1, 128), F32)
    lng[z, p, 0:1, 0:64] = ln_ref[...]
    entry_barrier(z, p, zs)
    loads[0].wait()
    ph('a_zsend')
    here = (z, p)

    def send(src_z, src_p, dev, way=0):
        recv = rpart.at[0] if way == 4 else xrecv.at[way, src_z]
        rcopy(xg.at[src_z, src_p], xg.at[src_z, src_p], xsend.at[0], recv, dev).start()

    def send_l(src_z, dev, phase):
        rcopy(lng.at[src_z, p], lng.at[src_z, p], lsend.at[0], lrecv.at[phase], dev).start()

    def wait_x(src_z, src_p, way):
        rcopy(xg.at[src_z, src_p], xg.at[src_z, src_p], xsend.at[0], xrecv.at[way, src_z], here).wait_recv()

    def stat(src_z, src_p):
        blk = xg[src_z, src_p].astype(F32).reshape(8, 8, 512)
        s1[...] += jnp.sum(blk, axis=0)
        s2[...] += jnp.sum(blk * blk, axis=0)

    spans = tuple((i, C1A) for i in range(0, C1, C1A))

    def w_piece(i, src, dst, dev):
        o, n = spans[i]
        return rcopy(
            wt.at[:, pl.ds(pl.multiple_of(dst * 256 + o, 16), n), :],
            w1f_ref.at[src, :, pl.ds(o, n), :],
            wsend.at[0], wrecv.at[0], dev)

    def send_w(i):
        for k in (3, 2, 1):
            w_piece(i, z, zs[k], (zs[k], p)).start()

    def turn(odd):
        def body(i, carry):
            lanes = pl.ds(pl.multiple_of(i * 256 + odd * 128, 128), 128)
            blk = wn[:, :, lanes].astype(F32)
            for g in range(2):
                wt[g, lanes, :] = blk[:, g, :].T.astype(BF16)
            return carry

        lax.fori_loop(0, NZ, body, 0)

    mid = 2 - z // 2
    far = 3 - 3 * (z // 2)
    zo = [z, zs[1], mid, far]
    inner = (z == 1) | (z == 2)
    send(z, p, (mid, p))
    send(z, p, (zs[1], p))
    for k in (3, 2, 1):
        send_l(z, (zs[k], p), 0)
    targets = ((diag, 3), (xn, 1), (yn, 2), (partner, 4))
    for dev, way in targets:
        send(z, p, (z, dev), way)
    for j in range(1, NP):
        send_l(z, (z, (p + j) % NP), 1)

    def attn_piece(q):
        return rcopy(wattn_ref.at[pl.ds(attn_start(q), 80), :], watt.at[z], asend.at[0], arecv.at[0], (q, p))

    def outward(k):
        return rcopy(xg.at[zo[k], p], xg.at[zo[k], p], osem.at[k - 2], xrecv.at[0, zo[k]], (zs[1], p))

    s1[...] = jnp.zeros_like(s1)
    s2[...] = jnp.zeros_like(s2)
    stat(z, p)
    loads[2].wait()
    watt[z] = wattn_ref[pl.ds(attn_start(z), 80), :]
    wload.wait()
    turn(0)
    attn_piece(mid).start()

    @pl.when(jnp.logical_not(inner))
    def _():
        attn_piece(zs[1]).start()


    def column(k):
        wait_x(zo[k], p, 0)
        if k >= 2:
            @pl.when(inner)
            def _():
                outward(k).start()
        for dev, way in targets:
            send(zo[k], p, (z, dev), way)
        stat(zo[k], p)

    def pass_on(k, src, way):
        wait_x(zo[k], src, way)
        send(zo[k], src, (z, partner), 4)
        stat(zo[k], src)

    ph('a_col1')
    column(1)
    column(2)
    ph('a_col3')
    column(3)
    ph('a_lnsend')
    rcopy(ldummy.at[pl.ds(0, 3)], ldummy.at[pl.ds(0, 3)], lsend.at[0], lrecv.at[0], here).wait_recv()
    for k in range(1, NZ):
        for j in range(1, NP):
            send_l(zs[k], (z, (p + j) % NP), 1)
    ph('a_nbr')
    for k in range(2):
        pass_on(k, xn, 1)
        pass_on(k, yn, 2)
    ph('a_wattn')
    attn_piece(far).start()

    @pl.when(inner)
    def _():
        attn_piece(zs[1]).start()

    send_w(0)
    ph('a_nbr2')
    pass_on(0, diag, 3)
    pass_on(1, diag, 3)
    ph('a_nbr3')
    for k in range(2, NZ):
        pass_on(k, xn, 1)
        pass_on(k, yn, 2)
        pass_on(k, diag, 3)
    send_w(1)
    ph('a_rest')
    half = xg.at[pl.ds(0, 2)]
    rcopy(half, half, xsend.at[0], rpart.at[0], here).wait_recv()
    for q in (partner, partner + xn - p, partner + yn - p, partner + diag - p):
        for k in range(NZ):
            stat(zo[k], q)
    rcopy(ldummy.at[pl.ds(0, 28)], ldummy.at[pl.ds(0, 28)], lsend.at[0], lrecv.at[1], here).wait_recv()

    ph('a_norm')
    mean = jnp.sum(s1[...], axis=0, keepdims=True) / 2048.0
    var = jnp.sum(s2[...], axis=0, keepdims=True) / 2048.0 - mean * mean
    rstd = lax.rsqrt(var + LN_EPS)
    lnT = jnp.concatenate([lng[i // NP, i % NP, 0:1, :] for i in range(32)] + [jnp.zeros((96, 128), F32)], axis=0).T
    for i in range(NZ * NP):
        sc = lnT[0:64, i:i + 1]
        hT_ref[i * 64:(i + 1) * 64, :] = ((xg[i // NP, i % NP].astype(F32) - mean) * rstd * sc).astype(BF16)

    hout = pltpu.make_async_copy(hT_ref, h_ref, lsem.at[5])
    hout.start()
    ph('a_attw')
    three = watt.at[pl.ds(0, 3)]
    rcopy(three, three, asend.at[0], arecv.at[0], here).wait_recv()
    ph('a_zdot')
    part = None
    for q in range(NZ):
        t = jnp.dot(watt[q], hT_ref[q * 512:(q + 1) * 512, :], preferred_element_type=F32)
        part = t if part is None else part + t
    part = part.astype(BF16)
    for q in range(NZ):
        zsend[q] = part[:, q * 128:(q + 1) * 128]
    for k in (3, 2, 1):
        rcopy(zsend.at[zs[k]], zrecv.at[z], zsend_sem.at[0], zrecv_sem.at[0], (zs[k], p)).start()
    zrecv[z] = zsend[z]
    ph('a_turn')
    turn(1)
    send_w(2)
    outs = [pltpu.make_async_copy(wt, w2_ref, lsem.at[1])]
    for i, ps_ref in enumerate((ps1_ref, ps2_ref, ps3_ref)):
        dst = (z + i + 1) % NZ
        outs.append(pltpu.make_async_copy(wt.at[:, pl.ds(pl.multiple_of(dst * 256 + C1, 16), C2), :], ps_ref, lsem.at[2 + i]))
    for c in outs[1:] + outs[:1]:
        c.start()
    ph('a_zwait')
    zthree = rcopy(zsend.at[pl.ds(0, 3)], zrecv.at[pl.ds(0, 3)], zsend_sem.at[0], zrecv_sem.at[0], here)
    zthree.wait_recv()
    ph('a_a2a')
    zt = jnp.concatenate([zrecv[0].astype(F32), zrecv[1].astype(F32)[16:80], zrecv[2].astype(F32), zrecv[3].astype(F32)[16:80]], axis=0)
    zq[...] = zt.T.astype(BF16).reshape(NP, 16, 288)
    for j in range(1, NP):
        q = (p + j) % NP
        rcopy(zq.at[q], qkv_ref.at[p], qsend.at[0], qrecv.at[0], (z, q)).start()
    qown = pltpu.make_async_copy(zq.at[p], qkv_ref.at[p], lsem.at[9])
    qown.start()
    qseven = rcopy(zq.at[pl.ds(0, 7)], qkv_ref.at[pl.ds(0, 7)], qsend.at[0], qrecv.at[0], here)
    qseven.wait_recv()
    ph('a_wwait')
    wthree = w1f_ref.at[pl.ds(0, 3)]
    wall = rcopy(wthree, wthree, wsend.at[0], wrecv.at[0], here)
    wall.wait_recv()
    ph('a_sendwait')
    hout.wait()
    qown.wait()
    for c in outs:
        c.wait()
    sent30 = w2_ref.at[:, pl.ds(0, 960), :]
    rcopy(sent30, sent30, xsend.at[0], rpart.at[0], here).wait_send()
    rcopy(ldummy, ldummy, lsend.at[0], lrecv.at[0], here).wait_send()
    rcopy(three, three, asend.at[0], arecv.at[0], here).wait_send()
    zthree.wait_send()
    qseven.wait_send()
    wall.wait_send()

    @pl.when(inner)
    def _():
        outward(2).wait_send()
        outward(3).wait_send()
    ph('')


def call_a(xT, ln, wattnT, w):
    hbm = pl.BlockSpec(memory_space=pl.ANY)
    return pl.pallas_call(
        kernel_a,
        out_shape=(
            jax.ShapeDtypeStruct((2048, 512), BF16),
            jax.ShapeDtypeStruct((NP, 16, 288), BF16),
            jax.ShapeDtypeStruct((NZ, 2, C1, 512), BF16),
            jax.ShapeDtypeStruct((2, 1024, 512), BF16),
        ) + (jax.ShapeDtypeStruct((2, C2, 512), BF16),) * 3,
        in_specs=[hbm] * 4,
        out_specs=(hbm,) * 7,
        scratch_shapes=[
            pltpu.VMEM((NZ, NP, 64, 512), BF16),
            pltpu.VMEM((NZ, NP, 1, 128), F32),
            pltpu.VMEM((NZ, 80, 512), BF16),
            pltpu.VMEM((NZ, 80, 128), BF16),
            pltpu.VMEM((NZ, 80, 128), BF16),
            pltpu.VMEM((NP, 16, 288), BF16),
            pltpu.VMEM((8, 512), F32),
            pltpu.VMEM((8, 512), F32),
            pltpu.VMEM((512, 2, 1024), BF16),
            pltpu.VMEM((2, 1024, 512), BF16),
            pltpu.VMEM((2048, 512), BF16),
            pltpu.VMEM((1, 64), F32),
            pltpu.VMEM((288, 512), BF16),
            pltpu.SemaphoreType.DMA((1,)),
            pltpu.SemaphoreType.DMA((4, NZ)),
            pltpu.SemaphoreType.DMA((1,)),
            pltpu.SemaphoreType.DMA((1,)),
            pltpu.SemaphoreType.DMA((2,)),
            pltpu.SemaphoreType.DMA((1,)),
            pltpu.SemaphoreType.DMA((1,)),
            pltpu.SemaphoreType.DMA((1,)),
            pltpu.SemaphoreType.DMA((1,)),
            pltpu.SemaphoreType.DMA((1,)),
            pltpu.SemaphoreType.DMA((1,)),
            pltpu.SemaphoreType.DMA((1,)),
            pltpu.SemaphoreType.DMA((1,)),
            pltpu.SemaphoreType.DMA((10,)),
            pltpu.SemaphoreType.DMA((2,)),
            pltpu.VMEM((31, 1, 128), F32),
        ],
        compiler_params=pltpu.CompilerParams(collective_id=0, has_side_effects=True, vmem_limit_bytes=56 * 1024 * 1024),
        name='gather_norm_qkv',
    )(xT, ln, wattnT, w)


def kernel_b(len_ref, q_ref, k_ref, v_ref, kc_ref, vc_ref, o_ref, kn_ref, vn_ref, kbuf, vbuf, oscr, isem, osem):
    rows = kbuf.shape[0]
    seq = kbuf.shape[1]

    def load(b, t):
        return pltpu.make_async_copy((kc_ref, vc_ref)[t].at[b], (kbuf, vbuf)[t].at[b], isem.at[b])

    def store(b, t):
        return pltpu.make_async_copy((kbuf, vbuf)[t].at[b], (kn_ref, vn_ref)[t].at[b], osem.at[0])

    for b in range(rows):
        load(b, 0).start()
        load(b, 1).start()

    def insert(buf, b, length, new):
        base = pl.multiple_of((length // 16) * 16, 16)
        hit = base + lax.broadcasted_iota(jnp.int32, (16, 128), 0) == length
        buf[b, pl.ds(base, 16), :] = jnp.where(hit, new.astype(F32), buf[b, pl.ds(base, 16), :].astype(F32)).astype(BF16)

    def attend(b, length, n):
        scores = lax.dot_general(q_ref[b], kbuf[b, 0:n, :], (((1,), (1,)), ((), ())), preferred_element_type=F32) * (128.0 ** -0.5)
        slot = lax.broadcasted_iota(jnp.int32, scores.shape, 1)
        scores = jnp.where(slot <= length, scores, -1e30)
        top = jnp.max(scores, axis=1, keepdims=True)
        e = jnp.exp(scores - top)
        probs = (e / jnp.sum(e, axis=1, keepdims=True)).astype(BF16)
        return jnp.dot(probs, vbuf[b, 0:n, :], preferred_element_type=F32)

    def pair(i, carry):
        b0 = 2 * i
        b1 = 2 * i + 1
        l0 = len_ref[b0]
        l1 = len_ref[b1]
        for b, length in ((b0, l0), (b1, l1)):
            pltpu.make_async_copy(kc_ref.at[pl.ds(0, 2)], kbuf.at[pl.ds(0, 2)], isem.at[b]).wait()
            insert(kbuf, b, length, k_ref[b])
            insert(vbuf, b, length, v_ref[b])
        last = jnp.maximum(l0, l1) // 512
        for t in range(seq // 512):
            @pl.when(last == t)
            def _():
                n = 512 * (t + 1)
                r0 = attend(b0, l0, n)
                r1 = attend(b1, l1, n)
                oscr[b0] = r0
                oscr[b1] = r1
        for b in (b0, b1):
            store(b, 0).start()
            store(b, 1).start()
        return carry

    lax.fori_loop(0, rows // 2, pair, 0)
    for h in range(16):
        o_ref[h // 2, :, (h % 2) * 128:(h % 2 + 1) * 128] = oscr[:, h, :].astype(BF16)
    pltpu.make_async_copy(kbuf, kn_ref, osem.at[0]).wait()
    pltpu.make_async_copy(vbuf, vn_ref, osem.at[0]).wait()


def call_b(lengths, q_rot, k_rot, v_tok, k_cache, v_cache):
    rows, seq, hd = k_cache.shape
    heads = q_rot.shape[1]
    vm = pl.BlockSpec(memory_space=pltpu.VMEM)
    hbm = pl.BlockSpec(memory_space=pl.ANY)
    return pl.pallas_call(
        kernel_b,
        in_specs=[pl.BlockSpec(memory_space=pltpu.SMEM), vm, vm, vm, hbm, hbm],
        out_specs=(vm, hbm, hbm),
        out_shape=(
            jax.ShapeDtypeStruct((NP, rows, heads * hd // NP), BF16),
            jax.ShapeDtypeStruct(k_cache.shape, BF16),
            jax.ShapeDtypeStruct(v_cache.shape, BF16),
        ),
        scratch_shapes=[
            pltpu.VMEM((rows, seq, hd), BF16),
            pltpu.VMEM((rows, seq, hd), BF16),
            pltpu.VMEM((rows, heads, hd), F32),
            pltpu.SemaphoreType.DMA((rows,)),
            pltpu.SemaphoreType.DMA((1,)),
        ],
        compiler_params=pltpu.CompilerParams(vmem_limit_bytes=58 * 1024 * 1024),
        cost_estimate=pl.CostEstimate(flops=12_000_000_000, bytes_accessed=33_000_000, transcendentals=0),
        name='attend',
    )(lengths, q_rot, k_rot, v_tok, k_cache, v_cache)


def kernel_c(hT, w2_ref, w1f_ref, p1_ref, p2_ref, p3_ref, wd, wo, o_ref, xT_ref, y_ref,
             wvA, wvB, wdAT, wdBT, woT, og, hidA, hidB, yA, ysum, r1, acc, r2,
             wsem, wbsend, wbrecv, osend, orecv, gsend, grecv, hasend, harecv, hbsend, hbrecv,
             r1send, r1recv, r2send, r2recv):
    z, p, core, partner, xn, yn, diag, zs = coords()
    ph('c_bar')
    local = [pltpu.make_async_copy(w2_ref.at[:, pl.ds(pl.multiple_of(z * 256, 256), CA), :], wvA.at[z], wsem.at[0])]
    for s, p_ref in ((1, p1_ref), (2, p2_ref), (3, p3_ref)):
        src = (z + NZ - s) % NZ
        local.append(pltpu.make_async_copy(w1f_ref.at[src], wvA.at[src, :, pl.ds(0, C1), :], wsem.at[0]))
        local.append(pltpu.make_async_copy(p_ref, wvA.at[src, :, pl.ds(C1, C2), :], wsem.at[0]))
    late = [
        pltpu.make_async_copy(w2_ref.at[:, pl.ds(pl.multiple_of(z * 256 + CA, 16), C3), :], wvB.at[z], wsem.at[1]),
    ]
    for c in local + late:
        c.start()
    entry_barrier(z, p, zs)
    here = (z, p)

    ph('c_send')
    spans = ((0, C3A), (C3A, C3 - C3A))

    def w_piece(i, src, dst, dev):
        o, n = spans[i]
        return rcopy(
            w2_ref.at[:, pl.ds(pl.multiple_of(dst * 256 + CA + o, 16), n), :],
            wvB.at[src, :, pl.ds(o, n), :], wbsend.at[0], wbrecv.at[0], dev)

    def send_w(i):
        for k in (3, 2, 1):
            w_piece(i, z, zs[k], (zs[k], p)).start()

    send_w(0)
    for j in range(1, NP):
        q = (p + j) % NP
        rcopy(o_ref.at[q], og.at[z, p], osend.at[0], orecv.at[0], (z, q)).start()
    og[z, p] = o_ref[p]

    def gated(wv, n):
        g = None
        for q in range(NZ):
            t = jnp.dot(wv[q].reshape(2 * n, 512), hT[q * 512:(q + 1) * 512, :], preferred_element_type=F32)
            g = t if g is None else g + t
        gate = g[0:n].astype(BF16).astype(F32)
        up = g[n:2 * n].astype(BF16).astype(F32)
        return (jax.nn.silu(gate) * up).astype(BF16)

    ra = Relay(z, p, lambda src, ch: hidA.at[ch, src], hidA.at[0], hasend, harecv)
    rb = Relay(z, p, lambda src, ch: hidB.at[ch, src], hidB.at[0], hbsend, hbrecv)
    ro = Relay(z, p, lambda src, ch: og.at[src], og.at[0], gsend, grecv)
    every = range(CHUNKS)

    ph('c_localwait')
    pltpu.make_async_copy(wvA, wvA, wsem.at[0]).wait()
    ph('c_gA')
    ha = gated(wvA, CA)
    for ch in every:
        hidA[ch, z] = ha[:, ch * LANES:(ch + 1) * LANES]

    ra.own(range(2))
    send_w(1)
    ph('c_owait')
    oseven = rcopy(o_ref.at[pl.ds(0, 7)], og.at[z, pl.ds(0, 7)], osend.at[0], orecv.at[0], here)
    oseven.wait_recv()
    ro.own(range(1))
    ph('c_transp')
    for c in late:
        c.wait()
    def by_core(ref, w):
        w = w.T.reshape(4, 2, 64, w.shape[0])
        for j in range(2):
            ref[j] = w[:, j].reshape(256, w.shape[3])

    by_core(wdAT, jnp.concatenate([wd[q * 256:q * 256 + CA, :] for q in range(NZ)], axis=0))
    by_core(wdBT, jnp.concatenate([wd[q * 256 + CA:(q + 1) * 256, :] for q in range(NZ)], axis=0))
    by_core(woT, wo[...])

    ph('c_wBwait')
    for ch in range(2):
        ra.step(1, ch)
    ro.step(1, 0)
    ph('c_wBwait2')
    wthree = wvB.at[pl.ds(0, 3)]
    wall = rcopy(wthree, wthree, wbsend.at[0], wbrecv.at[0], here)
    wall.wait_recv()
    ph('c_gB')
    hb = gated(wvB, C3)
    for ch in range(CHUNKS):
        hidB[ch, z] = hb[:, ch * LANES:(ch + 1) * LANES]
    ph('c_own')
    rb.own(range(2))
    for ch in range(2, CHUNKS):
        ra.own((ch,))
        rb.own((ch,))
    ph('c_own2')
    for ch in range(2):
        ra.step(2, ch)

    chip = p // 2
    others = [diag // 2, xn // 2, yn // 2]

    def d2d(ch):
        return rcopy(ysum.at[ch, 1 - core], r1.at[ch], r1send.at[0], r1recv.at[ch], (z, partner))

    def hop(ch, i, dev):
        return rcopy(acc.at[ch, i], r2.at[ch, i], r2send.at[0], r2recv.at[ch], (z, dev))

    def stage0(ch):
        o_rows = og[ch * NZ // CHUNKS].reshape(128, 256)
        for j in (1 - core, core):
            yA[j] = jnp.dot(wdAT[j], hidA[ch].reshape(NZ * CA, LANES), preferred_element_type=F32) + lax.dot_general(
                woT[j], o_rows, (((1,), (1,)), ((), ())), preferred_element_type=F32)

    def half(ch, j):
        yt = yA[j] + jnp.dot(wdBT[j], hidB[ch].reshape(NZ * C3, LANES), preferred_element_type=F32)
        ysum[ch, j] = yt.reshape(4, 64, LANES)

    def stage1(ch):
        half(ch, 1 - core)
        d2d(ch).start()
        half(ch, core)

    def stage2(ch):
        d2d(ch).wait_recv()
        for i, (t, dev) in enumerate(zip(others, (diag, xn, yn))):
            acc[ch, i] = ysum[ch, core, t] + r1[ch, t]
            hop(ch, i, dev).start()

    def stage3(ch):
        lanes = slice(ch * LANES, (ch + 1) * LANES)
        mine = ysum[ch, core, chip] + r1[ch, chip]
        rcopy(acc.at[ch], r2.at[ch], r2send.at[0], r2recv.at[ch], here).wait_recv()
        for i in range(3):
            mine = mine + r2[ch, i]
        y_ref[:, lanes] = (xT_ref[:, lanes].astype(F32) + mine).astype(BF16)

    for t in range(1, CHUNKS + 3):
        ph(f'c_wave{t}')
        for k in range(1, NZ - 1):
            ch = t - k
            if 0 <= ch < CHUNKS:
                if ch >= 2:
                    ra.step(k, ch)
                rb.step(k, ch)
        if t < 3:
            ro.step(t + 1, 0)
        ph(f'c_sum{t}')
        if t >= 3:
            ra.step(3, t - 3)
            stage0(t - 3)
            rb.step(3, t - 3)
            stage1(t - 3)
        if t >= 4:
            stage2(t - 4)
    ph('c_last2')
    stage2(CHUNKS - 1)
    ph('c_last3')
    for ch in every:
        stage3(ch)

    ph('c_end')
    wall.wait_send()
    oseven.wait_send()
    rcopy(r1, r1, r1send.at[0], r1recv.at[0], here).wait_send()
    rcopy(acc, acc, r2send.at[0], r2recv.at[0], here).wait_send()
    ra.drain()
    rb.drain()
    ro.drain()
    ph('')


def call_c(hT, w2, w1f, ps, wd, wo, o8, xT):
    vm = pl.BlockSpec(memory_space=pltpu.VMEM)
    hbm = pl.BlockSpec(memory_space=pl.ANY)
    return pl.pallas_call(
        kernel_c,
        out_shape=jax.ShapeDtypeStruct((64, 512), BF16),
        in_specs=[vm] + [hbm] * 5 + [vm] * 4,
        out_specs=vm,
        scratch_shapes=[
            pltpu.VMEM((NZ, 2, CA, 512), BF16),
            pltpu.VMEM((NZ, 2, C3, 512), BF16),
            pltpu.VMEM((2, 256, NZ * CA), BF16),
            pltpu.VMEM((2, 256, NZ * C3), BF16),
            pltpu.VMEM((2, 256, 256), BF16),
            pltpu.VMEM((NZ, NP, 16, 256), BF16),
            pltpu.VMEM((CHUNKS, NZ, CA, LANES), BF16),
            pltpu.VMEM((CHUNKS, NZ, C3, LANES), BF16),
            pltpu.VMEM((2, 256, LANES), F32),
            pltpu.VMEM((CHUNKS, 2, 4, 64, LANES), F32),
            pltpu.VMEM((CHUNKS, 4, 64, LANES), F32),
            pltpu.VMEM((CHUNKS, 3, 64, LANES), F32),
            pltpu.VMEM((CHUNKS, 3, 64, LANES), F32),
            pltpu.SemaphoreType.DMA((2,)),
            pltpu.SemaphoreType.DMA((1,)),
            pltpu.SemaphoreType.DMA((1,)),
            pltpu.SemaphoreType.DMA((1,)),
            pltpu.SemaphoreType.DMA((1,)),
            pltpu.SemaphoreType.DMA((6,)),
            pltpu.SemaphoreType.DMA((NZ, 1)),
            pltpu.SemaphoreType.DMA((6,)),
            pltpu.SemaphoreType.DMA((NZ, CHUNKS)),
            pltpu.SemaphoreType.DMA((6,)),
            pltpu.SemaphoreType.DMA((NZ, CHUNKS)),
            pltpu.SemaphoreType.DMA((1,)),
            pltpu.SemaphoreType.DMA((CHUNKS,)),
            pltpu.SemaphoreType.DMA((1,)),
            pltpu.SemaphoreType.DMA((CHUNKS,)),
        ],
        compiler_params=pltpu.CompilerParams(collective_id=1, has_side_effects=True, vmem_limit_bytes=40 * 1024 * 1024),
        cost_estimate=pl.CostEstimate(flops=12_000_000_000, bytes_accessed=6_000_000, transcendentals=0),
        name='mlp_out',
    )(hT, w2, w1f, *ps, wd, wo, o8, xT)


def solution(mesh):
    all_axes = ('x', 'yz')

    def local_step(x_in, ln_scale, w_gate_up, w_attn, w_down, w_out, k_cache, v_cache, lengths, positions):
        xT = x_in.T
        wattnT = w_attn.T
        hT, qkv, w1f, w2, *pieces = call_a(xT, ln_scale[None, :], wattnT, w_gate_up)
        ps = [lax.ppermute(pieces[i], 'x', [(q, (q + i + 1) % NZ) for q in range(NZ)]) for i in range(NZ - 1)]
        proj = jnp.transpose(qkv, (1, 0, 2)).reshape(16, 2304)
        q_raw = proj[:, :2048].reshape(16, 16, 128)
        k_tok = proj[:, 2048:2176]
        v_tok = proj[:, 2176:]
        q_rot = rotary(q_raw.astype(F32), positions).astype(BF16)
        k_rot = rotary(k_tok[:, None, :].astype(F32), positions).astype(BF16)
        o8, k_new, v_new = call_b(lengths, q_rot, k_rot, v_tok[:, None, :], k_cache, v_cache)
        yT = call_c(hT, w2, w1f, ps, w_down, w_out, o8, xT)
        return yT.T, k_new, v_new

    row_spec = P(None, all_axes)
    vec_spec = P(all_axes)
    cache_spec = P(all_axes, None, None)
    return jax.shard_map(
        local_step,
        mesh=mesh,
        in_specs=(row_spec, vec_spec, P('x', None, 'yz'), P('x', 'yz'), P('yz', 'x'), P('yz', 'x'), cache_spec, cache_spec, vec_spec, vec_spec),
        out_specs=(row_spec, cache_spec, cache_spec),
        check_vma=False,
    )
```

```python
import functools

import jax
import jax.numpy as jnp
from jax import lax
from jax.experimental import pallas as pl
from jax.experimental.pallas import tpu as pltpu
from jax.sharding import PartitionSpec as P

LN_EPS = 1e-6
ROPE_BASE = 10000.0
MESH = pl.DeviceIdType.MESH


class Phase:
    cm = None

    def __call__(self, name):
        if self.cm is not None:
            self.cm.__exit__(None, None, None)
            self.cm = None
        if name:
            self.cm = jax.named_scope(name)
            self.cm.__enter__()


ph = Phase()
F32 = jnp.float32
BF16 = jnp.bfloat16

NZ = 4
NP = 8
C1A = 16
C1 = 48
C2 = 128
C3 = 80
CA = C1 + C2
CHUNKS = 4
LANES = 512 // CHUNKS


def rotary(values, positions):
    half_dim = values.shape[-1] // 2
    inv_freq = ROPE_BASE ** (-jnp.arange(half_dim, dtype=jnp.float32) / half_dim)
    angles = positions.astype(jnp.float32)[:, None, None] * inv_freq
    cos_part = jnp.cos(angles)
    sin_part = jnp.sin(angles)
    lo_half = values[..., :half_dim]
    hi_half = values[..., half_dim:]
    return jnp.concatenate([lo_half * cos_part - hi_half * sin_part, hi_half * cos_part + lo_half * sin_part], axis=-1)


def coords():
    z = lax.axis_index('x')
    p = lax.axis_index('yz')
    core = p % 2
    xx = (p // 2) % 2
    y = p // 4
    partner = p + 1 - 2 * core
    xn = p + 2 - 4 * xx
    yn = p + 4 - 8 * y
    diag = xn + 4 - 8 * y
    z1 = z % 2
    z2 = z // 2
    zs = [z, 2 * z2 + 1 - z1, 2 * (1 - z2) + z1, 3 - z]
    return z, p, core, partner, xn, yn, diag, zs


def entry_barrier(z, p, zs):
    sem = pltpu.get_barrier_semaphore()
    for k in range(1, NZ):
        pl.semaphore_signal(sem, inc=1, device_id=(zs[k], p), device_id_type=MESH)
    for k in range(1, NP):
        pl.semaphore_signal(sem, inc=1, device_id=(z, (p + k) % NP), device_id_type=MESH)
    pl.semaphore_wait(sem, NZ - 1 + NP - 1)


def rcopy(src, dst, send, recv, dev):
    return pltpu.make_async_remote_copy(src_ref=src, dst_ref=dst, send_sem=send, recv_sem=recv, device_id=dev, device_id_type=MESH)


class Relay:
    def __init__(self, z, p, at, whole, send, recv):
        self.z, self.p, self.at, self.whole, self.send, self.recv = z, p, at, whole, send, recv

    def copy(self, way, src, ch, dev):
        ref = self.at(src, ch)
        return rcopy(ref, ref, self.send.at[way], self.recv.at[src, ch], (dev, self.p))

    def inward(self, chunks):
        z = self.z

        @pl.when(z < 2)
        def _():
            for ch in chunks:
                self.copy(0, z, ch, z + 1).start()

        @pl.when(z >= 2)
        def _():
            for ch in chunks:
                self.copy(1, z, ch, z - 1).start()

    def outward(self, chunks):
        z = self.z

        @pl.when(z == 1)
        def _():
            for ch in chunks:
                self.copy(1, z, ch, z - 1).start()

        @pl.when(z == 2)
        def _():
            for ch in chunks:
                self.copy(0, z, ch, z + 1).start()

    def step(self, k, ch):
        z = self.z

        @pl.when(z >= k)
        def _():
            self.copy(0, z - k, ch, z).wait_recv()

            @pl.when(z < 3)
            def _():
                self.copy(2 * k, z - k, ch, z + 1).start()

        @pl.when(z + k <= 3)
        def _():
            self.copy(0, z + k, ch, z).wait_recv()

            @pl.when(z > 0)
            def _():
                self.copy(2 * k + 1, z + k, ch, z - 1).start()

    def sent(self, way):
        rcopy(self.whole, self.whole, self.send.at[way], self.recv.at[0, 0], (self.z, self.p)).wait_send()

    def drain(self):
        z = self.z
        for k in range(NZ - 1):
            @pl.when((z >= k) & (z < 3))
            def _():
                self.sent(2 * k)

            @pl.when((z + k <= 3) & (z > 0))
            def _():
                self.sent(2 * k + 1)


def attn_start(q):
    return pl.multiple_of(64 * q + 16 * (q // 2), 16)


def kernel_a(xT_hbm, ln_hbm, wattn_hbm, w_ref, h_ref, qkv_ref, w1f_ref, w2_ref, ps1_ref, ps2_ref, ps3_ref,
             xg, lng, watt, zsend, zrecv, zq, s1, s2, wn, wt, hT_ref, ln_ref, wattn_ref,
             xsend, xrecv, rpart, lsend, lrecv, asend, arecv, zsend_sem, zrecv_sem, qsend, qrecv, wsend, wrecv, lsem, osem, ldummy):
    z, p, core, partner, xn, yn, diag, zs = coords()
    ph('a_bar')
    wload = pltpu.make_async_copy(w_ref, wn, lsem.at[0])
    loads = [
        pltpu.make_async_copy(xT_hbm, xg.at[z, p], lsem.at[6]),
        pltpu.make_async_copy(ln_hbm, ln_ref, lsem.at[7]),
        pltpu.make_async_copy(wattn_hbm, wattn_ref, lsem.at[8]),
        wload,
    ]
    for c in loads:
        c.start()
    loads[1].wait()
    lng[z, p] = jnp.zeros((1, 128), F32)
    lng[z, p, 0:1, 0:64] = ln_ref[...]
    entry_barrier(z, p, zs)
    loads[0].wait()
    ph('a_zsend')
    here = (z, p)

    def send(src_z, src_p, dev, way=0):
        recv = rpart.at[0] if way == 4 else xrecv.at[way, src_z]
        rcopy(xg.at[src_z, src_p], xg.at[src_z, src_p], xsend.at[0], recv, dev).start()

    def send_l(src_z, dev, phase):
        rcopy(lng.at[src_z, p], lng.at[src_z, p], lsend.at[0], lrecv.at[phase], dev).start()

    def wait_x(src_z, src_p, way):
        rcopy(xg.at[src_z, src_p], xg.at[src_z, src_p], xsend.at[0], xrecv.at[way, src_z], here).wait_recv()

    def stat(src_z, src_p):
        blk = xg[src_z, src_p].astype(F32).reshape(8, 8, 512)
        s1[...] += jnp.sum(blk, axis=0)
        s2[...] += jnp.sum(blk * blk, axis=0)

    spans = tuple((i, C1A) for i in range(0, C1, C1A))

    def w_piece(i, src, dst, dev):
        o, n = spans[i]
        return rcopy(
            wt.at[:, pl.ds(pl.multiple_of(dst * 256 + o, 16), n), :],
            w1f_ref.at[src, :, pl.ds(o, n), :],
            wsend.at[0], wrecv.at[0], dev)

    def send_w(i):
        for k in (3, 2, 1):
            w_piece(i, z, zs[k], (zs[k], p)).start()

    def turn(odd):
        def body(i, carry):
            lanes = pl.ds(pl.multiple_of(i * 256 + odd * 128, 128), 128)
            blk = wn[:, :, lanes].astype(F32)
            for g in range(2):
                wt[g, lanes, :] = blk[:, g, :].T.astype(BF16)
            return carry

        lax.fori_loop(0, NZ, body, 0)

    mid = 2 - z // 2
    far = 3 - 3 * (z // 2)
    zo = [z, zs[1], mid, far]
    inner = (z == 1) | (z == 2)
    send(z, p, (mid, p))
    send(z, p, (zs[1], p))
    for k in (3, 2, 1):
        send_l(z, (zs[k], p), 0)
    targets = ((diag, 3), (xn, 1), (yn, 2), (partner, 4))
    for dev, way in targets:
        send(z, p, (z, dev), way)
    for j in range(1, NP):
        send_l(z, (z, (p + j) % NP), 1)

    def attn_piece(q):
        return rcopy(wattn_ref.at[pl.ds(attn_start(q), 80), :], watt.at[z], asend.at[0], arecv.at[0], (q, p))

    def outward(k):
        return rcopy(xg.at[zo[k], p], xg.at[zo[k], p], osem.at[k - 2], xrecv.at[0, zo[k]], (zs[1], p))

    s1[...] = jnp.zeros_like(s1)
    s2[...] = jnp.zeros_like(s2)
    stat(z, p)
    loads[2].wait()
    watt[z] = wattn_ref[pl.ds(attn_start(z), 80), :]
    wload.wait()
    turn(0)
    attn_piece(mid).start()

    @pl.when(jnp.logical_not(inner))
    def _():
        attn_piece(zs[1]).start()


    def column(k):
        wait_x(zo[k], p, 0)
        if k >= 2:
            @pl.when(inner)
            def _():
                outward(k).start()
        for dev, way in targets:
            send(zo[k], p, (z, dev), way)
        stat(zo[k], p)

    def pass_on(k, src, way):
        wait_x(zo[k], src, way)
        send(zo[k], src, (z, partner), 4)
        stat(zo[k], src)

    ph('a_col1')
    column(1)
    column(2)
    ph('a_col3')
    column(3)
    ph('a_lnsend')
    rcopy(ldummy.at[pl.ds(0, 3)], ldummy.at[pl.ds(0, 3)], lsend.at[0], lrecv.at[0], here).wait_recv()
    for k in range(1, NZ):
        for j in range(1, NP):
            send_l(zs[k], (z, (p + j) % NP), 1)
    ph('a_nbr')
    for k in range(2):
        pass_on(k, xn, 1)
        pass_on(k, yn, 2)
    ph('a_wattn')
    attn_piece(far).start()

    @pl.when(inner)
    def _():
        attn_piece(zs[1]).start()

    send_w(0)
    ph('a_nbr2')
    pass_on(0, diag, 3)
    pass_on(1, diag, 3)
    ph('a_nbr3')
    for k in range(2, NZ):
        pass_on(k, xn, 1)
        pass_on(k, yn, 2)
        pass_on(k, diag, 3)
    send_w(1)
    ph('a_rest')
    half = xg.at[pl.ds(0, 2)]
    rcopy(half, half, xsend.at[0], rpart.at[0], here).wait_recv()
    for q in (partner, partner + xn - p, partner + yn - p, partner + diag - p):
        for k in range(NZ):
            stat(zo[k], q)
    rcopy(ldummy.at[pl.ds(0, 28)], ldummy.at[pl.ds(0, 28)], lsend.at[0], lrecv.at[1], here).wait_recv()

    ph('a_norm')
    mean = jnp.sum(s1[...], axis=0, keepdims=True) / 2048.0
    var = jnp.sum(s2[...], axis=0, keepdims=True) / 2048.0 - mean * mean
    rstd = lax.rsqrt(var + LN_EPS)
    lnT = jnp.concatenate([lng[i // NP, i % NP, 0:1, :] for i in range(32)] + [jnp.zeros((96, 128), F32)], axis=0).T
    for i in range(NZ * NP):
        sc = lnT[0:64, i:i + 1]
        hT_ref[i * 64:(i + 1) * 64, :] = ((xg[i // NP, i % NP].astype(F32) - mean) * rstd * sc).astype(BF16)

    hout = pltpu.make_async_copy(hT_ref, h_ref, lsem.at[5])
    hout.start()
    ph('a_attw')
    three = watt.at[pl.ds(0, 3)]
    rcopy(three, three, asend.at[0], arecv.at[0], here).wait_recv()
    ph('a_zdot')
    part = None
    for q in range(NZ):
        t = jnp.dot(watt[q], hT_ref[q * 512:(q + 1) * 512, :], preferred_element_type=F32)
        part = t if part is None else part + t
    part = part.astype(BF16)
    for q in range(NZ):
        zsend[q] = part[:, q * 128:(q + 1) * 128]
    for k in (3, 2, 1):
        rcopy(zsend.at[zs[k]], zrecv.at[z], zsend_sem.at[0], zrecv_sem.at[0], (zs[k], p)).start()
    zrecv[z] = zsend[z]
    ph('a_turn')
    turn(1)
    send_w(2)
    outs = [pltpu.make_async_copy(wt, w2_ref, lsem.at[1])]
    for i, ps_ref in enumerate((ps1_ref, ps2_ref, ps3_ref)):
        dst = (z + i + 1) % NZ
        outs.append(pltpu.make_async_copy(wt.at[:, pl.ds(pl.multiple_of(dst * 256 + C1, 16), C2), :], ps_ref, lsem.at[2 + i]))
    for c in outs[1:] + outs[:1]:
        c.start()
    ph('a_zwait')
    zthree = rcopy(zsend.at[pl.ds(0, 3)], zrecv.at[pl.ds(0, 3)], zsend_sem.at[0], zrecv_sem.at[0], here)
    zthree.wait_recv()
    ph('a_a2a')
    zt = jnp.concatenate([zrecv[0].astype(F32), zrecv[1].astype(F32)[16:80], zrecv[2].astype(F32), zrecv[3].astype(F32)[16:80]], axis=0)
    zq[...] = zt.T.astype(BF16).reshape(NP, 16, 288)
    for j in range(1, NP):
        q = (p + j) % NP
        rcopy(zq.at[q], qkv_ref.at[p], qsend.at[0], qrecv.at[0], (z, q)).start()
    qown = pltpu.make_async_copy(zq.at[p], qkv_ref.at[p], lsem.at[9])
    qown.start()
    qseven = rcopy(zq.at[pl.ds(0, 7)], qkv_ref.at[pl.ds(0, 7)], qsend.at[0], qrecv.at[0], here)
    qseven.wait_recv()
    ph('a_wwait')
    wthree = w1f_ref.at[pl.ds(0, 3)]
    wall = rcopy(wthree, wthree, wsend.at[0], wrecv.at[0], here)
    wall.wait_recv()
    ph('a_sendwait')
    hout.wait()
    qown.wait()
    for c in outs:
        c.wait()
    sent30 = w2_ref.at[:, pl.ds(0, 960), :]
    rcopy(sent30, sent30, xsend.at[0], rpart.at[0], here).wait_send()
    rcopy(ldummy, ldummy, lsend.at[0], lrecv.at[0], here).wait_send()
    rcopy(three, three, asend.at[0], arecv.at[0], here).wait_send()
    zthree.wait_send()
    qseven.wait_send()
    wall.wait_send()

    @pl.when(inner)
    def _():
        outward(2).wait_send()
        outward(3).wait_send()
    ph('')


def call_a(xT, ln, wattnT, w):
    hbm = pl.BlockSpec(memory_space=pl.ANY)
    return pl.pallas_call(
        kernel_a,
        out_shape=(
            jax.ShapeDtypeStruct((2048, 512), BF16),
            jax.ShapeDtypeStruct((NP, 16, 288), BF16),
            jax.ShapeDtypeStruct((NZ, 2, C1, 512), BF16),
            jax.ShapeDtypeStruct((2, 1024, 512), BF16),
        ) + (jax.ShapeDtypeStruct((2, C2, 512), BF16),) * 3,
        in_specs=[hbm] * 4,
        out_specs=(hbm,) * 7,
        scratch_shapes=[
            pltpu.VMEM((NZ, NP, 64, 512), BF16),
            pltpu.VMEM((NZ, NP, 1, 128), F32),
            pltpu.VMEM((NZ, 80, 512), BF16),
            pltpu.VMEM((NZ, 80, 128), BF16),
            pltpu.VMEM((NZ, 80, 128), BF16),
            pltpu.VMEM((NP, 16, 288), BF16),
            pltpu.VMEM((8, 512), F32),
            pltpu.VMEM((8, 512), F32),
            pltpu.VMEM((512, 2, 1024), BF16),
            pltpu.VMEM((2, 1024, 512), BF16),
            pltpu.VMEM((2048, 512), BF16),
            pltpu.VMEM((1, 64), F32),
            pltpu.VMEM((288, 512), BF16),
            pltpu.SemaphoreType.DMA((1,)),
            pltpu.SemaphoreType.DMA((4, NZ)),
            pltpu.SemaphoreType.DMA((1,)),
            pltpu.SemaphoreType.DMA((1,)),
            pltpu.SemaphoreType.DMA((2,)),
            pltpu.SemaphoreType.DMA((1,)),
            pltpu.SemaphoreType.DMA((1,)),
            pltpu.SemaphoreType.DMA((1,)),
            pltpu.SemaphoreType.DMA((1,)),
            pltpu.SemaphoreType.DMA((1,)),
            pltpu.SemaphoreType.DMA((1,)),
            pltpu.SemaphoreType.DMA((1,)),
            pltpu.SemaphoreType.DMA((1,)),
            pltpu.SemaphoreType.DMA((10,)),
            pltpu.SemaphoreType.DMA((2,)),
            pltpu.VMEM((31, 1, 128), F32),
        ],
        compiler_params=pltpu.CompilerParams(collective_id=0, has_side_effects=True, vmem_limit_bytes=56 * 1024 * 1024),
        name='gather_norm_qkv',
    )(xT, ln, wattnT, w)


def kernel_b(len_ref, q_ref, k_ref, v_ref, kc_ref, vc_ref, o_ref, kn_ref, vn_ref, kbuf, vbuf, oscr, isem, osem):
    rows = kbuf.shape[0]
    seq = kbuf.shape[1]

    def load(b, t):
        return pltpu.make_async_copy((kc_ref, vc_ref)[t].at[b], (kbuf, vbuf)[t].at[b], isem.at[b])

    def store(b, t):
        return pltpu.make_async_copy((kbuf, vbuf)[t].at[b], (kn_ref, vn_ref)[t].at[b], osem.at[0])

    for b in range(rows):
        load(b, 0).start()
        load(b, 1).start()

    def insert(buf, b, length, new):
        base = pl.multiple_of((length // 16) * 16, 16)
        hit = base + lax.broadcasted_iota(jnp.int32, (16, 128), 0) == length
        buf[b, pl.ds(base, 16), :] = jnp.where(hit, new.astype(F32), buf[b, pl.ds(base, 16), :].astype(F32)).astype(BF16)

    def attend(b, length, n):
        scores = lax.dot_general(q_ref[b], kbuf[b, 0:n, :], (((1,), (1,)), ((), ())), preferred_element_type=F32) * (128.0 ** -0.5)
        slot = lax.broadcasted_iota(jnp.int32, scores.shape, 1)
        scores = jnp.where(slot <= length, scores, -1e30)
        top = jnp.max(scores, axis=1, keepdims=True)
        e = jnp.exp(scores - top)
        probs = (e / jnp.sum(e, axis=1, keepdims=True)).astype(BF16)
        return jnp.dot(probs, vbuf[b, 0:n, :], preferred_element_type=F32)

    def pair(i, carry):
        b0 = 2 * i
        b1 = 2 * i + 1
        l0 = len_ref[b0]
        l1 = len_ref[b1]
        for b, length in ((b0, l0), (b1, l1)):
            pltpu.make_async_copy(kc_ref.at[pl.ds(0, 2)], kbuf.at[pl.ds(0, 2)], isem.at[b]).wait()
            insert(kbuf, b, length, k_ref[b])
            insert(vbuf, b, length, v_ref[b])
        last = jnp.maximum(l0, l1) // 512
        for t in range(seq // 512):
            @pl.when(last == t)
            def _():
                n = 512 * (t + 1)
                r0 = attend(b0, l0, n)
                r1 = attend(b1, l1, n)
                oscr[b0] = r0
                oscr[b1] = r1
        for b in (b0, b1):
            store(b, 0).start()
            store(b, 1).start()
        return carry

    lax.fori_loop(0, rows // 2, pair, 0)
    for h in range(16):
        o_ref[h // 2, :, (h % 2) * 128:(h % 2 + 1) * 128] = oscr[:, h, :].astype(BF16)
    pltpu.make_async_copy(kbuf, kn_ref, osem.at[0]).wait()
    pltpu.make_async_copy(vbuf, vn_ref, osem.at[0]).wait()


def call_b(lengths, q_rot, k_rot, v_tok, k_cache, v_cache):
    rows, seq, hd = k_cache.shape
    heads = q_rot.shape[1]
    vm = pl.BlockSpec(memory_space=pltpu.VMEM)
    hbm = pl.BlockSpec(memory_space=pl.ANY)
    return pl.pallas_call(
        kernel_b,
        in_specs=[pl.BlockSpec(memory_space=pltpu.SMEM), vm, vm, vm, hbm, hbm],
        out_specs=(vm, hbm, hbm),
        out_shape=(
            jax.ShapeDtypeStruct((NP, rows, heads * hd // NP), BF16),
            jax.ShapeDtypeStruct(k_cache.shape, BF16),
            jax.ShapeDtypeStruct(v_cache.shape, BF16),
        ),
        scratch_shapes=[
            pltpu.VMEM((rows, seq, hd), BF16),
            pltpu.VMEM((rows, seq, hd), BF16),
            pltpu.VMEM((rows, heads, hd), F32),
            pltpu.SemaphoreType.DMA((rows,)),
            pltpu.SemaphoreType.DMA((1,)),
        ],
        compiler_params=pltpu.CompilerParams(vmem_limit_bytes=58 * 1024 * 1024),
        cost_estimate=pl.CostEstimate(flops=12_000_000_000, bytes_accessed=33_000_000, transcendentals=0),
        name='attend',
    )(lengths, q_rot, k_rot, v_tok, k_cache, v_cache)


def kernel_c(hT, w2_ref, w1f_ref, p1_ref, p2_ref, p3_ref, wd, wo, o_ref, xT_ref, y_ref,
             wvA, wvB, wdAT, wdBT, woT, og, hidA, hidB, yA, ysum, r1, acc, r2,
             wsem, wbsend, wbrecv, osend, orecv, gsend, grecv, hasend, harecv, hbsend, hbrecv,
             r1send, r1recv, r2send, r2recv):
    z, p, core, partner, xn, yn, diag, zs = coords()
    ph('c_bar')
    local = [pltpu.make_async_copy(w2_ref.at[:, pl.ds(pl.multiple_of(z * 256, 256), CA), :], wvA.at[z], wsem.at[0])]
    for s, p_ref in ((1, p1_ref), (2, p2_ref), (3, p3_ref)):
        src = (z + NZ - s) % NZ
        local.append(pltpu.make_async_copy(w1f_ref.at[src], wvA.at[src, :, pl.ds(0, C1), :], wsem.at[0]))
        local.append(pltpu.make_async_copy(p_ref, wvA.at[src, :, pl.ds(C1, C2), :], wsem.at[0]))
    late = [
        pltpu.make_async_copy(w2_ref.at[:, pl.ds(pl.multiple_of(z * 256 + CA, 16), C3), :], wvB.at[z], wsem.at[1]),
    ]
    for c in local + late:
        c.start()
    entry_barrier(z, p, zs)
    here = (z, p)

    ph('c_send')
    def w_piece(src, dst, dev):
        return rcopy(
            w2_ref.at[:, pl.ds(pl.multiple_of(dst * 256 + CA, 16), C3), :],
            wvB.at[src], wbsend.at[0], wbrecv.at[0], dev)

    for k in (3, 2, 1):
        w_piece(z, zs[k], (zs[k], p)).start()
    for j in range(1, NP):
        q = (p + j) % NP
        rcopy(o_ref.at[q], og.at[z, p], osend.at[0], orecv.at[0], (z, q)).start()
    og[z, p] = o_ref[p]

    def gated(wv, n):
        g = None
        for q in range(NZ):
            t = jnp.dot(wv[q].reshape(2 * n, 512), hT[q * 512:(q + 1) * 512, :], preferred_element_type=F32)
            g = t if g is None else g + t
        gate = g[0:n].astype(BF16).astype(F32)
        up = g[n:2 * n].astype(BF16).astype(F32)
        return (jax.nn.silu(gate) * up).astype(BF16)

    ra = Relay(z, p, lambda src, ch: hidA.at[ch, src], hidA.at[0], hasend, harecv)
    rb = Relay(z, p, lambda src, ch: hidB.at[ch, src], hidB.at[0], hbsend, hbrecv)
    ro = Relay(z, p, lambda src, ch: og.at[src], og.at[0], gsend, grecv)
    every = range(CHUNKS)

    ph('c_localwait')
    pltpu.make_async_copy(wvA, wvA, wsem.at[0]).wait()
    ph('c_gA')
    ha = gated(wvA, CA)
    for ch in every:
        hidA[ch, z] = ha[:, ch * LANES:(ch + 1) * LANES]

    ra.outward(every)
    ra.inward(range(2))
    ph('c_owait')
    oseven = rcopy(o_ref.at[pl.ds(0, 7)], og.at[z, pl.ds(0, 7)], osend.at[0], orecv.at[0], here)
    oseven.wait_recv()
    ro.outward(range(1))
    ro.inward(range(1))
    ph('c_transp')
    for c in late:
        c.wait()
    def by_core(ref, w):
        w = w.T.reshape(4, 2, 64, w.shape[0])
        for j in range(2):
            ref[j] = w[:, j].reshape(256, w.shape[3])

    by_core(wdAT, jnp.concatenate([wd[q * 256:q * 256 + CA, :] for q in range(NZ)], axis=0))
    by_core(wdBT, jnp.concatenate([wd[q * 256 + CA:(q + 1) * 256, :] for q in range(NZ)], axis=0))
    by_core(woT, wo[...])

    ph('c_wBwait')
    ph('c_wBwait2')
    wthree = wvB.at[pl.ds(0, 3)]
    wall = rcopy(wthree, wthree, wbsend.at[0], wbrecv.at[0], here)
    wall.wait_recv()
    ph('c_gB')
    hb = gated(wvB, C3)
    for ch in range(CHUNKS):
        hidB[ch, z] = hb[:, ch * LANES:(ch + 1) * LANES]
    ph('c_own')
    rb.outward(every)
    rb.inward(range(2))
    for ch in range(2, CHUNKS):
        ra.inward((ch,))
        rb.inward((ch,))
    ph('c_step1')
    ro.step(1, 0)
    for ch in range(2):
        ra.step(1, ch)
    ph('c_step2')
    for ch in range(2):
        ra.step(2, ch)

    chip = p // 2
    others = [diag // 2, xn // 2, yn // 2]

    def d2d(ch):
        return rcopy(ysum.at[ch, 1 - core], r1.at[ch], r1send.at[0], r1recv.at[ch], (z, partner))

    def hop(ch, i, dev):
        return rcopy(acc.at[ch, i], r2.at[ch, i], r2send.at[0], r2recv.at[ch], (z, dev))

    def stage0(ch):
        o_rows = og[ch * NZ // CHUNKS].reshape(128, 256)
        for j in (1 - core, core):
            yA[j] = jnp.dot(wdAT[j], hidA[ch].reshape(NZ * CA, LANES), preferred_element_type=F32) + lax.dot_general(
                woT[j], o_rows, (((1,), (1,)), ((), ())), preferred_element_type=F32)

    def half(ch, j):
        yt = yA[j] + jnp.dot(wdBT[j], hidB[ch].reshape(NZ * C3, LANES), preferred_element_type=F32)
        ysum[ch, j] = yt.reshape(4, 64, LANES)

    def stage1(ch):
        half(ch, 1 - core)
        d2d(ch).start()
        half(ch, core)

    def stage2(ch):
        d2d(ch).wait_recv()
        for i, (t, dev) in enumerate(zip(others, (diag, xn, yn))):
            acc[ch, i] = ysum[ch, core, t] + r1[ch, t]
            hop(ch, i, dev).start()

    def stage3(ch):
        lanes = slice(ch * LANES, (ch + 1) * LANES)
        mine = ysum[ch, core, chip] + r1[ch, chip]
        rcopy(acc.at[ch], r2.at[ch], r2send.at[0], r2recv.at[ch], here).wait_recv()
        for i in range(3):
            mine = mine + r2[ch, i]
        y_ref[:, lanes] = (xT_ref[:, lanes].astype(F32) + mine).astype(BF16)

    for t in range(1, CHUNKS + 3):
        ph(f'c_wave{t}')
        for k in range(1, NZ - 1):
            ch = t - k
            if 0 <= ch < CHUNKS:
                if ch >= 2:
                    ra.step(k, ch)
                rb.step(k, ch)
        if t < 3:
            ro.step(t + 1, 0)
        ph(f'c_sum{t}')
        if t >= 3:
            ra.step(3, t - 3)
            stage0(t - 3)
            rb.step(3, t - 3)
            stage1(t - 3)
        if t >= 4:
            stage2(t - 4)
    ph('c_last2')
    stage2(CHUNKS - 1)
    ph('c_last3')
    for ch in every:
        stage3(ch)

    ph('c_end')
    wall.wait_send()
    oseven.wait_send()
    rcopy(r1, r1, r1send.at[0], r1recv.at[0], here).wait_send()
    rcopy(acc, acc, r2send.at[0], r2recv.at[0], here).wait_send()
    ra.drain()
    rb.drain()
    ro.drain()
    ph('')


def call_c(hT, w2, w1f, ps, wd, wo, o8, xT):
    vm = pl.BlockSpec(memory_space=pltpu.VMEM)
    hbm = pl.BlockSpec(memory_space=pl.ANY)
    return pl.pallas_call(
        kernel_c,
        out_shape=jax.ShapeDtypeStruct((64, 512), BF16),
        in_specs=[vm] + [hbm] * 5 + [vm] * 4,
        out_specs=vm,
        scratch_shapes=[
            pltpu.VMEM((NZ, 2, CA, 512), BF16),
            pltpu.VMEM((NZ, 2, C3, 512), BF16),
            pltpu.VMEM((2, 256, NZ * CA), BF16),
            pltpu.VMEM((2, 256, NZ * C3), BF16),
            pltpu.VMEM((2, 256, 256), BF16),
            pltpu.VMEM((NZ, NP, 16, 256), BF16),
            pltpu.VMEM((CHUNKS, NZ, CA, LANES), BF16),
            pltpu.VMEM((CHUNKS, NZ, C3, LANES), BF16),
            pltpu.VMEM((2, 256, LANES), F32),
            pltpu.VMEM((CHUNKS, 2, 4, 64, LANES), F32),
            pltpu.VMEM((CHUNKS, 4, 64, LANES), F32),
            pltpu.VMEM((CHUNKS, 3, 64, LANES), F32),
            pltpu.VMEM((CHUNKS, 3, 64, LANES), F32),
            pltpu.SemaphoreType.DMA((2,)),
            pltpu.SemaphoreType.DMA((1,)),
            pltpu.SemaphoreType.DMA((1,)),
            pltpu.SemaphoreType.DMA((1,)),
            pltpu.SemaphoreType.DMA((1,)),
            pltpu.SemaphoreType.DMA((6,)),
            pltpu.SemaphoreType.DMA((NZ, 1)),
            pltpu.SemaphoreType.DMA((6,)),
            pltpu.SemaphoreType.DMA((NZ, CHUNKS)),
            pltpu.SemaphoreType.DMA((6,)),
            pltpu.SemaphoreType.DMA((NZ, CHUNKS)),
            pltpu.SemaphoreType.DMA((1,)),
            pltpu.SemaphoreType.DMA((CHUNKS,)),
            pltpu.SemaphoreType.DMA((1,)),
            pltpu.SemaphoreType.DMA((CHUNKS,)),
        ],
        compiler_params=pltpu.CompilerParams(collective_id=1, has_side_effects=True, vmem_limit_bytes=40 * 1024 * 1024),
        cost_estimate=pl.CostEstimate(flops=12_000_000_000, bytes_accessed=6_000_000, transcendentals=0),
        name='mlp_out',
    )(hT, w2, w1f, *ps, wd, wo, o8, xT)


def solution(mesh):
    all_axes = ('x', 'yz')

    def local_step(x_in, ln_scale, w_gate_up, w_attn, w_down, w_out, k_cache, v_cache, lengths, positions):
        xT = x_in.T
        wattnT = w_attn.T
        hT, qkv, w1f, w2, *pieces = call_a(xT, ln_scale[None, :], wattnT, w_gate_up)
        ps = [lax.ppermute(pieces[i], 'x', [(q, (q + i + 1) % NZ) for q in range(NZ)]) for i in range(NZ - 1)]
        proj = jnp.transpose(qkv, (1, 0, 2)).reshape(16, 2304)
        q_raw = proj[:, :2048].reshape(16, 16, 128)
        k_tok = proj[:, 2048:2176]
        v_tok = proj[:, 2176:]
        q_rot = rotary(q_raw.astype(F32), positions).astype(BF16)
        k_rot = rotary(k_tok[:, None, :].astype(F32), positions).astype(BF16)
        o8, k_new, v_new = call_b(lengths, q_rot, k_rot, v_tok[:, None, :], k_cache, v_cache)
        yT = call_c(hT, w2, w1f, ps, w_down, w_out, o8, xT)
        return yT.T, k_new, v_new

    row_spec = P(None, all_axes)
    vec_spec = P(all_axes)
    cache_spec = P(all_axes, None, None)
    return jax.shard_map(
        local_step,
        mesh=mesh,
        in_specs=(row_spec, vec_spec, P('x', None, 'yz'), P('x', 'yz'), P('yz', 'x'), P('yz', 'x'), cache_spec, cache_spec, vec_spec, vec_spec),
        out_specs=(row_spec, cache_spec, cache_spec),
        check_vma=False,
    )
```

```python
import functools

import jax
import jax.numpy as jnp
from jax import lax
from jax.experimental import pallas as pl
from jax.experimental.pallas import tpu as pltpu
from jax.sharding import PartitionSpec as P

LN_EPS = 1e-6
ROPE_BASE = 10000.0
MESH = pl.DeviceIdType.MESH


class Phase:
    cm = None

    def __call__(self, name):
        if self.cm is not None:
            self.cm.__exit__(None, None, None)
            self.cm = None
        if name:
            self.cm = jax.named_scope(name)
            self.cm.__enter__()


ph = Phase()
F32 = jnp.float32
BF16 = jnp.bfloat16

NZ = 4
NP = 8
C1A = 16
C1 = 48
C2 = 128
C3 = 80
CA = C1 + C2
CHUNKS = 4
LANES = 512 // CHUNKS


def rotary(values, positions):
    half_dim = values.shape[-1] // 2
    inv_freq = ROPE_BASE ** (-jnp.arange(half_dim, dtype=jnp.float32) / half_dim)
    angles = positions.astype(jnp.float32)[:, None, None] * inv_freq
    cos_part = jnp.cos(angles)
    sin_part = jnp.sin(angles)
    lo_half = values[..., :half_dim]
    hi_half = values[..., half_dim:]
    return jnp.concatenate([lo_half * cos_part - hi_half * sin_part, hi_half * cos_part + lo_half * sin_part], axis=-1)


def coords():
    z = lax.axis_index('x')
    p = lax.axis_index('yz')
    core = p % 2
    xx = (p // 2) % 2
    y = p // 4
    partner = p + 1 - 2 * core
    xn = p + 2 - 4 * xx
    yn = p + 4 - 8 * y
    diag = xn + 4 - 8 * y
    z1 = z % 2
    z2 = z // 2
    zs = [z, 2 * z2 + 1 - z1, 2 * (1 - z2) + z1, 3 - z]
    return z, p, core, partner, xn, yn, diag, zs


def entry_barrier(z, p, zs):
    sem = pltpu.get_barrier_semaphore()
    for k in range(1, NZ):
        pl.semaphore_signal(sem, inc=1, device_id=(zs[k], p), device_id_type=MESH)
    for k in range(1, NP):
        pl.semaphore_signal(sem, inc=1, device_id=(z, (p + k) % NP), device_id_type=MESH)
    pl.semaphore_wait(sem, NZ - 1 + NP - 1)


def rcopy(src, dst, send, recv, dev):
    return pltpu.make_async_remote_copy(src_ref=src, dst_ref=dst, send_sem=send, recv_sem=recv, device_id=dev, device_id_type=MESH)


class Relay:
    def __init__(self, z, p, at, whole, send, recv):
        self.z, self.p, self.at, self.whole, self.send, self.recv = z, p, at, whole, send, recv

    def copy(self, way, src, ch, dev):
        ref = self.at(src, ch)
        return rcopy(ref, ref, self.send.at[way], self.recv.at[src, ch], (dev, self.p))

    def inward(self, chunks):
        z = self.z

        @pl.when(z < 2)
        def _():
            for ch in chunks:
                self.copy(0, z, ch, z + 1).start()

        @pl.when(z >= 2)
        def _():
            for ch in chunks:
                self.copy(1, z, ch, z - 1).start()

    def outward(self, chunks):
        z = self.z

        @pl.when(z == 1)
        def _():
            for ch in chunks:
                self.copy(1, z, ch, z - 1).start()

        @pl.when(z == 2)
        def _():
            for ch in chunks:
                self.copy(0, z, ch, z + 1).start()

    def step(self, k, ch):
        z = self.z

        @pl.when(z >= k)
        def _():
            self.copy(0, z - k, ch, z).wait_recv()

            @pl.when(z < 3)
            def _():
                self.copy(2 * k, z - k, ch, z + 1).start()

        @pl.when(z + k <= 3)
        def _():
            self.copy(0, z + k, ch, z).wait_recv()

            @pl.when(z > 0)
            def _():
                self.copy(2 * k + 1, z + k, ch, z - 1).start()

    def sent(self, way):
        rcopy(self.whole, self.whole, self.send.at[way], self.recv.at[0, 0], (self.z, self.p)).wait_send()

    def drain(self):
        z = self.z
        for k in range(NZ - 1):
            @pl.when((z >= k) & (z < 3))
            def _():
                self.sent(2 * k)

            @pl.when((z + k <= 3) & (z > 0))
            def _():
                self.sent(2 * k + 1)


def attn_start(q):
    return pl.multiple_of(64 * q + 16 * (q // 2), 16)


def kernel_a(xT_hbm, ln_hbm, wattn_hbm, w_ref, h_ref, qkv_ref, w1f_ref, w2_ref, ps1_ref, ps2_ref, ps3_ref,
             xg, lng, watt, zsend, zrecv, zq, s1, s2, wn, wt, hT_ref, ln_ref, wattn_ref,
             xsend, xrecv, rpart, lsend, lrecv, asend, arecv, zsend_sem, zrecv_sem, qsend, qrecv, wsend, wrecv, lsem, osem, ldummy):
    z, p, core, partner, xn, yn, diag, zs = coords()
    ph('a_bar')
    wload = pltpu.make_async_copy(w_ref, wn, lsem.at[0])
    loads = [
        pltpu.make_async_copy(xT_hbm, xg.at[z, p], lsem.at[6]),
        pltpu.make_async_copy(ln_hbm, ln_ref, lsem.at[7]),
        pltpu.make_async_copy(wattn_hbm, wattn_ref, lsem.at[8]),
        wload,
    ]
    for c in loads:
        c.start()
    loads[1].wait()
    lng[z, p] = jnp.zeros((1, 128), F32)
    lng[z, p, 0:1, 0:64] = ln_ref[...]
    entry_barrier(z, p, zs)
    loads[0].wait()
    ph('a_zsend')
    here = (z, p)

    def send(src_z, src_p, dev, way=0):
        recv = rpart.at[0] if way == 4 else xrecv.at[way, src_z]
        rcopy(xg.at[src_z, src_p], xg.at[src_z, src_p], xsend.at[0], recv, dev).start()

    def send_l(src_z, dev, phase):
        rcopy(lng.at[src_z, p], lng.at[src_z, p], lsend.at[0], lrecv.at[phase], dev).start()

    def wait_x(src_z, src_p, way):
        rcopy(xg.at[src_z, src_p], xg.at[src_z, src_p], xsend.at[0], xrecv.at[way, src_z], here).wait_recv()

    def stat(src_z, src_p):
        blk = xg[src_z, src_p].astype(F32).reshape(8, 8, 512)
        s1[...] += jnp.sum(blk, axis=0)
        s2[...] += jnp.sum(blk * blk, axis=0)

    spans = tuple((i, C1A) for i in range(0, C1, C1A))

    def w_piece(i, src, dst, dev):
        o, n = spans[i]
        return rcopy(
            wt.at[:, pl.ds(pl.multiple_of(dst * 256 + o, 16), n), :],
            w1f_ref.at[src, :, pl.ds(o, n), :],
            wsend.at[0], wrecv.at[0], dev)

    def send_w(i):
        for k in (3, 2, 1):
            w_piece(i, z, zs[k], (zs[k], p)).start()

    def turn(odd):
        def body(i, carry):
            lanes = pl.ds(pl.multiple_of(i * 256 + odd * 128, 128), 128)
            blk = wn[:, :, lanes].astype(F32)
            for g in range(2):
                wt[g, lanes, :] = blk[:, g, :].T.astype(BF16)
            return carry

        lax.fori_loop(0, NZ, body, 0)

    mid = 2 - z // 2
    far = 3 - 3 * (z // 2)
    zo = [z, zs[1], mid, far]
    inner = (z == 1) | (z == 2)
    send(z, p, (mid, p))
    send(z, p, (zs[1], p))
    for k in (3, 2, 1):
        send_l(z, (zs[k], p), 0)
    targets = ((diag, 3), (xn, 1), (yn, 2), (partner, 4))
    for dev, way in targets:
        send(z, p, (z, dev), way)
    for j in range(1, NP):
        send_l(z, (z, (p + j) % NP), 1)

    def attn_piece(q):
        return rcopy(wattn_ref.at[pl.ds(attn_start(q), 80), :], watt.at[z], asend.at[0], arecv.at[0], (q, p))

    def outward(k):
        return rcopy(xg.at[zo[k], p], xg.at[zo[k], p], osem.at[k - 2], xrecv.at[0, zo[k]], (zs[1], p))

    s1[...] = jnp.zeros_like(s1)
    s2[...] = jnp.zeros_like(s2)
    stat(z, p)
    loads[2].wait()
    watt[z] = wattn_ref[pl.ds(attn_start(z), 80), :]
    wload.wait()
    turn(0)
    attn_piece(mid).start()

    @pl.when(jnp.logical_not(inner))
    def _():
        attn_piece(zs[1]).start()


    def column(k):
        wait_x(zo[k], p, 0)
        if k >= 2:
            @pl.when(inner)
            def _():
                outward(k).start()
        for dev, way in targets:
            send(zo[k], p, (z, dev), way)
        stat(zo[k], p)

    def pass_on(k, src, way):
        wait_x(zo[k], src, way)
        send(zo[k], src, (z, partner), 4)
        stat(zo[k], src)

    ph('a_col1')
    column(1)
    column(2)
    ph('a_col3')
    column(3)
    ph('a_lnsend')
    rcopy(ldummy.at[pl.ds(0, 3)], ldummy.at[pl.ds(0, 3)], lsend.at[0], lrecv.at[0], here).wait_recv()
    for k in range(1, NZ):
        for j in range(1, NP):
            send_l(zs[k], (z, (p + j) % NP), 1)
    ph('a_nbr')
    for k in range(2):
        pass_on(k, xn, 1)
        pass_on(k, yn, 2)
    ph('a_wattn')
    attn_piece(far).start()

    @pl.when(inner)
    def _():
        attn_piece(zs[1]).start()

    send_w(0)
    ph('a_nbr2')
    pass_on(0, diag, 3)
    pass_on(1, diag, 3)
    ph('a_nbr3')
    for k in range(2, NZ):
        pass_on(k, xn, 1)
        pass_on(k, yn, 2)
        pass_on(k, diag, 3)
    send_w(1)
    ph('a_rest')
    half = xg.at[pl.ds(0, 2)]
    rcopy(half, half, xsend.at[0], rpart.at[0], here).wait_recv()
    for q in (partner, partner + xn - p, partner + yn - p, partner + diag - p):
        for k in range(NZ):
            stat(zo[k], q)
    rcopy(ldummy.at[pl.ds(0, 28)], ldummy.at[pl.ds(0, 28)], lsend.at[0], lrecv.at[1], here).wait_recv()

    ph('a_norm')
    mean = jnp.sum(s1[...], axis=0, keepdims=True) / 2048.0
    var = jnp.sum(s2[...], axis=0, keepdims=True) / 2048.0 - mean * mean
    rstd = lax.rsqrt(var + LN_EPS)
    lnT = jnp.concatenate([lng[i // NP, i % NP, 0:1, :] for i in range(32)] + [jnp.zeros((96, 128), F32)], axis=0).T
    for i in range(NZ * NP):
        sc = lnT[0:64, i:i + 1]
        hT_ref[i * 64:(i + 1) * 64, :] = ((xg[i // NP, i % NP].astype(F32) - mean) * rstd * sc).astype(BF16)

    hout = pltpu.make_async_copy(hT_ref, h_ref, lsem.at[5])
    hout.start()
    ph('a_attw')
    three = watt.at[pl.ds(0, 3)]
    rcopy(three, three, asend.at[0], arecv.at[0], here).wait_recv()
    ph('a_zdot')
    part = None
    for q in range(NZ):
        t = jnp.dot(watt[q], hT_ref[q * 512:(q + 1) * 512, :], preferred_element_type=F32)
        part = t if part is None else part + t
    part = part.astype(BF16)
    for q in range(NZ):
        zsend[q] = part[:, q * 128:(q + 1) * 128]
    for k in (3, 2, 1):
        rcopy(zsend.at[zs[k]], zrecv.at[z], zsend_sem.at[0], zrecv_sem.at[0], (zs[k], p)).start()
    zrecv[z] = zsend[z]
    ph('a_turn')
    turn(1)
    send_w(2)
    outs = [pltpu.make_async_copy(wt, w2_ref, lsem.at[1])]
    for i, ps_ref in enumerate((ps1_ref, ps2_ref, ps3_ref)):
        n = ps_ref.shape[1]
        outs.append(pltpu.make_async_copy(wt.at[:, pl.ds(pl.multiple_of(zs[i + 1] * 256 + C1, 16), n), :], ps_ref, lsem.at[2 + i]))
    for c in outs[1:] + outs[:1]:
        c.start()
    ph('a_zwait')
    zthree = rcopy(zsend.at[pl.ds(0, 3)], zrecv.at[pl.ds(0, 3)], zsend_sem.at[0], zrecv_sem.at[0], here)
    zthree.wait_recv()
    ph('a_a2a')
    zt = jnp.concatenate([zrecv[0].astype(F32), zrecv[1].astype(F32)[16:80], zrecv[2].astype(F32), zrecv[3].astype(F32)[16:80]], axis=0)
    zq[...] = zt.T.astype(BF16).reshape(NP, 16, 288)
    for j in range(1, NP):
        q = (p + j) % NP
        rcopy(zq.at[q], qkv_ref.at[p], qsend.at[0], qrecv.at[0], (z, q)).start()
    qown = pltpu.make_async_copy(zq.at[p], qkv_ref.at[p], lsem.at[9])
    qown.start()
    qseven = rcopy(zq.at[pl.ds(0, 7)], qkv_ref.at[pl.ds(0, 7)], qsend.at[0], qrecv.at[0], here)
    qseven.wait_recv()
    ph('a_wwait')
    wthree = w1f_ref.at[pl.ds(0, 3)]
    wall = rcopy(wthree, wthree, wsend.at[0], wrecv.at[0], here)
    wall.wait_recv()
    ph('a_sendwait')
    hout.wait()
    qown.wait()
    for c in outs:
        c.wait()
    sent30 = w2_ref.at[:, pl.ds(0, 960), :]
    rcopy(sent30, sent30, xsend.at[0], rpart.at[0], here).wait_send()
    rcopy(ldummy, ldummy, lsend.at[0], lrecv.at[0], here).wait_send()
    rcopy(three, three, asend.at[0], arecv.at[0], here).wait_send()
    zthree.wait_send()
    qseven.wait_send()
    wall.wait_send()

    @pl.when(inner)
    def _():
        outward(2).wait_send()
        outward(3).wait_send()
    ph('')


def call_a(xT, ln, wattnT, w):
    hbm = pl.BlockSpec(memory_space=pl.ANY)
    return pl.pallas_call(
        kernel_a,
        out_shape=(
            jax.ShapeDtypeStruct((2048, 512), BF16),
            jax.ShapeDtypeStruct((NP, 16, 288), BF16),
            jax.ShapeDtypeStruct((NZ, 2, C1, 512), BF16),
            jax.ShapeDtypeStruct((2, 1024, 512), BF16),
                    jax.ShapeDtypeStruct((2, C2 + C3, 512), BF16),
            jax.ShapeDtypeStruct((2, C2, 512), BF16),
            jax.ShapeDtypeStruct((2, C2, 512), BF16),
        ),
        in_specs=[hbm] * 4,
        out_specs=(hbm,) * 7,
        scratch_shapes=[
            pltpu.VMEM((NZ, NP, 64, 512), BF16),
            pltpu.VMEM((NZ, NP, 1, 128), F32),
            pltpu.VMEM((NZ, 80, 512), BF16),
            pltpu.VMEM((NZ, 80, 128), BF16),
            pltpu.VMEM((NZ, 80, 128), BF16),
            pltpu.VMEM((NP, 16, 288), BF16),
            pltpu.VMEM((8, 512), F32),
            pltpu.VMEM((8, 512), F32),
            pltpu.VMEM((512, 2, 1024), BF16),
            pltpu.VMEM((2, 1024, 512), BF16),
            pltpu.VMEM((2048, 512), BF16),
            pltpu.VMEM((1, 64), F32),
            pltpu.VMEM((288, 512), BF16),
            pltpu.SemaphoreType.DMA((1,)),
            pltpu.SemaphoreType.DMA((4, NZ)),
            pltpu.SemaphoreType.DMA((1,)),
            pltpu.SemaphoreType.DMA((1,)),
            pltpu.SemaphoreType.DMA((2,)),
            pltpu.SemaphoreType.DMA((1,)),
            pltpu.SemaphoreType.DMA((1,)),
            pltpu.SemaphoreType.DMA((1,)),
            pltpu.SemaphoreType.DMA((1,)),
            pltpu.SemaphoreType.DMA((1,)),
            pltpu.SemaphoreType.DMA((1,)),
            pltpu.SemaphoreType.DMA((1,)),
            pltpu.SemaphoreType.DMA((1,)),
            pltpu.SemaphoreType.DMA((10,)),
            pltpu.SemaphoreType.DMA((2,)),
            pltpu.VMEM((31, 1, 128), F32),
        ],
        compiler_params=pltpu.CompilerParams(collective_id=0, has_side_effects=True, vmem_limit_bytes=56 * 1024 * 1024),
        name='gather_norm_qkv',
    )(xT, ln, wattnT, w)


def kernel_b(len_ref, q_ref, k_ref, v_ref, kc_ref, vc_ref, o_ref, kn_ref, vn_ref, kbuf, vbuf, oscr, isem, osem):
    rows = kbuf.shape[0]
    seq = kbuf.shape[1]

    def load(b, t):
        return pltpu.make_async_copy((kc_ref, vc_ref)[t].at[b], (kbuf, vbuf)[t].at[b], isem.at[b])

    def store(b, t):
        return pltpu.make_async_copy((kbuf, vbuf)[t].at[b], (kn_ref, vn_ref)[t].at[b], osem.at[0])

    for b in range(rows):
        load(b, 0).start()
        load(b, 1).start()

    def insert(buf, b, length, new):
        base = pl.multiple_of((length // 16) * 16, 16)
        hit = base + lax.broadcasted_iota(jnp.int32, (16, 128), 0) == length
        buf[b, pl.ds(base, 16), :] = jnp.where(hit, new.astype(F32), buf[b, pl.ds(base, 16), :].astype(F32)).astype(BF16)

    def attend(b, length, n):
        scores = lax.dot_general(q_ref[b], kbuf[b, 0:n, :], (((1,), (1,)), ((), ())), preferred_element_type=F32) * (128.0 ** -0.5)
        slot = lax.broadcasted_iota(jnp.int32, scores.shape, 1)
        scores = jnp.where(slot <= length, scores, -1e30)
        top = jnp.max(scores, axis=1, keepdims=True)
        e = jnp.exp(scores - top)
        probs = (e / jnp.sum(e, axis=1, keepdims=True)).astype(BF16)
        return jnp.dot(probs, vbuf[b, 0:n, :], preferred_element_type=F32)

    def pair(i, carry):
        b0 = 2 * i
        b1 = 2 * i + 1
        l0 = len_ref[b0]
        l1 = len_ref[b1]
        for b, length in ((b0, l0), (b1, l1)):
            pltpu.make_async_copy(kc_ref.at[pl.ds(0, 2)], kbuf.at[pl.ds(0, 2)], isem.at[b]).wait()
            insert(kbuf, b, length, k_ref[b])
            insert(vbuf, b, length, v_ref[b])
        last = jnp.maximum(l0, l1) // 512
        for t in range(seq // 512):
            @pl.when(last == t)
            def _():
                n = 512 * (t + 1)
                r0 = attend(b0, l0, n)
                r1 = attend(b1, l1, n)
                oscr[b0] = r0
                oscr[b1] = r1
        for b in (b0, b1):
            store(b, 0).start()
            store(b, 1).start()
        return carry

    lax.fori_loop(0, rows // 2, pair, 0)
    for h in range(16):
        o_ref[h // 2, :, (h % 2) * 128:(h % 2 + 1) * 128] = oscr[:, h, :].astype(BF16)
    pltpu.make_async_copy(kbuf, kn_ref, osem.at[0]).wait()
    pltpu.make_async_copy(vbuf, vn_ref, osem.at[0]).wait()


def call_b(lengths, q_rot, k_rot, v_tok, k_cache, v_cache):
    rows, seq, hd = k_cache.shape
    heads = q_rot.shape[1]
    vm = pl.BlockSpec(memory_space=pltpu.VMEM)
    hbm = pl.BlockSpec(memory_space=pl.ANY)
    return pl.pallas_call(
        kernel_b,
        in_specs=[pl.BlockSpec(memory_space=pltpu.SMEM), vm, vm, vm, hbm, hbm],
        out_specs=(vm, hbm, hbm),
        out_shape=(
            jax.ShapeDtypeStruct((NP, rows, heads * hd // NP), BF16),
            jax.ShapeDtypeStruct(k_cache.shape, BF16),
            jax.ShapeDtypeStruct(v_cache.shape, BF16),
        ),
        scratch_shapes=[
            pltpu.VMEM((rows, seq, hd), BF16),
            pltpu.VMEM((rows, seq, hd), BF16),
            pltpu.VMEM((rows, heads, hd), F32),
            pltpu.SemaphoreType.DMA((rows,)),
            pltpu.SemaphoreType.DMA((1,)),
        ],
        compiler_params=pltpu.CompilerParams(vmem_limit_bytes=58 * 1024 * 1024),
        cost_estimate=pl.CostEstimate(flops=12_000_000_000, bytes_accessed=33_000_000, transcendentals=0),
        name='attend',
    )(lengths, q_rot, k_rot, v_tok, k_cache, v_cache)


def kernel_c(hT, w2_ref, w1f_ref, p1_ref, p2_ref, p3_ref, wd, wo, o_ref, xT_ref, y_ref,
             wvA, wvB, wdAT, wdBT, woT, og, hidA, hidB, yA, ysum, r1, acc, r2,
             wsem, wbsend, wbrecv, osend, orecv, gsend, grecv, hasend, harecv, hbsend, hbrecv,
             r1send, r1recv, r2send, r2recv):
    z, p, core, partner, xn, yn, diag, zs = coords()
    ph('c_bar')
    local = [pltpu.make_async_copy(w2_ref.at[:, pl.ds(pl.multiple_of(z * 256, 256), CA), :], wvA.at[z], wsem.at[0])]
    for s, p_ref in ((1, p1_ref), (2, p2_ref), (3, p3_ref)):
        src = zs[s]
        local.append(pltpu.make_async_copy(w1f_ref.at[src], wvA.at[src, :, pl.ds(0, C1), :], wsem.at[0]))
        local.append(pltpu.make_async_copy(p_ref.at[:, pl.ds(0, C2), :], wvA.at[src, :, pl.ds(C1, C2), :], wsem.at[0]))
    late = [
        pltpu.make_async_copy(w2_ref.at[:, pl.ds(pl.multiple_of(z * 256 + CA, 16), C3), :], wvB.at[z], wsem.at[1]),
        pltpu.make_async_copy(p1_ref.at[:, pl.ds(C2, C3), :], wvB.at[zs[1]], wsem.at[1]),
    ]
    for c in local + late:
        c.start()
    entry_barrier(z, p, zs)
    here = (z, p)

    ph('c_send')
    def w_piece(src, dst, dev):
        return rcopy(
            w2_ref.at[:, pl.ds(pl.multiple_of(dst * 256 + CA, 16), C3), :],
            wvB.at[src], wbsend.at[0], wbrecv.at[0], dev)

    for k in (3, 2):
        w_piece(z, zs[k], (zs[k], p)).start()
    for j in range(1, NP):
        q = (p + j) % NP
        rcopy(o_ref.at[q], og.at[z, p], osend.at[0], orecv.at[0], (z, q)).start()
    og[z, p] = o_ref[p]

    def gated(wv, n):
        g = None
        for q in range(NZ):
            t = jnp.dot(wv[q].reshape(2 * n, 512), hT[q * 512:(q + 1) * 512, :], preferred_element_type=F32)
            g = t if g is None else g + t
        gate = g[0:n].astype(BF16).astype(F32)
        up = g[n:2 * n].astype(BF16).astype(F32)
        return (jax.nn.silu(gate) * up).astype(BF16)

    ra = Relay(z, p, lambda src, ch: hidA.at[ch, src], hidA.at[0], hasend, harecv)
    rb = Relay(z, p, lambda src, ch: hidB.at[ch, src], hidB.at[0], hbsend, hbrecv)
    ro = Relay(z, p, lambda src, ch: og.at[src], og.at[0], gsend, grecv)
    every = range(CHUNKS)

    ph('c_localwait')
    pltpu.make_async_copy(wvA, wvA, wsem.at[0]).wait()
    ph('c_gA')
    ha = gated(wvA, CA)
    for ch in every:
        hidA[ch, z] = ha[:, ch * LANES:(ch + 1) * LANES]

    ra.outward(every)
    ra.inward(range(2))
    ph('c_owait')
    oseven = rcopy(o_ref.at[pl.ds(0, 7)], og.at[z, pl.ds(0, 7)], osend.at[0], orecv.at[0], here)
    oseven.wait_recv()
    ro.outward(range(1))
    ro.inward(range(1))
    ph('c_transp')
    pltpu.make_async_copy(wvB.at[pl.ds(0, 2)], wvB.at[pl.ds(0, 2)], wsem.at[1]).wait()
    def by_core(ref, w):
        w = w.T.reshape(4, 2, 64, w.shape[0])
        for j in range(2):
            ref[j] = w[:, j].reshape(256, w.shape[3])

    by_core(wdAT, jnp.concatenate([wd[q * 256:q * 256 + CA, :] for q in range(NZ)], axis=0))
    by_core(wdBT, jnp.concatenate([wd[q * 256 + CA:(q + 1) * 256, :] for q in range(NZ)], axis=0))
    by_core(woT, wo[...])

    ph('c_wBwait')
    ph('c_wBwait2')
    wtwo = wvB.at[pl.ds(0, 2)]
    wall = rcopy(wtwo, wtwo, wbsend.at[0], wbrecv.at[0], here)
    wall.wait_recv()
    ph('c_gB')
    hb = gated(wvB, C3)
    for ch in range(CHUNKS):
        hidB[ch, z] = hb[:, ch * LANES:(ch + 1) * LANES]
    ph('c_own')
    rb.outward(every)
    rb.inward(range(2))
    for ch in range(2, CHUNKS):
        ra.inward((ch,))
        rb.inward((ch,))
    ph('c_step1')
    ro.step(1, 0)
    for ch in range(2):
        ra.step(1, ch)
    ph('c_step2')
    for ch in range(2):
        ra.step(2, ch)

    chip = p // 2
    others = [diag // 2, xn // 2, yn // 2]

    def d2d(ch):
        return rcopy(ysum.at[ch, 1 - core], r1.at[ch], r1send.at[0], r1recv.at[ch], (z, partner))

    def hop(ch, i, dev):
        return rcopy(acc.at[ch, i], r2.at[ch, i], r2send.at[0], r2recv.at[ch], (z, dev))

    def stage0(ch):
        o_rows = og[ch * NZ // CHUNKS].reshape(128, 256)
        for j in (1 - core, core):
            yA[j] = jnp.dot(wdAT[j], hidA[ch].reshape(NZ * CA, LANES), preferred_element_type=F32) + lax.dot_general(
                woT[j], o_rows, (((1,), (1,)), ((), ())), preferred_element_type=F32)

    def half(ch, j):
        yt = yA[j] + jnp.dot(wdBT[j], hidB[ch].reshape(NZ * C3, LANES), preferred_element_type=F32)
        ysum[ch, j] = yt.reshape(4, 64, LANES)

    def stage1(ch):
        half(ch, 1 - core)
        d2d(ch).start()
        half(ch, core)

    def stage2(ch):
        d2d(ch).wait_recv()
        for i, (t, dev) in enumerate(zip(others, (diag, xn, yn))):
            acc[ch, i] = ysum[ch, core, t] + r1[ch, t]
            hop(ch, i, dev).start()

    def stage3(ch):
        lanes = slice(ch * LANES, (ch + 1) * LANES)
        mine = ysum[ch, core, chip] + r1[ch, chip]
        rcopy(acc.at[ch], r2.at[ch], r2send.at[0], r2recv.at[ch], here).wait_recv()
        for i in range(3):
            mine = mine + r2[ch, i]
        y_ref[:, lanes] = (xT_ref[:, lanes].astype(F32) + mine).astype(BF16)

    for t in range(1, CHUNKS + 3):
        ph(f'c_wave{t}')
        for k in range(1, NZ - 1):
            ch = t - k
            if 0 <= ch < CHUNKS:
                if ch >= 2:
                    ra.step(k, ch)
                rb.step(k, ch)
        if t < 3:
            ro.step(t + 1, 0)
        ph(f'c_sum{t}')
        if t >= 3:
            ra.step(3, t - 3)
            stage0(t - 3)
            rb.step(3, t - 3)
            stage1(t - 3)
        if t >= 4:
            stage2(t - 4)
    ph('c_last2')
    stage2(CHUNKS - 1)
    ph('c_last3')
    for ch in every:
        stage3(ch)

    ph('c_end')
    wall.wait_send()
    oseven.wait_send()
    rcopy(r1, r1, r1send.at[0], r1recv.at[0], here).wait_send()
    rcopy(acc, acc, r2send.at[0], r2recv.at[0], here).wait_send()
    ra.drain()
    rb.drain()
    ro.drain()
    ph('')


def call_c(hT, w2, w1f, ps, wd, wo, o8, xT):
    vm = pl.BlockSpec(memory_space=pltpu.VMEM)
    hbm = pl.BlockSpec(memory_space=pl.ANY)
    return pl.pallas_call(
        kernel_c,
        out_shape=jax.ShapeDtypeStruct((64, 512), BF16),
        in_specs=[vm] + [hbm] * 5 + [vm] * 4,
        out_specs=vm,
        scratch_shapes=[
            pltpu.VMEM((NZ, 2, CA, 512), BF16),
            pltpu.VMEM((NZ, 2, C3, 512), BF16),
            pltpu.VMEM((2, 256, NZ * CA), BF16),
            pltpu.VMEM((2, 256, NZ * C3), BF16),
            pltpu.VMEM((2, 256, 256), BF16),
            pltpu.VMEM((NZ, NP, 16, 256), BF16),
            pltpu.VMEM((CHUNKS, NZ, CA, LANES), BF16),
            pltpu.VMEM((CHUNKS, NZ, C3, LANES), BF16),
            pltpu.VMEM((2, 256, LANES), F32),
            pltpu.VMEM((CHUNKS, 2, 4, 64, LANES), F32),
            pltpu.VMEM((CHUNKS, 4, 64, LANES), F32),
            pltpu.VMEM((CHUNKS, 3, 64, LANES), F32),
            pltpu.VMEM((CHUNKS, 3, 64, LANES), F32),
            pltpu.SemaphoreType.DMA((2,)),
            pltpu.SemaphoreType.DMA((1,)),
            pltpu.SemaphoreType.DMA((1,)),
            pltpu.SemaphoreType.DMA((1,)),
            pltpu.SemaphoreType.DMA((1,)),
            pltpu.SemaphoreType.DMA((6,)),
            pltpu.SemaphoreType.DMA((NZ, 1)),
            pltpu.SemaphoreType.DMA((6,)),
            pltpu.SemaphoreType.DMA((NZ, CHUNKS)),
            pltpu.SemaphoreType.DMA((6,)),
            pltpu.SemaphoreType.DMA((NZ, CHUNKS)),
            pltpu.SemaphoreType.DMA((1,)),
            pltpu.SemaphoreType.DMA((CHUNKS,)),
            pltpu.SemaphoreType.DMA((1,)),
            pltpu.SemaphoreType.DMA((CHUNKS,)),
        ],
        compiler_params=pltpu.CompilerParams(collective_id=1, has_side_effects=True, vmem_limit_bytes=40 * 1024 * 1024),
        cost_estimate=pl.CostEstimate(flops=12_000_000_000, bytes_accessed=6_000_000, transcendentals=0),
        name='mlp_out',
    )(hT, w2, w1f, *ps, wd, wo, o8, xT)


def solution(mesh):
    all_axes = ('x', 'yz')

    def local_step(x_in, ln_scale, w_gate_up, w_attn, w_down, w_out, k_cache, v_cache, lengths, positions):
        xT = x_in.T
        wattnT = w_attn.T
        hT, qkv, w1f, w2, *pieces = call_a(xT, ln_scale[None, :], wattnT, w_gate_up)
        ps = [lax.ppermute(pieces[i], 'x', [(q, q ^ (i + 1)) for q in range(NZ)]) for i in range(NZ - 1)]
        proj = jnp.transpose(qkv, (1, 0, 2)).reshape(16, 2304)
        q_raw = proj[:, :2048].reshape(16, 16, 128)
        k_tok = proj[:, 2048:2176]
        v_tok = proj[:, 2176:]
        q_rot = rotary(q_raw.astype(F32), positions).astype(BF16)
        k_rot = rotary(k_tok[:, None, :].astype(F32), positions).astype(BF16)
        o8, k_new, v_new = call_b(lengths, q_rot, k_rot, v_tok[:, None, :], k_cache, v_cache)
        yT = call_c(hT, w2, w1f, ps, w_down, w_out, o8, xT)
        return yT.T, k_new, v_new

    row_spec = P(None, all_axes)
    vec_spec = P(all_axes)
    cache_spec = P(all_axes, None, None)
    return jax.shard_map(
        local_step,
        mesh=mesh,
        in_specs=(row_spec, vec_spec, P('x', None, 'yz'), P('x', 'yz'), P('yz', 'x'), P('yz', 'x'), cache_spec, cache_spec, vec_spec, vec_spec),
        out_specs=(row_spec, cache_spec, cache_spec),
        check_vma=False,
    )
```

```python
import functools

import jax
import jax.numpy as jnp
from jax import lax
from jax.experimental import pallas as pl
from jax.experimental.pallas import tpu as pltpu
from jax.sharding import PartitionSpec as P

LN_EPS = 1e-6
ROPE_BASE = 10000.0
MESH = pl.DeviceIdType.MESH


class Phase:
    cm = None

    def __call__(self, name):
        if self.cm is not None:
            self.cm.__exit__(None, None, None)
            self.cm = None
        if name:
            self.cm = jax.named_scope(name)
            self.cm.__enter__()


ph = Phase()
F32 = jnp.float32
BF16 = jnp.bfloat16

NZ = 4
NP = 8
C1A = 16
C1 = 48
C2 = 128
C3 = 80
CA = C1 + C2
CHUNKS = 4
LANES = 512 // CHUNKS


def rotary(values, positions):
    half_dim = values.shape[-1] // 2
    inv_freq = ROPE_BASE ** (-jnp.arange(half_dim, dtype=jnp.float32) / half_dim)
    angles = positions.astype(jnp.float32)[:, None, None] * inv_freq
    cos_part = jnp.cos(angles)
    sin_part = jnp.sin(angles)
    lo_half = values[..., :half_dim]
    hi_half = values[..., half_dim:]
    return jnp.concatenate([lo_half * cos_part - hi_half * sin_part, hi_half * cos_part + lo_half * sin_part], axis=-1)


def coords():
    z = lax.axis_index('x')
    p = lax.axis_index('yz')
    core = p % 2
    xx = (p // 2) % 2
    y = p // 4
    partner = p + 1 - 2 * core
    xn = p + 2 - 4 * xx
    yn = p + 4 - 8 * y
    diag = xn + 4 - 8 * y
    z1 = z % 2
    z2 = z // 2
    zs = [z, 2 * z2 + 1 - z1, 2 * (1 - z2) + z1, 3 - z]
    return z, p, core, partner, xn, yn, diag, zs


def entry_barrier(z, p, zs):
    sem = pltpu.get_barrier_semaphore()
    for k in range(1, NZ):
        pl.semaphore_signal(sem, inc=1, device_id=(zs[k], p), device_id_type=MESH)
    for k in range(1, NP):
        pl.semaphore_signal(sem, inc=1, device_id=(z, (p + k) % NP), device_id_type=MESH)
    pl.semaphore_wait(sem, NZ - 1 + NP - 1)


def rcopy(src, dst, send, recv, dev):
    return pltpu.make_async_remote_copy(src_ref=src, dst_ref=dst, send_sem=send, recv_sem=recv, device_id=dev, device_id_type=MESH)


class Relay:
    def __init__(self, z, p, at, whole, send, recv):
        self.z, self.p, self.at, self.whole, self.send, self.recv = z, p, at, whole, send, recv

    def copy(self, way, src, ch, dev):
        ref = self.at(src, ch)
        return rcopy(ref, ref, self.send.at[way], self.recv.at[src, ch], (dev, self.p))

    def inward(self, chunks, planes=(0, 1, 2, 3)):
        z = self.z
        for q in planes:
            @pl.when(z == q)
            def _():
                for ch in chunks:
                    if q < 2:
                        self.copy(0, z, ch, z + 1).start()
                    else:
                        self.copy(1, z, ch, z - 1).start()

    def from_outer(self, ch):
        z = self.z

        @pl.when(z == 1)
        def _():
            self.copy(0, z - 1, ch, z).wait_recv()
            self.copy(2, z - 1, ch, z + 1).start()

        @pl.when(z == 2)
        def _():
            self.copy(0, z + 1, ch, z).wait_recv()
            self.copy(3, z + 1, ch, z - 1).start()

    def from_inner(self, ch):
        z = self.z

        @pl.when(z <= 1)
        def _():
            self.copy(0, z + 1, ch, z).wait_recv()

        @pl.when(z == 1)
        def _():
            self.copy(3, z + 1, ch, z - 1).start()

        @pl.when(z >= 2)
        def _():
            self.copy(0, z - 1, ch, z).wait_recv()

        @pl.when(z == 2)
        def _():
            self.copy(2, z - 1, ch, z + 1).start()

    def outward(self, chunks):
        z = self.z

        @pl.when(z == 1)
        def _():
            for ch in chunks:
                self.copy(1, z, ch, z - 1).start()

        @pl.when(z == 2)
        def _():
            for ch in chunks:
                self.copy(0, z, ch, z + 1).start()

    def step(self, k, ch):
        z = self.z

        @pl.when(z >= k)
        def _():
            self.copy(0, z - k, ch, z).wait_recv()

            @pl.when(z < 3)
            def _():
                self.copy(2 * k, z - k, ch, z + 1).start()

        @pl.when(z + k <= 3)
        def _():
            self.copy(0, z + k, ch, z).wait_recv()

            @pl.when(z > 0)
            def _():
                self.copy(2 * k + 1, z + k, ch, z - 1).start()

    def sent(self, way):
        rcopy(self.whole, self.whole, self.send.at[way], self.recv.at[0, 0], (self.z, self.p)).wait_send()

    def drain(self):
        z = self.z
        for k in range(NZ - 1):
            @pl.when((z >= k) & (z < 3))
            def _():
                self.sent(2 * k)

            @pl.when((z + k <= 3) & (z > 0))
            def _():
                self.sent(2 * k + 1)


def attn_start(q):
    return pl.multiple_of(64 * q + 16 * (q // 2), 16)


def kernel_a(xT_hbm, ln_hbm, wattn_hbm, w_ref, h_ref, qkv_ref, w1f_ref, w2_ref, ps1_ref, ps2_ref, ps3_ref,
             xg, lng, watt, zsend, zrecv, zq, s1, s2, wn, wt, hT_ref, ln_ref, wattn_ref,
             xsend, xrecv, rpart, lsend, lrecv, asend, arecv, zsend_sem, zrecv_sem, qsend, qrecv, wsend, wrecv, lsem, osem, ldummy):
    z, p, core, partner, xn, yn, diag, zs = coords()
    ph('a_bar')
    wload = pltpu.make_async_copy(w_ref, wn, lsem.at[0])
    loads = [
        pltpu.make_async_copy(xT_hbm, xg.at[z, p], lsem.at[6]),
        pltpu.make_async_copy(ln_hbm, ln_ref, lsem.at[7]),
        pltpu.make_async_copy(wattn_hbm, wattn_ref, lsem.at[8]),
        wload,
    ]
    for c in loads:
        c.start()
    loads[1].wait()
    lng[z, p] = jnp.zeros((1, 128), F32)
    lng[z, p, 0:1, 0:64] = ln_ref[...]
    entry_barrier(z, p, zs)
    loads[0].wait()
    ph('a_zsend')
    here = (z, p)

    def send(src_z, src_p, dev, way=0):
        recv = rpart.at[0] if way == 4 else xrecv.at[way, src_z]
        rcopy(xg.at[src_z, src_p], xg.at[src_z, src_p], xsend.at[0], recv, dev).start()

    def send_l(src_z, dev, phase):
        rcopy(lng.at[src_z, p], lng.at[src_z, p], lsend.at[0], lrecv.at[phase], dev).start()

    def wait_x(src_z, src_p, way):
        rcopy(xg.at[src_z, src_p], xg.at[src_z, src_p], xsend.at[0], xrecv.at[way, src_z], here).wait_recv()

    def stat(src_z, src_p):
        blk = xg[src_z, src_p].astype(F32).reshape(8, 8, 512)
        s1[...] += jnp.sum(blk, axis=0)
        s2[...] += jnp.sum(blk * blk, axis=0)

    spans = tuple((i, C1A) for i in range(0, C1, C1A))

    def w_piece(i, src, dst, dev):
        o, n = spans[i]
        return rcopy(
            wt.at[:, pl.ds(pl.multiple_of(dst * 256 + o, 16), n), :],
            w1f_ref.at[src, :, pl.ds(o, n), :],
            wsend.at[0], wrecv.at[0], dev)

    def send_w(i):
        for k in (3, 2, 1):
            w_piece(i, z, zs[k], (zs[k], p)).start()

    def turn(odd):
        def body(i, carry):
            lanes = pl.ds(pl.multiple_of(i * 256 + odd * 128, 128), 128)
            blk = wn[:, :, lanes].astype(F32)
            for g in range(2):
                wt[g, lanes, :] = blk[:, g, :].T.astype(BF16)
            return carry

        lax.fori_loop(0, NZ, body, 0)

    mid = 2 - z // 2
    far = 3 - 3 * (z // 2)
    zo = [z, zs[1], mid, far]
    inner = (z == 1) | (z == 2)
    send(z, p, (mid, p))
    send(z, p, (zs[1], p))
    for k in (3, 2, 1):
        send_l(z, (zs[k], p), 0)
    targets = ((diag, 3), (xn, 1), (yn, 2), (partner, 4))
    for dev, way in targets:
        send(z, p, (z, dev), way)
    for j in range(1, NP):
        send_l(z, (z, (p + j) % NP), 1)

    def attn_piece(q):
        return rcopy(wattn_ref.at[pl.ds(attn_start(q), 80), :], watt.at[z], asend.at[0], arecv.at[0], (q, p))

    def outward(k):
        return rcopy(xg.at[zo[k], p], xg.at[zo[k], p], osem.at[k - 2], xrecv.at[0, zo[k]], (zs[1], p))

    s1[...] = jnp.zeros_like(s1)
    s2[...] = jnp.zeros_like(s2)
    stat(z, p)
    loads[2].wait()
    watt[z] = wattn_ref[pl.ds(attn_start(z), 80), :]
    wload.wait()
    turn(0)
    attn_piece(mid).start()

    @pl.when(jnp.logical_not(inner))
    def _():
        attn_piece(zs[1]).start()


    def column(k):
        wait_x(zo[k], p, 0)
        if k >= 2:
            @pl.when(inner)
            def _():
                outward(k).start()
        for dev, way in targets:
            send(zo[k], p, (z, dev), way)
        stat(zo[k], p)

    def pass_on(k, src, way):
        wait_x(zo[k], src, way)
        send(zo[k], src, (z, partner), 4)
        stat(zo[k], src)

    ph('a_col1')
    column(1)
    column(2)
    ph('a_col3')
    column(3)
    ph('a_lnsend')
    rcopy(ldummy.at[pl.ds(0, 3)], ldummy.at[pl.ds(0, 3)], lsend.at[0], lrecv.at[0], here).wait_recv()
    for k in range(1, NZ):
        for j in range(1, NP):
            send_l(zs[k], (z, (p + j) % NP), 1)
    ph('a_nbr')
    for k in range(2):
        pass_on(k, xn, 1)
        pass_on(k, yn, 2)
    ph('a_wattn')
    attn_piece(far).start()

    @pl.when(inner)
    def _():
        attn_piece(zs[1]).start()

    send_w(0)
    ph('a_nbr2')
    pass_on(0, diag, 3)
    pass_on(1, diag, 3)
    ph('a_nbr3')
    for k in range(2, NZ):
        pass_on(k, xn, 1)
        pass_on(k, yn, 2)
        pass_on(k, diag, 3)
    send_w(1)
    ph('a_rest')
    half = xg.at[pl.ds(0, 2)]
    rcopy(half, half, xsend.at[0], rpart.at[0], here).wait_recv()
    for q in (partner, partner + xn - p, partner + yn - p, partner + diag - p):
        for k in range(NZ):
            stat(zo[k], q)
    rcopy(ldummy.at[pl.ds(0, 28)], ldummy.at[pl.ds(0, 28)], lsend.at[0], lrecv.at[1], here).wait_recv()

    ph('a_norm')
    mean = jnp.sum(s1[...], axis=0, keepdims=True) / 2048.0
    var = jnp.sum(s2[...], axis=0, keepdims=True) / 2048.0 - mean * mean
    rstd = lax.rsqrt(var + LN_EPS)
    lnT = jnp.concatenate([lng[i // NP, i % NP, 0:1, :] for i in range(32)] + [jnp.zeros((96, 128), F32)], axis=0).T
    for i in range(NZ * NP):
        sc = lnT[0:64, i:i + 1]
        hT_ref[i * 64:(i + 1) * 64, :] = ((xg[i // NP, i % NP].astype(F32) - mean) * rstd * sc).astype(BF16)

    hout = pltpu.make_async_copy(hT_ref, h_ref, lsem.at[5])
    hout.start()
    ph('a_attw')
    three = watt.at[pl.ds(0, 3)]
    rcopy(three, three, asend.at[0], arecv.at[0], here).wait_recv()
    ph('a_zdot')
    part = None
    for q in range(NZ):
        t = jnp.dot(watt[q], hT_ref[q * 512:(q + 1) * 512, :], preferred_element_type=F32)
        part = t if part is None else part + t
    part = part.astype(BF16)
    for q in range(NZ):
        zsend[q] = part[:, q * 128:(q + 1) * 128]
    for k in (3, 2, 1):
        rcopy(zsend.at[zs[k]], zrecv.at[z], zsend_sem.at[0], zrecv_sem.at[0], (zs[k], p)).start()
    zrecv[z] = zsend[z]
    ph('a_turn')
    turn(1)
    send_w(2)
    outs = [pltpu.make_async_copy(wt, w2_ref, lsem.at[1])]
    for i, ps_ref in enumerate((ps1_ref, ps2_ref, ps3_ref)):
        dst = (z + i + 1) % NZ
        outs.append(pltpu.make_async_copy(wt.at[:, pl.ds(pl.multiple_of(dst * 256 + C1, 16), C2), :], ps_ref, lsem.at[2 + i]))
    for c in outs[1:] + outs[:1]:
        c.start()
    ph('a_zwait')
    zthree = rcopy(zsend.at[pl.ds(0, 3)], zrecv.at[pl.ds(0, 3)], zsend_sem.at[0], zrecv_sem.at[0], here)
    zthree.wait_recv()
    ph('a_a2a')
    zt = jnp.concatenate([zrecv[0].astype(F32), zrecv[1].astype(F32)[16:80], zrecv[2].astype(F32), zrecv[3].astype(F32)[16:80]], axis=0)
    zq[...] = zt.T.astype(BF16).reshape(NP, 16, 288)
    for j in range(1, NP):
        q = (p + j) % NP
        rcopy(zq.at[q], qkv_ref.at[p], qsend.at[0], qrecv.at[0], (z, q)).start()
    qown = pltpu.make_async_copy(zq.at[p], qkv_ref.at[p], lsem.at[9])
    qown.start()
    qseven = rcopy(zq.at[pl.ds(0, 7)], qkv_ref.at[pl.ds(0, 7)], qsend.at[0], qrecv.at[0], here)
    qseven.wait_recv()
    ph('a_wwait')
    wthree = w1f_ref.at[pl.ds(0, 3)]
    wall = rcopy(wthree, wthree, wsend.at[0], wrecv.at[0], here)
    wall.wait_recv()
    ph('a_sendwait')
    hout.wait()
    qown.wait()
    for c in outs:
        c.wait()
    sent30 = w2_ref.at[:, pl.ds(0, 960), :]
    rcopy(sent30, sent30, xsend.at[0], rpart.at[0], here).wait_send()
    rcopy(ldummy, ldummy, lsend.at[0], lrecv.at[0], here).wait_send()
    rcopy(three, three, asend.at[0], arecv.at[0], here).wait_send()
    zthree.wait_send()
    qseven.wait_send()
    wall.wait_send()

    @pl.when(inner)
    def _():
        outward(2).wait_send()
        outward(3).wait_send()
    ph('')


def call_a(xT, ln, wattnT, w):
    hbm = pl.BlockSpec(memory_space=pl.ANY)
    return pl.pallas_call(
        kernel_a,
        out_shape=(
            jax.ShapeDtypeStruct((2048, 512), BF16),
            jax.ShapeDtypeStruct((NP, 16, 288), BF16),
            jax.ShapeDtypeStruct((NZ, 2, C1, 512), BF16),
            jax.ShapeDtypeStruct((2, 1024, 512), BF16),
        ) + (jax.ShapeDtypeStruct((2, C2, 512), BF16),) * 3,
        in_specs=[hbm] * 4,
        out_specs=(hbm,) * 7,
        scratch_shapes=[
            pltpu.VMEM((NZ, NP, 64, 512), BF16),
            pltpu.VMEM((NZ, NP, 1, 128), F32),
            pltpu.VMEM((NZ, 80, 512), BF16),
            pltpu.VMEM((NZ, 80, 128), BF16),
            pltpu.VMEM((NZ, 80, 128), BF16),
            pltpu.VMEM((NP, 16, 288), BF16),
            pltpu.VMEM((8, 512), F32),
            pltpu.VMEM((8, 512), F32),
            pltpu.VMEM((512, 2, 1024), BF16),
            pltpu.VMEM((2, 1024, 512), BF16),
            pltpu.VMEM((2048, 512), BF16),
            pltpu.VMEM((1, 64), F32),
            pltpu.VMEM((288, 512), BF16),
            pltpu.SemaphoreType.DMA((1,)),
            pltpu.SemaphoreType.DMA((4, NZ)),
            pltpu.SemaphoreType.DMA((1,)),
            pltpu.SemaphoreType.DMA((1,)),
            pltpu.SemaphoreType.DMA((2,)),
            pltpu.SemaphoreType.DMA((1,)),
            pltpu.SemaphoreType.DMA((1,)),
            pltpu.SemaphoreType.DMA((1,)),
            pltpu.SemaphoreType.DMA((1,)),
            pltpu.SemaphoreType.DMA((1,)),
            pltpu.SemaphoreType.DMA((1,)),
            pltpu.SemaphoreType.DMA((1,)),
            pltpu.SemaphoreType.DMA((1,)),
            pltpu.SemaphoreType.DMA((10,)),
            pltpu.SemaphoreType.DMA((2,)),
            pltpu.VMEM((31, 1, 128), F32),
        ],
        compiler_params=pltpu.CompilerParams(collective_id=0, has_side_effects=True, vmem_limit_bytes=56 * 1024 * 1024),
        name='gather_norm_qkv',
    )(xT, ln, wattnT, w)


def kernel_b(len_ref, q_ref, k_ref, v_ref, kc_ref, vc_ref, o_ref, kn_ref, vn_ref, kbuf, vbuf, oscr, isem, osem):
    rows = kbuf.shape[0]
    seq = kbuf.shape[1]

    def load(b, t):
        return pltpu.make_async_copy((kc_ref, vc_ref)[t].at[b], (kbuf, vbuf)[t].at[b], isem.at[b])

    def store(b, t):
        return pltpu.make_async_copy((kbuf, vbuf)[t].at[b], (kn_ref, vn_ref)[t].at[b], osem.at[0])

    for b in range(rows):
        load(b, 0).start()
        load(b, 1).start()

    def insert(buf, b, length, new):
        base = pl.multiple_of((length // 16) * 16, 16)
        hit = base + lax.broadcasted_iota(jnp.int32, (16, 128), 0) == length
        buf[b, pl.ds(base, 16), :] = jnp.where(hit, new.astype(F32), buf[b, pl.ds(base, 16), :].astype(F32)).astype(BF16)

    def attend(b, length, n):
        scores = lax.dot_general(q_ref[b], kbuf[b, 0:n, :], (((1,), (1,)), ((), ())), preferred_element_type=F32) * (128.0 ** -0.5)
        slot = lax.broadcasted_iota(jnp.int32, scores.shape, 1)
        scores = jnp.where(slot <= length, scores, -1e30)
        top = jnp.max(scores, axis=1, keepdims=True)
        e = jnp.exp(scores - top)
        probs = (e / jnp.sum(e, axis=1, keepdims=True)).astype(BF16)
        return jnp.dot(probs, vbuf[b, 0:n, :], preferred_element_type=F32)

    def pair(i, carry):
        b0 = 2 * i
        b1 = 2 * i + 1
        l0 = len_ref[b0]
        l1 = len_ref[b1]
        for b, length in ((b0, l0), (b1, l1)):
            pltpu.make_async_copy(kc_ref.at[pl.ds(0, 2)], kbuf.at[pl.ds(0, 2)], isem.at[b]).wait()
            insert(kbuf, b, length, k_ref[b])
            insert(vbuf, b, length, v_ref[b])
        last = jnp.maximum(l0, l1) // 512
        for t in range(seq // 512):
            @pl.when(last == t)
            def _():
                n = 512 * (t + 1)
                r0 = attend(b0, l0, n)
                r1 = attend(b1, l1, n)
                oscr[b0] = r0
                oscr[b1] = r1
        for b in (b0, b1):
            store(b, 0).start()
            store(b, 1).start()
        return carry

    lax.fori_loop(0, rows // 2, pair, 0)
    for h in range(16):
        o_ref[h // 2, :, (h % 2) * 128:(h % 2 + 1) * 128] = oscr[:, h, :].astype(BF16)
    pltpu.make_async_copy(kbuf, kn_ref, osem.at[0]).wait()
    pltpu.make_async_copy(vbuf, vn_ref, osem.at[0]).wait()


def call_b(lengths, q_rot, k_rot, v_tok, k_cache, v_cache):
    rows, seq, hd = k_cache.shape
    heads = q_rot.shape[1]
    vm = pl.BlockSpec(memory_space=pltpu.VMEM)
    hbm = pl.BlockSpec(memory_space=pl.ANY)
    return pl.pallas_call(
        kernel_b,
        in_specs=[pl.BlockSpec(memory_space=pltpu.SMEM), vm, vm, vm, hbm, hbm],
        out_specs=(vm, hbm, hbm),
        out_shape=(
            jax.ShapeDtypeStruct((NP, rows, heads * hd // NP), BF16),
            jax.ShapeDtypeStruct(k_cache.shape, BF16),
            jax.ShapeDtypeStruct(v_cache.shape, BF16),
        ),
        scratch_shapes=[
            pltpu.VMEM((rows, seq, hd), BF16),
            pltpu.VMEM((rows, seq, hd), BF16),
            pltpu.VMEM((rows, heads, hd), F32),
            pltpu.SemaphoreType.DMA((rows,)),
            pltpu.SemaphoreType.DMA((1,)),
        ],
        compiler_params=pltpu.CompilerParams(vmem_limit_bytes=58 * 1024 * 1024),
        cost_estimate=pl.CostEstimate(flops=12_000_000_000, bytes_accessed=33_000_000, transcendentals=0),
        name='attend',
    )(lengths, q_rot, k_rot, v_tok, k_cache, v_cache)


def kernel_c(hT, w2_ref, w1f_ref, p1_ref, p2_ref, p3_ref, wd, wo, o_ref, xT_ref, y_ref,
             wvA, wvB, wdAT, wdBT, woT, og, hidA, hidB, yA, ysum, r1, acc, r2,
             wsem, wbsend, wbrecv, osend, orecv, gsend, grecv, hasend, harecv, hbsend, hbrecv,
             r1send, r1recv, r2send, r2recv):
    z, p, core, partner, xn, yn, diag, zs = coords()
    ph('c_bar')
    local = [pltpu.make_async_copy(w2_ref.at[:, pl.ds(pl.multiple_of(z * 256, 256), CA), :], wvA.at[z], wsem.at[0])]
    for s, p_ref in ((1, p1_ref), (2, p2_ref), (3, p3_ref)):
        src = (z + NZ - s) % NZ
        local.append(pltpu.make_async_copy(w1f_ref.at[src], wvA.at[src, :, pl.ds(0, C1), :], wsem.at[0]))
        local.append(pltpu.make_async_copy(p_ref, wvA.at[src, :, pl.ds(C1, C2), :], wsem.at[0]))
    late = [
        pltpu.make_async_copy(w2_ref.at[:, pl.ds(pl.multiple_of(z * 256 + CA, 16), C3), :], wvB.at[z], wsem.at[1]),
    ]
    for c in local + late:
        c.start()
    entry_barrier(z, p, zs)
    here = (z, p)

    ph('c_send')
    def w_piece(src, dst, dev):
        return rcopy(
            w2_ref.at[:, pl.ds(pl.multiple_of(dst * 256 + CA, 16), C3), :],
            wvB.at[src], wbsend.at[0], wbrecv.at[0], dev)

    def send_w():
        for k in (3, 2, 1):
            w_piece(z, zs[k], (zs[k], p)).start()

    inner = (z == 1) | (z == 2)
    pl.when(inner)(send_w)
    for j in range(1, NP):
        q = (p + j) % NP
        rcopy(o_ref.at[q], og.at[z, p], osend.at[0], orecv.at[0], (z, q)).start()
    og[z, p] = o_ref[p]

    def gated(wv, n):
        g = None
        for q in range(NZ):
            t = jnp.dot(wv[q].reshape(2 * n, 512), hT[q * 512:(q + 1) * 512, :], preferred_element_type=F32)
            g = t if g is None else g + t
        gate = g[0:n].astype(BF16).astype(F32)
        up = g[n:2 * n].astype(BF16).astype(F32)
        return (jax.nn.silu(gate) * up).astype(BF16)

    ra = Relay(z, p, lambda src, ch: hidA.at[ch, src], hidA.at[0], hasend, harecv)
    rb = Relay(z, p, lambda src, ch: hidB.at[ch, src], hidB.at[0], hbsend, hbrecv)
    ro = Relay(z, p, lambda src, ch: og.at[src], og.at[0], gsend, grecv)
    every = range(CHUNKS)

    ph('c_localwait')
    pltpu.make_async_copy(wvA, wvA, wsem.at[0]).wait()
    ph('c_gA')
    ha = gated(wvA, CA)
    for ch in every:
        hidA[ch, z] = ha[:, ch * LANES:(ch + 1) * LANES]

    ra.outward(every)
    ra.inward(range(2), (1, 2))
    ra.inward(every, (0, 3))
    pl.when(jnp.logical_not(inner))(send_w)
    ph('c_owait')
    oseven = rcopy(o_ref.at[pl.ds(0, 7)], og.at[z, pl.ds(0, 7)], osend.at[0], orecv.at[0], here)
    oseven.wait_recv()
    ro.outward(range(1))
    ro.inward(range(1))
    ph('c_transp')
    for c in late:
        c.wait()
    def by_core(ref, w):
        w = w.T.reshape(4, 2, 64, w.shape[0])
        for j in range(2):
            ref[j] = w[:, j].reshape(256, w.shape[3])

    by_core(wdAT, jnp.concatenate([wd[q * 256:q * 256 + CA, :] for q in range(NZ)], axis=0))
    by_core(wdBT, jnp.concatenate([wd[q * 256 + CA:(q + 1) * 256, :] for q in range(NZ)], axis=0))
    by_core(woT, wo[...])

    ph('c_wBwait')
    for ch in every:
        ra.from_outer(ch)
    ph('c_wBwait2')
    wthree = wvB.at[pl.ds(0, 3)]
    wall = rcopy(wthree, wthree, wbsend.at[0], wbrecv.at[0], here)
    wall.wait_recv()
    ph('c_gB')
    hb = gated(wvB, C3)
    for ch in range(CHUNKS):
        hidB[ch, z] = hb[:, ch * LANES:(ch + 1) * LANES]
    ph('c_own')
    rb.outward(every)
    rb.inward(range(2))
    for ch in range(2, CHUNKS):
        ra.inward((ch,), (1, 2))
        rb.inward((ch,))
    ph('c_step1')
    ro.step(1, 0)
    for ch in range(2):
        ra.from_inner(ch)
    ph('c_step2')
    for ch in range(2):
        ra.step(2, ch)

    chip = p // 2
    others = [diag // 2, xn // 2, yn // 2]

    def d2d(ch):
        return rcopy(ysum.at[ch, 1 - core], r1.at[ch], r1send.at[0], r1recv.at[ch], (z, partner))

    def hop(ch, i, dev):
        return rcopy(acc.at[ch, i], r2.at[ch, i], r2send.at[0], r2recv.at[ch], (z, dev))

    def stage0(ch):
        o_rows = og[ch * NZ // CHUNKS].reshape(128, 256)
        for j in (1 - core, core):
            yA[j] = jnp.dot(wdAT[j], hidA[ch].reshape(NZ * CA, LANES), preferred_element_type=F32) + lax.dot_general(
                woT[j], o_rows, (((1,), (1,)), ((), ())), preferred_element_type=F32)

    def half(ch, j):
        yt = yA[j] + jnp.dot(wdBT[j], hidB[ch].reshape(NZ * C3, LANES), preferred_element_type=F32)
        ysum[ch, j] = yt.reshape(4, 64, LANES)

    def stage1(ch):
        half(ch, 1 - core)
        d2d(ch).start()
        half(ch, core)

    def stage2(ch):
        d2d(ch).wait_recv()
        for i, (t, dev) in enumerate(zip(others, (diag, xn, yn))):
            acc[ch, i] = ysum[ch, core, t] + r1[ch, t]
            hop(ch, i, dev).start()

    def stage3(ch):
        lanes = slice(ch * LANES, (ch + 1) * LANES)
        mine = ysum[ch, core, chip] + r1[ch, chip]
        rcopy(acc.at[ch], r2.at[ch], r2send.at[0], r2recv.at[ch], here).wait_recv()
        for i in range(3):
            mine = mine + r2[ch, i]
        y_ref[:, lanes] = (xT_ref[:, lanes].astype(F32) + mine).astype(BF16)

    for t in range(1, CHUNKS + 3):
        ph(f'c_wave{t}')
        for k in range(1, NZ - 1):
            ch = t - k
            if 0 <= ch < CHUNKS:
                if ch >= 2:
                    if k == 1:
                        ra.from_inner(ch)
                    else:
                        ra.step(k, ch)
                rb.step(k, ch)
        if t < 3:
            ro.step(t + 1, 0)
        ph(f'c_sum{t}')
        if t >= 3:
            ra.step(3, t - 3)
            stage0(t - 3)
            rb.step(3, t - 3)
            stage1(t - 3)
        if t >= 4:
            stage2(t - 4)
    ph('c_last2')
    stage2(CHUNKS - 1)
    ph('c_last3')
    for ch in every:
        stage3(ch)

    ph('c_end')
    wall.wait_send()
    oseven.wait_send()
    rcopy(r1, r1, r1send.at[0], r1recv.at[0], here).wait_send()
    rcopy(acc, acc, r2send.at[0], r2recv.at[0], here).wait_send()
    ra.drain()
    rb.drain()
    ro.drain()
    ph('')


def call_c(hT, w2, w1f, ps, wd, wo, o8, xT):
    vm = pl.BlockSpec(memory_space=pltpu.VMEM)
    hbm = pl.BlockSpec(memory_space=pl.ANY)
    return pl.pallas_call(
        kernel_c,
        out_shape=jax.ShapeDtypeStruct((64, 512), BF16),
        in_specs=[vm] + [hbm] * 5 + [vm] * 4,
        out_specs=vm,
        scratch_shapes=[
            pltpu.VMEM((NZ, 2, CA, 512), BF16),
            pltpu.VMEM((NZ, 2, C3, 512), BF16),
            pltpu.VMEM((2, 256, NZ * CA), BF16),
            pltpu.VMEM((2, 256, NZ * C3), BF16),
            pltpu.VMEM((2, 256, 256), BF16),
            pltpu.VMEM((NZ, NP, 16, 256), BF16),
            pltpu.VMEM((CHUNKS, NZ, CA, LANES), BF16),
            pltpu.VMEM((CHUNKS, NZ, C3, LANES), BF16),
            pltpu.VMEM((2, 256, LANES), F32),
            pltpu.VMEM((CHUNKS, 2, 4, 64, LANES), F32),
            pltpu.VMEM((CHUNKS, 4, 64, LANES), F32),
            pltpu.VMEM((CHUNKS, 3, 64, LANES), F32),
            pltpu.VMEM((CHUNKS, 3, 64, LANES), F32),
            pltpu.SemaphoreType.DMA((2,)),
            pltpu.SemaphoreType.DMA((1,)),
            pltpu.SemaphoreType.DMA((1,)),
            pltpu.SemaphoreType.DMA((1,)),
            pltpu.SemaphoreType.DMA((1,)),
            pltpu.SemaphoreType.DMA((6,)),
            pltpu.SemaphoreType.DMA((NZ, 1)),
            pltpu.SemaphoreType.DMA((6,)),
            pltpu.SemaphoreType.DMA((NZ, CHUNKS)),
            pltpu.SemaphoreType.DMA((6,)),
            pltpu.SemaphoreType.DMA((NZ, CHUNKS)),
            pltpu.SemaphoreType.DMA((1,)),
            pltpu.SemaphoreType.DMA((CHUNKS,)),
            pltpu.SemaphoreType.DMA((1,)),
            pltpu.SemaphoreType.DMA((CHUNKS,)),
        ],
        compiler_params=pltpu.CompilerParams(collective_id=1, has_side_effects=True, vmem_limit_bytes=40 * 1024 * 1024),
        cost_estimate=pl.CostEstimate(flops=12_000_000_000, bytes_accessed=6_000_000, transcendentals=0),
        name='mlp_out',
    )(hT, w2, w1f, *ps, wd, wo, o8, xT)


def solution(mesh):
    all_axes = ('x', 'yz')

    def local_step(x_in, ln_scale, w_gate_up, w_attn, w_down, w_out, k_cache, v_cache, lengths, positions):
        xT = x_in.T
        wattnT = w_attn.T
        hT, qkv, w1f, w2, *pieces = call_a(xT, ln_scale[None, :], wattnT, w_gate_up)
        ps = [lax.ppermute(pieces[i], 'x', [(q, (q + i + 1) % NZ) for q in range(NZ)]) for i in range(NZ - 1)]
        proj = jnp.transpose(qkv, (1, 0, 2)).reshape(16, 2304)
        q_raw = proj[:, :2048].reshape(16, 16, 128)
        k_tok = proj[:, 2048:2176]
        v_tok = proj[:, 2176:]
        q_rot = rotary(q_raw.astype(F32), positions).astype(BF16)
        k_rot = rotary(k_tok[:, None, :].astype(F32), positions).astype(BF16)
        o8, k_new, v_new = call_b(lengths, q_rot, k_rot, v_tok[:, None, :], k_cache, v_cache)
        yT = call_c(hT, w2, w1f, ps, w_down, w_out, o8, xT)
        return yT.T, k_new, v_new

    row_spec = P(None, all_axes)
    vec_spec = P(all_axes)
    cache_spec = P(all_axes, None, None)
    return jax.shard_map(
        local_step,
        mesh=mesh,
        in_specs=(row_spec, vec_spec, P('x', None, 'yz'), P('x', 'yz'), P('yz', 'x'), P('yz', 'x'), cache_spec, cache_spec, vec_spec, vec_spec),
        out_specs=(row_spec, cache_spec, cache_spec),
        check_vma=False,
    )
```

```python
import functools

import jax
import jax.numpy as jnp
from jax import lax
from jax.experimental import pallas as pl
from jax.experimental.pallas import tpu as pltpu
from jax.sharding import PartitionSpec as P

LN_EPS = 1e-6
ROPE_BASE = 10000.0
MESH = pl.DeviceIdType.MESH
F32 = jnp.float32
BF16 = jnp.bfloat16

NZ = 4
NP = 8
C1A = 16
C1 = 48
C2 = 128
C3 = 80
CA = C1 + C2
CHUNKS = 4
LANES = 512 // CHUNKS


def rotary(values, positions):
    half_dim = values.shape[-1] // 2
    inv_freq = ROPE_BASE ** (-jnp.arange(half_dim, dtype=jnp.float32) / half_dim)
    angles = positions.astype(jnp.float32)[:, None, None] * inv_freq
    cos_part = jnp.cos(angles)
    sin_part = jnp.sin(angles)
    lo_half = values[..., :half_dim]
    hi_half = values[..., half_dim:]
    return jnp.concatenate([lo_half * cos_part - hi_half * sin_part, hi_half * cos_part + lo_half * sin_part], axis=-1)


def coords():
    z = lax.axis_index('x')
    p = lax.axis_index('yz')
    core = p % 2
    xx = (p // 2) % 2
    y = p // 4
    partner = p + 1 - 2 * core
    xn = p + 2 - 4 * xx
    yn = p + 4 - 8 * y
    diag = xn + 4 - 8 * y
    z1 = z % 2
    z2 = z // 2
    zs = [z, 2 * z2 + 1 - z1, 2 * (1 - z2) + z1, 3 - z]
    return z, p, core, partner, xn, yn, diag, zs


def entry_signal(z, p, zs):
    sem = pltpu.get_barrier_semaphore()
    for k in range(1, NZ):
        pl.semaphore_signal(sem, inc=1, device_id=(zs[k], p), device_id_type=MESH)
    for k in range(1, NP):
        pl.semaphore_signal(sem, inc=1, device_id=(z, (p + k) % NP), device_id_type=MESH)


def entry_wait():
    pl.semaphore_wait(pltpu.get_barrier_semaphore(), NZ - 1 + NP - 1)


def rcopy(src, dst, send, recv, dev):
    return pltpu.make_async_remote_copy(src_ref=src, dst_ref=dst, send_sem=send, recv_sem=recv, device_id=dev, device_id_type=MESH)


class Relay:
    def __init__(self, z, p, at, whole, send, recv):
        self.z, self.p, self.at, self.whole, self.send, self.recv = z, p, at, whole, send, recv

    def copy(self, way, src, ch, dev):
        ref = self.at(src, ch)
        return rcopy(ref, ref, self.send.at[way], self.recv.at[src, ch], (dev, self.p))

    def inward(self, chunks):
        z = self.z

        @pl.when(z < 2)
        def _():
            for ch in chunks:
                self.copy(0, z, ch, z + 1).start()

        @pl.when(z >= 2)
        def _():
            for ch in chunks:
                self.copy(1, z, ch, z - 1).start()

    def outward(self, chunks):
        z = self.z

        @pl.when(z == 1)
        def _():
            for ch in chunks:
                self.copy(1, z, ch, z - 1).start()

        @pl.when(z == 2)
        def _():
            for ch in chunks:
                self.copy(0, z, ch, z + 1).start()

    def step(self, k, ch):
        z = self.z

        @pl.when(z >= k)
        def _():
            self.copy(0, z - k, ch, z).wait_recv()

            @pl.when(z < 3)
            def _():
                self.copy(2 * k, z - k, ch, z + 1).start()

        @pl.when(z + k <= 3)
        def _():
            self.copy(0, z + k, ch, z).wait_recv()

            @pl.when(z > 0)
            def _():
                self.copy(2 * k + 1, z + k, ch, z - 1).start()

    def sent(self, way):
        rcopy(self.whole, self.whole, self.send.at[way], self.recv.at[0, 0], (self.z, self.p)).wait_send()

    def drain(self):
        z = self.z
        for k in range(NZ - 1):
            @pl.when((z >= k) & (z < 3))
            def _():
                self.sent(2 * k)

            @pl.when((z + k <= 3) & (z > 0))
            def _():
                self.sent(2 * k + 1)


def attn_start(q):
    return pl.multiple_of(64 * q + 16 * (q // 2), 16)


def kernel_a(xT_hbm, ln_hbm, wattn_hbm, w_ref, h_ref, qkv_ref, w1f_ref, w2_ref, ps1_ref, ps2_ref, ps3_ref,
             xg, lng, watt, zsend, zrecv, zq, s1, s2, wn, wt, hT_ref, ln_ref, wattn_ref,
             xsend, xrecv, rpart, lsend, lrecv, asend, arecv, zsend_sem, zrecv_sem, qsend, qrecv, wsend, wrecv, lsem, osem, ldummy):
    z, p, core, partner, xn, yn, diag, zs = coords()
    entry_signal(z, p, zs)
    wload = pltpu.make_async_copy(w_ref, wn, lsem.at[0])
    loads = [
        pltpu.make_async_copy(xT_hbm, xg.at[z, p], lsem.at[6]),
        pltpu.make_async_copy(ln_hbm, ln_ref, lsem.at[7]),
        pltpu.make_async_copy(wattn_hbm, wattn_ref, lsem.at[8]),
        wload,
    ]
    for c in loads:
        c.start()
    lng[z, p] = jnp.zeros((1, 128), F32)
    loads[1].wait()
    lng[z, p, 0:1, 0:64] = ln_ref[...]
    loads[0].wait()
    entry_wait()
    here = (z, p)

    def send(src_z, src_p, dev, way=0):
        recv = rpart.at[0] if way == 4 else xrecv.at[way, src_z]
        rcopy(xg.at[src_z, src_p], xg.at[src_z, src_p], xsend.at[0], recv, dev).start()

    def send_l(src_z, dev, phase):
        rcopy(lng.at[src_z, p], lng.at[src_z, p], lsend.at[0], lrecv.at[phase], dev).start()

    def wait_x(src_z, src_p, way):
        rcopy(xg.at[src_z, src_p], xg.at[src_z, src_p], xsend.at[0], xrecv.at[way, src_z], here).wait_recv()

    def stat(src_z, src_p):
        blk = xg[src_z, src_p].astype(F32).reshape(8, 8, 512)
        s1[...] += jnp.sum(blk, axis=0)
        s2[...] += jnp.sum(blk * blk, axis=0)

    spans = tuple((i, C1A) for i in range(0, C1, C1A))

    def w_piece(i, src, dst, dev):
        o, n = spans[i]
        return rcopy(
            wt.at[:, pl.ds(pl.multiple_of(dst * 256 + o, 16), n), :],
            w1f_ref.at[src, :, pl.ds(o, n), :],
            wsend.at[0], wrecv.at[0], dev)

    def send_w(i):
        for k in (3, 2, 1):
            w_piece(i, z, zs[k], (zs[k], p)).start()

    def turn(odd):
        def body(i, carry):
            lanes = pl.ds(pl.multiple_of(i * 256 + odd * 128, 128), 128)
            blk = wn[:, :, lanes].astype(F32)
            for g in range(2):
                wt[g, lanes, :] = blk[:, g, :].T.astype(BF16)
            return carry

        lax.fori_loop(0, NZ, body, 0)

    mid = 2 - z // 2
    far = 3 - 3 * (z // 2)
    zo = [z, zs[1], mid, far]
    inner = (z == 1) | (z == 2)
    send(z, p, (mid, p))
    send(z, p, (zs[1], p))
    for k in (3, 2, 1):
        send_l(z, (zs[k], p), 0)
    targets = ((diag, 3), (xn, 1), (yn, 2), (partner, 4))
    for dev, way in targets:
        send(z, p, (z, dev), way)
    for j in range(1, NP):
        send_l(z, (z, (p + j) % NP), 1)

    def attn_piece(q):
        return rcopy(wattn_ref.at[pl.ds(attn_start(q), 80), :], watt.at[z], asend.at[0], arecv.at[0], (q, p))

    def outward(k):
        return rcopy(xg.at[zo[k], p], xg.at[zo[k], p], osem.at[k - 2], xrecv.at[0, zo[k]], (zs[1], p))

    s1[...] = jnp.zeros_like(s1)
    s2[...] = jnp.zeros_like(s2)
    stat(z, p)
    loads[2].wait()
    watt[z] = wattn_ref[pl.ds(attn_start(z), 80), :]
    wload.wait()
    turn(0)
    attn_piece(mid).start()

    @pl.when(jnp.logical_not(inner))
    def _():
        attn_piece(zs[1]).start()


    def column(k):
        wait_x(zo[k], p, 0)
        if k >= 2:
            @pl.when(inner)
            def _():
                outward(k).start()
        for dev, way in targets:
            send(zo[k], p, (z, dev), way)
        stat(zo[k], p)

    def pass_on(k, src, way):
        wait_x(zo[k], src, way)
        send(zo[k], src, (z, partner), 4)
        stat(zo[k], src)

    column(1)
    column(2)
    column(3)
    rcopy(ldummy.at[pl.ds(0, 3)], ldummy.at[pl.ds(0, 3)], lsend.at[0], lrecv.at[0], here).wait_recv()
    for k in range(1, NZ):
        for j in range(1, NP):
            send_l(zs[k], (z, (p + j) % NP), 1)
    for k in range(2):
        pass_on(k, xn, 1)
        pass_on(k, yn, 2)
    attn_piece(far).start()

    @pl.when(inner)
    def _():
        attn_piece(zs[1]).start()

    send_w(0)
    pass_on(0, diag, 3)
    pass_on(1, diag, 3)
    for k in range(2, NZ):
        pass_on(k, xn, 1)
        pass_on(k, yn, 2)
        pass_on(k, diag, 3)
    send_w(1)
    half = xg.at[pl.ds(0, 2)]
    rcopy(half, half, xsend.at[0], rpart.at[0], here).wait_recv()
    for q in (partner, partner + xn - p, partner + yn - p, partner + diag - p):
        for k in range(NZ):
            stat(zo[k], q)
    rcopy(ldummy.at[pl.ds(0, 28)], ldummy.at[pl.ds(0, 28)], lsend.at[0], lrecv.at[1], here).wait_recv()

    mean = jnp.sum(s1[...], axis=0, keepdims=True) / 2048.0
    var = jnp.sum(s2[...], axis=0, keepdims=True) / 2048.0 - mean * mean
    rstd = lax.rsqrt(var + LN_EPS)
    lnT = jnp.concatenate([lng[i // NP, i % NP, 0:1, :] for i in range(32)] + [jnp.zeros((96, 128), F32)], axis=0).T
    for i in range(NZ * NP):
        sc = lnT[0:64, i:i + 1]
        hT_ref[i * 64:(i + 1) * 64, :] = ((xg[i // NP, i % NP].astype(F32) - mean) * rstd * sc).astype(BF16)

    hout = pltpu.make_async_copy(hT_ref, h_ref, lsem.at[5])
    hout.start()
    three = watt.at[pl.ds(0, 3)]
    rcopy(three, three, asend.at[0], arecv.at[0], here).wait_recv()
    part = None
    for q in range(NZ):
        t = jnp.dot(watt[q], hT_ref[q * 512:(q + 1) * 512, :], preferred_element_type=F32)
        part = t if part is None else part + t
    part = part.astype(BF16)
    for q in range(NZ):
        zsend[q] = part[:, q * 128:(q + 1) * 128]
    for k in (3, 2, 1):
        rcopy(zsend.at[zs[k]], zrecv.at[z], zsend_sem.at[0], zrecv_sem.at[0], (zs[k], p)).start()
    zrecv[z] = zsend[z]
    turn(1)
    send_w(2)
    outs = [pltpu.make_async_copy(wt, w2_ref, lsem.at[1])]
    for i, ps_ref in enumerate((ps1_ref, ps2_ref, ps3_ref)):
        dst = (z + i + 1) % NZ
        outs.append(pltpu.make_async_copy(wt.at[:, pl.ds(pl.multiple_of(dst * 256 + C1, 16), C2), :], ps_ref, lsem.at[2 + i]))
    for c in outs[1:] + outs[:1]:
        c.start()
    zthree = rcopy(zsend.at[pl.ds(0, 3)], zrecv.at[pl.ds(0, 3)], zsend_sem.at[0], zrecv_sem.at[0], here)
    zthree.wait_recv()
    zt = jnp.concatenate([zrecv[0].astype(F32), zrecv[1].astype(F32)[16:80], zrecv[2].astype(F32), zrecv[3].astype(F32)[16:80]], axis=0)
    zq[...] = zt.T.astype(BF16).reshape(NP, 16, 288)
    for j in range(1, NP):
        q = (p + j) % NP
        rcopy(zq.at[q], qkv_ref.at[p], qsend.at[0], qrecv.at[0], (z, q)).start()
    qown = pltpu.make_async_copy(zq.at[p], qkv_ref.at[p], lsem.at[9])
    qown.start()
    qseven = rcopy(zq.at[pl.ds(0, 7)], qkv_ref.at[pl.ds(0, 7)], qsend.at[0], qrecv.at[0], here)
    qseven.wait_recv()
    wthree = w1f_ref.at[pl.ds(0, 3)]
    wall = rcopy(wthree, wthree, wsend.at[0], wrecv.at[0], here)
    wall.wait_recv()
    hout.wait()
    qown.wait()
    for c in outs:
        c.wait()
    sent30 = w2_ref.at[:, pl.ds(0, 960), :]
    rcopy(sent30, sent30, xsend.at[0], rpart.at[0], here).wait_send()
    rcopy(ldummy, ldummy, lsend.at[0], lrecv.at[0], here).wait_send()
    rcopy(three, three, asend.at[0], arecv.at[0], here).wait_send()
    zthree.wait_send()
    qseven.wait_send()
    wall.wait_send()

    @pl.when(inner)
    def _():
        outward(2).wait_send()
        outward(3).wait_send()


def call_a(xT, ln, wattnT, w):
    hbm = pl.BlockSpec(memory_space=pl.ANY)
    return pl.pallas_call(
        kernel_a,
        out_shape=(
            jax.ShapeDtypeStruct((2048, 512), BF16),
            jax.ShapeDtypeStruct((NP, 16, 288), BF16),
            jax.ShapeDtypeStruct((NZ, 2, C1, 512), BF16),
            jax.ShapeDtypeStruct((2, 1024, 512), BF16),
        ) + (jax.ShapeDtypeStruct((2, C2, 512), BF16),) * 3,
        in_specs=[hbm] * 4,
        out_specs=(hbm,) * 7,
        scratch_shapes=[
            pltpu.VMEM((NZ, NP, 64, 512), BF16),
            pltpu.VMEM((NZ, NP, 1, 128), F32),
            pltpu.VMEM((NZ, 80, 512), BF16),
            pltpu.VMEM((NZ, 80, 128), BF16),
            pltpu.VMEM((NZ, 80, 128), BF16),
            pltpu.VMEM((NP, 16, 288), BF16),
            pltpu.VMEM((8, 512), F32),
            pltpu.VMEM((8, 512), F32),
            pltpu.VMEM((512, 2, 1024), BF16),
            pltpu.VMEM((2, 1024, 512), BF16),
            pltpu.VMEM((2048, 512), BF16),
            pltpu.VMEM((1, 64), F32),
            pltpu.VMEM((288, 512), BF16),
            pltpu.SemaphoreType.DMA((1,)),
            pltpu.SemaphoreType.DMA((4, NZ)),
            pltpu.SemaphoreType.DMA((1,)),
            pltpu.SemaphoreType.DMA((1,)),
            pltpu.SemaphoreType.DMA((2,)),
            pltpu.SemaphoreType.DMA((1,)),
            pltpu.SemaphoreType.DMA((1,)),
            pltpu.SemaphoreType.DMA((1,)),
            pltpu.SemaphoreType.DMA((1,)),
            pltpu.SemaphoreType.DMA((1,)),
            pltpu.SemaphoreType.DMA((1,)),
            pltpu.SemaphoreType.DMA((1,)),
            pltpu.SemaphoreType.DMA((1,)),
            pltpu.SemaphoreType.DMA((10,)),
            pltpu.SemaphoreType.DMA((2,)),
            pltpu.VMEM((31, 1, 128), F32),
        ],
        compiler_params=pltpu.CompilerParams(collective_id=0, has_side_effects=True, vmem_limit_bytes=56 * 1024 * 1024),
        name='gather_norm_qkv',
    )(xT, ln, wattnT, w)


def kernel_b(len_ref, q_ref, k_ref, v_ref, kc_ref, vc_ref, o_ref, kn_ref, vn_ref, kbuf, vbuf, oscr, isem, osem):
    rows = kbuf.shape[0]
    seq = kbuf.shape[1]

    def load(b, t):
        return pltpu.make_async_copy((kc_ref, vc_ref)[t].at[b], (kbuf, vbuf)[t].at[b], isem.at[b])

    def store(b, t):
        return pltpu.make_async_copy((kbuf, vbuf)[t].at[b], (kn_ref, vn_ref)[t].at[b], osem.at[0])

    for b in range(rows):
        load(b, 0).start()
        load(b, 1).start()

    def insert(buf, b, length, new):
        base = pl.multiple_of((length // 16) * 16, 16)
        hit = base + lax.broadcasted_iota(jnp.int32, (16, 128), 0) == length
        buf[b, pl.ds(base, 16), :] = jnp.where(hit, new.astype(F32), buf[b, pl.ds(base, 16), :].astype(F32)).astype(BF16)

    def attend(b, length, n):
        scores = lax.dot_general(q_ref[b], kbuf[b, 0:n, :], (((1,), (1,)), ((), ())), preferred_element_type=F32) * (128.0 ** -0.5)
        slot = lax.broadcasted_iota(jnp.int32, scores.shape, 1)
        scores = jnp.where(slot <= length, scores, -1e30)
        top = jnp.max(scores, axis=1, keepdims=True)
        e = jnp.exp(scores - top)
        probs = (e / jnp.sum(e, axis=1, keepdims=True)).astype(BF16)
        return jnp.dot(probs, vbuf[b, 0:n, :], preferred_element_type=F32)

    def pair(i, carry):
        b0 = 2 * i
        b1 = 2 * i + 1
        l0 = len_ref[b0]
        l1 = len_ref[b1]
        for b, length in ((b0, l0), (b1, l1)):
            pltpu.make_async_copy(kc_ref.at[pl.ds(0, 2)], kbuf.at[pl.ds(0, 2)], isem.at[b]).wait()
            insert(kbuf, b, length, k_ref[b])
            insert(vbuf, b, length, v_ref[b])
        last = jnp.maximum(l0, l1) // 512
        for t in range(seq // 512):
            @pl.when(last == t)
            def _():
                n = 512 * (t + 1)
                r0 = attend(b0, l0, n)
                r1 = attend(b1, l1, n)
                oscr[b0] = r0
                oscr[b1] = r1
        for b in (b0, b1):
            store(b, 0).start()
            store(b, 1).start()
        return carry

    lax.fori_loop(0, rows // 2, pair, 0)
    for h in range(16):
        o_ref[h // 2, :, (h % 2) * 128:(h % 2 + 1) * 128] = oscr[:, h, :].astype(BF16)
    pltpu.make_async_copy(kbuf, kn_ref, osem.at[0]).wait()
    pltpu.make_async_copy(vbuf, vn_ref, osem.at[0]).wait()


def call_b(lengths, q_rot, k_rot, v_tok, k_cache, v_cache):
    rows, seq, hd = k_cache.shape
    heads = q_rot.shape[1]
    vm = pl.BlockSpec(memory_space=pltpu.VMEM)
    hbm = pl.BlockSpec(memory_space=pl.ANY)
    return pl.pallas_call(
        kernel_b,
        in_specs=[pl.BlockSpec(memory_space=pltpu.SMEM), vm, vm, vm, hbm, hbm],
        out_specs=(vm, hbm, hbm),
        out_shape=(
            jax.ShapeDtypeStruct((NP, rows, heads * hd // NP), BF16),
            jax.ShapeDtypeStruct(k_cache.shape, BF16),
            jax.ShapeDtypeStruct(v_cache.shape, BF16),
        ),
        scratch_shapes=[
            pltpu.VMEM((rows, seq, hd), BF16),
            pltpu.VMEM((rows, seq, hd), BF16),
            pltpu.VMEM((rows, heads, hd), F32),
            pltpu.SemaphoreType.DMA((rows,)),
            pltpu.SemaphoreType.DMA((1,)),
        ],
        compiler_params=pltpu.CompilerParams(vmem_limit_bytes=58 * 1024 * 1024),
        cost_estimate=pl.CostEstimate(flops=12_000_000_000, bytes_accessed=33_000_000, transcendentals=0),
        name='attend',
    )(lengths, q_rot, k_rot, v_tok, k_cache, v_cache)


def kernel_c(hT, w2_ref, w1f_ref, p1_ref, p2_ref, p3_ref, wd, wo, o_ref, xT_ref, y_ref,
             wvA, wvB, wdAT, wdBT, woT, og, hidA, hidB, yA, ysum, r1, acc, r2,
             wsem, wbsend, wbrecv, osend, orecv, gsend, grecv, hasend, harecv, hbsend, hbrecv,
             r1send, r1recv, r2send, r2recv):
    z, p, core, partner, xn, yn, diag, zs = coords()
    entry_signal(z, p, zs)
    local = [pltpu.make_async_copy(w2_ref.at[:, pl.ds(pl.multiple_of(z * 256, 256), CA), :], wvA.at[z], wsem.at[0])]
    for s, p_ref in ((1, p1_ref), (2, p2_ref), (3, p3_ref)):
        src = (z + NZ - s) % NZ
        local.append(pltpu.make_async_copy(w1f_ref.at[src], wvA.at[src, :, pl.ds(0, C1), :], wsem.at[0]))
        local.append(pltpu.make_async_copy(p_ref, wvA.at[src, :, pl.ds(C1, C2), :], wsem.at[0]))
    late = [
        pltpu.make_async_copy(w2_ref.at[:, pl.ds(pl.multiple_of(z * 256 + CA, 16), C3), :], wvB.at[z], wsem.at[1]),
    ]
    for c in local + late:
        c.start()
    entry_wait()
    here = (z, p)

    def w_piece(src, dst, dev):
        return rcopy(
            w2_ref.at[:, pl.ds(pl.multiple_of(dst * 256 + CA, 16), C3), :],
            wvB.at[src], wbsend.at[0], wbrecv.at[0], dev)

    for k in (3, 2, 1):
        w_piece(z, zs[k], (zs[k], p)).start()
    for j in range(1, NP):
        q = (p + j) % NP
        rcopy(o_ref.at[q], og.at[z, p], osend.at[0], orecv.at[0], (z, q)).start()
    og[z, p] = o_ref[p]

    def gated(wv, n):
        g = None
        for q in range(NZ):
            t = jnp.dot(wv[q].reshape(2 * n, 512), hT[q * 512:(q + 1) * 512, :], preferred_element_type=F32)
            g = t if g is None else g + t
        gate = g[0:n].astype(BF16).astype(F32)
        up = g[n:2 * n].astype(BF16).astype(F32)
        return (jax.nn.silu(gate) * up).astype(BF16)

    ra = Relay(z, p, lambda src, ch: hidA.at[ch, src], hidA.at[0], hasend, harecv)
    rb = Relay(z, p, lambda src, ch: hidB.at[ch, src], hidB.at[0], hbsend, hbrecv)
    ro = Relay(z, p, lambda src, ch: og.at[src], og.at[0], gsend, grecv)
    every = range(CHUNKS)

    pltpu.make_async_copy(wvA, wvA, wsem.at[0]).wait()
    ha = gated(wvA, CA)
    for ch in every:
        hidA[ch, z] = ha[:, ch * LANES:(ch + 1) * LANES]

    ra.outward(every)
    ra.inward(range(2))
    oseven = rcopy(o_ref.at[pl.ds(0, 7)], og.at[z, pl.ds(0, 7)], osend.at[0], orecv.at[0], here)
    oseven.wait_recv()
    ro.outward(range(1))
    ro.inward(range(1))
    for c in late:
        c.wait()
    def by_core(ref, w):
        w = w.T.reshape(4, 2, 64, w.shape[0])
        for j in range(2):
            ref[j] = w[:, j].reshape(256, w.shape[3])

    by_core(wdAT, jnp.concatenate([wd[q * 256:q * 256 + CA, :] for q in range(NZ)], axis=0))
    by_core(wdBT, jnp.concatenate([wd[q * 256 + CA:(q + 1) * 256, :] for q in range(NZ)], axis=0))
    by_core(woT, wo[...])

    wthree = wvB.at[pl.ds(0, 3)]
    wall = rcopy(wthree, wthree, wbsend.at[0], wbrecv.at[0], here)
    wall.wait_recv()
    hb = gated(wvB, C3)
    for ch in range(CHUNKS):
        hidB[ch, z] = hb[:, ch * LANES:(ch + 1) * LANES]
    rb.outward(every)
    rb.inward(range(2))
    for ch in range(2, CHUNKS):
        ra.inward((ch,))
        rb.inward((ch,))
    ro.step(1, 0)
    for ch in range(2):
        ra.step(1, ch)
    for ch in range(2):
        ra.step(2, ch)

    chip = p // 2
    others = [diag // 2, xn // 2, yn // 2]

    def d2d(ch):
        return rcopy(ysum.at[ch, 1 - core], r1.at[ch], r1send.at[0], r1recv.at[ch], (z, partner))

    def hop(ch, i, dev):
        return rcopy(acc.at[ch, i], r2.at[ch, i], r2send.at[0], r2recv.at[ch], (z, dev))

    def stage0(ch):
        o_rows = og[ch * NZ // CHUNKS].reshape(128, 256)
        for j in (1 - core, core):
            yA[j] = jnp.dot(wdAT[j], hidA[ch].reshape(NZ * CA, LANES), preferred_element_type=F32) + lax.dot_general(
                woT[j], o_rows, (((1,), (1,)), ((), ())), preferred_element_type=F32)

    def half(ch, j):
        yt = yA[j] + jnp.dot(wdBT[j], hidB[ch].reshape(NZ * C3, LANES), preferred_element_type=F32)
        ysum[ch, j] = yt.reshape(4, 64, LANES)

    def stage1(ch):
        half(ch, 1 - core)
        d2d(ch).start()
        half(ch, core)

    def stage2(ch):
        d2d(ch).wait_recv()
        for i, (t, dev) in enumerate(zip(others, (diag, xn, yn))):
            acc[ch, i] = ysum[ch, core, t] + r1[ch, t]
            hop(ch, i, dev).start()

    def stage3(ch):
        lanes = slice(ch * LANES, (ch + 1) * LANES)
        mine = ysum[ch, core, chip] + r1[ch, chip]
        rcopy(acc.at[ch], r2.at[ch], r2send.at[0], r2recv.at[ch], here).wait_recv()
        for i in range(3):
            mine = mine + r2[ch, i]
        y_ref[:, lanes] = (xT_ref[:, lanes].astype(F32) + mine).astype(BF16)

    for t in range(1, CHUNKS + 3):
        for k in range(1, NZ - 1):
            ch = t - k
            if 0 <= ch < CHUNKS:
                if ch >= 2:
                    ra.step(k, ch)
                rb.step(k, ch)
        if t < 3:
            ro.step(t + 1, 0)
        if t >= 3:
            ra.step(3, t - 3)
            stage0(t - 3)
            rb.step(3, t - 3)
            stage1(t - 3)
        if t >= 4:
            stage2(t - 4)
    stage2(CHUNKS - 1)
    for ch in every:
        stage3(ch)

    wall.wait_send()
    oseven.wait_send()
    rcopy(r1, r1, r1send.at[0], r1recv.at[0], here).wait_send()
    rcopy(acc, acc, r2send.at[0], r2recv.at[0], here).wait_send()
    ra.drain()
    rb.drain()
    ro.drain()


def call_c(hT, w2, w1f, ps, wd, wo, o8, xT):
    vm = pl.BlockSpec(memory_space=pltpu.VMEM)
    hbm = pl.BlockSpec(memory_space=pl.ANY)
    return pl.pallas_call(
        kernel_c,
        out_shape=jax.ShapeDtypeStruct((64, 512), BF16),
        in_specs=[vm] + [hbm] * 5 + [vm] * 4,
        out_specs=vm,
        scratch_shapes=[
            pltpu.VMEM((NZ, 2, CA, 512), BF16),
            pltpu.VMEM((NZ, 2, C3, 512), BF16),
            pltpu.VMEM((2, 256, NZ * CA), BF16),
            pltpu.VMEM((2, 256, NZ * C3), BF16),
            pltpu.VMEM((2, 256, 256), BF16),
            pltpu.VMEM((NZ, NP, 16, 256), BF16),
            pltpu.VMEM((CHUNKS, NZ, CA, LANES), BF16),
            pltpu.VMEM((CHUNKS, NZ, C3, LANES), BF16),
            pltpu.VMEM((2, 256, LANES), F32),
            pltpu.VMEM((CHUNKS, 2, 4, 64, LANES), F32),
            pltpu.VMEM((CHUNKS, 4, 64, LANES), F32),
            pltpu.VMEM((CHUNKS, 3, 64, LANES), F32),
            pltpu.VMEM((CHUNKS, 3, 64, LANES), F32),
            pltpu.SemaphoreType.DMA((2,)),
            pltpu.SemaphoreType.DMA((1,)),
            pltpu.SemaphoreType.DMA((1,)),
            pltpu.SemaphoreType.DMA((1,)),
            pltpu.SemaphoreType.DMA((1,)),
            pltpu.SemaphoreType.DMA((6,)),
            pltpu.SemaphoreType.DMA((NZ, 1)),
            pltpu.SemaphoreType.DMA((6,)),
            pltpu.SemaphoreType.DMA((NZ, CHUNKS)),
            pltpu.SemaphoreType.DMA((6,)),
            pltpu.SemaphoreType.DMA((NZ, CHUNKS)),
            pltpu.SemaphoreType.DMA((1,)),
            pltpu.SemaphoreType.DMA((CHUNKS,)),
            pltpu.SemaphoreType.DMA((1,)),
            pltpu.SemaphoreType.DMA((CHUNKS,)),
        ],
        compiler_params=pltpu.CompilerParams(collective_id=1, has_side_effects=True, vmem_limit_bytes=40 * 1024 * 1024),
        cost_estimate=pl.CostEstimate(flops=12_000_000_000, bytes_accessed=6_000_000, transcendentals=0),
        name='mlp_out',
    )(hT, w2, w1f, *ps, wd, wo, o8, xT)


def solution(mesh):
    all_axes = ('x', 'yz')

    def local_step(x_in, ln_scale, w_gate_up, w_attn, w_down, w_out, k_cache, v_cache, lengths, positions):
        xT = x_in.T
        wattnT = w_attn.T
        hT, qkv, w1f, w2, *pieces = call_a(xT, ln_scale[None, :], wattnT, w_gate_up)
        ps = [lax.ppermute(pieces[i], 'x', [(q, (q + i + 1) % NZ) for q in range(NZ)]) for i in range(NZ - 1)]
        proj = jnp.transpose(qkv, (1, 0, 2)).reshape(16, 2304)
        q_raw = proj[:, :2048].reshape(16, 16, 128)
        k_tok = proj[:, 2048:2176]
        v_tok = proj[:, 2176:]
        q_rot = rotary(q_raw.astype(F32), positions).astype(BF16)
        k_rot = rotary(k_tok[:, None, :].astype(F32), positions).astype(BF16)
        o8, k_new, v_new = call_b(lengths, q_rot, k_rot, v_tok[:, None, :], k_cache, v_cache)
        yT = call_c(hT, w2, w1f, ps, w_down, w_out, o8, xT)
        return yT.T, k_new, v_new

    row_spec = P(None, all_axes)
    vec_spec = P(all_axes)
    cache_spec = P(all_axes, None, None)
    return jax.shard_map(
        local_step,
        mesh=mesh,
        in_specs=(row_spec, vec_spec, P('x', None, 'yz'), P('x', 'yz'), P('yz', 'x'), P('yz', 'x'), cache_spec, cache_spec, vec_spec, vec_spec),
        out_specs=(row_spec, cache_spec, cache_spec),
        check_vma=False,
    )
```

```python
import functools

import jax
import jax.numpy as jnp
from jax import lax
from jax.experimental import pallas as pl
from jax.experimental.pallas import tpu as pltpu
from jax.sharding import PartitionSpec as P

LN_EPS = 1e-6
ROPE_BASE = 10000.0
MESH = pl.DeviceIdType.MESH
F32 = jnp.float32
BF16 = jnp.bfloat16

NZ = 4
NP = 8
C1A = 16
C1 = 48
C2 = 128
C3 = 80
CA = C1 + C2
CHUNKS = 4
LANES = 512 // CHUNKS


def rotary(values, positions):
    half_dim = values.shape[-1] // 2
    inv_freq = ROPE_BASE ** (-jnp.arange(half_dim, dtype=jnp.float32) / half_dim)
    angles = positions.astype(jnp.float32)[:, None, None] * inv_freq
    cos_part = jnp.cos(angles)
    sin_part = jnp.sin(angles)
    lo_half = values[..., :half_dim]
    hi_half = values[..., half_dim:]
    return jnp.concatenate([lo_half * cos_part - hi_half * sin_part, hi_half * cos_part + lo_half * sin_part], axis=-1)


def coords():
    z = lax.axis_index('x')
    p = lax.axis_index('yz')
    core = p % 2
    xx = (p // 2) % 2
    y = p // 4
    partner = p + 1 - 2 * core
    xn = p + 2 - 4 * xx
    yn = p + 4 - 8 * y
    diag = xn + 4 - 8 * y
    z1 = z % 2
    z2 = z // 2
    zs = [z, 2 * z2 + 1 - z1, 2 * (1 - z2) + z1, 3 - z]
    return z, p, core, partner, xn, yn, diag, zs


def entry_signal(z, p, zs):
    sem = pltpu.get_barrier_semaphore()
    for k in range(1, NZ):
        pl.semaphore_signal(sem, inc=1, device_id=(zs[k], p), device_id_type=MESH)
    for k in range(1, NP):
        pl.semaphore_signal(sem, inc=1, device_id=(z, (p + k) % NP), device_id_type=MESH)


def entry_wait():
    pl.semaphore_wait(pltpu.get_barrier_semaphore(), NZ - 1 + NP - 1)


def rcopy(src, dst, send, recv, dev):
    return pltpu.make_async_remote_copy(src_ref=src, dst_ref=dst, send_sem=send, recv_sem=recv, device_id=dev, device_id_type=MESH)


class Relay:
    def __init__(self, z, p, at, whole, send, recv):
        self.z, self.p, self.at, self.whole, self.send, self.recv = z, p, at, whole, send, recv

    def copy(self, way, src, ch, dev):
        ref = self.at(src, ch)
        return rcopy(ref, ref, self.send.at[way], self.recv.at[src, ch], (dev, self.p))

    def inward(self, chunks):
        z = self.z

        @pl.when(z < 2)
        def _():
            for ch in chunks:
                self.copy(0, z, ch, z + 1).start()

        @pl.when(z >= 2)
        def _():
            for ch in chunks:
                self.copy(1, z, ch, z - 1).start()

    def outward(self, chunks):
        z = self.z

        @pl.when(z == 1)
        def _():
            for ch in chunks:
                self.copy(1, z, ch, z - 1).start()

        @pl.when(z == 2)
        def _():
            for ch in chunks:
                self.copy(0, z, ch, z + 1).start()

    def step(self, k, ch):
        z = self.z

        @pl.when(z >= k)
        def _():
            self.copy(0, z - k, ch, z).wait_recv()

            @pl.when(z < 3)
            def _():
                self.copy(2 * k, z - k, ch, z + 1).start()

        @pl.when(z + k <= 3)
        def _():
            self.copy(0, z + k, ch, z).wait_recv()

            @pl.when(z > 0)
            def _():
                self.copy(2 * k + 1, z + k, ch, z - 1).start()

    def sent(self, way):
        rcopy(self.whole, self.whole, self.send.at[way], self.recv.at[0, 0], (self.z, self.p)).wait_send()

    def drain(self):
        z = self.z
        for k in range(NZ - 1):
            @pl.when((z >= k) & (z < 3))
            def _():
                self.sent(2 * k)

            @pl.when((z + k <= 3) & (z > 0))
            def _():
                self.sent(2 * k + 1)


def attn_start(q):
    return pl.multiple_of(64 * q + 16 * (q // 2), 16)


def kernel_a(xT_hbm, ln_hbm, wattn_hbm, w_ref, h_ref, qkv_ref, w1f_ref, w2_ref, ps1_ref, ps2_ref, ps3_ref,
             xg, lng, watt, zsend, zrecv, zq, s1, s2, wn, wt, hT_ref, ln_ref, wattn_ref,
             xsend, xrecv, rpart, lsend, lrecv, asend, arecv, zsend_sem, zrecv_sem, qsend, qrecv, wsend, wrecv, lsem, osem, ldummy):
    z, p, core, partner, xn, yn, diag, zs = coords()
    entry_signal(z, p, zs)
    wload = pltpu.make_async_copy(w_ref, wn, lsem.at[0])
    loads = [
        pltpu.make_async_copy(xT_hbm, xg.at[z, p], lsem.at[6]),
        pltpu.make_async_copy(ln_hbm, ln_ref, lsem.at[7]),
        pltpu.make_async_copy(wattn_hbm, wattn_ref, lsem.at[8]),
        wload,
    ]
    for c in loads:
        c.start()
    lng[z, p] = jnp.zeros((1, 128), F32)
    loads[1].wait()
    lng[z, p, 0:1, 0:64] = ln_ref[...]
    loads[0].wait()
    entry_wait()
    here = (z, p)

    def send(src_z, src_p, dev, way=0):
        recv = rpart.at[0] if way == 4 else xrecv.at[way, src_z]
        rcopy(xg.at[src_z, src_p], xg.at[src_z, src_p], xsend.at[0], recv, dev).start()

    def send_l(src_z, dev, phase):
        rcopy(lng.at[src_z, p], lng.at[src_z, p], lsend.at[0], lrecv.at[phase], dev).start()

    def wait_x(src_z, src_p, way):
        rcopy(xg.at[src_z, src_p], xg.at[src_z, src_p], xsend.at[0], xrecv.at[way, src_z], here).wait_recv()

    def stat(src_z, src_p):
        blk = xg[src_z, src_p].astype(F32).reshape(8, 8, 512)
        s1[...] += jnp.sum(blk, axis=0)
        s2[...] += jnp.sum(blk * blk, axis=0)

    spans = tuple((i, C1A) for i in range(0, C1, C1A))

    def w_piece(i, src, dst, dev):
        o, n = spans[i]
        return rcopy(
            wt.at[:, pl.ds(pl.multiple_of(dst * 256 + o, 16), n), :],
            w1f_ref.at[src, :, pl.ds(o, n), :],
            wsend.at[0], wrecv.at[0], dev)

    def send_w(i):
        for k in (3, 2, 1):
            w_piece(i, z, zs[k], (zs[k], p)).start()

    def turn(odd):
        def body(i, carry):
            lanes = pl.ds(pl.multiple_of(i * 256 + odd * 128, 128), 128)
            blk = wn[:, :, lanes].astype(F32)
            for g in range(2):
                wt[g, lanes, :] = blk[:, g, :].T.astype(BF16)
            return carry

        lax.fori_loop(0, NZ, body, 0)

    mid = 2 - z // 2
    far = 3 - 3 * (z // 2)
    zo = [z, zs[1], mid, far]
    inner = (z == 1) | (z == 2)
    send(z, p, (mid, p))
    send(z, p, (zs[1], p))
    for k in (3, 2, 1):
        send_l(z, (zs[k], p), 0)
    targets = ((diag, 3), (xn, 1), (yn, 2), (partner, 4))
    for dev, way in targets:
        send(z, p, (z, dev), way)
    for j in range(1, NP):
        send_l(z, (z, (p + j) % NP), 1)

    def attn_piece(q):
        return rcopy(wattn_ref.at[pl.ds(attn_start(q), 80), :], watt.at[z], asend.at[0], arecv.at[0], (q, p))

    def outward(k):
        return rcopy(xg.at[zo[k], p], xg.at[zo[k], p], osem.at[k - 2], xrecv.at[0, zo[k]], (zs[1], p))

    s1[...] = jnp.zeros_like(s1)
    s2[...] = jnp.zeros_like(s2)
    stat(z, p)
    loads[2].wait()
    watt[z] = wattn_ref[pl.ds(attn_start(z), 80), :]
    wload.wait()
    turn(0)
    attn_piece(mid).start()

    @pl.when(jnp.logical_not(inner))
    def _():
        attn_piece(zs[1]).start()


    def column(k):
        wait_x(zo[k], p, 0)
        if k >= 2:
            @pl.when(inner)
            def _():
                outward(k).start()
        for dev, way in targets:
            send(zo[k], p, (z, dev), way)
        stat(zo[k], p)

    def pass_on(k, src, way):
        wait_x(zo[k], src, way)
        send(zo[k], src, (z, partner), 4)
        stat(zo[k], src)

    column(1)
    column(2)
    column(3)
    rcopy(ldummy.at[pl.ds(0, 3)], ldummy.at[pl.ds(0, 3)], lsend.at[0], lrecv.at[0], here).wait_recv()
    for k in range(1, NZ):
        for j in range(1, NP):
            send_l(zs[k], (z, (p + j) % NP), 1)
    for k in range(2):
        pass_on(k, xn, 1)
        pass_on(k, yn, 2)
    attn_piece(far).start()

    @pl.when(inner)
    def _():
        attn_piece(zs[1]).start()

    send_w(0)
    pass_on(0, diag, 3)
    pass_on(1, diag, 3)
    for k in range(2, NZ):
        pass_on(k, xn, 1)
        pass_on(k, yn, 2)
        pass_on(k, diag, 3)
    send_w(1)
    half = xg.at[pl.ds(0, 2)]
    rcopy(half, half, xsend.at[0], rpart.at[0], here).wait_recv()
    for q in (partner, partner + xn - p, partner + yn - p, partner + diag - p):
        for k in range(NZ):
            stat(zo[k], q)
    rcopy(ldummy.at[pl.ds(0, 28)], ldummy.at[pl.ds(0, 28)], lsend.at[0], lrecv.at[1], here).wait_recv()

    mean = jnp.sum(s1[...], axis=0, keepdims=True) / 2048.0
    var = jnp.sum(s2[...], axis=0, keepdims=True) / 2048.0 - mean * mean
    rstd = lax.rsqrt(var + LN_EPS)
    lnT = jnp.concatenate([lng[i // NP, i % NP, 0:1, :] for i in range(32)] + [jnp.zeros((96, 128), F32)], axis=0).T
    for i in range(NZ * NP):
        sc = lnT[0:64, i:i + 1]
        hT_ref[i * 64:(i + 1) * 64, :] = ((xg[i // NP, i % NP].astype(F32) - mean) * rstd * sc).astype(BF16)

    hout = pltpu.make_async_copy(hT_ref, h_ref, lsem.at[5])
    hout.start()
    three = watt.at[pl.ds(0, 3)]
    rcopy(three, three, asend.at[0], arecv.at[0], here).wait_recv()
    part = None
    for q in range(NZ):
        t = jnp.dot(watt[q], hT_ref[q * 512:(q + 1) * 512, :], preferred_element_type=F32)
        part = t if part is None else part + t
    part = part.astype(BF16)
    for q in range(NZ):
        zsend[q] = part[:, q * 128:(q + 1) * 128]
    for k in (3, 2, 1):
        rcopy(zsend.at[zs[k]], zrecv.at[z], zsend_sem.at[0], zrecv_sem.at[0], (zs[k], p)).start()
    zrecv[z] = zsend[z]
    turn(1)
    send_w(2)
    outs = [pltpu.make_async_copy(wt, w2_ref, lsem.at[1])]
    for i, ps_ref in enumerate((ps1_ref, ps2_ref, ps3_ref)):
        dst = (z + i + 1) % NZ
        outs.append(pltpu.make_async_copy(wt.at[:, pl.ds(pl.multiple_of(dst * 256 + C1, 16), C2), :], ps_ref, lsem.at[2 + i]))
    for c in outs[1:] + outs[:1]:
        c.start()
    zthree = rcopy(zsend.at[pl.ds(0, 3)], zrecv.at[pl.ds(0, 3)], zsend_sem.at[0], zrecv_sem.at[0], here)
    zthree.wait_recv()
    zt = jnp.concatenate([zrecv[0].astype(F32), zrecv[1].astype(F32)[16:80], zrecv[2].astype(F32), zrecv[3].astype(F32)[16:80]], axis=0)
    zq[...] = zt.T.astype(BF16).reshape(NP, 16, 288)
    for j in range(1, NP):
        q = (p + j) % NP
        rcopy(zq.at[q], qkv_ref.at[p], qsend.at[0], qrecv.at[0], (z, q)).start()
    qown = pltpu.make_async_copy(zq.at[p], qkv_ref.at[p], lsem.at[9])
    qown.start()
    qseven = rcopy(zq.at[pl.ds(0, 7)], qkv_ref.at[pl.ds(0, 7)], qsend.at[0], qrecv.at[0], here)
    qseven.wait_recv()
    wthree = w1f_ref.at[pl.ds(0, 3)]
    wall = rcopy(wthree, wthree, wsend.at[0], wrecv.at[0], here)
    wall.wait_recv()
    hout.wait()
    qown.wait()
    for c in outs:
        c.wait()
    sent30 = w2_ref.at[:, pl.ds(0, 960), :]
    rcopy(sent30, sent30, xsend.at[0], rpart.at[0], here).wait_send()
    rcopy(ldummy, ldummy, lsend.at[0], lrecv.at[0], here).wait_send()
    rcopy(three, three, asend.at[0], arecv.at[0], here).wait_send()
    zthree.wait_send()
    qseven.wait_send()
    wall.wait_send()

    @pl.when(inner)
    def _():
        outward(2).wait_send()
        outward(3).wait_send()


def call_a(xT, ln, wattnT, w):
    hbm = pl.BlockSpec(memory_space=pl.ANY)
    return pl.pallas_call(
        kernel_a,
        out_shape=(
            jax.ShapeDtypeStruct((2048, 512), BF16),
            jax.ShapeDtypeStruct((NP, 16, 288), BF16),
            jax.ShapeDtypeStruct((NZ, 2, C1, 512), BF16),
            jax.ShapeDtypeStruct((2, 1024, 512), BF16),
        ) + (jax.ShapeDtypeStruct((2, C2, 512), BF16),) * 3,
        in_specs=[hbm] * 4,
        out_specs=(hbm,) * 7,
        scratch_shapes=[
            pltpu.VMEM((NZ, NP, 64, 512), BF16),
            pltpu.VMEM((NZ, NP, 1, 128), F32),
            pltpu.VMEM((NZ, 80, 512), BF16),
            pltpu.VMEM((NZ, 80, 128), BF16),
            pltpu.VMEM((NZ, 80, 128), BF16),
            pltpu.VMEM((NP, 16, 288), BF16),
            pltpu.VMEM((8, 512), F32),
            pltpu.VMEM((8, 512), F32),
            pltpu.VMEM((512, 2, 1024), BF16),
            pltpu.VMEM((2, 1024, 512), BF16),
            pltpu.VMEM((2048, 512), BF16),
            pltpu.VMEM((1, 64), F32),
            pltpu.VMEM((288, 512), BF16),
            pltpu.SemaphoreType.DMA((1,)),
            pltpu.SemaphoreType.DMA((4, NZ)),
            pltpu.SemaphoreType.DMA((1,)),
            pltpu.SemaphoreType.DMA((1,)),
            pltpu.SemaphoreType.DMA((2,)),
            pltpu.SemaphoreType.DMA((1,)),
            pltpu.SemaphoreType.DMA((1,)),
            pltpu.SemaphoreType.DMA((1,)),
            pltpu.SemaphoreType.DMA((1,)),
            pltpu.SemaphoreType.DMA((1,)),
            pltpu.SemaphoreType.DMA((1,)),
            pltpu.SemaphoreType.DMA((1,)),
            pltpu.SemaphoreType.DMA((1,)),
            pltpu.SemaphoreType.DMA((10,)),
            pltpu.SemaphoreType.DMA((2,)),
            pltpu.VMEM((31, 1, 128), F32),
        ],
        compiler_params=pltpu.CompilerParams(collective_id=0, has_side_effects=True, vmem_limit_bytes=56 * 1024 * 1024),
        name='gather_norm_qkv',
    )(xT, ln, wattnT, w)


def kernel_b(len_ref, q_ref, k_ref, v_ref, kc_ref, vc_ref, o_ref, kn_ref, vn_ref, kbuf, vbuf, oscr, isem, osem):
    rows = kbuf.shape[0]
    seq = kbuf.shape[1]

    def load(b, t):
        return pltpu.make_async_copy((kc_ref, vc_ref)[t].at[b], (kbuf, vbuf)[t].at[b], isem.at[b])

    def store(b, t):
        return pltpu.make_async_copy((kbuf, vbuf)[t].at[b], (kn_ref, vn_ref)[t].at[b], osem.at[0])

    for b in range(rows):
        load(b, 0).start()
        load(b, 1).start()

    def insert(buf, b, length, new):
        base = pl.multiple_of((length // 16) * 16, 16)
        hit = base + lax.broadcasted_iota(jnp.int32, (16, 128), 0) == length
        buf[b, pl.ds(base, 16), :] = jnp.where(hit, new.astype(F32), buf[b, pl.ds(base, 16), :].astype(F32)).astype(BF16)

    def attend(b, length, n):
        scores = lax.dot_general(q_ref[b], kbuf[b, 0:n, :], (((1,), (1,)), ((), ())), preferred_element_type=F32) * (128.0 ** -0.5)
        slot = lax.broadcasted_iota(jnp.int32, scores.shape, 1)
        scores = jnp.where(slot <= length, scores, -1e30)
        top = jnp.max(scores, axis=1, keepdims=True)
        e = jnp.exp(scores - top)
        probs = (e / jnp.sum(e, axis=1, keepdims=True)).astype(BF16)
        return jnp.dot(probs, vbuf[b, 0:n, :], preferred_element_type=F32)

    def pair(i, carry):
        b0 = 2 * i
        b1 = 2 * i + 1
        l0 = len_ref[b0]
        l1 = len_ref[b1]
        for b, length in ((b0, l0), (b1, l1)):
            pltpu.make_async_copy(kc_ref.at[pl.ds(0, 2)], kbuf.at[pl.ds(0, 2)], isem.at[b]).wait()
            insert(kbuf, b, length, k_ref[b])
            insert(vbuf, b, length, v_ref[b])
        last = jnp.maximum(l0, l1) // 512
        for t in range(seq // 512):
            @pl.when(last == t)
            def _():
                n = 512 * (t + 1)
                r0 = attend(b0, l0, n)
                r1 = attend(b1, l1, n)
                oscr[b0] = r0
                oscr[b1] = r1
        for b in (b0, b1):
            store(b, 0).start()
            store(b, 1).start()
        return carry

    lax.fori_loop(0, rows // 2, pair, 0)
    for h in range(16):
        o_ref[h // 2, :, (h % 2) * 128:(h % 2 + 1) * 128] = oscr[:, h, :].astype(BF16)
    pltpu.make_async_copy(kbuf, kn_ref, osem.at[0]).wait()
    pltpu.make_async_copy(vbuf, vn_ref, osem.at[0]).wait()


def call_b(lengths, q_rot, k_rot, v_tok, k_cache, v_cache):
    rows, seq, hd = k_cache.shape
    heads = q_rot.shape[1]
    vm = pl.BlockSpec(memory_space=pltpu.VMEM)
    hbm = pl.BlockSpec(memory_space=pl.ANY)
    return pl.pallas_call(
        kernel_b,
        in_specs=[pl.BlockSpec(memory_space=pltpu.SMEM), vm, vm, vm, hbm, hbm],
        out_specs=(vm, hbm, hbm),
        out_shape=(
            jax.ShapeDtypeStruct((NP, rows, heads * hd // NP), BF16),
            jax.ShapeDtypeStruct(k_cache.shape, BF16),
            jax.ShapeDtypeStruct(v_cache.shape, BF16),
        ),
        scratch_shapes=[
            pltpu.VMEM((rows, seq, hd), BF16),
            pltpu.VMEM((rows, seq, hd), BF16),
            pltpu.VMEM((rows, heads, hd), F32),
            pltpu.SemaphoreType.DMA((rows,)),
            pltpu.SemaphoreType.DMA((1,)),
        ],
        compiler_params=pltpu.CompilerParams(vmem_limit_bytes=52 * 1024 * 1024),
        cost_estimate=pl.CostEstimate(flops=12_000_000_000, bytes_accessed=33_000_000, transcendentals=0),
        name='attend',
    )(lengths, q_rot, k_rot, v_tok, k_cache, v_cache)


def kernel_c(hT, w2_ref, w1f_ref, p1_ref, p2_ref, p3_ref, wd, wo, o_ref, xT_ref, y_ref,
             wvA, wvB, wdAT, wdBT, woT, og, hidA, hidB, yA, ysum, r1, acc, r2,
             wsem, wbsend, wbrecv, osend, orecv, gsend, grecv, hasend, harecv, hbsend, hbrecv,
             r1send, r1recv, r2send, r2recv):
    z, p, core, partner, xn, yn, diag, zs = coords()
    entry_signal(z, p, zs)
    local = [pltpu.make_async_copy(w2_ref.at[:, pl.ds(pl.multiple_of(z * 256, 256), CA), :], wvA.at[z], wsem.at[0])]
    for s, p_ref in ((1, p1_ref), (2, p2_ref), (3, p3_ref)):
        src = (z + NZ - s) % NZ
        local.append(pltpu.make_async_copy(w1f_ref.at[src], wvA.at[src, :, pl.ds(0, C1), :], wsem.at[0]))
        local.append(pltpu.make_async_copy(p_ref, wvA.at[src, :, pl.ds(C1, C2), :], wsem.at[0]))
    late = [
        pltpu.make_async_copy(w2_ref.at[:, pl.ds(pl.multiple_of(z * 256 + CA, 16), C3), :], wvB.at[z], wsem.at[1]),
    ]
    for c in local + late:
        c.start()
    entry_wait()
    here = (z, p)

    def w_piece(src, dst, dev):
        return rcopy(
            w2_ref.at[:, pl.ds(pl.multiple_of(dst * 256 + CA, 16), C3), :],
            wvB.at[src], wbsend.at[0], wbrecv.at[0], dev)

    for k in (3, 2, 1):
        w_piece(z, zs[k], (zs[k], p)).start()
    for j in range(1, NP):
        q = (p + j) % NP
        rcopy(o_ref.at[q], og.at[z, p], osend.at[0], orecv.at[0], (z, q)).start()
    og[z, p] = o_ref[p]

    def gated(wv, n):
        g = None
        for q in range(NZ):
            t = jnp.dot(wv[q].reshape(2 * n, 512), hT[q * 512:(q + 1) * 512, :], preferred_element_type=F32)
            g = t if g is None else g + t
        gate = g[0:n].astype(BF16).astype(F32)
        up = g[n:2 * n].astype(BF16).astype(F32)
        return (jax.nn.silu(gate) * up).astype(BF16)

    ra = Relay(z, p, lambda src, ch: hidA.at[ch, src], hidA.at[0], hasend, harecv)
    rb = Relay(z, p, lambda src, ch: hidB.at[ch, src], hidB.at[0], hbsend, hbrecv)
    ro = Relay(z, p, lambda src, ch: og.at[src], og.at[0], gsend, grecv)
    every = range(CHUNKS)

    pltpu.make_async_copy(wvA, wvA, wsem.at[0]).wait()
    ha = gated(wvA, CA)
    for ch in every:
        hidA[ch, z] = ha[:, ch * LANES:(ch + 1) * LANES]

    ra.outward(every)
    ra.inward(range(2))
    oseven = rcopy(o_ref.at[pl.ds(0, 7)], og.at[z, pl.ds(0, 7)], osend.at[0], orecv.at[0], here)
    oseven.wait_recv()
    ro.outward(range(1))
    ro.inward(range(1))
    for c in late:
        c.wait()
    def by_core(ref, w):
        w = w.T.reshape(4, 2, 64, w.shape[0])
        for j in range(2):
            ref[j] = w[:, j].reshape(256, w.shape[3])

    by_core(wdAT, jnp.concatenate([wd[q * 256:q * 256 + CA, :] for q in range(NZ)], axis=0))
    by_core(wdBT, jnp.concatenate([wd[q * 256 + CA:(q + 1) * 256, :] for q in range(NZ)], axis=0))
    by_core(woT, wo[...])

    wthree = wvB.at[pl.ds(0, 3)]
    wall = rcopy(wthree, wthree, wbsend.at[0], wbrecv.at[0], here)
    wall.wait_recv()
    hb = gated(wvB, C3)
    for ch in range(CHUNKS):
        hidB[ch, z] = hb[:, ch * LANES:(ch + 1) * LANES]
    rb.outward(every)
    rb.inward(range(2))
    for ch in range(2, CHUNKS):
        ra.inward((ch,))
        rb.inward((ch,))
    ro.step(1, 0)
    for ch in range(2):
        ra.step(1, ch)
    for ch in range(2):
        ra.step(2, ch)

    chip = p // 2
    others = [diag // 2, xn // 2, yn // 2]

    def d2d(ch):
        return rcopy(ysum.at[ch, 1 - core], r1.at[ch], r1send.at[0], r1recv.at[ch], (z, partner))

    def hop(ch, i, dev):
        return rcopy(acc.at[ch, i], r2.at[ch, i], r2send.at[0], r2recv.at[ch], (z, dev))

    def stage0(ch):
        o_rows = og[ch * NZ // CHUNKS].reshape(128, 256)
        for j in (1 - core, core):
            yA[j] = jnp.dot(wdAT[j], hidA[ch].reshape(NZ * CA, LANES), preferred_element_type=F32) + lax.dot_general(
                woT[j], o_rows, (((1,), (1,)), ((), ())), preferred_element_type=F32)

    def half(ch, j):
        yt = yA[j] + jnp.dot(wdBT[j], hidB[ch].reshape(NZ * C3, LANES), preferred_element_type=F32)
        ysum[ch, j] = yt.reshape(4, 64, LANES)

    def stage1(ch):
        half(ch, 1 - core)
        d2d(ch).start()
        half(ch, core)

    def stage2(ch):
        d2d(ch).wait_recv()
        for i, (t, dev) in enumerate(zip(others, (diag, xn, yn))):
            acc[ch, i] = ysum[ch, core, t] + r1[ch, t]
            hop(ch, i, dev).start()

    def stage3(ch):
        lanes = slice(ch * LANES, (ch + 1) * LANES)
        mine = ysum[ch, core, chip] + r1[ch, chip]
        rcopy(acc.at[ch], r2.at[ch], r2send.at[0], r2recv.at[ch], here).wait_recv()
        for i in range(3):
            mine = mine + r2[ch, i]
        y_ref[:, lanes] = (xT_ref[:, lanes].astype(F32) + mine).astype(BF16)

    for t in range(1, CHUNKS + 3):
        for k in range(1, NZ - 1):
            ch = t - k
            if 0 <= ch < CHUNKS:
                if ch >= 2:
                    ra.step(k, ch)
                rb.step(k, ch)
        if t < 3:
            ro.step(t + 1, 0)
        if t >= 3:
            ra.step(3, t - 3)
            stage0(t - 3)
            rb.step(3, t - 3)
            stage1(t - 3)
        if t >= 4:
            stage2(t - 4)
    stage2(CHUNKS - 1)
    for ch in every:
        stage3(ch)

    wall.wait_send()
    oseven.wait_send()
    rcopy(r1, r1, r1send.at[0], r1recv.at[0], here).wait_send()
    rcopy(acc, acc, r2send.at[0], r2recv.at[0], here).wait_send()
    ra.drain()
    rb.drain()
    ro.drain()


def call_c(hT, w2, w1f, ps, wd, wo, o8, xT):
    vm = pl.BlockSpec(memory_space=pltpu.VMEM)
    hbm = pl.BlockSpec(memory_space=pl.ANY)
    return pl.pallas_call(
        kernel_c,
        out_shape=jax.ShapeDtypeStruct((64, 512), BF16),
        in_specs=[vm] + [hbm] * 5 + [vm] * 4,
        out_specs=vm,
        scratch_shapes=[
            pltpu.VMEM((NZ, 2, CA, 512), BF16),
            pltpu.VMEM((NZ, 2, C3, 512), BF16),
            pltpu.VMEM((2, 256, NZ * CA), BF16),
            pltpu.VMEM((2, 256, NZ * C3), BF16),
            pltpu.VMEM((2, 256, 256), BF16),
            pltpu.VMEM((NZ, NP, 16, 256), BF16),
            pltpu.VMEM((CHUNKS, NZ, CA, LANES), BF16),
            pltpu.VMEM((CHUNKS, NZ, C3, LANES), BF16),
            pltpu.VMEM((2, 256, LANES), F32),
            pltpu.VMEM((CHUNKS, 2, 4, 64, LANES), F32),
            pltpu.VMEM((CHUNKS, 4, 64, LANES), F32),
            pltpu.VMEM((CHUNKS, 3, 64, LANES), F32),
            pltpu.VMEM((CHUNKS, 3, 64, LANES), F32),
            pltpu.SemaphoreType.DMA((2,)),
            pltpu.SemaphoreType.DMA((1,)),
            pltpu.SemaphoreType.DMA((1,)),
            pltpu.SemaphoreType.DMA((1,)),
            pltpu.SemaphoreType.DMA((1,)),
            pltpu.SemaphoreType.DMA((6,)),
            pltpu.SemaphoreType.DMA((NZ, 1)),
            pltpu.SemaphoreType.DMA((6,)),
            pltpu.SemaphoreType.DMA((NZ, CHUNKS)),
            pltpu.SemaphoreType.DMA((6,)),
            pltpu.SemaphoreType.DMA((NZ, CHUNKS)),
            pltpu.SemaphoreType.DMA((1,)),
            pltpu.SemaphoreType.DMA((CHUNKS,)),
            pltpu.SemaphoreType.DMA((1,)),
            pltpu.SemaphoreType.DMA((CHUNKS,)),
        ],
        compiler_params=pltpu.CompilerParams(collective_id=1, has_side_effects=True, vmem_limit_bytes=40 * 1024 * 1024),
        cost_estimate=pl.CostEstimate(flops=12_000_000_000, bytes_accessed=6_000_000, transcendentals=0),
        name='mlp_out',
    )(hT, w2, w1f, *ps, wd, wo, o8, xT)


def solution(mesh):
    all_axes = ('x', 'yz')

    def local_step(x_in, ln_scale, w_gate_up, w_attn, w_down, w_out, k_cache, v_cache, lengths, positions):
        xT = x_in.T
        wattnT = w_attn.T
        hT, qkv, w1f, w2, *pieces = call_a(xT, ln_scale[None, :], wattnT, w_gate_up)
        ps = [lax.ppermute(pieces[i], 'x', [(q, (q + i + 1) % NZ) for q in range(NZ)]) for i in range(NZ - 1)]
        proj = jnp.transpose(qkv, (1, 0, 2)).reshape(16, 2304)
        q_raw = proj[:, :2048].reshape(16, 16, 128)
        k_tok = proj[:, 2048:2176]
        v_tok = proj[:, 2176:]
        q_rot = rotary(q_raw.astype(F32), positions).astype(BF16)
        k_rot = rotary(k_tok[:, None, :].astype(F32), positions).astype(BF16)
        o8, k_new, v_new = call_b(lengths, q_rot, k_rot, v_tok[:, None, :], k_cache, v_cache)
        yT = call_c(hT, w2, w1f, ps, w_down, w_out, o8, xT)
        return yT.T, k_new, v_new

    row_spec = P(None, all_axes)
    vec_spec = P(all_axes)
    cache_spec = P(all_axes, None, None)
    return jax.shard_map(
        local_step,
        mesh=mesh,
        in_specs=(row_spec, vec_spec, P('x', None, 'yz'), P('x', 'yz'), P('yz', 'x'), P('yz', 'x'), cache_spec, cache_spec, vec_spec, vec_spec),
        out_specs=(row_spec, cache_spec, cache_spec),
        check_vma=False,
    )
```

```python
import functools

import jax
import jax.numpy as jnp
from jax import lax
from jax.experimental import pallas as pl
from jax.experimental.pallas import tpu as pltpu
from jax.sharding import PartitionSpec as P

LN_EPS = 1e-6
ROPE_BASE = 10000.0
MESH = pl.DeviceIdType.MESH
F32 = jnp.float32
BF16 = jnp.bfloat16

NZ = 4
NP = 8
C1A = 16
C1 = 48
C2 = 112
C3 = 96
CA = C1 + C2
CHUNKS = 4
LANES = 512 // CHUNKS


def rotary(values, positions):
    half_dim = values.shape[-1] // 2
    inv_freq = ROPE_BASE ** (-jnp.arange(half_dim, dtype=jnp.float32) / half_dim)
    angles = positions.astype(jnp.float32)[:, None, None] * inv_freq
    cos_part = jnp.cos(angles)
    sin_part = jnp.sin(angles)
    lo_half = values[..., :half_dim]
    hi_half = values[..., half_dim:]
    return jnp.concatenate([lo_half * cos_part - hi_half * sin_part, hi_half * cos_part + lo_half * sin_part], axis=-1)


def coords():
    z = lax.axis_index('x')
    p = lax.axis_index('yz')
    core = p % 2
    xx = (p // 2) % 2
    y = p // 4
    partner = p + 1 - 2 * core
    xn = p + 2 - 4 * xx
    yn = p + 4 - 8 * y
    diag = xn + 4 - 8 * y
    z1 = z % 2
    z2 = z // 2
    zs = [z, 2 * z2 + 1 - z1, 2 * (1 - z2) + z1, 3 - z]
    return z, p, core, partner, xn, yn, diag, zs


def entry_signal(z, p, zs):
    sem = pltpu.get_barrier_semaphore()
    for k in range(1, NZ):
        pl.semaphore_signal(sem, inc=1, device_id=(zs[k], p), device_id_type=MESH)
    for k in range(1, NP):
        pl.semaphore_signal(sem, inc=1, device_id=(z, (p + k) % NP), device_id_type=MESH)


def entry_wait():
    pl.semaphore_wait(pltpu.get_barrier_semaphore(), NZ - 1 + NP - 1)


def rcopy(src, dst, send, recv, dev):
    return pltpu.make_async_remote_copy(src_ref=src, dst_ref=dst, send_sem=send, recv_sem=recv, device_id=dev, device_id_type=MESH)


class Relay:
    def __init__(self, z, p, at, whole, send, recv):
        self.z, self.p, self.at, self.whole, self.send, self.recv = z, p, at, whole, send, recv

    def copy(self, way, src, ch, dev):
        ref = self.at(src, ch)
        return rcopy(ref, ref, self.send.at[way], self.recv.at[src, ch], (dev, self.p))

    def inward(self, chunks):
        z = self.z

        @pl.when(z < 2)
        def _():
            for ch in chunks:
                self.copy(0, z, ch, z + 1).start()

        @pl.when(z >= 2)
        def _():
            for ch in chunks:
                self.copy(1, z, ch, z - 1).start()

    def outward(self, chunks):
        z = self.z

        @pl.when(z == 1)
        def _():
            for ch in chunks:
                self.copy(1, z, ch, z - 1).start()

        @pl.when(z == 2)
        def _():
            for ch in chunks:
                self.copy(0, z, ch, z + 1).start()

    def step(self, k, ch):
        z = self.z

        @pl.when(z >= k)
        def _():
            self.copy(0, z - k, ch, z).wait_recv()

            @pl.when(z < 3)
            def _():
                self.copy(2 * k, z - k, ch, z + 1).start()

        @pl.when(z + k <= 3)
        def _():
            self.copy(0, z + k, ch, z).wait_recv()

            @pl.when(z > 0)
            def _():
                self.copy(2 * k + 1, z + k, ch, z - 1).start()

    def sent(self, way):
        rcopy(self.whole, self.whole, self.send.at[way], self.recv.at[0, 0], (self.z, self.p)).wait_send()

    def drain(self):
        z = self.z
        for k in range(NZ - 1):
            @pl.when((z >= k) & (z < 3))
            def _():
                self.sent(2 * k)

            @pl.when((z + k <= 3) & (z > 0))
            def _():
                self.sent(2 * k + 1)


def attn_start(q):
    return pl.multiple_of(64 * q + 16 * (q // 2), 16)


def kernel_a(xT_hbm, ln_hbm, wattn_hbm, w_ref, h_ref, qkv_ref, w1f_ref, w2_ref, ps1_ref, ps2_ref, ps3_ref,
             xg, lng, watt, zsend, zrecv, zq, s1, s2, wn, wt, hT_ref, ln_ref, wattn_ref,
             xsend, xrecv, rpart, lsend, lrecv, asend, arecv, zsend_sem, zrecv_sem, qsend, qrecv, wsend, wrecv, lsem, osem, ldummy):
    z, p, core, partner, xn, yn, diag, zs = coords()
    entry_signal(z, p, zs)
    wload = pltpu.make_async_copy(w_ref, wn, lsem.at[0])
    loads = [
        pltpu.make_async_copy(xT_hbm, xg.at[z, p], lsem.at[6]),
        pltpu.make_async_copy(ln_hbm, ln_ref, lsem.at[7]),
        pltpu.make_async_copy(wattn_hbm, wattn_ref, lsem.at[8]),
        wload,
    ]
    for c in loads:
        c.start()
    lng[z, p] = jnp.zeros((1, 128), F32)
    loads[1].wait()
    lng[z, p, 0:1, 0:64] = ln_ref[...]
    loads[0].wait()
    entry_wait()
    here = (z, p)

    def send(src_z, src_p, dev, way=0):
        recv = rpart.at[0] if way == 4 else xrecv.at[way, src_z]
        rcopy(xg.at[src_z, src_p], xg.at[src_z, src_p], xsend.at[0], recv, dev).start()

    def send_l(src_z, dev, phase):
        rcopy(lng.at[src_z, p], lng.at[src_z, p], lsend.at[0], lrecv.at[phase], dev).start()

    def wait_x(src_z, src_p, way):
        rcopy(xg.at[src_z, src_p], xg.at[src_z, src_p], xsend.at[0], xrecv.at[way, src_z], here).wait_recv()

    def stat(src_z, src_p):
        blk = xg[src_z, src_p].astype(F32).reshape(8, 8, 512)
        s1[...] += jnp.sum(blk, axis=0)
        s2[...] += jnp.sum(blk * blk, axis=0)

    spans = tuple((i, C1A) for i in range(0, C1, C1A))

    def w_piece(i, src, dst, dev):
        o, n = spans[i]
        return rcopy(
            wt.at[:, pl.ds(pl.multiple_of(dst * 256 + o, 16), n), :],
            w1f_ref.at[src, :, pl.ds(o, n), :],
            wsend.at[0], wrecv.at[0], dev)

    def send_w(i):
        for k in (3, 2, 1):
            w_piece(i, z, zs[k], (zs[k], p)).start()

    def turn(odd):
        def body(i, carry):
            lanes = pl.ds(pl.multiple_of(i * 256 + odd * 128, 128), 128)
            blk = wn[:, :, lanes].astype(F32)
            for g in range(2):
                wt[g, lanes, :] = blk[:, g, :].T.astype(BF16)
            return carry

        lax.fori_loop(0, NZ, body, 0)

    mid = 2 - z // 2
    far = 3 - 3 * (z // 2)
    zo = [z, zs[1], mid, far]
    inner = (z == 1) | (z == 2)
    send(z, p, (mid, p))
    send(z, p, (zs[1], p))
    for k in (3, 2, 1):
        send_l(z, (zs[k], p), 0)
    targets = ((diag, 3), (xn, 1), (yn, 2), (partner, 4))
    for dev, way in targets:
        send(z, p, (z, dev), way)
    for j in range(1, NP):
        send_l(z, (z, (p + j) % NP), 1)

    def attn_piece(q):
        return rcopy(wattn_ref.at[pl.ds(attn_start(q), 80), :], watt.at[z], asend.at[0], arecv.at[0], (q, p))

    def outward(k):
        return rcopy(xg.at[zo[k], p], xg.at[zo[k], p], osem.at[k - 2], xrecv.at[0, zo[k]], (zs[1], p))

    s1[...] = jnp.zeros_like(s1)
    s2[...] = jnp.zeros_like(s2)
    stat(z, p)
    loads[2].wait()
    watt[z] = wattn_ref[pl.ds(attn_start(z), 80), :]
    wload.wait()
    turn(0)
    attn_piece(mid).start()

    @pl.when(jnp.logical_not(inner))
    def _():
        attn_piece(zs[1]).start()


    def column(k):
        wait_x(zo[k], p, 0)
        if k >= 2:
            @pl.when(inner)
            def _():
                outward(k).start()
        for dev, way in targets:
            send(zo[k], p, (z, dev), way)
        stat(zo[k], p)

    def pass_on(k, src, way):
        wait_x(zo[k], src, way)
        send(zo[k], src, (z, partner), 4)
        stat(zo[k], src)

    column(1)
    column(2)
    column(3)
    rcopy(ldummy.at[pl.ds(0, 3)], ldummy.at[pl.ds(0, 3)], lsend.at[0], lrecv.at[0], here).wait_recv()
    for k in range(1, NZ):
        for j in range(1, NP):
            send_l(zs[k], (z, (p + j) % NP), 1)
    for k in range(2):
        pass_on(k, xn, 1)
        pass_on(k, yn, 2)
    attn_piece(far).start()

    @pl.when(inner)
    def _():
        attn_piece(zs[1]).start()

    send_w(0)
    pass_on(0, diag, 3)
    pass_on(1, diag, 3)
    for k in range(2, NZ):
        pass_on(k, xn, 1)
        pass_on(k, yn, 2)
        pass_on(k, diag, 3)
    send_w(1)
    half = xg.at[pl.ds(0, 2)]
    rcopy(half, half, xsend.at[0], rpart.at[0], here).wait_recv()
    for q in (partner, partner + xn - p, partner + yn - p, partner + diag - p):
        for k in range(NZ):
            stat(zo[k], q)
    rcopy(ldummy.at[pl.ds(0, 28)], ldummy.at[pl.ds(0, 28)], lsend.at[0], lrecv.at[1], here).wait_recv()

    mean = jnp.sum(s1[...], axis=0, keepdims=True) / 2048.0
    var = jnp.sum(s2[...], axis=0, keepdims=True) / 2048.0 - mean * mean
    rstd = lax.rsqrt(var + LN_EPS)
    lnT = jnp.concatenate([lng[i // NP, i % NP, 0:1, :] for i in range(32)] + [jnp.zeros((96, 128), F32)], axis=0).T
    for i in range(NZ * NP):
        sc = lnT[0:64, i:i + 1]
        hT_ref[i * 64:(i + 1) * 64, :] = ((xg[i // NP, i % NP].astype(F32) - mean) * rstd * sc).astype(BF16)

    hout = pltpu.make_async_copy(hT_ref, h_ref, lsem.at[5])
    hout.start()
    three = watt.at[pl.ds(0, 3)]
    rcopy(three, three, asend.at[0], arecv.at[0], here).wait_recv()
    part = None
    for q in range(NZ):
        t = jnp.dot(watt[q], hT_ref[q * 512:(q + 1) * 512, :], preferred_element_type=F32)
        part = t if part is None else part + t
    part = part.astype(BF16)
    for q in range(NZ):
        zsend[q] = part[:, q * 128:(q + 1) * 128]
    for k in (3, 2, 1):
        rcopy(zsend.at[zs[k]], zrecv.at[z], zsend_sem.at[0], zrecv_sem.at[0], (zs[k], p)).start()
    zrecv[z] = zsend[z]
    turn(1)
    send_w(2)
    outs = [pltpu.make_async_copy(wt, w2_ref, lsem.at[1])]
    for i, ps_ref in enumerate((ps1_ref, ps2_ref, ps3_ref)):
        dst = (z + i + 1) % NZ
        outs.append(pltpu.make_async_copy(wt.at[:, pl.ds(pl.multiple_of(dst * 256 + C1, 16), C2), :], ps_ref, lsem.at[2 + i]))
    for c in outs[1:] + outs[:1]:
        c.start()
    zthree = rcopy(zsend.at[pl.ds(0, 3)], zrecv.at[pl.ds(0, 3)], zsend_sem.at[0], zrecv_sem.at[0], here)
    zthree.wait_recv()
    zt = jnp.concatenate([zrecv[0].astype(F32), zrecv[1].astype(F32)[16:80], zrecv[2].astype(F32), zrecv[3].astype(F32)[16:80]], axis=0)
    zq[...] = zt.T.astype(BF16).reshape(NP, 16, 288)
    for j in range(1, NP):
        q = (p + j) % NP
        rcopy(zq.at[q], qkv_ref.at[p], qsend.at[0], qrecv.at[0], (z, q)).start()
    qown = pltpu.make_async_copy(zq.at[p], qkv_ref.at[p], lsem.at[9])
    qown.start()
    qseven = rcopy(zq.at[pl.ds(0, 7)], qkv_ref.at[pl.ds(0, 7)], qsend.at[0], qrecv.at[0], here)
    qseven.wait_recv()
    wthree = w1f_ref.at[pl.ds(0, 3)]
    wall = rcopy(wthree, wthree, wsend.at[0], wrecv.at[0], here)
    wall.wait_recv()
    hout.wait()
    qown.wait()
    for c in outs:
        c.wait()
    sent30 = w2_ref.at[:, pl.ds(0, 960), :]
    rcopy(sent30, sent30, xsend.at[0], rpart.at[0], here).wait_send()
    rcopy(ldummy, ldummy, lsend.at[0], lrecv.at[0], here).wait_send()
    rcopy(three, three, asend.at[0], arecv.at[0], here).wait_send()
    zthree.wait_send()
    qseven.wait_send()
    wall.wait_send()

    @pl.when(inner)
    def _():
        outward(2).wait_send()
        outward(3).wait_send()


def call_a(xT, ln, wattnT, w):
    hbm = pl.BlockSpec(memory_space=pl.ANY)
    return pl.pallas_call(
        kernel_a,
        out_shape=(
            jax.ShapeDtypeStruct((2048, 512), BF16),
            jax.ShapeDtypeStruct((NP, 16, 288), BF16),
            jax.ShapeDtypeStruct((NZ, 2, C1, 512), BF16),
            jax.ShapeDtypeStruct((2, 1024, 512), BF16),
        ) + (jax.ShapeDtypeStruct((2, C2, 512), BF16),) * 3,
        in_specs=[hbm] * 4,
        out_specs=(hbm,) * 7,
        scratch_shapes=[
            pltpu.VMEM((NZ, NP, 64, 512), BF16),
            pltpu.VMEM((NZ, NP, 1, 128), F32),
            pltpu.VMEM((NZ, 80, 512), BF16),
            pltpu.VMEM((NZ, 80, 128), BF16),
            pltpu.VMEM((NZ, 80, 128), BF16),
            pltpu.VMEM((NP, 16, 288), BF16),
            pltpu.VMEM((8, 512), F32),
            pltpu.VMEM((8, 512), F32),
            pltpu.VMEM((512, 2, 1024), BF16),
            pltpu.VMEM((2, 1024, 512), BF16),
            pltpu.VMEM((2048, 512), BF16),
            pltpu.VMEM((1, 64), F32),
            pltpu.VMEM((288, 512), BF16),
            pltpu.SemaphoreType.DMA((1,)),
            pltpu.SemaphoreType.DMA((4, NZ)),
            pltpu.SemaphoreType.DMA((1,)),
            pltpu.SemaphoreType.DMA((1,)),
            pltpu.SemaphoreType.DMA((2,)),
            pltpu.SemaphoreType.DMA((1,)),
            pltpu.SemaphoreType.DMA((1,)),
            pltpu.SemaphoreType.DMA((1,)),
            pltpu.SemaphoreType.DMA((1,)),
            pltpu.SemaphoreType.DMA((1,)),
            pltpu.SemaphoreType.DMA((1,)),
            pltpu.SemaphoreType.DMA((1,)),
            pltpu.SemaphoreType.DMA((1,)),
            pltpu.SemaphoreType.DMA((10,)),
            pltpu.SemaphoreType.DMA((2,)),
            pltpu.VMEM((31, 1, 128), F32),
        ],
        compiler_params=pltpu.CompilerParams(collective_id=0, has_side_effects=True, vmem_limit_bytes=56 * 1024 * 1024),
        name='gather_norm_qkv',
    )(xT, ln, wattnT, w)


def kernel_b(len_ref, q_ref, k_ref, v_ref, kc_ref, vc_ref, o_ref, kn_ref, vn_ref, kbuf, vbuf, oscr, isem, osem):
    rows = kbuf.shape[0]
    seq = kbuf.shape[1]

    def load(b, t):
        return pltpu.make_async_copy((kc_ref, vc_ref)[t].at[b], (kbuf, vbuf)[t].at[b], isem.at[b])

    def store(b, t):
        return pltpu.make_async_copy((kbuf, vbuf)[t].at[b], (kn_ref, vn_ref)[t].at[b], osem.at[0])

    for b in range(rows):
        load(b, 0).start()
        load(b, 1).start()

    def insert(buf, b, length, new):
        base = pl.multiple_of((length // 16) * 16, 16)
        hit = base + lax.broadcasted_iota(jnp.int32, (16, 128), 0) == length
        buf[b, pl.ds(base, 16), :] = jnp.where(hit, new.astype(F32), buf[b, pl.ds(base, 16), :].astype(F32)).astype(BF16)

    def attend(b, length, n):
        scores = lax.dot_general(q_ref[b], kbuf[b, 0:n, :], (((1,), (1,)), ((), ())), preferred_element_type=F32) * (128.0 ** -0.5)
        slot = lax.broadcasted_iota(jnp.int32, scores.shape, 1)
        scores = jnp.where(slot <= length, scores, -1e30)
        top = jnp.max(scores, axis=1, keepdims=True)
        e = jnp.exp(scores - top)
        probs = (e / jnp.sum(e, axis=1, keepdims=True)).astype(BF16)
        return jnp.dot(probs, vbuf[b, 0:n, :], preferred_element_type=F32)

    def pair(i, carry):
        b0 = 2 * i
        b1 = 2 * i + 1
        l0 = len_ref[b0]
        l1 = len_ref[b1]
        for b, length in ((b0, l0), (b1, l1)):
            pltpu.make_async_copy(kc_ref.at[pl.ds(0, 2)], kbuf.at[pl.ds(0, 2)], isem.at[b]).wait()
            insert(kbuf, b, length, k_ref[b])
            insert(vbuf, b, length, v_ref[b])
        last = jnp.maximum(l0, l1) // 512
        for t in range(seq // 512):
            @pl.when(last == t)
            def _():
                n = 512 * (t + 1)
                r0 = attend(b0, l0, n)
                r1 = attend(b1, l1, n)
                oscr[b0] = r0
                oscr[b1] = r1
        for b in (b0, b1):
            store(b, 0).start()
            store(b, 1).start()
        return carry

    lax.fori_loop(0, rows // 2, pair, 0)
    for h in range(16):
        o_ref[h // 2, :, (h % 2) * 128:(h % 2 + 1) * 128] = oscr[:, h, :].astype(BF16)
    pltpu.make_async_copy(kbuf, kn_ref, osem.at[0]).wait()
    pltpu.make_async_copy(vbuf, vn_ref, osem.at[0]).wait()


def call_b(lengths, q_rot, k_rot, v_tok, k_cache, v_cache):
    rows, seq, hd = k_cache.shape
    heads = q_rot.shape[1]
    vm = pl.BlockSpec(memory_space=pltpu.VMEM)
    hbm = pl.BlockSpec(memory_space=pl.ANY)
    return pl.pallas_call(
        kernel_b,
        in_specs=[pl.BlockSpec(memory_space=pltpu.SMEM), vm, vm, vm, hbm, hbm],
        out_specs=(vm, hbm, hbm),
        out_shape=(
            jax.ShapeDtypeStruct((NP, rows, heads * hd // NP), BF16),
            jax.ShapeDtypeStruct(k_cache.shape, BF16),
            jax.ShapeDtypeStruct(v_cache.shape, BF16),
        ),
        scratch_shapes=[
            pltpu.VMEM((rows, seq, hd), BF16),
            pltpu.VMEM((rows, seq, hd), BF16),
            pltpu.VMEM((rows, heads, hd), F32),
            pltpu.SemaphoreType.DMA((rows,)),
            pltpu.SemaphoreType.DMA((1,)),
        ],
        compiler_params=pltpu.CompilerParams(vmem_limit_bytes=52 * 1024 * 1024),
        cost_estimate=pl.CostEstimate(flops=12_000_000_000, bytes_accessed=33_000_000, transcendentals=0),
        name='attend',
    )(lengths, q_rot, k_rot, v_tok, k_cache, v_cache)


def kernel_c(hT, w2_ref, w1f_ref, p1_ref, p2_ref, p3_ref, wd, wo, o_ref, xT_ref, y_ref,
             wvA, wvB, wdAT, wdBT, woT, og, hidA, hidB, yA, ysum, r1, acc, r2,
             wsem, wbsend, wbrecv, osend, orecv, gsend, grecv, hasend, harecv, hbsend, hbrecv,
             r1send, r1recv, r2send, r2recv):
    z, p, core, partner, xn, yn, diag, zs = coords()
    entry_signal(z, p, zs)
    local = [pltpu.make_async_copy(w2_ref.at[:, pl.ds(pl.multiple_of(z * 256, 256), CA), :], wvA.at[z], wsem.at[0])]
    for s, p_ref in ((1, p1_ref), (2, p2_ref), (3, p3_ref)):
        src = (z + NZ - s) % NZ
        local.append(pltpu.make_async_copy(w1f_ref.at[src], wvA.at[src, :, pl.ds(0, C1), :], wsem.at[0]))
        local.append(pltpu.make_async_copy(p_ref, wvA.at[src, :, pl.ds(C1, C2), :], wsem.at[0]))
    late = [
        pltpu.make_async_copy(w2_ref.at[:, pl.ds(pl.multiple_of(z * 256 + CA, 16), C3), :], wvB.at[z], wsem.at[1]),
    ]
    for c in local + late:
        c.start()
    entry_wait()
    here = (z, p)

    def w_piece(src, dst, dev):
        return rcopy(
            w2_ref.at[:, pl.ds(pl.multiple_of(dst * 256 + CA, 16), C3), :],
            wvB.at[src], wbsend.at[0], wbrecv.at[0], dev)

    for k in (3, 2, 1):
        w_piece(z, zs[k], (zs[k], p)).start()
    for j in range(1, NP):
        q = (p + j) % NP
        rcopy(o_ref.at[q], og.at[z, p], osend.at[0], orecv.at[0], (z, q)).start()
    og[z, p] = o_ref[p]

    def gated(wv, n):
        g = None
        for q in range(NZ):
            t = jnp.dot(wv[q].reshape(2 * n, 512), hT[q * 512:(q + 1) * 512, :], preferred_element_type=F32)
            g = t if g is None else g + t
        gate = g[0:n].astype(BF16).astype(F32)
        up = g[n:2 * n].astype(BF16).astype(F32)
        return (jax.nn.silu(gate) * up).astype(BF16)

    ra = Relay(z, p, lambda src, ch: hidA.at[ch, src], hidA.at[0], hasend, harecv)
    rb = Relay(z, p, lambda src, ch: hidB.at[ch, src], hidB.at[0], hbsend, hbrecv)
    ro = Relay(z, p, lambda src, ch: og.at[src], og.at[0], gsend, grecv)
    every = range(CHUNKS)

    pltpu.make_async_copy(wvA, wvA, wsem.at[0]).wait()
    ha = gated(wvA, CA)
    for ch in every:
        hidA[ch, z] = ha[:, ch * LANES:(ch + 1) * LANES]

    ra.outward(every)
    ra.inward(range(2))
    oseven = rcopy(o_ref.at[pl.ds(0, 7)], og.at[z, pl.ds(0, 7)], osend.at[0], orecv.at[0], here)
    oseven.wait_recv()
    ro.outward(range(1))
    ro.inward(range(1))
    for c in late:
        c.wait()
    def by_core(ref, w):
        w = w.T.reshape(4, 2, 64, w.shape[0])
        for j in range(2):
            ref[j] = w[:, j].reshape(256, w.shape[3])

    by_core(wdAT, jnp.concatenate([wd[q * 256:q * 256 + CA, :] for q in range(NZ)], axis=0))
    by_core(wdBT, jnp.concatenate([wd[q * 256 + CA:(q + 1) * 256, :] for q in range(NZ)], axis=0))
    by_core(woT, wo[...])

    wthree = wvB.at[pl.ds(0, 3)]
    wall = rcopy(wthree, wthree, wbsend.at[0], wbrecv.at[0], here)
    wall.wait_recv()
    hb = gated(wvB, C3)
    for ch in range(CHUNKS):
        hidB[ch, z] = hb[:, ch * LANES:(ch + 1) * LANES]
    rb.outward(every)
    rb.inward(range(2))
    for ch in range(2, CHUNKS):
        ra.inward((ch,))
        rb.inward((ch,))
    ro.step(1, 0)
    for ch in range(2):
        ra.step(1, ch)
    for ch in range(2):
        ra.step(2, ch)

    chip = p // 2
    others = [diag // 2, xn // 2, yn // 2]

    def d2d(ch):
        return rcopy(ysum.at[ch, 1 - core], r1.at[ch], r1send.at[0], r1recv.at[ch], (z, partner))

    def hop(ch, i, dev):
        return rcopy(acc.at[ch, i], r2.at[ch, i], r2send.at[0], r2recv.at[ch], (z, dev))

    def stage0(ch):
        o_rows = og[ch * NZ // CHUNKS].reshape(128, 256)
        for j in (1 - core, core):
            yA[j] = jnp.dot(wdAT[j], hidA[ch].reshape(NZ * CA, LANES), preferred_element_type=F32) + lax.dot_general(
                woT[j], o_rows, (((1,), (1,)), ((), ())), preferred_element_type=F32)

    def half(ch, j):
        yt = yA[j] + jnp.dot(wdBT[j], hidB[ch].reshape(NZ * C3, LANES), preferred_element_type=F32)
        ysum[ch, j] = yt.reshape(4, 64, LANES)

    def stage1(ch):
        half(ch, 1 - core)
        d2d(ch).start()
        half(ch, core)

    def stage2(ch):
        d2d(ch).wait_recv()
        for i, (t, dev) in enumerate(zip(others, (diag, xn, yn))):
            acc[ch, i] = ysum[ch, core, t] + r1[ch, t]
            hop(ch, i, dev).start()

    def stage3(ch):
        lanes = slice(ch * LANES, (ch + 1) * LANES)
        mine = ysum[ch, core, chip] + r1[ch, chip]
        rcopy(acc.at[ch], r2.at[ch], r2send.at[0], r2recv.at[ch], here).wait_recv()
        for i in range(3):
            mine = mine + r2[ch, i]
        y_ref[:, lanes] = (xT_ref[:, lanes].astype(F32) + mine).astype(BF16)

    for t in range(1, CHUNKS + 3):
        for k in range(1, NZ - 1):
            ch = t - k
            if 0 <= ch < CHUNKS:
                if ch >= 2:
                    ra.step(k, ch)
                rb.step(k, ch)
        if t < 3:
            ro.step(t + 1, 0)
        if t >= 3:
            ra.step(3, t - 3)
            stage0(t - 3)
            rb.step(3, t - 3)
            stage1(t - 3)
        if t >= 4:
            stage2(t - 4)
    stage2(CHUNKS - 1)
    for ch in every:
        stage3(ch)

    wall.wait_send()
    oseven.wait_send()
    rcopy(r1, r1, r1send.at[0], r1recv.at[0], here).wait_send()
    rcopy(acc, acc, r2send.at[0], r2recv.at[0], here).wait_send()
    ra.drain()
    rb.drain()
    ro.drain()


def call_c(hT, w2, w1f, ps, wd, wo, o8, xT):
    vm = pl.BlockSpec(memory_space=pltpu.VMEM)
    hbm = pl.BlockSpec(memory_space=pl.ANY)
    return pl.pallas_call(
        kernel_c,
        out_shape=jax.ShapeDtypeStruct((64, 512), BF16),
        in_specs=[vm] + [hbm] * 5 + [vm] * 4,
        out_specs=vm,
        scratch_shapes=[
            pltpu.VMEM((NZ, 2, CA, 512), BF16),
            pltpu.VMEM((NZ, 2, C3, 512), BF16),
            pltpu.VMEM((2, 256, NZ * CA), BF16),
            pltpu.VMEM((2, 256, NZ * C3), BF16),
            pltpu.VMEM((2, 256, 256), BF16),
            pltpu.VMEM((NZ, NP, 16, 256), BF16),
            pltpu.VMEM((CHUNKS, NZ, CA, LANES), BF16),
            pltpu.VMEM((CHUNKS, NZ, C3, LANES), BF16),
            pltpu.VMEM((2, 256, LANES), F32),
            pltpu.VMEM((CHUNKS, 2, 4, 64, LANES), F32),
            pltpu.VMEM((CHUNKS, 4, 64, LANES), F32),
            pltpu.VMEM((CHUNKS, 3, 64, LANES), F32),
            pltpu.VMEM((CHUNKS, 3, 64, LANES), F32),
            pltpu.SemaphoreType.DMA((2,)),
            pltpu.SemaphoreType.DMA((1,)),
            pltpu.SemaphoreType.DMA((1,)),
            pltpu.SemaphoreType.DMA((1,)),
            pltpu.SemaphoreType.DMA((1,)),
            pltpu.SemaphoreType.DMA((6,)),
            pltpu.SemaphoreType.DMA((NZ, 1)),
            pltpu.SemaphoreType.DMA((6,)),
            pltpu.SemaphoreType.DMA((NZ, CHUNKS)),
            pltpu.SemaphoreType.DMA((6,)),
            pltpu.SemaphoreType.DMA((NZ, CHUNKS)),
            pltpu.SemaphoreType.DMA((1,)),
            pltpu.SemaphoreType.DMA((CHUNKS,)),
            pltpu.SemaphoreType.DMA((1,)),
            pltpu.SemaphoreType.DMA((CHUNKS,)),
        ],
        compiler_params=pltpu.CompilerParams(collective_id=1, has_side_effects=True, vmem_limit_bytes=40 * 1024 * 1024),
        cost_estimate=pl.CostEstimate(flops=12_000_000_000, bytes_accessed=6_000_000, transcendentals=0),
        name='mlp_out',
    )(hT, w2, w1f, *ps, wd, wo, o8, xT)


def solution(mesh):
    all_axes = ('x', 'yz')

    def local_step(x_in, ln_scale, w_gate_up, w_attn, w_down, w_out, k_cache, v_cache, lengths, positions):
        xT = x_in.T
        wattnT = w_attn.T
        hT, qkv, w1f, w2, *pieces = call_a(xT, ln_scale[None, :], wattnT, w_gate_up)
        ps = [lax.ppermute(pieces[i], 'x', [(q, (q + i + 1) % NZ) for q in range(NZ)]) for i in range(NZ - 1)]
        proj = jnp.transpose(qkv, (1, 0, 2)).reshape(16, 2304)
        q_raw = proj[:, :2048].reshape(16, 16, 128)
        k_tok = proj[:, 2048:2176]
        v_tok = proj[:, 2176:]
        q_rot = rotary(q_raw.astype(F32), positions).astype(BF16)
        k_rot = rotary(k_tok[:, None, :].astype(F32), positions).astype(BF16)
        o8, k_new, v_new = call_b(lengths, q_rot, k_rot, v_tok[:, None, :], k_cache, v_cache)
        yT = call_c(hT, w2, w1f, ps, w_down, w_out, o8, xT)
        return yT.T, k_new, v_new

    row_spec = P(None, all_axes)
    vec_spec = P(all_axes)
    cache_spec = P(all_axes, None, None)
    return jax.shard_map(
        local_step,
        mesh=mesh,
        in_specs=(row_spec, vec_spec, P('x', None, 'yz'), P('x', 'yz'), P('yz', 'x'), P('yz', 'x'), cache_spec, cache_spec, vec_spec, vec_spec),
        out_specs=(row_spec, cache_spec, cache_spec),
        check_vma=False,
    )
```
